64 devices in a mesh: member: 4 (over x, y), lat: 16 (over z, core).
Axes of the slice: x: 2, y: 2, z: 8, core: 2. Of those that a mesh axis runs over, the one named last changes fastest.
The devices are a block of a 4x4x8 slice.
Arguments:
- field_in: float32 [48, 128, 96, 192], P('member', None, 'lat'), parts along dimension 0
- grad_out: float32 [48, 128, 96, 192], P('member', None, 'lat'), parts along dimension 0
- p_fwd: float32 [96, 96, 96], replicated
- p_inv: float32 [96, 96, 96], replicated
- w_mix: float32 [96, 128, 128, 2], replicated
Outputs:
- output 1: float32 [48, 128, 96, 192], P('member', None, 'lat'), parts along dimension 0
- output 2: float32 [384, 128, 128, 2], P('member'), parts along dimension 0
There are 4 independent parts. The reference program is written for one: setup_inputs(seed, part) draws one part's arguments, and reference() takes and returns one part's arrays. A program takes and returns all parts, laid end to end along the dimension named above; an argument that names none is the same for every part.
All inputs are finite; a program needn't handle non-finite values.
Results may differ from the reference program's by a relative error of at most 0.0062904.
Values are sent between devices in bfloat16 or wider.
A program may use at most 768 MiB of HBM per device.

```python
import math
import jax
import jax.numpy as jnp
from jax import lax

BATCH = 12
CHANNELS = 128
NLAT = 96

NLON = 2 * NLAT


def setup_inputs(seed: int = 0, part: int = 0) -> dict:
    part_key = jax.random.fold_in(jax.random.key(seed), part)
    key_field, key_grad = jax.random.split(part_key, 2)
    key_fwd, key_inv, key_mix = jax.random.split(jax.random.key(seed + 1), 3)
    field_in = jax.random.normal(key_field, (BATCH, CHANNELS, NLAT, NLON), jnp.float32)
    grad_out = jax.random.normal(key_grad, (BATCH, CHANNELS, NLAT, NLON), jnp.float32)
    wave_num = jnp.arange(NLAT)[:, None, None]
    degree = jnp.arange(NLAT)[None, :, None]
    lower_tri = (degree >= wave_num).astype(jnp.float32)
    fwd_scale = lower_tri / math.sqrt(NLAT)
    inv_scale = lower_tri / jnp.sqrt((NLAT - wave_num).astype(jnp.float32))
    p_fwd = jax.random.normal(key_fwd, (NLAT, NLAT, NLAT), jnp.float32) * fwd_scale
    p_inv = jax.random.normal(key_inv, (NLAT, NLAT, NLAT), jnp.float32) * inv_scale
    w_mix = jax.random.normal(key_mix, (NLAT, CHANNELS, CHANNELS, 2), jnp.float32) / math.sqrt(2 * CHANNELS)
    return {'field_in': field_in, 'grad_out': grad_out, 'p_fwd': p_fwd, 'p_inv': p_inv, 'w_mix': w_mix}


def to_bf16(values):
    return values.astype(jnp.bfloat16).astype(jnp.float32)


def gelu_grad(values):
    cumulative = 0.5 * (1.0 + lax.erf(values * math.sqrt(0.5)))
    density = jnp.exp(-0.5 * values * values) / math.sqrt(2.0 * math.pi)
    return cumulative + values * density


def mix_matrix(w_mix):
    w_real = w_mix[..., 0]
    w_imag = w_mix[..., 1]
    upper_half = jnp.stack([w_real, -w_imag], axis=-1)
    lower_half = jnp.stack([w_imag, w_real], axis=-1)
    return jnp.stack([upper_half, lower_half], axis=2)


def analysis(values, mode_gains):
    spectrum = jnp.fft.rfft(values, axis=-1)[..., :NLAT] * mode_gains
    return jnp.stack([spectrum.real, spectrum.imag], axis=-2)


def synthesis(spec_pair, mode_gains):
    complex_spec = lax.complex(spec_pair[..., 0, :], spec_pair[..., 1, :]) * mode_gains
    padded = jnp.pad(complex_spec, [(0, 0)] * (complex_spec.ndim - 1) + [(0, NLON // 2 + 1 - NLAT)])
    return jnp.fft.irfft(padded, n=NLON, axis=-1)


def reference(field_in, grad_out, p_fwd, p_inv, w_mix):
    root_lon = math.sqrt(NLON)
    is_mean = jnp.arange(NLAT) == 0
    pw_half = to_bf16(p_fwd)
    pi_half = to_bf16(p_inv)
    w_big = to_bf16(mix_matrix(w_mix))
    four_lat = to_bf16(analysis(field_in, 1.0 / root_lon))
    coeffs = to_bf16(jnp.einsum('mlt,bctrm->bclrm', pw_half, four_lat))
    mixed_coef = to_bf16(jnp.einsum('losir,bilrm->bolsm', w_big, coeffs))
    back_lat = to_bf16(jnp.einsum('mlt,bclrm->bctrm', pi_half, mixed_coef))
    hidden = synthesis(back_lat, root_lon)
    grad_hidden = grad_out * gelu_grad(hidden)
    grad_back = to_bf16(analysis(grad_hidden, jnp.where(is_mean, 1.0, 2.0) / root_lon))
    grad_mixed = to_bf16(jnp.einsum('mlt,bctrm->bclrm', pi_half, grad_back))
    grad_big = jnp.einsum('bolsm,bilrm->losir', grad_mixed, coeffs)
    grad_coef = to_bf16(jnp.einsum('losir,bolsm->bilrm', w_big, grad_mixed))
    grad_four = to_bf16(jnp.einsum('mlt,bclrm->bctrm', pw_half, grad_coef))
    grad_field = grad_out + synthesis(grad_four, jnp.where(is_mean, 1.0, 0.5) * root_lon)
    grad_wmix = jnp.stack([grad_big[:, :, 0, :, 0] + grad_big[:, :, 1, :, 1], grad_big[:, :, 1, :, 0] - grad_big[:, :, 0, :, 1]], axis=-1)
    return grad_field, grad_wmix
```

```python
import functools
import math

import jax
import jax.numpy as jnp
import numpy as np
from jax import lax
from jax.experimental import pallas as pl
from jax.experimental.pallas import tpu as pltpu
from jax.sharding import PartitionSpec as P

F32 = jnp.float32
BF16 = jnp.bfloat16
SEND_SLOTS = 4


def split_const(matrix):
    head = matrix.astype(BF16)
    tail = (matrix - head.astype(np.float64)).astype(BF16)
    return [head, tail]


def fourier_tables(modes, lons):
    angle = 2.0 * np.pi * (np.outer(np.arange(modes), np.arange(lons)) % lons) / lons
    forward = np.stack([np.cos(angle), -np.sin(angle)], axis=1).reshape(2 * modes, lons) / math.sqrt(lons)
    gains = np.repeat(np.where(np.arange(modes) == 0, 1.0, 2.0), 2)[:, None]
    doubled = forward * gains
    tables = split_const(forward) + split_const(doubled) + split_const(doubled.T) + split_const(forward.T)
    return [jnp.asarray(t) for t in tables]


def gelu_grad(values):
    cumulative = 0.5 * (1.0 + lax.erf(values * math.sqrt(0.5)))
    density = jnp.exp(-0.5 * values * values) / math.sqrt(2.0 * math.pi)
    return cumulative + values * density


def dot(a, b, dims=((1,), (0,))):
    return lax.dot_general(a, b, (dims, ((), ())), preferred_element_type=F32)


def layer_kernel(
    axis, n, nb,
    f_hbm, dg_hbm, w_hbm, pw_ref, pi_ref, pwt_ref, pit_ref,
    fwd_h, fwd_l, dbl_h, dbl_l, syn_h, syn_l, adj_h, adj_l,
    df_hbm, dw_hbm,
    recv, send, t1, t2, xb, coef, dq, vmix, wbuf, inbuf, outbuf, gather, dwbuf,
    send_sem, recv_sem, in_sem, out_sem, w_sem,
):
    me = lax.axis_index(axis)
    batch, tl, lons, chans = f_hbm.shape
    ml, degs, lats = pw_ref.shape
    chunks = batch // nb
    tile = 2 * nb
    rows = ml * tile
    pitch = rows + 1
    modes2 = 2 * n * ml
    units = chunks * tl

    barrier = pltpu.get_barrier_semaphore()

    def announce(k, _):
        pl.semaphore_signal(barrier, inc=1, device_id={axis: lax.rem(me + k, n)}, device_id_type=pl.DeviceIdType.MESH)
        return 0

    lax.fori_loop(1, n, announce, 0)

    def unit_in(src, unit):
        ch, t = lax.div(unit, tl), lax.rem(unit, tl)
        slot = lax.rem(unit, 2)
        return pltpu.make_async_copy(src.at[pl.ds(ch * nb, nb), t], inbuf.at[slot], in_sem.at[slot])

    def unit_out(unit):
        ch, t = lax.div(unit, tl), lax.rem(unit, tl)
        slot = lax.rem(unit, 2)
        return pltpu.make_async_copy(outbuf.at[slot], df_hbm.at[pl.ds(ch * nb, nb), t], out_sem.at[slot])

    def step_in(src, unit):
        @pl.when(unit + 1 < units)
        def _():
            unit_in(src, unit + 1).start()
        unit_in(src, unit).wait()

    def ship(stage, ch):
        index = stage * chunks + ch
        slot = lax.rem(index, SEND_SLOTS)

        def one(k, _):
            peer = lax.rem(me + k, n)
            pltpu.make_async_remote_copy(
                src_ref=send.at[slot, peer], dst_ref=recv.at[stage, ch, me],
                send_sem=send_sem.at[index], recv_sem=recv_sem.at[index],
                device_id={axis: peer}, device_id_type=pl.DeviceIdType.MESH,
            ).start()
            return 0

        lax.fori_loop(1, n, one, 0)
        recv[stage, ch, me] = send[slot, me]

    def arrived(stage, ch):
        others = recv.at[stage, ch, pl.ds(0, n - 1)]
        pltpu.make_async_copy(others, others, recv_sem.at[stage * chunks + ch]).wait()

    def wait_sent(index):
        others = send.at[lax.rem(index, SEND_SLOTS), pl.ds(0, n - 1)]
        pltpu.make_async_copy(others, others, send_sem.at[index]).wait()

    def free_slot(stage, ch):
        index = stage * chunks + ch

        @pl.when(index >= SEND_SLOTS)
        def _():
            wait_sent(index - SEND_SLOTS)

        return lax.rem(index, SEND_SLOTS)

    def put_rows(slot, t):
        send[slot, :, t] = gather[...].reshape(n, rows, chans).astype(BF16)

    def transform(values, head, tail):
        high = values.astype(BF16)
        low = (values - high.astype(F32)).astype(BF16)
        return dot(head[...], high) + (dot(tail[...], high) + dot(head[...], low))

    unit_in(f_hbm, 0).start()

    def step1_chunk(ch, _):
        slot = free_slot(0, ch)

        def row(t, _):
            unit = ch * tl + t
            step_in(f_hbm, unit)
            buf = lax.rem(unit, 2)
            for b in range(0, nb, 2):
                pair = jnp.concatenate([inbuf[buf, b], inbuf[buf, b + 1]], axis=1)
                spec = transform(pair, fwd_h, fwd_l)
                gather[pl.ds(b, modes2, stride=nb), :] = spec[:, :chans]
                gather[pl.ds(b + 1, modes2, stride=nb), :] = spec[:, chans:]
            put_rows(slot, t)
            return 0

        lax.fori_loop(0, tl, row, 0)

        @pl.when(ch == 0)
        def _():
            pl.semaphore_wait(barrier, n - 1)

        ship(0, ch)
        return 0

    lax.fori_loop(0, chunks, step1_chunk, 0)
    unit_in(dg_hbm, 0).start()

    per = wbuf.shape[1] // (2 * chans)
    parts = degs // per

    def w_in(k):
        slot = lax.rem(k, 2)
        return pltpu.make_async_copy(w_hbm.at[pl.ds(k * per * 2 * chans, per * 2 * chans)], wbuf.at[slot], w_sem.at[slot])

    w_in(0).start()

    def load_w(k, _):
        @pl.when(k + 1 < parts)
        def _():
            w_in(k + 1).start()
        w_in(k).wait()
        slot = lax.rem(k, 2)
        for j in range(per):
            for part in range(2):
                vmix[k * per + j, pl.ds(part * chans, chans)] = wbuf[
                    slot, pl.ds(j * 2 * chans + part, chans, stride=2), :].astype(BF16)
        return 0

    lax.fori_loop(0, parts, load_w, 0)

    sign = jnp.where(lax.broadcasted_iota(jnp.int32, (tile, chans), 0) < nb, -1.0, 1.0).astype(F32)

    def turn(values):
        groups = values.reshape(ml, tile, chans)
        return (pltpu.roll(groups, nb, 1) * sign[None]).reshape(rows, chans)

    def legendre(src, dst, mats):
        def mode(m, _):
            for k in range(tile):
                xb[:, k * chans:(k + 1) * chans] = src[pl.ds(m * tile + k, lats, stride=pitch), :].astype(BF16)
            out = dot(mats[m], xb[...])
            for k in range(tile):
                dst[pl.ds(m * tile + k, degs, stride=pitch), :] = out[:, k * chans:(k + 1) * chans]
            return 0

        lax.fori_loop(0, ml, mode, 0)

    def unload(stage, ch):
        def body(src, _):
            for t in range(tl):
                t1[pl.ds((src * tl + t) * pitch, rows), :] = recv[stage, ch, src, t].astype(F32)
            return 0

        lax.fori_loop(0, n, body, 0)

    def load(slot):
        def body(dev, _):
            for t in range(tl):
                send[slot, dev, t] = t2[pl.ds((dev * tl + t) * pitch, rows), :].astype(BF16)
            return 0

        lax.fori_loop(0, n, body, 0)

    def spectral(stage, ch, into, outof, kept, mix):
        arrived(stage - 1, ch)
        unload(stage - 1, ch)
        legendre(t1, t2, into)

        def degree(l, _):
            x = t2[pl.ds(l * pitch, rows), :].astype(BF16)
            kept[l, ch] = x
            t1[pl.ds(l * pitch, rows), :] = mix(l, x)
            return 0

        lax.fori_loop(0, degs, degree, 0, unroll=2)
        legendre(t1, t2, outof)
        load(free_slot(stage, ch))
        ship(stage, ch)

    def mix_forward(l, x):
        both = dot(x, vmix[l], ((1,), (1,)))
        return both[:, :chans] + turn(both[:, chans:])

    def mix_adjoint(l, x):
        real = dot(x, vmix[l, pl.ds(0, chans)])
        imag = dot(x, vmix[l, pl.ds(chans, chans)])
        return real - turn(imag)

    def step2_chunk(ch, _):
        spectral(1, ch, pw_ref, pit_ref, coef, mix_forward)
        return 0

    lax.fori_loop(0, chunks, step2_chunk, 0)

    def fetch_rows(stage, ch, t):
        for src in range(n):
            gather[pl.ds(src * rows, rows), :] = recv[stage, ch, src, t].astype(F32)

    def fetch_pair(b):
        return jnp.concatenate(
            [gather[pl.ds(b, modes2, stride=nb), :], gather[pl.ds(b + 1, modes2, stride=nb), :]], axis=1).astype(BF16)

    def step3_chunk(ch, _):
        slot = free_slot(2, ch)
        arrived(1, ch)

        def row(t, _):
            unit = ch * tl + t
            step_in(dg_hbm, unit)
            buf = lax.rem(unit, 2)
            fetch_rows(1, ch, t)
            for b in range(0, nb, 2):
                g = fetch_pair(b)
                hidden = dot(syn_h[...], g) + dot(syn_l[...], g)
                pair = jnp.concatenate([inbuf[buf, b], inbuf[buf, b + 1]], axis=1)
                spec = transform(pair * gelu_grad(hidden), dbl_h, dbl_l)
                gather[pl.ds(b, modes2, stride=nb), :] = spec[:, :chans]
                gather[pl.ds(b + 1, modes2, stride=nb), :] = spec[:, chans:]
            put_rows(slot, t)
            return 0

        lax.fori_loop(0, tl, row, 0)
        ship(2, ch)
        return 0

    lax.fori_loop(0, chunks, step3_chunk, 0)
    unit_in(dg_hbm, 0).start()

    def step4_chunk(ch, _):
        spectral(3, ch, pi_ref, pwt_ref, dq, mix_adjoint)
        return 0

    lax.fori_loop(0, chunks, step4_chunk, 0)

    def dw_out(l):
        slot = lax.rem(l, 2)
        return pltpu.make_async_copy(dwbuf.at[slot], dw_hbm.at[pl.ds(l * 2 * chans, 2 * chans)], w_sem.at[slot])

    def weight_grad(l, _):
        @pl.when(l >= 2)
        def _():
            dw_out(l - 2).wait()
        slot = lax.rem(l, 2)
        real = jnp.zeros((chans, chans), F32)
        imag = jnp.zeros((chans, chans), F32)
        for ch in range(chunks):
            y = dq[l, ch]
            x = coef[l, ch]
            real += dot(y, x, ((0,), (0,)))
            imag -= dot(turn(y.astype(F32)).astype(BF16), x, ((0,), (0,)))
        dwbuf[slot, pl.ds(0, chans, stride=2), :] = real
        dwbuf[slot, pl.ds(1, chans, stride=2), :] = imag
        dw_out(l).start()
        return 0

    lax.fori_loop(0, degs, weight_grad, 0)
    dw_out(degs - 2).wait()
    dw_out(degs - 1).wait()

    def step5_chunk(ch, _):
        arrived(3, ch)

        def row(t, _):
            unit = ch * tl + t
            step_in(dg_hbm, unit)
            buf = lax.rem(unit, 2)

            @pl.when(unit >= 2)
            def _():
                unit_out(unit - 2).wait()

            fetch_rows(3, ch, t)
            for b in range(0, nb, 2):
                g = fetch_pair(b)
                change = dot(adj_h[...], g) + dot(adj_l[...], g)
                outbuf[buf, b] = inbuf[buf, b] + change[:, :chans]
                outbuf[buf, b + 1] = inbuf[buf, b + 1] + change[:, chans:]
            unit_out(unit).start()
            return 0

        lax.fori_loop(0, tl, row, 0)
        return 0

    lax.fori_loop(0, chunks, step5_chunk, 0)
    unit_out(units - 2).wait()
    unit_out(units - 1).wait()
    for index in range(4 * chunks - SEND_SLOTS, 4 * chunks):
        wait_sent(index)


def solution(mesh):
    n = mesh.shape['lat']
    field_spec = P('member', None, 'lat', None)

    def local_step(field_loc, grad_loc, p_fwd, p_inv, w_mix):
        batch, chans, tl, lons = field_loc.shape
        degs, lats = p_fwd.shape[1:]
        ml = p_fwd.shape[0] // n
        nb = 4
        chunks = batch // nb
        rows = ml * 2 * nb
        pitch = rows + 1
        m_start = lax.axis_index('lat') * ml
        pw = lax.dynamic_slice_in_dim(p_fwd, m_start, ml, axis=0).astype(BF16)
        pi = lax.dynamic_slice_in_dim(p_inv, m_start, ml, axis=0).astype(BF16)
        tables = fourier_tables(n * ml, lons)
        anywhere = pl.BlockSpec(memory_space=pl.ANY)
        vmem = pl.BlockSpec(memory_space=pltpu.VMEM)
        grad_field, grad_w = pl.pallas_call(
            functools.partial(layer_kernel, 'lat', n, nb),
            name='layer',
            out_shape=(
                jax.ShapeDtypeStruct((batch, tl, lons, chans), F32),
                jax.ShapeDtypeStruct((degs * 2 * chans, chans), F32),
            ),
            in_specs=[anywhere] * 3 + [vmem] * (4 + len(tables)),
            out_specs=(anywhere, anywhere),
            scratch_shapes=[
                pltpu.VMEM((4, chunks, n, tl, rows, chans), BF16),
                pltpu.VMEM((SEND_SLOTS, n, tl, rows, chans), BF16),
                pltpu.VMEM((lats * pitch, chans), F32),
                pltpu.VMEM((lats * pitch, chans), F32),
                pltpu.VMEM((lats, 2 * nb * chans), BF16),
                pltpu.VMEM((degs, chunks, rows, chans), BF16),
                pltpu.VMEM((degs, chunks, rows, chans), BF16),
                pltpu.VMEM((degs, 2 * chans, chans), BF16),
                pltpu.VMEM((2, 8 * 2 * chans, chans), F32),
                pltpu.VMEM((2, nb, lons, chans), F32),
                pltpu.VMEM((2, nb, lons, chans), F32),
                pltpu.VMEM((n * rows, chans), F32),
                pltpu.VMEM((2, 2 * chans, chans), F32),
                pltpu.SemaphoreType.DMA((4 * chunks,)),
                pltpu.SemaphoreType.DMA((4 * chunks,)),
                pltpu.SemaphoreType.DMA((2,)),
                pltpu.SemaphoreType.DMA((2,)),
                pltpu.SemaphoreType.DMA((2,)),
            ],
            compiler_params=pltpu.CompilerParams(
                collective_id=0, has_side_effects=True, vmem_limit_bytes=60 * 1024 * 1024),
        )(
            field_loc.transpose(0, 2, 3, 1), grad_loc.transpose(0, 2, 3, 1),
            w_mix.transpose(0, 1, 3, 2).reshape(degs * 2 * chans, chans),
            pw, pi, pw.transpose(0, 2, 1), pi.transpose(0, 2, 1), *tables)
        total = lax.psum(grad_w, 'lat')
        return grad_field.transpose(0, 3, 1, 2), total.reshape(degs, chans, 2, chans).transpose(0, 1, 3, 2)

    return jax.shard_map(
        local_step, mesh=mesh, in_specs=(field_spec, field_spec, P(), P(), P()),
        out_specs=(field_spec, P('member', None, None, None)), check_vma=False)
```

```python
import functools
import math

import jax
import jax.numpy as jnp
import numpy as np
from jax import lax
from jax.experimental import pallas as pl
from jax.experimental.pallas import tpu as pltpu
from jax.sharding import PartitionSpec as P

F32 = jnp.float32
BF16 = jnp.bfloat16
SEND_SLOTS = 4


def split_const(matrix):
    head = matrix.astype(BF16)
    tail = (matrix - head.astype(np.float64)).astype(BF16)
    return [head, tail]


def fourier_tables(n, ml, lons):
    modes = n * ml
    order = np.arange(modes).reshape(ml, n).T.reshape(-1)
    angle = 2.0 * np.pi * (np.outer(order, np.arange(lons)) % lons) / lons
    forward = np.stack([np.cos(angle), -np.sin(angle)], axis=1).reshape(2 * modes, lons) / math.sqrt(lons)
    gains = np.repeat(np.where(order == 0, 1.0, 2.0), 2)[:, None]
    doubled = forward * gains
    tables = split_const(forward) + split_const(doubled) + split_const(doubled.T) + split_const(forward.T)
    return [jnp.asarray(t) for t in tables]


def gelu_grad(values):
    cumulative = 0.5 * (1.0 + lax.erf(values * math.sqrt(0.5)))
    density = jnp.exp(-0.5 * values * values) / math.sqrt(2.0 * math.pi)
    return cumulative + values * density


def dot(a, b, dims=((1,), (0,))):
    return lax.dot_general(a, b, (dims, ((), ())), preferred_element_type=F32)


def layer_kernel(
    axis, n, nb, pieces,
    f_hbm, dg_hbm, w_hbm, pf_hbm, pv_hbm,
    fwd_h, fwd_l, dbl_h, dbl_l, syn_h, syn_l, adj_h, adj_l,
    df_hbm, dw_hbm,
    recv, send, t1, t2, xb, coef, dq, vmix, wbuf, inbuf, outbuf, gather, pbuf, pmat, mine, theirs, ring,
    send_sem, recv_sem, in_sem, out_sem, w_sem, p_sem, pair_send, pair_recv, rs_send, rs_recv, ag_send, ag_recv, dw_sem,
):
    me = lax.axis_index(axis)
    batch, tl, lons, chans = f_hbm.shape
    ml, degs, lats = pmat.shape[1:]
    chunks = batch // nb
    tile = 2 * nb
    rows = ml * tile
    pitch = rows + 1
    modes2 = 2 * n * ml
    units = chunks * tl

    barrier = pltpu.get_barrier_semaphore()

    def announce(k, _):
        pl.semaphore_signal(barrier, inc=1, device_id={axis: lax.rem(me + k, n)}, device_id_type=pl.DeviceIdType.MESH)
        return 0

    lax.fori_loop(1, n, announce, 0)

    def unit_of(unit):
        return lax.div(unit, tl), lax.rem(unit, tl)

    def unit_in(src, unit):
        ch, t = unit_of(unit)
        slot = lax.rem(unit, 2)
        return pltpu.make_async_copy(src.at[pl.ds(ch * nb, nb), t], inbuf.at[slot], in_sem.at[slot])

    def unit_out(unit):
        ch, t = unit_of(unit)
        slot = lax.rem(unit, 2)
        return pltpu.make_async_copy(outbuf.at[slot], df_hbm.at[pl.ds(ch * nb, nb), t], out_sem.at[slot])

    def step_in(src, unit):
        @pl.when(unit + 1 < units)
        def _():
            unit_in(src, unit + 1).start()
        unit_in(src, unit).wait()

    def ship(stage, ch, t0, nt):
        index = stage * chunks + ch
        slot = lax.rem(index, SEND_SLOTS)
        part = pl.ds(t0, nt)

        def one(k, _):
            peer = lax.rem(me + k, n)
            pltpu.make_async_remote_copy(
                src_ref=send.at[slot, peer, part], dst_ref=recv.at[stage % 2, ch, me, part],
                send_sem=send_sem.at[index], recv_sem=recv_sem.at[index],
                device_id={axis: peer}, device_id_type=pl.DeviceIdType.MESH,
            ).start()
            return 0

        lax.fori_loop(1, n, one, 0)
        recv[stage % 2, ch, me, part] = send[slot, me, part]

    def arrived(stage, ch):
        others = recv.at[stage % 2, ch, pl.ds(0, n - 1)]
        pltpu.make_async_copy(others, others, recv_sem.at[stage * chunks + ch]).wait()

    def wait_sent(index):
        others = send.at[lax.rem(index, SEND_SLOTS), pl.ds(0, n - 1)]
        pltpu.make_async_copy(others, others, send_sem.at[index]).wait()

    def free_slot(stage, ch):
        index = stage * chunks + ch

        @pl.when(index >= SEND_SLOTS)
        def _():
            wait_sent(index - SEND_SLOTS)

        return lax.rem(index, SEND_SLOTS)

    def put_rows(slot, t):
        send[slot, :, t] = gather[...].reshape(n, rows, chans).astype(BF16)

    def transform(values, head, tail):
        high = values.astype(BF16)
        low = (values - high.astype(F32)).astype(BF16)
        return dot(head[...], high) + (dot(tail[...], high) + dot(head[...], low))

    unit_in(f_hbm, 0).start()
    for which, source in enumerate((pf_hbm, pv_hbm)):
        for k in range(ml):
            pltpu.make_async_copy(source.at[me + n * k], pbuf.at[which, k], p_sem.at[which]).start()

    group = 2 if tl % 2 == 0 else 1

    def by_rows(stage, ch, row):
        slot = free_slot(stage, ch)

        def part(p, _):
            def one(j, _):
                row(slot, p * group + j)
                return 0

            lax.fori_loop(0, group, one, 0)
            if stage == 0:
                @pl.when(ch + p == 0)
                def _():
                    pl.semaphore_wait(barrier, n - 1)
            ship(stage, ch, p * group, group)
            return 0

        lax.fori_loop(0, tl // group, part, 0)

    def step1_chunk(ch, _):
        def row(slot, t):
            unit = ch * tl + t
            step_in(f_hbm, unit)
            buf = lax.rem(unit, 2)
            for b in range(0, nb, 2):
                pair = jnp.concatenate([inbuf[buf, b], inbuf[buf, b + 1]], axis=1)
                spec = transform(pair, fwd_h, fwd_l)
                gather[pl.ds(b, modes2, stride=nb), :] = spec[:, :chans]
                gather[pl.ds(b + 1, modes2, stride=nb), :] = spec[:, chans:]
            put_rows(slot, t)

        by_rows(0, ch, row)
        return 0

    lax.fori_loop(0, chunks, step1_chunk, 0)
    unit_in(dg_hbm, 0).start()
    for which in range(2):
        pltpu.make_async_copy(pbuf.at[which], pbuf.at[which], p_sem.at[which]).wait()
    pmat[...] = pbuf[...].astype(BF16)

    per = wbuf.shape[1] // (2 * chans)
    parts = degs // per

    def w_in(k):
        slot = lax.rem(k, 2)
        return pltpu.make_async_copy(w_hbm.at[pl.ds(k * per * 2 * chans, per * 2 * chans)], wbuf.at[slot], w_sem.at[slot])

    w_in(0).start()

    def load_w(k, _):
        @pl.when(k + 1 < parts)
        def _():
            w_in(k + 1).start()
        w_in(k).wait()
        slot = lax.rem(k, 2)
        for j in range(per):
            for part in range(2):
                vmix[k * per + j, pl.ds(part * chans, chans)] = wbuf[
                    slot, pl.ds(j * 2 * chans + part, chans, stride=2), :].astype(BF16)
        return 0

    lax.fori_loop(0, parts, load_w, 0)

    sign = jnp.where(lax.broadcasted_iota(jnp.int32, (tile, chans), 0) < nb, -1.0, 1.0).astype(F32)

    def turn(values):
        groups = values.reshape(ml, tile, chans)
        return (pltpu.roll(groups, nb, 1) * sign[None]).reshape(rows, chans)

    def legendre(src, dst, which, over):
        def mode(m, _):
            for k in range(tile):
                xb[:, k * chans:(k + 1) * chans] = src[pl.ds(m * tile + k, lats, stride=pitch), :].astype(BF16)
            out = dot(pmat[which, m], xb[...], ((over,), (0,)))
            for k in range(tile):
                dst[pl.ds(m * tile + k, degs, stride=pitch), :] = out[:, k * chans:(k + 1) * chans]
            return 0

        lax.fori_loop(0, ml, mode, 0)

    def unload(stage, ch):
        def body(src, _):
            for t in range(tl):
                t1[pl.ds((src * tl + t) * pitch, rows), :] = recv[stage % 2, ch, src, t].astype(F32)
            return 0

        lax.fori_loop(0, n, body, 0)

    def load(slot):
        def body(dev, _):
            for t in range(tl):
                send[slot, dev, t] = t2[pl.ds((dev * tl + t) * pitch, rows), :].astype(BF16)
            return 0

        lax.fori_loop(0, n, body, 0)

    def spectral(stage, ch, into, kept, mix):
        arrived(stage - 1, ch)
        unload(stage - 1, ch)
        legendre(t1, t2, into, 1)

        def degree(l, _):
            x = t2[pl.ds(l * pitch, rows), :].astype(BF16)
            kept[l, ch] = x
            t1[pl.ds(l * pitch, rows), :] = mix(l, x)
            return 0

        lax.fori_loop(0, degs, degree, 0, unroll=2)
        legendre(t1, t2, 1 - into, 0)
        load(free_slot(stage, ch))
        ship(stage, ch, 0, tl)

    def mix_forward(l, x):
        both = dot(x, vmix[l], ((1,), (1,)))
        return both[:, :chans] + turn(both[:, chans:])

    def mix_adjoint(l, x):
        real = dot(x, vmix[l, pl.ds(0, chans)])
        imag = dot(x, vmix[l, pl.ds(chans, chans)])
        return real - turn(imag)

    def step2_chunk(ch, _):
        spectral(1, ch, 0, coef, mix_forward)
        return 0

    lax.fori_loop(0, chunks, step2_chunk, 0)

    def fetch_rows(stage, ch, t):
        for src in range(n):
            gather[pl.ds(src * rows, rows), :] = recv[stage % 2, ch, src, t].astype(F32)

    def fetch_pair(b):
        return jnp.concatenate(
            [gather[pl.ds(b, modes2, stride=nb), :], gather[pl.ds(b + 1, modes2, stride=nb), :]], axis=1).astype(BF16)

    def step3_chunk(ch, _):
        arrived(1, ch)

        def row(slot, t):
            unit = ch * tl + t
            step_in(dg_hbm, unit)
            buf = lax.rem(unit, 2)
            fetch_rows(1, ch, t)
            for b in range(0, nb, 2):
                g = fetch_pair(b)
                hidden = dot(syn_h[...], g) + dot(syn_l[...], g)
                pair = jnp.concatenate([inbuf[buf, b], inbuf[buf, b + 1]], axis=1)
                spec = transform(pair * gelu_grad(hidden), dbl_h, dbl_l)
                gather[pl.ds(b, modes2, stride=nb), :] = spec[:, :chans]
                gather[pl.ds(b + 1, modes2, stride=nb), :] = spec[:, chans:]
            put_rows(slot, t)

        by_rows(2, ch, row)
        return 0

    lax.fori_loop(0, chunks, step3_chunk, 0)
    unit_in(dg_hbm, 0).start()

    def step4_chunk(ch, _):
        spectral(3, ch, 1, dq, mix_adjoint)
        return 0

    lax.fori_loop(0, chunks, step4_chunk, 0)

    chip, core = lax.div(me, 2), lax.rem(me, 2)
    chips = n // 2
    way = 1 - 2 * core
    sibling = me + way
    onward = 2 * lax.rem(chip + way + chips, chips) + core
    half = degs // n
    piece = half // pieces * 2 * chans
    wide = 2 * chans

    def block_at(k, direction):
        return lax.rem(chip - direction * (1 + k) + 2 * chips, chips)

    def to(device, src, dst, sent, got):
        return pltpu.make_async_remote_copy(
            src_ref=src, dst_ref=dst, send_sem=sent, recv_sem=got,
            device_id={axis: device}, device_id_type=pl.DeviceIdType.MESH)

    def weight_grad(dst, degree, count):
        def one(j, _):
            real = jnp.zeros((chans, chans), F32)
            imag = jnp.zeros((chans, chans), F32)
            for ch in range(chunks):
                y = dq[degree + j, ch]
                x = coef[degree + j, ch]
                real += dot(y, x, ((0,), (0,)))
                imag -= dot(turn(y.astype(F32)).astype(BF16), x, ((0,), (0,)))
            dst[pl.ds(j * wide, chans, stride=2), :] = real
            dst[pl.ds(j * wide + 1, chans, stride=2), :] = imag
            return 0

        lax.fori_loop(0, count, one, 0)

    def pair_copy(k):
        slot = lax.rem(k, 2)
        return to(sibling, wbuf.at[slot, pl.ds(0, half * wide)], theirs.at[block_at(k, -way)],
                  pair_send.at[slot], pair_recv.at[k])

    def weight_block(k, _):
        @pl.when(k >= 2)
        def _():
            pair_copy(k - 2).wait_send()
        weight_grad(wbuf.at[lax.rem(k, 2)], (2 * block_at(k, -way) + 1 - core) * half, half)
        pair_copy(k).start()
        block = block_at(k, way)
        weight_grad(mine.at[block], (2 * block + core) * half, half)
        return 0

    lax.fori_loop(0, chips, weight_block, 0)
    pair_copy(chips - 2).wait_send()
    pair_copy(chips - 1).wait_send()

    def final_rows(unit):
        ch, t = unit_of(unit)

        @pl.when(t == 0)
        def _():
            arrived(3, ch)

        step_in(dg_hbm, unit)
        buf = lax.rem(unit, 2)

        @pl.when(unit >= 2)
        def _():
            unit_out(unit - 2).wait()

        fetch_rows(3, ch, t)
        for b in range(0, nb, 2):
            g = fetch_pair(b)
            change = dot(adj_h[...], g) + dot(adj_l[...], g)
            outbuf[buf, b] = inbuf[buf, b] + change[:, :chans]
            outbuf[buf, b + 1] = inbuf[buf, b + 1] + change[:, chans:]
        unit_out(unit).start()

    hops = (chips - 1) * pieces

    def add_up(i):
        k, part = lax.div(i, pieces), pl.ds(lax.rem(i, pieces) * piece, piece)
        block = block_at(k, way)

        @pl.when(lax.rem(i, pieces) == 0)
        def _():
            pair_copy(k).wait_recv()

        mine[block, part] += theirs[block, part]

        @pl.when(k > 0)
        def _():
            rs_copy(i - pieces).wait_recv()
            mine[block, part] += ring[block, part]

        return block, part

    def rs_copy(i):
        k, part = lax.div(i, pieces), pl.ds(lax.rem(i, pieces) * piece, piece)
        block = block_at(k, way)
        return to(onward, mine.at[block, part], ring.at[block, part], rs_send, rs_recv.at[i])

    def rs_step(i, _):
        add_up(i)
        rs_copy(i).start()

        @pl.when(i < units)
        def _():
            final_rows(i)

        return 0

    lax.fori_loop(0, hops, rs_step, 0)

    def publish(source, block, i):
        rows_out = pl.ds(((2 * block + core) * half) * wide + lax.rem(i, pieces) * piece, piece)
        pltpu.make_async_copy(source, dw_hbm.at[rows_out], dw_sem.at[0]).start()
        to(sibling, source, dw_hbm.at[rows_out], dw_sem.at[1], dw_sem.at[2]).start()

    def own_piece(s, _):
        block, part = add_up(hops + s)
        to(onward, mine.at[block, part], ring.at[block, part], ag_send, ag_recv.at[s]).start()
        publish(mine.at[block, part], block, s)
        return 0

    lax.fori_loop(0, pieces, own_piece, 0)

    def ag_step(i, _):
        part = pl.ds(lax.rem(i, pieces) * piece, piece)
        block = block_at(lax.div(i, pieces), way)
        held = ring.at[block, part]
        to(onward, held, held, ag_send, ag_recv.at[i]).wait_recv()

        @pl.when(i + pieces < hops)
        def _():
            to(onward, held, held, ag_send, ag_recv.at[i + pieces]).start()

        publish(held, block, i)
        return 0

    lax.fori_loop(0, hops, ag_step, 0)

    def rest(unit, _):
        final_rows(unit)
        return 0

    lax.fori_loop(min(hops, units), units, rest, 0)

    unit_out(units - 2).wait()
    unit_out(units - 1).wait()
    for index in range(4 * chunks - SEND_SLOTS, 4 * chunks):
        wait_sent(index)
    sent = ring.at[pl.ds(0, chips - 1)]
    pltpu.make_async_copy(sent, sent, rs_send).wait()
    pltpu.make_async_copy(sent, sent, ag_send).wait()
    shared = dw_hbm.at[pl.ds(0, degs // 2 * wide)]
    for which in range(3):
        pltpu.make_async_copy(shared, shared, dw_sem.at[which]).wait()


def solution(mesh):
    n = mesh.shape['lat']
    field_spec = P('member', None, 'lat', None)

    def local_step(field_loc, grad_loc, p_fwd, p_inv, w_mix):
        batch, chans, tl, lons = field_loc.shape
        degs, lats = p_fwd.shape[1:]
        ml = p_fwd.shape[0] // n
        nb = 4
        chunks = batch // nb
        rows = ml * 2 * nb
        pitch = rows + 1
        half = degs // n
        pieces = 3 if half % 3 == 0 else 1
        hops = (n // 2 - 1) * pieces
        ringed = pltpu.VMEM((n // 2, half * 2 * chans, chans), F32)
        tables = fourier_tables(n, ml, lons)
        anywhere = pl.BlockSpec(memory_space=pl.ANY)
        vmem = pl.BlockSpec(memory_space=pltpu.VMEM)
        grad_field, grad_w = pl.pallas_call(
            functools.partial(layer_kernel, 'lat', n, nb, pieces),
            name='layer',
            out_shape=(
                jax.ShapeDtypeStruct((batch, tl, lons, chans), F32),
                jax.ShapeDtypeStruct((degs * 2 * chans, chans), F32),
            ),
            in_specs=[anywhere] * 5 + [vmem] * len(tables),
            out_specs=(anywhere, anywhere),
            scratch_shapes=[
                pltpu.VMEM((2, chunks, n, tl, rows, chans), BF16),
                pltpu.VMEM((SEND_SLOTS, n, tl, rows, chans), BF16),
                pltpu.VMEM((lats * pitch, chans), F32),
                pltpu.VMEM((lats * pitch, chans), F32),
                pltpu.VMEM((lats, 2 * nb * chans), BF16),
                pltpu.VMEM((degs, chunks, rows, chans), BF16),
                pltpu.VMEM((degs, chunks, rows, chans), BF16),
                pltpu.VMEM((degs, 2 * chans, chans), BF16),
                pltpu.VMEM((2, 8 * 2 * chans, chans), F32),
                pltpu.VMEM((2, nb, lons, chans), F32),
                pltpu.VMEM((2, nb, lons, chans), F32),
                pltpu.VMEM((n * rows, chans), F32),
                pltpu.VMEM((2, ml, degs, lats), F32),
                pltpu.VMEM((2, ml, degs, lats), BF16),
                ringed, ringed, ringed,
                pltpu.SemaphoreType.DMA((4 * chunks,)),
                pltpu.SemaphoreType.DMA((4 * chunks,)),
                pltpu.SemaphoreType.DMA((2,)),
                pltpu.SemaphoreType.DMA((2,)),
                pltpu.SemaphoreType.DMA((2,)),
                pltpu.SemaphoreType.DMA((2,)),
                pltpu.SemaphoreType.DMA((2,)),
                pltpu.SemaphoreType.DMA((n // 2,)),
                pltpu.SemaphoreType.DMA,
                pltpu.SemaphoreType.DMA((hops,)),
                pltpu.SemaphoreType.DMA,
                pltpu.SemaphoreType.DMA((hops,)),
                pltpu.SemaphoreType.DMA((3,)),
            ],
            compiler_params=pltpu.CompilerParams(
                collective_id=0, has_side_effects=True, vmem_limit_bytes=62 * 1024 * 1024),
        )(
            field_loc.transpose(0, 2, 3, 1), grad_loc.transpose(0, 2, 3, 1),
            w_mix.transpose(0, 1, 3, 2).reshape(degs * 2 * chans, chans),
            p_fwd, p_inv, *tables)
        return grad_field.transpose(0, 3, 1, 2), grad_w.reshape(degs, chans, 2, chans).transpose(0, 1, 3, 2)

    return jax.shard_map(
        local_step, mesh=mesh, in_specs=(field_spec, field_spec, P(), P(), P()),
        out_specs=(field_spec, P('member', None, None, None)), check_vma=False)
```

```python
import functools
import math

import jax
import jax.numpy as jnp
import numpy as np
from jax import lax
from jax.experimental import pallas as pl
from jax.experimental.pallas import tpu as pltpu
from jax.sharding import PartitionSpec as P

F32 = jnp.float32
BF16 = jnp.bfloat16
SEND_SLOTS = 4


def split_const(matrix):
    head = matrix.astype(BF16)
    tail = (matrix - head.astype(np.float64)).astype(BF16)
    return [head, tail]


def fourier_tables(n, ml, lons):
    modes = n * ml
    order = np.arange(modes).reshape(ml, n).T.reshape(-1)
    angle = 2.0 * np.pi * (np.outer(order, np.arange(lons)) % lons) / lons
    forward = np.stack([np.cos(angle), -np.sin(angle)], axis=1).reshape(2 * modes, lons) / math.sqrt(lons)
    gains = np.repeat(np.where(order == 0, 1.0, 2.0), 2)[:, None]
    doubled = forward * gains
    tables = split_const(forward) + split_const(doubled) + split_const(doubled.T) + split_const(forward.T)
    return [jnp.asarray(t) for t in tables]


def gelu_grad(values):
    cumulative = 0.5 * (1.0 + lax.erf(values * math.sqrt(0.5)))
    density = jnp.exp(-0.5 * values * values) / math.sqrt(2.0 * math.pi)
    return cumulative + values * density


def dot(a, b, dims=((1,), (0,))):
    return lax.dot_general(a, b, (dims, ((), ())), preferred_element_type=F32)


def layer_kernel(
    axis, n, nb, pieces,
    f_hbm, dg_hbm, w_hbm, pf_hbm, pv_hbm,
    fwd_h, fwd_l, dbl_h, dbl_l, syn_h, syn_l, adj_h, adj_l,
    df_out, dw_out,
    recv, send, t1, t2, xb, coef, dq, vmix, wbuf, inbuf, gather, pbuf, pmat, mine, low,
    send_sem, recv_sem, in_sem, w_sem, p_sem, pair_send, pair_recv, rs_send, rs_recv, ag_send, ag_recv,
    low_send, low_recv, free_sem, pub_send, pub_recv,
):
    me = lax.axis_index(axis)
    batch, tl, lons, chans = f_hbm.shape
    ml, degs, lats = pmat.shape[1:]
    chunks = batch // nb
    tile = 2 * nb
    rows = ml * tile
    pitch = rows + 1
    modes2 = 2 * n * ml
    units = chunks * tl

    barrier = pltpu.get_barrier_semaphore()

    def announce(k, _):
        pl.semaphore_signal(barrier, inc=1, device_id={axis: lax.rem(me + k, n)}, device_id_type=pl.DeviceIdType.MESH)
        return 0

    lax.fori_loop(1, n, announce, 0)

    def unit_of(unit):
        return lax.div(unit, tl), lax.rem(unit, tl)

    def unit_in(src, unit):
        ch, t = unit_of(unit)
        slot = lax.rem(unit, 2)
        return pltpu.make_async_copy(src.at[pl.ds(ch * nb, nb), t], inbuf.at[slot], in_sem.at[slot])

    def step_in(src, unit):
        @pl.when(unit + 1 < units)
        def _():
            unit_in(src, unit + 1).start()
        unit_in(src, unit).wait()

    def ship(stage, ch, t0, nt):
        index = stage * chunks + ch
        slot = lax.rem(index, SEND_SLOTS)
        part = pl.ds(t0, nt)

        def one(k, _):
            peer = lax.rem(me + k, n)
            pltpu.make_async_remote_copy(
                src_ref=send.at[slot, peer, part], dst_ref=recv.at[stage % 2, ch, me, part],
                send_sem=send_sem.at[index], recv_sem=recv_sem.at[index],
                device_id={axis: peer}, device_id_type=pl.DeviceIdType.MESH,
            ).start()
            return 0

        lax.fori_loop(1, n, one, 0)
        recv[stage % 2, ch, me, part] = send[slot, me, part]

    def arrived(stage, ch):
        others = recv.at[stage % 2, ch, pl.ds(0, n - 1)]
        pltpu.make_async_copy(others, others, recv_sem.at[stage * chunks + ch]).wait()

    def wait_sent(index):
        others = send.at[lax.rem(index, SEND_SLOTS), pl.ds(0, n - 1)]
        pltpu.make_async_copy(others, others, send_sem.at[index]).wait()

    def free_slot(stage, ch):
        index = stage * chunks + ch

        @pl.when(index >= SEND_SLOTS)
        def _():
            wait_sent(index - SEND_SLOTS)

        return lax.rem(index, SEND_SLOTS)

    def put_rows(slot, t):
        send[slot, :, t] = gather[...].reshape(n, rows, chans).astype(BF16)

    def transform(values, head, tail):
        high = values.astype(BF16)
        low = (values - high.astype(F32)).astype(BF16)
        return dot(head[...], high) + (dot(tail[...], high) + dot(head[...], low))

    unit_in(f_hbm, 0).start()
    for which, source in enumerate((pf_hbm, pv_hbm)):
        for k in range(ml):
            pltpu.make_async_copy(source.at[me + n * k], pbuf.at[which, k], p_sem.at[which]).start()

    group = 2 if tl % 2 == 0 else 1

    def by_rows(stage, ch, row):
        slot = free_slot(stage, ch)

        def part(p, _):
            def one(j, _):
                row(slot, p * group + j)
                return 0

            lax.fori_loop(0, group, one, 0)
            if stage == 0:
                @pl.when(ch + p == 0)
                def _():
                    pl.semaphore_wait(barrier, n - 1)
            ship(stage, ch, p * group, group)
            return 0

        lax.fori_loop(0, tl // group, part, 0)

    def step1_chunk(ch, _):
        def row(slot, t):
            unit = ch * tl + t
            step_in(f_hbm, unit)
            buf = lax.rem(unit, 2)
            for b in range(0, nb, 2):
                pair = jnp.concatenate([inbuf[buf, b], inbuf[buf, b + 1]], axis=1)
                spec = transform(pair, fwd_h, fwd_l)
                gather[pl.ds(b, modes2, stride=nb), :] = spec[:, :chans]
                gather[pl.ds(b + 1, modes2, stride=nb), :] = spec[:, chans:]
            put_rows(slot, t)

        by_rows(0, ch, row)
        return 0

    lax.fori_loop(0, chunks, step1_chunk, 0)
    unit_in(dg_hbm, 0).start()
    for which in range(2):
        pltpu.make_async_copy(pbuf.at[which], pbuf.at[which], p_sem.at[which]).wait()
    pmat[...] = pbuf[...].astype(BF16)

    per = wbuf.shape[1] // (2 * chans)
    parts = degs // per

    def w_in(k):
        slot = lax.rem(k, 2)
        return pltpu.make_async_copy(w_hbm.at[pl.ds(k * per * 2 * chans, per * 2 * chans)], wbuf.at[slot], w_sem.at[slot])

    w_in(0).start()

    def load_w(k, _):
        @pl.when(k + 1 < parts)
        def _():
            w_in(k + 1).start()
        w_in(k).wait()
        slot = lax.rem(k, 2)
        for j in range(per):
            for part in range(2):
                vmix[k * per + j, pl.ds(part * chans, chans)] = wbuf[
                    slot, pl.ds(j * 2 * chans + part, chans, stride=2), :].astype(BF16)
        return 0

    lax.fori_loop(0, parts, load_w, 0)

    sign = jnp.where(lax.broadcasted_iota(jnp.int32, (tile, chans), 0) < nb, -1.0, 1.0).astype(F32)

    def turn(values):
        groups = values.reshape(-1, tile, chans)
        return (pltpu.roll(groups, nb, 1) * sign[None]).reshape(values.shape)

    def legendre(src, dst, which, over):
        def mode(m, _):
            for k in range(tile):
                xb[:, k * chans:(k + 1) * chans] = src[pl.ds(m * tile + k, lats, stride=pitch), :].astype(BF16)
            out = dot(pmat[which, m], xb[...], ((over,), (0,)))
            for k in range(tile):
                dst[pl.ds(m * tile + k, degs, stride=pitch), :] = out[:, k * chans:(k + 1) * chans]
            return 0

        lax.fori_loop(0, ml, mode, 0)

    def unload(stage, ch):
        def body(src, _):
            for t in range(tl):
                t1[pl.ds((src * tl + t) * pitch, rows), :] = recv[stage % 2, ch, src, t].astype(F32)
            return 0

        lax.fori_loop(0, n, body, 0)

    def load(slot):
        def body(dev, _):
            for t in range(tl):
                send[slot, dev, t] = t2[pl.ds((dev * tl + t) * pitch, rows), :].astype(BF16)
            return 0

        lax.fori_loop(0, n, body, 0)

    def spectral(stage, ch, into, kept, mix):
        arrived(stage - 1, ch)
        unload(stage - 1, ch)
        legendre(t1, t2, into, 1)

        def degree(l, _):
            x = t2[pl.ds(l * pitch, rows), :].astype(BF16)
            kept[l, ch] = x
            t1[pl.ds(l * pitch, rows), :] = mix(l, x)
            return 0

        lax.fori_loop(0, degs, degree, 0, unroll=2)
        legendre(t1, t2, 1 - into, 0)
        load(free_slot(stage, ch))
        ship(stage, ch, 0, tl)

    def mix_forward(l, x):
        both = dot(x, vmix[l], ((1,), (1,)))
        return both[:, :chans] + turn(both[:, chans:])

    def mix_adjoint(l, x):
        real = dot(x, vmix[l, pl.ds(0, chans)])
        imag = dot(x, vmix[l, pl.ds(chans, chans)])
        return real - turn(imag)

    def step2_chunk(ch, _):
        spectral(1, ch, 0, coef, mix_forward)
        return 0

    lax.fori_loop(0, chunks, step2_chunk, 0)

    def send_low(which, kept):
        def one(k, _):
            peer = lax.rem(me + k, n)
            pltpu.make_async_remote_copy(
                src_ref=kept.at[peer, :, pl.ds(0, tile)], dst_ref=low.at[which, me],
                send_sem=low_send.at[which], recv_sem=low_recv.at[which],
                device_id={axis: peer}, device_id_type=pl.DeviceIdType.MESH,
            ).start()
            return 0

        lax.fori_loop(1, n, one, 0)
        low[which, me] = kept[me, :, pl.ds(0, tile)]

    send_low(0, coef)

    def fetch_rows(stage, ch, t):
        for src in range(n):
            gather[pl.ds(src * rows, rows), :] = recv[stage % 2, ch, src, t].astype(F32)

    def fetch_pair(b):
        return jnp.concatenate(
            [gather[pl.ds(b, modes2, stride=nb), :], gather[pl.ds(b + 1, modes2, stride=nb), :]], axis=1).astype(BF16)

    def step3_chunk(ch, _):
        arrived(1, ch)

        def row(slot, t):
            unit = ch * tl + t
            step_in(dg_hbm, unit)
            buf = lax.rem(unit, 2)
            fetch_rows(1, ch, t)
            for b in range(0, nb, 2):
                g = fetch_pair(b)
                hidden = dot(syn_h[...], g) + dot(syn_l[...], g)
                pair = jnp.concatenate([inbuf[buf, b], inbuf[buf, b + 1]], axis=1)
                spec = transform(pair * gelu_grad(hidden), dbl_h, dbl_l)
                gather[pl.ds(b, modes2, stride=nb), :] = spec[:, :chans]
                gather[pl.ds(b + 1, modes2, stride=nb), :] = spec[:, chans:]
            put_rows(slot, t)

        by_rows(2, ch, row)
        return 0

    lax.fori_loop(0, chunks, step3_chunk, 0)
    unit_in(dg_hbm, 0).start()

    def step4_chunk(ch, _):
        spectral(3, ch, 1, dq, mix_adjoint)
        return 0

    lax.fori_loop(0, chunks, step4_chunk, 0)
    send_low(1, dq)

    chip, core = lax.div(me, 2), lax.rem(me, 2)
    chips = n // 2
    way = 1 - 2 * core
    sibling = me + way
    onward = 2 * lax.rem(chip + way + chips, chips) + core
    half = degs // n - 1
    wide = 2 * chans
    piece = half * wide // pieces
    hops = (chips - 1) * pieces

    def block_at(k, direction):
        return lax.rem(chip - direction * (1 + k) + 2 * chips, chips)

    def to(device, src, dst, sent, got):
        return pltpu.make_async_remote_copy(
            src_ref=src, dst_ref=dst, send_sem=sent, recv_sem=got,
            device_id={axis: device}, device_id_type=pl.DeviceIdType.MESH)

    def outer(dst, row, pairs):
        real = jnp.zeros((chans, chans), F32)
        imag = jnp.zeros((chans, chans), F32)
        for y, x in pairs:
            real += dot(y, x, ((0,), (0,)))
            imag -= dot(turn(y.astype(F32)).astype(BF16), x, ((0,), (0,)))
        dst[pl.ds(row, chans, stride=2), :] = real
        dst[pl.ds(row + 1, chans, stride=2), :] = imag

    def first_degree(block, of_core):
        return n + (2 * block + of_core) * half

    def weight_grad(dst, degree):
        def one(j, _):
            outer(dst, j * wide, [(dq[degree + j, ch], coef[degree + j, ch]) for ch in range(chunks)])
            return 0

        lax.fori_loop(0, half, one, 0)

    def pair_copy(k):
        slot = lax.rem(k, 2)
        rows_there = pl.ds(first_degree(block_at(k, -way), core) * wide, half * wide)
        return to(sibling, wbuf.at[slot, pl.ds(0, half * wide)], dw_out.at[rows_there],
                  pair_send.at[slot], pair_recv.at[k])

    def weight_block(k, _):
        @pl.when(k >= 2)
        def _():
            pair_copy(k - 2).wait_send()
        weight_grad(wbuf.at[lax.rem(k, 2)], first_degree(block_at(k, -way), 1 - core))
        pair_copy(k).start()
        block = block_at(k, way)
        weight_grad(mine.at[block], first_degree(block, core))
        return 0

    lax.fori_loop(0, chips, weight_block, 0)
    pair_copy(chips - 2).wait_send()
    pair_copy(chips - 1).wait_send()

    def final_rows(unit):
        ch, t = unit_of(unit)

        @pl.when(t == 0)
        def _():
            arrived(3, ch)

        step_in(dg_hbm, unit)
        buf = lax.rem(unit, 2)

        fetch_rows(3, ch, t)
        for b in range(0, nb, 2):
            g = fetch_pair(b)
            change = dot(adj_h[...], g) + dot(adj_l[...], g)
            df_out[ch * nb + b, t] = inbuf[buf, b] + change[:, :chans]
            df_out[ch * nb + b + 1, t] = inbuf[buf, b + 1] + change[:, chans:]

    def place(i, of_core):
        block = block_at(lax.div(i, pieces), way)
        start = lax.rem(i, pieces) * piece
        return block, pl.ds(start, piece), pl.ds(first_degree(block, of_core) * wide + start, piece)

    def rs_copy(i):
        block, part, there = place(i, core)
        return to(onward, mine.at[block, part], dw_out.at[there], rs_send, rs_recv.at[i])

    def add_pair(i):
        block, part, _ = place(i, core)
        _, _, passed = place(i, 1 - core)

        @pl.when(lax.rem(i, pieces) == 0)
        def _():
            pair_copy(lax.div(i, pieces)).wait_recv()

        mine[block, part] += dw_out[passed]

    def rs_step(i, _):
        add_pair(i)

        @pl.when(i >= pieces)
        def _():
            rs_copy(i - pieces).wait_recv()
            block, part, there = place(i, core)
            mine[block, part] += dw_out[there]

        rs_copy(i).start()

        @pl.when(i < units)
        def _():
            final_rows(i)

        return 0

    lax.fori_loop(0, hops, rs_step, 0)

    def own_sum(s, _):
        i = hops + s
        add_pair(i)
        rs_copy(i - pieces).wait_recv()
        block, part, there = place(i, core)
        dw_out[there] += mine[block, part]
        return 0

    lax.fori_loop(0, pieces, own_sum, 0)
    pl.semaphore_signal(free_sem, inc=1, device_id={axis: sibling}, device_id_type=pl.DeviceIdType.MESH)

    for which in range(2):
        others = low.at[which, pl.ds(0, n - 1)]
        pltpu.make_async_copy(others, others, low_recv.at[which]).wait()
    outer(wbuf.at[0], 0, [(low[1].reshape(-1, chans), low[0].reshape(-1, chans))])
    dw_out[pl.ds(me * wide, wide)] = wbuf[0, pl.ds(0, wide)]

    def spot(i):
        return pl.ds(first_degree(block_at(lax.div(i, pieces), way), core) * wide + lax.rem(i, pieces) * piece, piece)

    def low_spot(k):
        return pl.ds((2 * block_at(k, way) + core) * wide, wide)

    def ag_copy(rows_out, got):
        return to(onward, dw_out.at[rows_out], dw_out.at[rows_out], ag_send, got)

    def publish(rows_out):
        to(sibling, dw_out.at[rows_out], dw_out.at[rows_out], pub_send, pub_recv).start()

    pl.semaphore_wait(free_sem, 1)

    def own_piece(s, _):
        rows_out = spot(hops + s)
        ag_copy(rows_out, ag_recv.at[s]).start()
        publish(rows_out)
        return 0

    lax.fori_loop(0, pieces, own_piece, 0)
    ag_copy(low_spot(chips - 1), ag_recv.at[hops]).start()
    publish(low_spot(chips - 1))

    def ag_step(i, _):
        rows_out = spot(i)
        ag_copy(rows_out, ag_recv.at[i]).wait_recv()

        @pl.when(i + pieces < hops)
        def _():
            ag_copy(rows_out, ag_recv.at[i + pieces]).start()

        publish(rows_out)

        @pl.when(lax.rem(i, pieces) == pieces - 1)
        def _():
            k = lax.div(i, pieces)
            low_out = low_spot(k)
            ag_copy(low_out, ag_recv.at[hops + k]).wait_recv()

            @pl.when(k < chips - 2)
            def _():
                ag_copy(low_out, ag_recv.at[hops + k + 1]).start()

            publish(low_out)

        return 0

    lax.fori_loop(0, hops, ag_step, 0)

    def rest(unit, _):
        final_rows(unit)
        return 0

    lax.fori_loop(min(hops, units), units, rest, 0)

    for index in range(4 * chunks - SEND_SLOTS, 4 * chunks):
        wait_sent(index)
    sent = mine.at[pl.ds(0, chips - 1)]
    pltpu.make_async_copy(sent, sent, rs_send).wait()
    sent = dw_out.at[pl.ds(0, (chips - 1) * (half + 1) * wide)]
    pltpu.make_async_copy(sent, sent, ag_send).wait()
    for which in range(2):
        others = low.at[which, pl.ds(0, n - 1)]
        pltpu.make_async_copy(others, others, low_send.at[which]).wait()
    shared = dw_out.at[pl.ds(0, degs // 2 * wide)]
    pltpu.make_async_copy(shared, shared, pub_send).wait()
    pltpu.make_async_copy(shared, shared, pub_recv).wait()


def solution(mesh):
    n = mesh.shape['lat']
    field_spec = P('member', None, 'lat', None)

    def local_step(field_loc, grad_loc, p_fwd, p_inv, w_mix):
        batch, chans, tl, lons = field_loc.shape
        degs, lats = p_fwd.shape[1:]
        ml = p_fwd.shape[0] // n
        nb = 4
        chunks = batch // nb
        rows = ml * 2 * nb
        pitch = rows + 1
        half = degs // n - 1
        pieces = 4 if half * 2 * chans % 32 == 0 else 1
        hops = (n // 2 - 1) * pieces
        tables = fourier_tables(n, ml, lons)
        anywhere = pl.BlockSpec(memory_space=pl.ANY)
        vmem = pl.BlockSpec(memory_space=pltpu.VMEM)
        grad_field, grad_w = pl.pallas_call(
            functools.partial(layer_kernel, 'lat', n, nb, pieces),
            name='layer',
            out_shape=(
                pltpu.VMEM((batch, tl, lons, chans), F32),
                pltpu.VMEM((degs * 2 * chans, chans), F32),
            ),
            in_specs=[anywhere] * 5 + [vmem] * len(tables),
            out_specs=(vmem, vmem),
            scratch_shapes=[
                pltpu.VMEM((2, chunks, n, tl, rows, chans), BF16),
                pltpu.VMEM((SEND_SLOTS, n, tl, rows, chans), BF16),
                pltpu.VMEM((lats * pitch, chans), F32),
                pltpu.VMEM((lats * pitch, chans), F32),
                pltpu.VMEM((lats, 2 * nb * chans), BF16),
                pltpu.VMEM((degs, chunks, rows, chans), BF16),
                pltpu.VMEM((degs, chunks, rows, chans), BF16),
                pltpu.VMEM((degs, 2 * chans, chans), BF16),
                pltpu.VMEM((2, 8 * 2 * chans, chans), F32),
                pltpu.VMEM((2, nb, lons, chans), F32),
                pltpu.VMEM((n * rows, chans), F32),
                pltpu.VMEM((2, ml, degs, lats), F32),
                pltpu.VMEM((2, ml, degs, lats), BF16),
                pltpu.VMEM((n // 2, half * 2 * chans, chans), F32),
                pltpu.VMEM((2, n, chunks, 2 * nb, chans), BF16),
                pltpu.SemaphoreType.DMA((4 * chunks,)),
                pltpu.SemaphoreType.DMA((4 * chunks,)),
                pltpu.SemaphoreType.DMA((2,)),
                pltpu.SemaphoreType.DMA((2,)),
                pltpu.SemaphoreType.DMA((2,)),
                pltpu.SemaphoreType.DMA((2,)),
                pltpu.SemaphoreType.DMA((n // 2,)),
                pltpu.SemaphoreType.DMA,
                pltpu.SemaphoreType.DMA((hops,)),
                pltpu.SemaphoreType.DMA,
                pltpu.SemaphoreType.DMA((hops + n // 2 - 1,)),
                pltpu.SemaphoreType.DMA((2,)),
                pltpu.SemaphoreType.DMA((2,)),
                pltpu.SemaphoreType.REGULAR,
                pltpu.SemaphoreType.DMA,
                pltpu.SemaphoreType.DMA,
            ],
            compiler_params=pltpu.CompilerParams(
                collective_id=0, has_side_effects=True, vmem_limit_bytes=42 * 1024 * 1024),
        )(
            field_loc.transpose(0, 2, 3, 1), grad_loc.transpose(0, 2, 3, 1),
            w_mix.transpose(0, 1, 3, 2).reshape(degs * 2 * chans, chans),
            p_fwd, p_inv, *tables)
        return grad_field.transpose(0, 3, 1, 2), grad_w.reshape(degs, chans, 2, chans).transpose(0, 1, 3, 2)

    return jax.shard_map(
        local_step, mesh=mesh, in_specs=(field_spec, field_spec, P(), P(), P()),
        out_specs=(field_spec, P('member', None, None, None)), check_vma=False)
```

```python
import functools
import math

import jax
import jax.numpy as jnp
import numpy as np
from jax import lax
from jax.experimental import pallas as pl
from jax.experimental.pallas import tpu as pltpu
from jax.sharding import PartitionSpec as P

F32 = jnp.float32
BF16 = jnp.bfloat16
SEND_SLOTS = 4


def split_const(matrix):
    head = matrix.astype(BF16)
    tail = (matrix - head.astype(np.float64)).astype(BF16)
    return [head, tail]


def fourier_tables(n, ml, lons):
    modes = n * ml
    device = np.arange(n)
    first = np.where(device % 2 == 0, device // 2, n - 1 - device // 2)
    order = (first[:, None] + n * np.arange(ml)[None, :]).reshape(-1)
    angle = 2.0 * np.pi * (np.outer(order, np.arange(lons)) % lons) / lons
    forward = np.stack([np.cos(angle), -np.sin(angle)], axis=1).reshape(2 * modes, lons) / math.sqrt(lons)
    gains = np.repeat(np.where(order == 0, 1.0, 2.0), 2)[:, None]
    doubled = forward * gains
    tables = split_const(forward) + split_const(doubled) + split_const(doubled.T) + split_const(forward.T)
    return [jnp.asarray(t) for t in tables]


def gelu_grad(values):
    cumulative = 0.5 * (1.0 + lax.erf(values * math.sqrt(0.5)))
    density = jnp.exp(-0.5 * values * values) / math.sqrt(2.0 * math.pi)
    return cumulative + values * density


def dot(a, b, dims=((1,), (0,))):
    return lax.dot_general(a, b, (dims, ((), ())), preferred_element_type=F32)


def layer_kernel(
    axis, n, nb, pieces, per,
    f_hbm, dg_hbm, w_hbm, pf_hbm, pv_hbm,
    fwd_h, fwd_l, dbl_h, dbl_l, syn_h, syn_l, adj_h, adj_l,
    df_out, dw_out,
    recv, send, work, xb, coef, dq, vmix, wbuf, inbuf, gather, pbuf, pmat, band, cmat, qs, own, other, packs, lowx,
    send_sem, recv_sem, in_sem, w_sem, p_sem, band_sem, pair_send, pair_recv, rs_send, rs_recv, ag_send, ag_recv,
    free_sem, pub_send, pub_recv, own_send, own_recv, pack_send, pack_recv, share_send, share_recv,
):
    me = lax.axis_index(axis)
    batch, tl, lons, chans = f_hbm.shape
    ml, degs, lats = pmat.shape[1:]
    chunks = batch // nb
    tile = 2 * nb
    rows = ml * tile
    pitch = rows + 1
    modes2 = 2 * n * ml
    units = chunks * tl
    area = lats * pitch
    top = n * (ml - 1)
    held = n // 2 + 1
    chip, core = lax.div(me, 2), lax.rem(me, 2)
    chips = n // 2
    way = 1 - 2 * core
    sibling = me + way
    onward = 2 * lax.rem(chip + way + chips, chips) + core

    def first_mode(device):
        z = lax.div(device, 2)
        return jnp.where(lax.rem(device, 2) == 0, z, n - 1 - z)

    def to(device, src, dst, sent, got):
        return pltpu.make_async_remote_copy(
            src_ref=src, dst_ref=dst, send_sem=sent, recv_sem=got,
            device_id={axis: device}, device_id_type=pl.DeviceIdType.MESH)

    barrier = pltpu.get_barrier_semaphore()

    def announce(k, _):
        pl.semaphore_signal(barrier, inc=1, device_id={axis: lax.rem(me + k, n)}, device_id_type=pl.DeviceIdType.MESH)
        return 0

    lax.fori_loop(1, n, announce, 0)

    def unit_of(unit):
        return lax.div(unit, tl), lax.rem(unit, tl)

    def unit_in(src, unit):
        ch, t = unit_of(unit)
        slot = lax.rem(unit, 2)
        return pltpu.make_async_copy(src.at[pl.ds(ch * nb, nb), t], inbuf.at[slot], in_sem.at[slot])

    def step_in(src, unit):
        @pl.when(unit + 1 < units)
        def _():
            unit_in(src, unit + 1).start()
        unit_in(src, unit).wait()

    def sent_rows(stage):
        return pl.ds(0, rows - tile if stage == 3 else rows)

    def ship(stage, ch, t0, nt):
        index = stage * chunks + ch
        slot = lax.rem(index, SEND_SLOTS)
        part, span = pl.ds(t0, nt), sent_rows(stage)

        def one(k, _):
            peer = lax.rem(me + k, n)
            to(peer, send.at[slot, peer, part, span], recv.at[stage % 2, ch, me, part, span],
               send_sem.at[index], recv_sem.at[index]).start()
            return 0

        lax.fori_loop(1, n, one, 0)
        recv[stage % 2, ch, me, part, span] = send[slot, me, part, span]

    def arrived(stage, ch):
        others = recv.at[stage % 2, ch, pl.ds(0, n - 1), :, sent_rows(stage)]
        pltpu.make_async_copy(others, others, recv_sem.at[stage * chunks + ch]).wait()

    def wait_sent(index, stage=0):
        others = send.at[lax.rem(index, SEND_SLOTS), pl.ds(0, n - 1), :, sent_rows(stage)]
        pltpu.make_async_copy(others, others, send_sem.at[index]).wait()

    def free_slot(stage, ch):
        index = stage * chunks + ch

        @pl.when(index >= SEND_SLOTS)
        def _():
            wait_sent(index - SEND_SLOTS)

        return lax.rem(index, SEND_SLOTS)

    def put_rows(slot, t):
        send[slot, :, t] = gather[...].reshape(n, rows, chans).astype(BF16)

    def transform(values, head, tail):
        high = values.astype(BF16)
        low = (values - high.astype(F32)).astype(BF16)
        return dot(head[...], high) + (dot(tail[...], high) + dot(head[...], low))

    unit_in(f_hbm, 0).start()
    for which, source in enumerate((pf_hbm, pv_hbm)):
        for k in range(ml):
            pltpu.make_async_copy(source.at[first_mode(me) + n * k], pbuf.at[which, k], p_sem.at[which]).start()

    def band_in(d, _):
        pltpu.make_async_copy(pf_hbm.at[top + first_mode(d), pl.ds(top, n)], band.at[d], band_sem).start()
        return 0

    lax.fori_loop(0, n, band_in, 0)

    group = 2 if tl % 2 == 0 else 1

    def by_rows(stage, ch, row):
        slot = free_slot(stage, ch)

        def part(p, _):
            def one(j, _):
                row(slot, p * group + j)
                return 0

            lax.fori_loop(0, group, one, 0)
            if stage == 0:
                @pl.when(ch + p == 0)
                def _():
                    pl.semaphore_wait(barrier, n - 1)
            ship(stage, ch, p * group, group)
            return 0

        lax.fori_loop(0, tl // group, part, 0)

    def step1_chunk(ch, _):
        def row(slot, t):
            unit = ch * tl + t
            step_in(f_hbm, unit)
            buf = lax.rem(unit, 2)
            for b in range(0, nb, 2):
                pair = jnp.concatenate([inbuf[buf, b], inbuf[buf, b + 1]], axis=1)
                spec = transform(pair, fwd_h, fwd_l)
                gather[pl.ds(b, modes2, stride=nb), :] = spec[:, :chans]
                gather[pl.ds(b + 1, modes2, stride=nb), :] = spec[:, chans:]
            put_rows(slot, t)

        by_rows(0, ch, row)
        return 0

    lax.fori_loop(0, chunks, step1_chunk, 0)
    unit_in(dg_hbm, 0).start()
    for which in range(2):
        pltpu.make_async_copy(pbuf.at[which], pbuf.at[which], p_sem.at[which]).wait()
    pmat[...] = pbuf[...].astype(BF16)

    parts = degs // per

    def w_in(k):
        slot = lax.rem(k, 2)
        return pltpu.make_async_copy(w_hbm.at[pl.ds(k * per * 2 * chans, per * 2 * chans)], wbuf.at[slot, pl.ds(0, per * 2 * chans)], w_sem.at[slot])

    w_in(0).start()

    def load_w(k, _):
        @pl.when(k + 1 < parts)
        def _():
            w_in(k + 1).start()
        w_in(k).wait()
        slot = lax.rem(k, 2)
        for j in range(per):
            for part in range(2):
                vmix[k * per + j, pl.ds(part * chans, chans)] = wbuf[
                    slot, pl.ds(j * 2 * chans + part, chans, stride=2), :].astype(BF16)
        return 0

    lax.fori_loop(0, parts, load_w, 0)

    sign = jnp.where(lax.broadcasted_iota(jnp.int32, (tile, chans), 0) < nb, -1.0, 1.0).astype(F32)

    def turn(values):
        groups = values.reshape(-1, tile, chans)
        return (pltpu.roll(groups, nb, 1) * sign[None]).reshape(values.shape)

    def legendre(src, dst, which, over):
        def mode(m, _):
            for k in range(tile):
                xb[:, k * chans:(k + 1) * chans] = work[
                    pl.ds(src + m * tile + k, lats, stride=pitch), :].astype(BF16)
            out = dot(pmat[which, m], xb[...], ((over,), (0,)))
            for k in range(tile):
                work[pl.ds(dst + m * tile + k, degs, stride=pitch), :] = out[:, k * chans:(k + 1) * chans]
            return 0

        lax.fori_loop(0, ml, mode, 0)

    def unload(stage, ch):
        def body(src, _):
            for t in range(tl):
                work[pl.ds((src * tl + t) * pitch, rows), :] = recv[stage % 2, ch, src, t].astype(F32)
            return 0

        lax.fori_loop(0, n, body, 0)

    def load(slot):
        def body(dev, _):
            for t in range(tl):
                send[slot, dev, t] = work[pl.ds(area + (dev * tl + t) * pitch, rows), :].astype(BF16)
            return 0

        lax.fori_loop(0, n, body, 0)

    def pack(store):
        def one(index, _):
            half_at, row = lax.div(index, held), lax.rem(index, held)
            p = half_at * (held - 1) + row
            degree = jnp.where(core == 0, jnp.minimum(chip + p, n - 1), jnp.maximum(p - 1, 0))
            store(half_at, row, degree, (p < n - chip) == (core == 0))
            return 0

        lax.fori_loop(0, 2 * held, one, 0)

    def only(ours, values):
        values = values.astype(F32)
        return jnp.where(ours, values, jnp.zeros_like(values)).astype(BF16)

    def spectral(stage, ch, into, kept, mix):
        arrived(stage - 1, ch)
        unload(stage - 1, ch)
        legendre(0, area, into, 1)

        def degree(l, _):
            x = work[pl.ds(area + l * pitch, rows), :].astype(BF16)
            kept[l, ch] = x
            work[pl.ds(l * pitch, rows), :] = mix(l, x)
            return 0

        lax.fori_loop(0, degs, degree, 0, unroll=2)
        if stage == 3:
            def keep_top(half_at, row, degree, ours):
                own[half_at, 2, ch, row] = only(ours, work[pl.ds((top + degree) * pitch + rows - tile, tile), :])

            pack(keep_top)
        legendre(0, area, 1 - into, 0)
        load(free_slot(stage, ch))
        ship(stage, ch, 0, tl)

    def mix_forward(l, x):
        both = dot(x, vmix[l], ((1,), (1,)))
        return both[:, :chans] + turn(both[:, chans:])

    def mix_adjoint(l, x):
        real = dot(x, vmix[l, pl.ds(0, chans)])
        imag = dot(x, vmix[l, pl.ds(chans, chans)])
        return real - turn(imag)

    def step2_chunk(ch, _):
        spectral(1, ch, 0, coef, mix_forward)
        return 0

    lax.fori_loop(0, chunks, step2_chunk, 0)

    def fetch_rows(stage, ch, t):
        for src in range(n):
            gather[pl.ds(src * rows, rows), :] = recv[stage % 2, ch, src, t].astype(F32)

    def fetch_pair(b):
        return jnp.concatenate(
            [gather[pl.ds(b, modes2, stride=nb), :], gather[pl.ds(b + 1, modes2, stride=nb), :]], axis=1).astype(BF16)

    def step3_chunk(ch, _):
        arrived(1, ch)

        def row(slot, t):
            unit = ch * tl + t
            step_in(dg_hbm, unit)
            buf = lax.rem(unit, 2)
            fetch_rows(1, ch, t)
            for b in range(0, nb, 2):
                g = fetch_pair(b)
                hidden = dot(syn_h[...], g) + dot(syn_l[...], g)
                pair = jnp.concatenate([inbuf[buf, b], inbuf[buf, b + 1]], axis=1)
                spec = transform(pair * gelu_grad(hidden), dbl_h, dbl_l)
                gather[pl.ds(b, modes2, stride=nb), :] = spec[:, :chans]
                gather[pl.ds(b + 1, modes2, stride=nb), :] = spec[:, chans:]
            put_rows(slot, t)

        by_rows(2, ch, row)
        return 0

    lax.fori_loop(0, chunks, step3_chunk, 0)
    unit_in(dg_hbm, 0).start()

    def step4_chunk(ch, _):
        spectral(3, ch, 1, dq, mix_adjoint)
        return 0

    lax.fori_loop(0, chunks, step4_chunk, 0)

    for which, kept in enumerate((coef, dq)):
        def keep_low(half_at, row, degree, ours):
            own[half_at, which, :, row] = only(ours, kept[degree, :, pl.ds(0, tile)])

        pack(keep_low)
    own_copy = to(sibling, own.at[1 - core], other, own_send, own_recv)
    own_copy.start()

    def pack_block(k):
        return packs.at[core, lax.rem(chip - way * k + chips, chips)]

    def pack_copy(k):
        return to(onward, pack_block(k), pack_block(k), pack_send, pack_recv.at[k])

    def share(k):
        to(sibling, pack_block(k), pack_block(k), share_send, share_recv).start()

    half = degs // n - 1
    wide = 2 * chans
    block_rows = half * wide
    piece = block_rows // pieces
    hops = (chips - 1) * pieces

    def block_at(k, direction):
        return lax.rem(chip - direction * (1 + k) + 2 * chips, chips)

    def outer(dst, row, pairs):
        real = jnp.zeros((chans, chans), F32)
        imag = jnp.zeros((chans, chans), F32)
        for y, x in pairs:
            real += dot(y, x, ((0,), (0,)))
            imag -= dot(turn(y.astype(F32)).astype(BF16), x, ((0,), (0,)))
        dst[pl.ds(row, chans, stride=2), :] = real
        dst[pl.ds(row + 1, chans, stride=2), :] = imag

    def first_degree(block, of_core):
        return n + (2 * block + of_core) * half

    def weight_grad(dst, degree):
        def one(j, _):
            outer(dst, j * wide, [(dq[degree + j, ch], coef[degree + j, ch]) for ch in range(chunks)])
            return 0

        lax.fori_loop(0, half, one, 0)

    def pair_copy(k):
        slot = lax.rem(k, 2)
        rows_there = pl.ds(first_degree(block_at(k, -way), core) * wide, block_rows)
        return to(sibling, wbuf.at[slot, pl.ds(0, block_rows)], dw_out.at[rows_there],
                  pair_send.at[slot], pair_recv.at[k])

    def weight_block(k, _):
        @pl.when(k >= 2)
        def _():
            pair_copy(k - 2).wait_send()
        weight_grad(wbuf.at[lax.rem(k, 2)], first_degree(block_at(k, -way), 1 - core))
        pair_copy(k).start()
        block = block_at(k, way)
        weight_grad(work.at[pl.ds(block * block_rows, block_rows)], first_degree(block, core))
        return 0

    lax.fori_loop(0, chips, weight_block, 0)
    pair_copy(chips - 2).wait_send()
    pair_copy(chips - 1).wait_send()
    own_copy.wait()
    packs[core, chip] = (own[core].astype(F32) + other[...].astype(F32)).astype(BF16)

    pltpu.make_async_copy(band, band, band_sem).wait()
    qs[...] = jnp.zeros_like(qs)
    span = cmat.shape[2]
    mine_t = (lax.broadcasted_iota(jnp.int32, (8, lats), 1) == me * tl + lax.broadcasted_iota(jnp.int32, (8, lats), 0))
    mine_t &= lax.broadcasted_iota(jnp.int32, (8, lats), 0) < tl
    mine_t = jnp.where(mine_t, 1.0, 0.0).astype(BF16)

    def tabulate(d, _):
        z, of_core = lax.div(d, 2), lax.rem(d, 2)
        row = lax.broadcasted_iota(jnp.int32, (n, span), 0)
        p = jnp.where(of_core == 0, row - z, row + 1)
        target = jnp.where(p > held - 1, p + 1, p)
        moved = jnp.where(target == lax.broadcasted_iota(jnp.int32, (n, span), 1), 1.0, 0.0).astype(BF16)
        picked = dot(mine_t, band[d].astype(BF16), ((1,), (1,))).astype(BF16)
        cmat[z, pl.ds(pl.multiple_of(of_core * 8, 8), 8), :] = dot(picked, moved)
        return 0

    lax.fori_loop(0, n, tabulate, 0)

    def apply_top(ch, z):
        for h in range(2):
            qs[pl.ds(h * held * tile, held * tile), :] = packs[h, z, 2, ch].reshape(held * tile, chans).astype(F32)
        for k in range(tile):
            xb[0:span, k * chans:(k + 1) * chans] = qs[pl.ds(k, span, stride=tile), :].astype(BF16)
        out = dot(cmat[z].astype(BF16), xb[0:span, :])
        for k in range(tile):
            gather[pl.ds(k, 16, stride=tile), :] = out[:, k * chans:(k + 1) * chans]
        for c in range(2):
            for t in range(tl):
                recv[1, ch, 2 * z + c, t, pl.ds(rows - tile, tile)] = gather[
                    pl.ds((8 * c + t) * tile, tile), :].astype(BF16)

    def low_degree(l):
        def one(z, _):
            for c in range(2):
                p = l - z if c == 0 else l + 1
                ours = p >= 0 if c == 0 else p >= n - z
                p = jnp.maximum(p, 0)
                h = jnp.where(p > held - 1, 1, 0)
                for which in range(2):
                    lowx[which, 2 * z + c] = only(ours, packs[h, z, which, :, p - h * (held - 1)])
            return 0

        lax.fori_loop(0, chips, one, 0)
        outer(wbuf.at[0], 0, [(lowx[1].reshape(-1, chans), lowx[0].reshape(-1, chans))])
        dw_out[pl.ds(l * wide, wide)] = wbuf[0, pl.ds(0, wide)]

    def final_rows(unit):
        ch, t = unit_of(unit)

        step_in(dg_hbm, unit)
        buf = lax.rem(unit, 2)

        fetch_rows(3, ch, t)
        for b in range(0, nb, 2):
            g = fetch_pair(b)
            change = dot(adj_h[...], g) + dot(adj_l[...], g)
            df_out[ch * nb + b, t] = inbuf[buf, b] + change[:, :chans]
            df_out[ch * nb + b + 1, t] = inbuf[buf, b + 1] + change[:, chans:]

    def place(i, of_core):
        block = block_at(lax.div(i, pieces), way)
        start = lax.rem(i, pieces) * piece
        return pl.ds(block * block_rows + start, piece), pl.ds(first_degree(block, of_core) * wide + start, piece)

    def rs_copy(i):
        here, there = place(i, core)
        return to(onward, work.at[here], dw_out.at[there], rs_send, rs_recv.at[i])

    def add_pair(i):
        here, passed = place(i, 1 - core)

        @pl.when(lax.rem(i, pieces) == 0)
        def _():
            pair_copy(lax.div(i, pieces)).wait_recv()

        work[here] += dw_out[passed]

    def rs_step(i, _):
        add_pair(i)

        @pl.when(i >= pieces)
        def _():
            rs_copy(i - pieces).wait_recv()
            here, there = place(i, core)
            work[here] += dw_out[there]

        rs_copy(i).start()

        @pl.when(lax.rem(i, pieces) == 0)
        def _():
            k = lax.div(i, pieces)

            @pl.when(k > 0)
            def _():
                pack_copy(k - 1).wait_recv()

            pack_copy(k).start()
            share(k)

        return 0

    lax.fori_loop(0, hops, rs_step, 0)
    pack_copy(chips - 2).wait_recv()
    share(chips - 1)

    def own_sum(s, _):
        i = hops + s
        add_pair(i)
        rs_copy(i - pieces).wait_recv()
        here, there = place(i, core)
        dw_out[there] += work[here]
        return 0

    lax.fori_loop(0, pieces, own_sum, 0)
    pl.semaphore_signal(free_sem, inc=1, device_id={axis: sibling}, device_id_type=pl.DeviceIdType.MESH)

    def ag_copy(i, got):
        _, there = place(i, core)
        return to(onward, dw_out.at[there], dw_out.at[there], ag_send, ag_recv.at[got])

    def publish(i):
        _, there = place(i, core)
        to(sibling, dw_out.at[there], dw_out.at[there], pub_send, pub_recv).start()

    pl.semaphore_wait(free_sem, 1)

    def own_piece(s, _):
        ag_copy(hops + s, s).start()
        publish(hops + s)
        return 0

    lax.fori_loop(0, pieces, own_piece, 0)
    gathered = packs.at[1 - core]
    pltpu.make_async_copy(gathered, gathered, share_recv).wait()

    def task(i):
        @pl.when(i < chips)
        def _():
            for ch in range(chunks):
                @pl.when(i == 0)
                def _():
                    arrived(3, ch)
                apply_top(ch, i)

        @pl.when((i >= chips) & (i < chips + units))
        def _():
            final_rows(i - chips)

        @pl.when(i < n)
        def _():
            low_degree(i)

    def ag_step(i, _):
        ag_copy(i, i).wait_recv()

        @pl.when(i + pieces < hops)
        def _():
            ag_copy(i, i + pieces).start()

        publish(i)
        task(i)
        return 0

    lax.fori_loop(0, hops, ag_step, 0)

    def rest(i, _):
        task(i)
        return 0

    lax.fori_loop(hops, max(hops, chips + units, n), rest, 0)

    wait_sent(3 * chunks - 1)
    for ch in range(chunks):
        wait_sent(3 * chunks + ch, 3)
    sent = work.at[pl.ds(0, (chips - 1) * block_rows)]
    pltpu.make_async_copy(sent, sent, rs_send).wait()
    pltpu.make_async_copy(sent, sent, ag_send).wait()
    sent = packs.at[0, pl.ds(0, chips - 1)]
    pltpu.make_async_copy(sent, sent, pack_send).wait()
    pltpu.make_async_copy(packs.at[0], packs.at[0], share_send).wait()
    shared = dw_out.at[pl.ds(0, chips * block_rows)]
    pltpu.make_async_copy(shared, shared, pub_send).wait()
    pltpu.make_async_copy(shared, shared, pub_recv).wait()


def solution(mesh):
    n = mesh.shape['lat']
    field_spec = P('member', None, 'lat', None)

    def local_step(field_loc, grad_loc, p_fwd, p_inv, w_mix):
        batch, chans, tl, lons = field_loc.shape
        degs, lats = p_fwd.shape[1:]
        ml = p_fwd.shape[0] // n
        nb = 4
        chunks = batch // nb
        rows = ml * 2 * nb
        pitch = rows + 1
        half = degs // n - 1
        pieces = 4 if half * 2 * chans % 32 == 0 else 1
        hops = (n // 2 - 1) * pieces
        per = 4
        held = n // 2 + 1
        packed = (3, chunks, held, 2 * nb, chans)
        tables = fourier_tables(n, ml, lons)
        anywhere = pl.BlockSpec(memory_space=pl.ANY)
        vmem = pl.BlockSpec(memory_space=pltpu.VMEM)
        grad_field, grad_w = pl.pallas_call(
            functools.partial(layer_kernel, 'lat', n, nb, pieces, per),
            name='layer',
            out_shape=(
                pltpu.VMEM((batch, tl, lons, chans), F32),
                pltpu.VMEM((degs * 2 * chans, chans), F32),
            ),
            in_specs=[anywhere] * 5 + [vmem] * len(tables),
            out_specs=(vmem, vmem),
            scratch_shapes=[
                pltpu.VMEM((2, chunks, n, tl, rows, chans), BF16),
                pltpu.VMEM((SEND_SLOTS, n, tl, rows, chans), BF16),
                pltpu.VMEM((max(2 * lats * pitch, n // 2 * half * 2 * chans), chans), F32),
                pltpu.VMEM((lats, 2 * nb * chans), BF16),
                pltpu.VMEM((degs, chunks, rows, chans), BF16),
                pltpu.VMEM((degs, chunks, rows, chans), BF16),
                pltpu.VMEM((degs, 2 * chans, chans), BF16),
                pltpu.VMEM((2, max(per, half) * 2 * chans, chans), F32),
                pltpu.VMEM((2, nb, lons, chans), F32),
                pltpu.VMEM((n * rows, chans), F32),
                pltpu.VMEM((2, ml, degs, lats), F32),
                pltpu.VMEM((2, ml, degs, lats), BF16),
                pltpu.VMEM((n, n, lats), F32),
                pltpu.VMEM((n // 2, 16, 32), F32),
                pltpu.VMEM((32 * 2 * nb, chans), F32),
                pltpu.VMEM((2,) + packed, BF16),
                pltpu.VMEM(packed, BF16),
                pltpu.VMEM((2, n // 2) + packed, BF16),
                pltpu.VMEM((2, n, chunks, 2 * nb, chans), BF16),
                pltpu.SemaphoreType.DMA((4 * chunks,)),
                pltpu.SemaphoreType.DMA((4 * chunks,)),
                pltpu.SemaphoreType.DMA((2,)),
                pltpu.SemaphoreType.DMA((2,)),
                pltpu.SemaphoreType.DMA((2,)),
                pltpu.SemaphoreType.DMA,
                pltpu.SemaphoreType.DMA((2,)),
                pltpu.SemaphoreType.DMA((n // 2,)),
                pltpu.SemaphoreType.DMA,
                pltpu.SemaphoreType.DMA((hops,)),
                pltpu.SemaphoreType.DMA,
                pltpu.SemaphoreType.DMA((hops,)),
                pltpu.SemaphoreType.REGULAR,
                pltpu.SemaphoreType.DMA,
                pltpu.SemaphoreType.DMA,
                pltpu.SemaphoreType.DMA,
                pltpu.SemaphoreType.DMA,
                pltpu.SemaphoreType.DMA,
                pltpu.SemaphoreType.DMA((n // 2 - 1,)),
                pltpu.SemaphoreType.DMA,
                pltpu.SemaphoreType.DMA,
            ],
            compiler_params=pltpu.CompilerParams(
                collective_id=0, has_side_effects=True, vmem_limit_bytes=42 * 1024 * 1024),
        )(
            field_loc.transpose(0, 2, 3, 1), grad_loc.transpose(0, 2, 3, 1),
            w_mix.transpose(0, 1, 3, 2).reshape(degs * 2 * chans, chans),
            p_fwd, p_inv, *tables)
        return grad_field.transpose(0, 3, 1, 2), grad_w.reshape(degs, chans, 2, chans).transpose(0, 1, 3, 2)

    return jax.shard_map(
        local_step, mesh=mesh, in_specs=(field_spec, field_spec, P(), P(), P()),
        out_specs=(field_spec, P('member', None, None, None)), check_vma=False)
```

```python
import functools
import math

import jax
import jax.numpy as jnp
import numpy as np
from jax import lax
from jax.experimental import pallas as pl
from jax.experimental.pallas import tpu as pltpu
from jax.sharding import PartitionSpec as P

F32 = jnp.float32
BF16 = jnp.bfloat16
SEND_SLOTS = 4


def split_const(matrix):
    head = matrix.astype(BF16)
    tail = (matrix - head.astype(np.float64)).astype(BF16)
    return [head, tail]


def fourier_tables(n, ml, lons):
    modes = n * ml
    device = np.arange(n)
    first = np.where(device % 2 == 0, device // 2, n - 1 - device // 2)
    order = (first[:, None] + n * np.arange(ml)[None, :]).reshape(-1)
    angle = 2.0 * np.pi * (np.outer(order, np.arange(lons)) % lons) / lons
    forward = np.stack([np.cos(angle), -np.sin(angle)], axis=1).reshape(2 * modes, lons) / math.sqrt(lons)
    gains = np.repeat(np.where(order == 0, 1.0, 2.0), 2)[:, None]
    doubled = forward * gains
    tables = split_const(forward) + split_const(doubled) + split_const(doubled.T) + split_const(forward.T)
    return [jnp.asarray(t) for t in tables]


def gelu_grad(values):
    cumulative = 0.5 * (1.0 + lax.erf(values * math.sqrt(0.5)))
    density = jnp.exp(-0.5 * values * values) / math.sqrt(2.0 * math.pi)
    return cumulative + values * density


def dot(a, b, dims=((1,), (0,))):
    return lax.dot_general(a, b, (dims, ((), ())), preferred_element_type=F32)


def layer_kernel(
    axis, n, nb, pieces, per,
    f_hbm, dg_hbm, w_hbm, pf_hbm, pv_hbm,
    fwd_h, fwd_l, dbl_h, dbl_l, syn_h, syn_l, adj_h, adj_l,
    df_out, dw_out,
    recv, send, work, xb, coef, dq, vmix, wbuf, inbuf, gather, pbuf, pmat, band, cmat, qs, own, other, packs, lowx,
    send_sem, recv_sem, in_sem, w_sem, p_sem, band_sem, pair_send, pair_recv, rs_send, rs_recv, ag_send, ag_recv,
    free_sem, pub_send, pub_recv, own_send, own_recv, pack_send, pack_recv, share_send, share_recv,
):
    me = lax.axis_index(axis)
    batch, tl, lons, chans = f_hbm.shape
    ml, degs, lats = pmat.shape[1:]
    chunks = batch // nb
    tile = 2 * nb
    rows = ml * tile
    pitch = rows + 1
    modes2 = 2 * n * ml
    units = chunks * tl
    area = lats * pitch
    top = n * (ml - 1)
    held = n // 2 + 1
    chip, core = lax.div(me, 2), lax.rem(me, 2)
    chips = n // 2
    way = 1 - 2 * core
    sibling = me + way
    onward = 2 * lax.rem(chip + way + chips, chips) + core

    def first_mode(device):
        z = lax.div(device, 2)
        return jnp.where(lax.rem(device, 2) == 0, z, n - 1 - z)

    def to(device, src, dst, sent, got):
        return pltpu.make_async_remote_copy(
            src_ref=src, dst_ref=dst, send_sem=sent, recv_sem=got,
            device_id={axis: device}, device_id_type=pl.DeviceIdType.MESH)

    barrier = pltpu.get_barrier_semaphore()

    def announce(k, _):
        pl.semaphore_signal(barrier, inc=1, device_id={axis: lax.rem(me + k, n)}, device_id_type=pl.DeviceIdType.MESH)
        return 0

    lax.fori_loop(1, n, announce, 0)

    def unit_of(unit):
        return lax.div(unit, tl), lax.rem(unit, tl)

    def unit_in(src, unit):
        ch, t = unit_of(unit)
        slot = lax.rem(unit, 2)
        return pltpu.make_async_copy(src.at[pl.ds(ch * nb, nb), t], inbuf.at[slot], in_sem.at[slot])

    def step_in(src, unit):
        @pl.when(unit + 1 < units)
        def _():
            unit_in(src, unit + 1).start()
        unit_in(src, unit).wait()

    def sent_rows(stage):
        return pl.ds(0, rows - tile if stage == 3 else rows)

    def ship(stage, ch, t0, nt):
        index = stage * chunks + ch
        slot = lax.rem(index, SEND_SLOTS)
        part, span = pl.ds(t0, nt), sent_rows(stage)

        def one(k, _):
            peer = lax.rem(me + k, n)
            to(peer, send.at[slot, peer, part, span], recv.at[stage % 2, ch, me, part, span],
               send_sem.at[index], recv_sem.at[index]).start()
            return 0

        lax.fori_loop(1, n, one, 0)
        recv[stage % 2, ch, me, part, span] = send[slot, me, part, span]

    def arrived(stage, ch):
        others = recv.at[stage % 2, ch, pl.ds(0, n - 1), :, sent_rows(stage)]
        pltpu.make_async_copy(others, others, recv_sem.at[stage * chunks + ch]).wait()

    def wait_sent(index, stage=0):
        others = send.at[lax.rem(index, SEND_SLOTS), pl.ds(0, n - 1), :, sent_rows(stage)]
        pltpu.make_async_copy(others, others, send_sem.at[index]).wait()

    def free_slot(stage, ch):
        index = stage * chunks + ch

        @pl.when(index >= SEND_SLOTS)
        def _():
            wait_sent(index - SEND_SLOTS)

        return lax.rem(index, SEND_SLOTS)

    def put_rows(slot, t):
        send[slot, :, t] = gather[...].reshape(n, rows, chans).astype(BF16)

    def transform(values, head, tail):
        high = values.astype(BF16)
        low = (values - high.astype(F32)).astype(BF16)
        return dot(head[...], high) + (dot(tail[...], high) + dot(head[...], low))

    unit_in(f_hbm, 0).start()
    for which, source in enumerate((pf_hbm, pv_hbm)):
        for k in range(ml):
            pltpu.make_async_copy(source.at[first_mode(me) + n * k], pbuf.at[which, k], p_sem.at[which]).start()

    def band_in(d, _):
        pltpu.make_async_copy(pf_hbm.at[top + first_mode(d), pl.ds(top, n)], band.at[d], band_sem).start()
        return 0

    lax.fori_loop(0, n, band_in, 0)

    group = 2 if tl % 2 == 0 else 1

    def by_rows(stage, ch, row):
        slot = free_slot(stage, ch)

        def part(p, _):
            def one(j, _):
                row(slot, p * group + j)
                return 0

            lax.fori_loop(0, group, one, 0)
            if stage == 0:
                @pl.when(ch + p == 0)
                def _():
                    pl.semaphore_wait(barrier, n - 1)
            ship(stage, ch, p * group, group)
            return 0

        lax.fori_loop(0, tl // group, part, 0)

    def step1_chunk(ch, _):
        def row(slot, t):
            unit = ch * tl + t
            step_in(f_hbm, unit)
            buf = lax.rem(unit, 2)
            for b in range(0, nb, 2):
                pair = jnp.concatenate([inbuf[buf, b], inbuf[buf, b + 1]], axis=1)
                spec = transform(pair, fwd_h, fwd_l)
                gather[pl.ds(b, modes2, stride=nb), :] = spec[:, :chans]
                gather[pl.ds(b + 1, modes2, stride=nb), :] = spec[:, chans:]
            put_rows(slot, t)

        by_rows(0, ch, row)
        return 0

    lax.fori_loop(0, chunks, step1_chunk, 0)
    unit_in(dg_hbm, 0).start()
    for which in range(2):
        pltpu.make_async_copy(pbuf.at[which], pbuf.at[which], p_sem.at[which]).wait()
    pmat[...] = pbuf[...].astype(BF16)

    parts = degs // per

    def w_in(k):
        slot = lax.rem(k, 2)
        return pltpu.make_async_copy(w_hbm.at[pl.ds(k * per * 2 * chans, per * 2 * chans)], wbuf.at[slot, pl.ds(0, per * 2 * chans)], w_sem.at[slot])

    w_in(0).start()

    def load_w(k, _):
        @pl.when(k + 1 < parts)
        def _():
            w_in(k + 1).start()
        w_in(k).wait()
        slot = lax.rem(k, 2)
        for j in range(per):
            for part in range(2):
                vmix[k * per + j, pl.ds(part * chans, chans)] = wbuf[
                    slot, pl.ds(j * 2 * chans + part, chans, stride=2), :].astype(BF16)
        return 0

    lax.fori_loop(0, parts, load_w, 0)

    sign = jnp.where(lax.broadcasted_iota(jnp.int32, (tile, chans), 0) < nb, -1.0, 1.0).astype(F32)

    def turn(values):
        groups = values.reshape(-1, tile, chans)
        return (pltpu.roll(groups, nb, 1) * sign[None]).reshape(values.shape)

    def legendre(src, dst, which, over):
        def mode(m, _):
            for k in range(tile):
                xb[:, k * chans:(k + 1) * chans] = work[
                    pl.ds(src + m * tile + k, lats, stride=pitch), :].astype(BF16)
            out = dot(pmat[which, m], xb[...], ((over,), (0,)))
            for k in range(tile):
                work[pl.ds(dst + m * tile + k, degs, stride=pitch), :] = out[:, k * chans:(k + 1) * chans]
            return 0

        lax.fori_loop(0, ml, mode, 0)

    def unload(stage, ch):
        def body(src, _):
            for t in range(tl):
                work[pl.ds((src * tl + t) * pitch, rows), :] = recv[stage % 2, ch, src, t].astype(F32)
            return 0

        lax.fori_loop(0, n, body, 0)

    def load(slot):
        def body(dev, _):
            for t in range(tl):
                send[slot, dev, t] = work[pl.ds(area + (dev * tl + t) * pitch, rows), :].astype(BF16)
            return 0

        lax.fori_loop(0, n, body, 0)

    def pack(store):
        def one(index, _):
            half_at, row = lax.div(index, held), lax.rem(index, held)
            p = half_at * (held - 1) + row
            degree = jnp.where(core == 0, jnp.minimum(chip + p, n - 1), jnp.maximum(p - 1, 0))
            store(half_at, row, degree, (p < n - chip) == (core == 0))
            return 0

        lax.fori_loop(0, 2 * held, one, 0)

    def only(ours, values):
        values = values.astype(F32)
        return jnp.where(ours, values, jnp.zeros_like(values)).astype(BF16)

    def spectral(stage, ch, into, kept, mix):
        arrived(stage - 1, ch)
        unload(stage - 1, ch)
        legendre(0, area, into, 1)

        def degree(l, _):
            x = work[pl.ds(area + l * pitch, rows), :].astype(BF16)
            kept[l, ch] = x
            work[pl.ds(l * pitch, rows), :] = mix(l, x)
            return 0

        lax.fori_loop(0, degs, degree, 0, unroll=2)
        if stage == 3:
            def keep_top(half_at, row, degree, ours):
                own[half_at, 2, ch, row] = only(ours, work[pl.ds((top + degree) * pitch + rows - tile, tile), :])

            pack(keep_top)
        legendre(0, area, 1 - into, 0)
        load(free_slot(stage, ch))
        ship(stage, ch, 0, tl)

    def mix_forward(l, x):
        both = dot(x, vmix[l], ((1,), (1,)))
        return both[:, :chans] + turn(both[:, chans:])

    def mix_adjoint(l, x):
        real = dot(x, vmix[l, pl.ds(0, chans)])
        imag = dot(x, vmix[l, pl.ds(chans, chans)])
        return real - turn(imag)

    def step2_chunk(ch, _):
        spectral(1, ch, 0, coef, mix_forward)
        return 0

    lax.fori_loop(0, chunks, step2_chunk, 0)

    def fetch_rows(stage, ch, t):
        for src in range(n):
            gather[pl.ds(src * rows, rows), :] = recv[stage % 2, ch, src, t].astype(F32)

    def fetch_pair(b):
        return jnp.concatenate(
            [gather[pl.ds(b, modes2, stride=nb), :], gather[pl.ds(b + 1, modes2, stride=nb), :]], axis=1).astype(BF16)

    def step3_chunk(ch, _):
        arrived(1, ch)

        def row(slot, t):
            unit = ch * tl + t
            step_in(dg_hbm, unit)
            buf = lax.rem(unit, 2)
            fetch_rows(1, ch, t)
            for b in range(0, nb, 2):
                g = fetch_pair(b)
                hidden = dot(syn_h[...], g) + dot(syn_l[...], g)
                pair = jnp.concatenate([inbuf[buf, b], inbuf[buf, b + 1]], axis=1)
                spec = transform(pair * gelu_grad(hidden), dbl_h, dbl_l)
                gather[pl.ds(b, modes2, stride=nb), :] = spec[:, :chans]
                gather[pl.ds(b + 1, modes2, stride=nb), :] = spec[:, chans:]
            put_rows(slot, t)

        by_rows(2, ch, row)
        return 0

    lax.fori_loop(0, chunks, step3_chunk, 0)
    unit_in(dg_hbm, 0).start()

    def step4_chunk(ch, _):
        spectral(3, ch, 1, dq, mix_adjoint)
        return 0

    lax.fori_loop(0, chunks, step4_chunk, 0)

    for which, kept in enumerate((coef, dq)):
        def keep_low(half_at, row, degree, ours):
            own[half_at, which, :, row] = only(ours, kept[degree, :, pl.ds(0, tile)])

        pack(keep_low)
    own_copy = to(sibling, own.at[1 - core], other, own_send, own_recv)
    own_copy.start()

    def pack_block(k):
        return packs.at[core, lax.rem(chip - way * k + chips, chips)]

    def pack_copy(k):
        return to(onward, pack_block(k), pack_block(k), pack_send, pack_recv.at[k])

    def share(k):
        to(sibling, pack_block(k), pack_block(k), share_send, share_recv).start()

    half = degs // n - 1
    wide = 2 * chans
    block_rows = half * wide
    piece = block_rows // pieces
    hops = (chips - 1) * pieces

    def block_at(k, direction):
        return lax.rem(chip - direction * (1 + k) + 2 * chips, chips)

    def outer(dst, row, pairs):
        real = jnp.zeros((chans, chans), F32)
        imag = jnp.zeros((chans, chans), F32)
        for y, x in pairs:
            real += dot(y, x, ((0,), (0,)))
            imag -= dot(turn(y.astype(F32)).astype(BF16), x, ((0,), (0,)))
        dst[pl.ds(row, chans, stride=2), :] = real
        dst[pl.ds(row + 1, chans, stride=2), :] = imag

    def first_degree(block, of_core):
        return n + (2 * block + of_core) * half

    def weight_grad(dst, degree):
        def one(j, _):
            outer(dst, j * wide, [(dq[degree + j, ch], coef[degree + j, ch]) for ch in range(chunks)])
            return 0

        lax.fori_loop(0, half, one, 0)

    def pair_copy(k):
        slot = lax.rem(k, 2)
        rows_there = pl.ds(first_degree(block_at(k, -way), core) * wide, block_rows)
        return to(sibling, wbuf.at[slot, pl.ds(0, block_rows)], dw_out.at[rows_there],
                  pair_send.at[slot], pair_recv.at[k])

    def weight_block(k, _):
        @pl.when(k >= 2)
        def _():
            pair_copy(k - 2).wait_send()
        weight_grad(wbuf.at[lax.rem(k, 2)], first_degree(block_at(k, -way), 1 - core))
        pair_copy(k).start()
        block = block_at(k, way)
        weight_grad(work.at[pl.ds(block * block_rows, block_rows)], first_degree(block, core))
        return 0

    lax.fori_loop(0, chips, weight_block, 0)
    pair_copy(chips - 2).wait_send()
    pair_copy(chips - 1).wait_send()
    own_copy.wait()
    packs[core, chip] = (own[core].astype(F32) + other[...].astype(F32)).astype(BF16)

    pltpu.make_async_copy(band, band, band_sem).wait()
    qs[...] = jnp.zeros_like(qs)
    span = cmat.shape[2]
    mine_t = (lax.broadcasted_iota(jnp.int32, (8, lats), 1) == me * tl + lax.broadcasted_iota(jnp.int32, (8, lats), 0))
    mine_t &= lax.broadcasted_iota(jnp.int32, (8, lats), 0) < tl
    mine_t = jnp.where(mine_t, 1.0, 0.0).astype(BF16)

    def tabulate(d, _):
        z, of_core = lax.div(d, 2), lax.rem(d, 2)
        row = lax.broadcasted_iota(jnp.int32, (n, span), 0)
        p = jnp.where(of_core == 0, row - z, row + 1)
        target = jnp.where(p > held - 1, p + 1, p)
        moved = jnp.where(target == lax.broadcasted_iota(jnp.int32, (n, span), 1), 1.0, 0.0).astype(BF16)
        picked = dot(mine_t, band[d].astype(BF16), ((1,), (1,))).astype(BF16)
        cmat[z, pl.ds(pl.multiple_of(of_core * 8, 8), 8), :] = dot(picked, moved)
        return 0

    lax.fori_loop(0, n, tabulate, 0)

    def apply_top(ch, z):
        for h in range(2):
            qs[pl.ds(h * held * tile, held * tile), :] = packs[h, z, 2, ch].reshape(held * tile, chans).astype(F32)
        for k in range(tile):
            xb[0:span, k * chans:(k + 1) * chans] = qs[pl.ds(k, span, stride=tile), :].astype(BF16)
        out = dot(cmat[z].astype(BF16), xb[0:span, :])
        for k in range(tile):
            gather[pl.ds(k, 16, stride=tile), :] = out[:, k * chans:(k + 1) * chans]
        for c in range(2):
            for t in range(tl):
                recv[1, ch, 2 * z + c, t, pl.ds(rows - tile, tile)] = gather[
                    pl.ds((8 * c + t) * tile, tile), :].astype(BF16)

    def low_degree(l):
        def one(z, _):
            for c in range(2):
                p = l - z if c == 0 else l + 1
                ours = p >= 0 if c == 0 else p >= n - z
                p = jnp.maximum(p, 0)
                h = jnp.where(p > held - 1, 1, 0)
                for which in range(2):
                    lowx[which, 2 * z + c] = only(ours, packs[h, z, which, :, p - h * (held - 1)])
            return 0

        lax.fori_loop(0, chips, one, 0)
        outer(wbuf.at[0], 0, [(lowx[1].reshape(-1, chans), lowx[0].reshape(-1, chans))])
        dw_out[pl.ds(l * wide, wide)] = wbuf[0, pl.ds(0, wide)]

    def final_rows(unit):
        ch, t = unit_of(unit)

        step_in(dg_hbm, unit)
        buf = lax.rem(unit, 2)

        fetch_rows(3, ch, t)
        for b in range(0, nb, 2):
            g = fetch_pair(b)
            change = dot(adj_h[...], g) + dot(adj_l[...], g)
            df_out[ch * nb + b, t] = inbuf[buf, b] + change[:, :chans]
            df_out[ch * nb + b + 1, t] = inbuf[buf, b + 1] + change[:, chans:]

    def place(i, of_core):
        block = block_at(lax.div(i, pieces), way)
        start = lax.rem(i, pieces) * piece
        return pl.ds(block * block_rows + start, piece), pl.ds(first_degree(block, of_core) * wide + start, piece)

    def rs_copy(i):
        here, there = place(i, core)
        return to(onward, work.at[here], dw_out.at[there], rs_send, rs_recv.at[i])

    def add_pair(i):
        here, passed = place(i, 1 - core)

        @pl.when(lax.rem(i, pieces) == 0)
        def _():
            pair_copy(lax.div(i, pieces)).wait_recv()

        work[here] += dw_out[passed]

    def rs_step(i, _):
        add_pair(i)

        @pl.when(i >= pieces)
        def _():
            rs_copy(i - pieces).wait_recv()
            here, there = place(i, core)
            work[here] += dw_out[there]

        rs_copy(i).start()

        @pl.when(lax.rem(i, pieces) == 0)
        def _():
            k = lax.div(i, pieces)

            @pl.when(k > 0)
            def _():
                pack_copy(k - 1).wait_recv()

            pack_copy(k).start()
            share(k)

        return 0

    lax.fori_loop(0, hops, rs_step, 0)
    pack_copy(chips - 2).wait_recv()
    share(chips - 1)

    def own_sum(s, _):
        i = hops + s
        add_pair(i)
        rs_copy(i - pieces).wait_recv()
        here, there = place(i, core)
        dw_out[there] += work[here]
        ag_copy(i, s).start()
        return 0

    def ag_copy(i, got):
        _, there = place(i, core)
        return to(onward, dw_out.at[there], dw_out.at[there], ag_send, ag_recv.at[got])

    def publish(i):
        _, there = place(i, core)
        to(sibling, dw_out.at[there], dw_out.at[there], pub_send, pub_recv).start()

    lax.fori_loop(0, pieces, own_sum, 0)

    pl.semaphore_signal(free_sem, inc=1, device_id={axis: sibling}, device_id_type=pl.DeviceIdType.MESH)
    pl.semaphore_wait(free_sem, 1)

    def own_piece(s, _):
        publish(hops + s)
        return 0

    lax.fori_loop(0, pieces, own_piece, 0)
    gathered = packs.at[1 - core]
    pltpu.make_async_copy(gathered, gathered, share_recv).wait()

    def task(i):
        @pl.when(i < chips)
        def _():
            for ch in range(chunks):
                @pl.when(i == 0)
                def _():
                    arrived(3, ch)
                apply_top(ch, i)

        @pl.when((i >= chips) & (i < chips + units))
        def _():
            final_rows(i - chips)

        @pl.when(i < n)
        def _():
            low_degree(i)

    def ag_step(i, _):
        ag_copy(i, i).wait_recv()

        @pl.when(i + pieces < hops)
        def _():
            ag_copy(i, i + pieces).start()

        publish(i)
        task(i)
        return 0

    lax.fori_loop(0, hops, ag_step, 0)

    def rest(i, _):
        task(i)
        return 0

    lax.fori_loop(hops, max(hops, chips + units, n), rest, 0)

    wait_sent(3 * chunks - 1)
    for ch in range(chunks):
        wait_sent(3 * chunks + ch, 3)
    sent = work.at[pl.ds(0, (chips - 1) * block_rows)]
    pltpu.make_async_copy(sent, sent, rs_send).wait()
    pltpu.make_async_copy(sent, sent, ag_send).wait()
    sent = packs.at[0, pl.ds(0, chips - 1)]
    pltpu.make_async_copy(sent, sent, pack_send).wait()
    pltpu.make_async_copy(packs.at[0], packs.at[0], share_send).wait()
    shared = dw_out.at[pl.ds(0, chips * block_rows)]
    pltpu.make_async_copy(shared, shared, pub_send).wait()
    pltpu.make_async_copy(shared, shared, pub_recv).wait()


def put_kernel(df_ref, dw_ref, df_hbm, dw_hbm, sems):
    copies = []
    for source, target, parts in ((df_ref, df_hbm, 3), (dw_ref, dw_hbm, 4)):
        size = source.shape[0] // parts
        for k in range(parts):
            part = pl.ds(k * size, size)
            copies.append(pltpu.make_async_copy(source.at[part], target.at[part], sems.at[len(copies)]))
    for copy in copies:
        copy.start()
    for copy in copies:
        copy.wait()


def solution(mesh):
    n = mesh.shape['lat']
    field_spec = P('member', None, 'lat', None)

    def local_step(field_loc, grad_loc, p_fwd, p_inv, w_mix):
        batch, chans, tl, lons = field_loc.shape
        degs, lats = p_fwd.shape[1:]
        ml = p_fwd.shape[0] // n
        nb = 4
        chunks = batch // nb
        rows = ml * 2 * nb
        pitch = rows + 1
        half = degs // n - 1
        pieces = 4 if half * 2 * chans % 32 == 0 else 1
        hops = (n // 2 - 1) * pieces
        per = 4
        held = n // 2 + 1
        packed = (3, chunks, held, 2 * nb, chans)
        tables = fourier_tables(n, ml, lons)
        anywhere = pl.BlockSpec(memory_space=pl.ANY)
        vmem = pl.BlockSpec(memory_space=pltpu.VMEM)
        grad_field, grad_w = pl.pallas_call(
            functools.partial(layer_kernel, 'lat', n, nb, pieces, per),
            name='layer',
            out_shape=(
                pltpu.VMEM((batch, tl, lons, chans), F32),
                pltpu.VMEM((degs * 2 * chans, chans), F32),
            ),
            in_specs=[anywhere] * 5 + [vmem] * len(tables),
            out_specs=(vmem, vmem),
            scratch_shapes=[
                pltpu.VMEM((2, chunks, n, tl, rows, chans), BF16),
                pltpu.VMEM((SEND_SLOTS, n, tl, rows, chans), BF16),
                pltpu.VMEM((max(2 * lats * pitch, n // 2 * half * 2 * chans), chans), F32),
                pltpu.VMEM((lats, 2 * nb * chans), BF16),
                pltpu.VMEM((degs, chunks, rows, chans), BF16),
                pltpu.VMEM((degs, chunks, rows, chans), BF16),
                pltpu.VMEM((degs, 2 * chans, chans), BF16),
                pltpu.VMEM((2, max(per, half) * 2 * chans, chans), F32),
                pltpu.VMEM((2, nb, lons, chans), F32),
                pltpu.VMEM((n * rows, chans), F32),
                pltpu.VMEM((2, ml, degs, lats), F32),
                pltpu.VMEM((2, ml, degs, lats), BF16),
                pltpu.VMEM((n, n, lats), F32),
                pltpu.VMEM((n // 2, 16, 32), F32),
                pltpu.VMEM((32 * 2 * nb, chans), F32),
                pltpu.VMEM((2,) + packed, BF16),
                pltpu.VMEM(packed, BF16),
                pltpu.VMEM((2, n // 2) + packed, BF16),
                pltpu.VMEM((2, n, chunks, 2 * nb, chans), BF16),
                pltpu.SemaphoreType.DMA((4 * chunks,)),
                pltpu.SemaphoreType.DMA((4 * chunks,)),
                pltpu.SemaphoreType.DMA((2,)),
                pltpu.SemaphoreType.DMA((2,)),
                pltpu.SemaphoreType.DMA((2,)),
                pltpu.SemaphoreType.DMA,
                pltpu.SemaphoreType.DMA((2,)),
                pltpu.SemaphoreType.DMA((n // 2,)),
                pltpu.SemaphoreType.DMA,
                pltpu.SemaphoreType.DMA((hops,)),
                pltpu.SemaphoreType.DMA,
                pltpu.SemaphoreType.DMA((hops,)),
                pltpu.SemaphoreType.REGULAR,
                pltpu.SemaphoreType.DMA,
                pltpu.SemaphoreType.DMA,
                pltpu.SemaphoreType.DMA,
                pltpu.SemaphoreType.DMA,
                pltpu.SemaphoreType.DMA,
                pltpu.SemaphoreType.DMA((n // 2 - 1,)),
                pltpu.SemaphoreType.DMA,
                pltpu.SemaphoreType.DMA,
            ],
            compiler_params=pltpu.CompilerParams(
                collective_id=0, has_side_effects=True, vmem_limit_bytes=42 * 1024 * 1024),
        )(
            field_loc.transpose(0, 2, 3, 1), grad_loc.transpose(0, 2, 3, 1),
            w_mix.transpose(0, 1, 3, 2).reshape(degs * 2 * chans, chans),
            p_fwd, p_inv, *tables)
        grad_field, grad_w = pl.pallas_call(
            put_kernel,
            name='put',
            out_shape=(
                jax.ShapeDtypeStruct(grad_field.shape, F32),
                jax.ShapeDtypeStruct(grad_w.shape, F32),
            ),
            in_specs=[vmem] * 2,
            out_specs=(anywhere, anywhere),
            scratch_shapes=[pltpu.SemaphoreType.DMA((7,))],
            compiler_params=pltpu.CompilerParams(vmem_limit_bytes=1024 * 1024),
        )(grad_field, grad_w)
        return grad_field.transpose(0, 3, 1, 2), grad_w.reshape(degs, chans, 2, chans).transpose(0, 1, 3, 2)

    return jax.shard_map(
        local_step, mesh=mesh, in_specs=(field_spec, field_spec, P(), P(), P()),
        out_specs=(field_spec, P('member', None, None, None)), check_vma=False)
```

```python
import functools
import math

import jax
import jax.numpy as jnp
import numpy as np
from jax import lax
from jax.experimental import pallas as pl
from jax.experimental.pallas import tpu as pltpu
from jax.sharding import PartitionSpec as P

F32 = jnp.float32
BF16 = jnp.bfloat16


def split_const(matrix):
    head = matrix.astype(BF16)
    tail = (matrix - head.astype(np.float64)).astype(BF16)
    return [head, tail]


def fourier_tables(n, ml, lons):
    modes = n * ml
    device = np.arange(n)
    first = np.where(device % 2 == 0, device // 2, n - 1 - device // 2)
    order = (first[:, None] + n * np.arange(ml)[None, :]).reshape(-1)
    angle = 2.0 * np.pi * (np.outer(order, np.arange(lons)) % lons) / lons
    forward = np.stack([np.cos(angle), -np.sin(angle)], axis=1).reshape(2 * modes, lons) / math.sqrt(lons)
    gains = np.repeat(np.where(order == 0, 1.0, 2.0), 2)[:, None]
    doubled = forward * gains
    tables = split_const(forward) + split_const(doubled) + split_const(doubled.T) + split_const(forward.T)
    return jnp.stack([jnp.asarray(t) for t in tables])


def gelu_grad(values):
    cumulative = 0.5 * (1.0 + lax.erf(values * math.sqrt(0.5)))
    density = jnp.exp(-0.5 * values * values) / math.sqrt(2.0 * math.pi)
    return cumulative + values * density


def dot(a, b, dims=((1,), (0,))):
    return lax.dot_general(a, b, (dims, ((), ())), preferred_element_type=F32)


def layer_kernel(
    axis, n, nb, pieces, per,
    f_hbm, dg_hbm, w_hbm, pf_hbm, pv_hbm, tab_hbm,
    df_out, dw_out,
    recv, send, work, xb, coef, dq, vmix, wbuf, inbuf, gather, pbuf, pmat, band, cmat, qs, own, other, packs, lowx, tab,
    send_sem, recv_sem, in_sem, w_sem, p_sem, band_sem, pair_send, pair_recv, rs_send, rs_recv, ag_send, ag_recv,
    free_sem, pub_send, pub_recv, own_send, own_recv, pack_send, pack_recv, share_send, share_recv,
    tab_sem, top_send, near_recv, far_recv, swap_send, swap_recv,
):
    me = lax.axis_index(axis)
    batch, tl, lons, chans = f_hbm.shape
    ml, degs, lats = pmat.shape[1:]
    chunks = batch // nb
    tile = 2 * nb
    rows = ml * tile
    pitch = rows + 1
    modes2 = 2 * n * ml
    units = chunks * tl
    slots = chunks + 1
    fwd_h, fwd_l, dbl_h, dbl_l, syn_h, syn_l, adj_h, adj_l = (tab.at[k] for k in range(8))
    area = lats * pitch
    top = n * (ml - 1)
    held = n // 2 + 1
    chip, core = lax.div(me, 2), lax.rem(me, 2)
    chips = n // 2
    way = 1 - 2 * core
    sibling = me + way
    onward = 2 * lax.rem(chip + way + chips, chips) + core

    def first_mode(device):
        z = lax.div(device, 2)
        return jnp.where(lax.rem(device, 2) == 0, z, n - 1 - z)

    def to(device, src, dst, sent, got):
        return pltpu.make_async_remote_copy(
            src_ref=src, dst_ref=dst, send_sem=sent, recv_sem=got,
            device_id={axis: device}, device_id_type=pl.DeviceIdType.MESH)

    def unit_of(unit):
        return lax.div(unit, tl), lax.rem(unit, tl)

    def unit_in(src, unit):
        ch, t = unit_of(unit)
        slot = lax.rem(unit, 2)
        return pltpu.make_async_copy(src.at[pl.ds(ch * nb, nb), t], inbuf.at[slot], in_sem.at[slot])

    def step_in(src, unit):
        @pl.when(unit + 1 < units)
        def _():
            unit_in(src, unit + 1).start()
        unit_in(src, unit).wait()

    def sent_rows(stage):
        return pl.ds(0, rows - tile if stage % 2 else rows)

    def ship(stage, ch, t0, nt):
        index = stage * chunks + ch
        slot = lax.rem(index, slots)
        part, span = pl.ds(t0, nt), sent_rows(stage)

        def one(k, _):
            peer = lax.rem(me + k, n)
            to(peer, send.at[slot, peer, part, span], recv.at[stage % 2, ch, me, part, span],
               send_sem.at[index], recv_sem.at[index]).start()
            return 0

        lax.fori_loop(1, n, one, 0)
        recv[stage % 2, ch, me, part, span] = send[slot, me, part, span]

    def arrived(stage, ch):
        others = recv.at[stage % 2, ch, pl.ds(0, n - 1), :, sent_rows(stage)]
        pltpu.make_async_copy(others, others, recv_sem.at[stage * chunks + ch]).wait()

    def wait_sent(index, stage):
        others = send.at[lax.rem(index, slots), pl.ds(0, n - 1), :, sent_rows(stage)]
        pltpu.make_async_copy(others, others, send_sem.at[index]).wait()

    def free_slot(stage, ch):
        index = stage * chunks + ch
        if stage >= 1:
            @pl.when(ch >= 1)
            def _():
                wait_sent(index - slots, stage - 1)
        if stage >= 2:
            @pl.when(ch == 0)
            def _():
                wait_sent(index - slots, stage - 2)
        return lax.rem(index, slots)

    def put_rows(slot, t):
        send[slot, :, t] = gather[...].reshape(n, rows, chans).astype(BF16)

    def transform(values, head, tail):
        high = values.astype(BF16)
        low = (values - high.astype(F32)).astype(BF16)
        return dot(head[...], high) + (dot(tail[...], high) + dot(head[...], low))

    unit_in(f_hbm, 0).start()
    first_tables = pltpu.make_async_copy(tab_hbm.at[pl.ds(0, 2)], tab.at[pl.ds(0, 2)], tab_sem.at[0])
    other_tables = pltpu.make_async_copy(tab_hbm.at[pl.ds(2, 6)], tab.at[pl.ds(2, 6)], tab_sem.at[1])
    first_tables.start()
    barrier = pltpu.get_barrier_semaphore()

    def announce(k, _):
        pl.semaphore_signal(barrier, inc=1, device_id={axis: lax.rem(me + k, n)}, device_id_type=pl.DeviceIdType.MESH)
        return 0

    lax.fori_loop(1, n, announce, 0)

    for which, source in enumerate((pf_hbm, pv_hbm)):
        for k in range(ml):
            pltpu.make_async_copy(source.at[first_mode(me) + n * k], pbuf.at[which, k], p_sem.at[which]).start()

    other_tables.start()

    def band_in(d, _):
        for which, source in enumerate((pf_hbm, pv_hbm)):
            pltpu.make_async_copy(
                source.at[top + first_mode(d), pl.ds(top, n)], band.at[which, d], band_sem.at[which]).start()
        return 0

    lax.fori_loop(0, n, band_in, 0)
    first_tables.wait()

    group = 2 if tl % 2 == 0 else 1

    def by_rows(stage, ch, row):
        slot = free_slot(stage, ch)

        def part(p, _):
            def one(j, _):
                row(slot, p * group + j)
                return 0

            lax.fori_loop(0, group, one, 0)
            if stage == 0:
                @pl.when(ch + p == 0)
                def _():
                    pl.semaphore_wait(barrier, n - 1)
            ship(stage, ch, p * group, group)
            return 0

        lax.fori_loop(0, tl // group, part, 0)

    parts = degs // per
    depth = min(parts, work.shape[0] // (per * 2 * chans))

    def w_in(k):
        slot = lax.rem(k, depth)
        return pltpu.make_async_copy(
            w_hbm.at[pl.ds(k * per * 2 * chans, per * 2 * chans)],
            work.at[pl.ds(slot * per * 2 * chans, per * 2 * chans)], w_sem.at[slot])

    def step1_chunk(ch, _):
        def row(slot, t):
            unit = ch * tl + t
            step_in(f_hbm, unit)
            buf = lax.rem(unit, 2)
            for b in range(0, nb, 2):
                pair = jnp.concatenate([inbuf[buf, b], inbuf[buf, b + 1]], axis=1)
                spec = transform(pair, fwd_h, fwd_l)
                gather[pl.ds(b, modes2, stride=nb), :] = spec[:, :chans]
                gather[pl.ds(b + 1, modes2, stride=nb), :] = spec[:, chans:]
            put_rows(slot, t)

        by_rows(0, ch, row)

        @pl.when(ch == 0)
        def _():
            for k in range(depth):
                w_in(k).start()

        return 0

    lax.fori_loop(0, chunks, step1_chunk, 0)
    unit_in(dg_hbm, 0).start()
    for which in range(2):
        pltpu.make_async_copy(pbuf.at[which], pbuf.at[which], p_sem.at[which]).wait()
    pmat[...] = pbuf[...].astype(BF16)
    other_tables.wait()

    def load_w(k, _):
        w_in(k).wait()
        base = lax.rem(k, depth) * per * 2 * chans
        for j in range(per):
            for part in range(2):
                vmix[k * per + j, pl.ds(part * chans, chans)] = work[
                    pl.ds(base + j * 2 * chans + part, chans, stride=2), :].astype(BF16)

        @pl.when(k + depth < parts)
        def _():
            w_in(k + depth).start()

        return 0

    lax.fori_loop(0, parts, load_w, 0)

    for which in range(2):
        pltpu.make_async_copy(band.at[which], band.at[which], band_sem.at[which]).wait()
    qs[...] = jnp.zeros_like(qs)
    span = cmat.shape[3]
    mine_t = (lax.broadcasted_iota(jnp.int32, (8, lats), 1) == me * tl + lax.broadcasted_iota(jnp.int32, (8, lats), 0))
    mine_t &= lax.broadcasted_iota(jnp.int32, (8, lats), 0) < tl
    mine_t = jnp.where(mine_t, 1.0, 0.0).astype(BF16)

    def tabulate(d, _):
        z, of_core = lax.div(d, 2), lax.rem(d, 2)
        row = lax.broadcasted_iota(jnp.int32, (n, span), 0)
        p = jnp.where(of_core == 0, row - z, row + 1)
        target = jnp.where(p > held - 1, p + 1, p)
        moved = jnp.where(target == lax.broadcasted_iota(jnp.int32, (n, span), 1), 1.0, 0.0).astype(BF16)
        for which in range(2):
            picked = dot(mine_t, band[which, d].astype(BF16), ((1,), (1,))).astype(BF16)
            cmat[which, z, pl.ds(pl.multiple_of(of_core * 8, 8), 8), :] = dot(picked, moved)
        return 0

    lax.fori_loop(0, n, tabulate, 0)

    sign = jnp.where(lax.broadcasted_iota(jnp.int32, (tile, chans), 0) < nb, -1.0, 1.0).astype(F32)

    def turn(values):
        groups = values.reshape(-1, tile, chans)
        return (pltpu.roll(groups, nb, 1) * sign[None]).reshape(values.shape)

    def legendre(src, dst, which, over):
        def mode(m, _):
            for k in range(tile):
                xb[:, k * chans:(k + 1) * chans] = work[
                    pl.ds(src + m * tile + k, lats, stride=pitch), :].astype(BF16)
            out = dot(pmat[which, m], xb[...], ((over,), (0,)))
            for k in range(tile):
                work[pl.ds(dst + m * tile + k, degs, stride=pitch), :] = out[:, k * chans:(k + 1) * chans]
            return 0

        lax.fori_loop(0, ml, mode, 0)

    def unload(stage, ch):
        def body(src, _):
            for t in range(tl):
                work[pl.ds((src * tl + t) * pitch, rows), :] = recv[stage % 2, ch, src, t].astype(F32)
            return 0

        lax.fori_loop(0, n, body, 0)

    def load(slot):
        def body(dev, _):
            for t in range(tl):
                send[slot, dev, t] = work[pl.ds(area + (dev * tl + t) * pitch, rows), :].astype(BF16)
            return 0

        lax.fori_loop(0, n, body, 0)

    def pack(store):
        def one(index, _):
            half_at, row = lax.div(index, held), lax.rem(index, held)
            p = half_at * (held - 1) + row
            degree = jnp.where(core == 0, jnp.minimum(chip + p, n - 1), jnp.maximum(p - 1, 0))
            store(half_at, row, degree, (p < n - chip) == (core == 0))
            return 0

        lax.fori_loop(0, 2 * held, one, 0)

    def only(ours, values):
        values = values.astype(F32)
        return jnp.where(ours, values, jnp.zeros_like(values)).astype(BF16)

    def spectral(stage, ch, into, kept, mix):
        arrived(stage - 1, ch)
        unload(stage - 1, ch)
        legendre(0, area, into, 1)

        def degree(l, _):
            x = work[pl.ds(area + l * pitch, rows), :].astype(BF16)
            kept[l, ch] = x
            work[pl.ds(l * pitch, rows), :] = mix(l, x)
            return 0

        lax.fori_loop(0, degs, degree, 0, unroll=2)

        def keep_top(half_at, row, degree, ours):
            own[half_at, 2, ch, row] = only(ours, work[pl.ds((top + degree) * pitch + rows - tile, tile), :])

        pack(keep_top)
        if stage == 1:
            swap = to(sibling, own.at[1 - core, 2, ch], other.at[2, ch], swap_send.at[ch], swap_recv.at[ch])
            swap.start()
        legendre(0, area, 1 - into, 0)
        load(free_slot(stage, ch))
        if stage == 1:
            swap.wait()
            packs[core, chip, 2, ch] = (own[core, 2, ch].astype(F32) + other[2, ch].astype(F32)).astype(BF16)

            @pl.when(ch >= 2)
            def _():
                relay_top(ch - 2)

            for away in (2, -2):
                top_copy(0, away, ch, near_recv).start()
        ship(stage, ch, 0, tl)

    def top_copy(source, away, ch, got):
        block = packs.at[core, lax.rem(chip + source + chips, chips), 2, ch]
        return to(2 * lax.rem(chip + away + chips, chips) + core, block, block, top_send, got.at[ch])

    def top_blocks(count, ch):
        return packs.at[core, pl.ds(0, count), 2, ch]

    def relay_top(ch):
        pltpu.make_async_copy(top_blocks(2, ch), top_blocks(2, ch), near_recv.at[ch]).wait()
        for source in (2, -2):
            for away in (1, -1):
                top_copy(source, away, ch, far_recv).start()
        top_copy(-2 * way, 2 * way, ch, far_recv).start()

    def apply_top(which, ch, z):
        for h in range(2):
            qs[pl.ds(h * held * tile, held * tile), :] = packs[h, z, 2, ch].reshape(held * tile, chans).astype(F32)
        for k in range(tile):
            xb[0:span, k * chans:(k + 1) * chans] = qs[pl.ds(k, span, stride=tile), :].astype(BF16)
        out = dot(cmat[which, z].astype(BF16), xb[0:span, :])
        for k in range(tile):
            gather[pl.ds(k, 16, stride=tile), :] = out[:, k * chans:(k + 1) * chans]
        for c in range(2):
            for t in range(tl):
                recv[1, ch, 2 * z + c, t, pl.ds(rows - tile, tile)] = gather[
                    pl.ds((8 * c + t) * tile, tile), :].astype(BF16)

    def mix_forward(l, x):
        both = dot(x, vmix[l], ((1,), (1,)))
        return both[:, :chans] + turn(both[:, chans:])

    def mix_adjoint(l, x):
        real = dot(x, vmix[l, pl.ds(0, chans)])
        imag = dot(x, vmix[l, pl.ds(chans, chans)])
        return real - turn(imag)

    def step2_chunk(ch, _):
        spectral(1, ch, 0, coef, mix_forward)
        return 0

    lax.fori_loop(0, chunks, step2_chunk, 0)
    relay_top(chunks - 2)

    def fetch_rows(stage, ch, t):
        for src in range(n):
            gather[pl.ds(src * rows, rows), :] = recv[stage % 2, ch, src, t].astype(F32)

    def fetch_pair(b):
        return jnp.concatenate(
            [gather[pl.ds(b, modes2, stride=nb), :], gather[pl.ds(b + 1, modes2, stride=nb), :]], axis=1).astype(BF16)

    def step3_chunk(ch, _):
        arrived(1, ch)
        pltpu.make_async_copy(top_blocks(5, ch), top_blocks(5, ch), far_recv.at[ch]).wait()
        swap = to(sibling, top_blocks(chips, ch), top_blocks(chips, ch), swap_send.at[ch], swap_recv.at[ch])
        swap.start()

        @pl.when(ch == 0)
        def _():
            relay_top(chunks - 1)

        swap.wait()

        @pl.when(ch == chunks - 1)
        def _():
            all_sent = packs.at[0, pl.ds(0, 7), 2]
            pltpu.make_async_copy(all_sent, all_sent, top_send).wait()

        def apply(z, _):
            apply_top(1, ch, z)
            return 0

        lax.fori_loop(0, chips, apply, 0)

        def row(slot, t):
            unit = ch * tl + t
            step_in(dg_hbm, unit)
            buf = lax.rem(unit, 2)
            fetch_rows(1, ch, t)
            for b in range(0, nb, 2):
                g = fetch_pair(b)
                hidden = dot(syn_h[...], g) + dot(syn_l[...], g)
                pair = jnp.concatenate([inbuf[buf, b], inbuf[buf, b + 1]], axis=1)
                spec = transform(pair * gelu_grad(hidden), dbl_h, dbl_l)
                gather[pl.ds(b, modes2, stride=nb), :] = spec[:, :chans]
                gather[pl.ds(b + 1, modes2, stride=nb), :] = spec[:, chans:]
            put_rows(slot, t)

        by_rows(2, ch, row)
        return 0

    lax.fori_loop(0, chunks, step3_chunk, 0)
    unit_in(dg_hbm, 0).start()

    def step4_chunk(ch, _):
        spectral(3, ch, 1, dq, mix_adjoint)
        return 0

    lax.fori_loop(0, chunks, step4_chunk, 0)

    for which, kept in enumerate((coef, dq)):
        def keep_low(half_at, row, degree, ours):
            own[half_at, which, :, row] = only(ours, kept[degree, :, pl.ds(0, tile)])

        pack(keep_low)
    own_copy = to(sibling, own.at[1 - core], other, own_send, own_recv)
    own_copy.start()

    def pack_block(k):
        return packs.at[core, lax.rem(chip - way * k + chips, chips)]

    def pack_copy(k):
        return to(onward, pack_block(k), pack_block(k), pack_send, pack_recv.at[k])

    def share(k):
        to(sibling, pack_block(k), pack_block(k), share_send, share_recv).start()

    half = degs // n - 1
    wide = 2 * chans
    block_rows = half * wide
    piece = block_rows // pieces
    hops = (chips - 1) * pieces

    def block_at(k, direction):
        return lax.rem(chip - direction * (1 + k) + 2 * chips, chips)

    def outer(dst, row, pairs):
        real = jnp.zeros((chans, chans), F32)
        imag = jnp.zeros((chans, chans), F32)
        for y, x in pairs:
            real += dot(y, x, ((0,), (0,)))
            imag -= dot(turn(y.astype(F32)).astype(BF16), x, ((0,), (0,)))
        dst[pl.ds(row, chans, stride=2), :] = real
        dst[pl.ds(row + 1, chans, stride=2), :] = imag

    def first_degree(block, of_core):
        return n + (2 * block + of_core) * half

    def weight_grad(dst, degree):
        def one(j, _):
            outer(dst, j * wide, [(dq[degree + j, ch], coef[degree + j, ch]) for ch in range(chunks)])
            return 0

        lax.fori_loop(0, half, one, 0)

    def pair_copy(k):
        slot = lax.rem(k, 2)
        rows_there = pl.ds(first_degree(block_at(k, -way), core) * wide, block_rows)
        return to(sibling, wbuf.at[slot, pl.ds(0, block_rows)], dw_out.at[rows_there],
                  pair_send.at[slot], pair_recv.at[k])

    def weight_block(k, _):
        @pl.when(k >= 2)
        def _():
            pair_copy(k - 2).wait_send()
        weight_grad(wbuf.at[lax.rem(k, 2)], first_degree(block_at(k, -way), 1 - core))
        pair_copy(k).start()
        block = block_at(k, way)
        weight_grad(work.at[pl.ds(block * block_rows, block_rows)], first_degree(block, core))
        return 0

    lax.fori_loop(0, chips, weight_block, 0)
    pair_copy(chips - 2).wait_send()
    pair_copy(chips - 1).wait_send()
    own_copy.wait()
    packs[core, chip] = (own[core].astype(F32) + other[...].astype(F32)).astype(BF16)

    def low_degree(l):
        def one(z, _):
            for c in range(2):
                p = l - z if c == 0 else l + 1
                ours = p >= 0 if c == 0 else p >= n - z
                p = jnp.maximum(p, 0)
                h = jnp.where(p > held - 1, 1, 0)
                for which in range(2):
                    lowx[which, 2 * z + c] = only(ours, packs[h, z, which, :, p - h * (held - 1)])
            return 0

        lax.fori_loop(0, chips, one, 0)
        outer(wbuf.at[0], 0, [(lowx[1].reshape(-1, chans), lowx[0].reshape(-1, chans))])
        dw_out[pl.ds(l * wide, wide)] = wbuf[0, pl.ds(0, wide)]

    def final_rows(unit):
        ch, t = unit_of(unit)

        step_in(dg_hbm, unit)
        buf = lax.rem(unit, 2)

        fetch_rows(3, ch, t)
        for b in range(0, nb, 2):
            g = fetch_pair(b)
            change = dot(adj_h[...], g) + dot(adj_l[...], g)
            df_out[ch * nb + b, t] = inbuf[buf, b] + change[:, :chans]
            df_out[ch * nb + b + 1, t] = inbuf[buf, b + 1] + change[:, chans:]

    def place(i, of_core):
        block = block_at(lax.div(i, pieces), way)
        start = lax.rem(i, pieces) * piece
        return pl.ds(block * block_rows + start, piece), pl.ds(first_degree(block, of_core) * wide + start, piece)

    def rs_copy(i):
        here, there = place(i, core)
        return to(onward, work.at[here], dw_out.at[there], rs_send, rs_recv.at[i])

    def add_pair(i):
        here, passed = place(i, 1 - core)

        @pl.when(lax.rem(i, pieces) == 0)
        def _():
            pair_copy(lax.div(i, pieces)).wait_recv()

        work[here] += dw_out[passed]

    def rs_step(i, _):
        add_pair(i)

        @pl.when(i >= pieces)
        def _():
            rs_copy(i - pieces).wait_recv()
            here, there = place(i, core)
            work[here] += dw_out[there]

        rs_copy(i).start()

        @pl.when(lax.rem(i, pieces) == 0)
        def _():
            k = lax.div(i, pieces)

            @pl.when(k > 0)
            def _():
                pack_copy(k - 1).wait_recv()

            pack_copy(k).start()
            share(k)

        return 0

    lax.fori_loop(0, hops, rs_step, 0)
    pack_copy(chips - 2).wait_recv()
    share(chips - 1)

    def own_sum(s, _):
        i = hops + s
        add_pair(i)
        rs_copy(i - pieces).wait_recv()
        here, there = place(i, core)
        dw_out[there] += work[here]
        ag_copy(i, s).start()
        return 0

    def ag_copy(i, got):
        _, there = place(i, core)
        return to(onward, dw_out.at[there], dw_out.at[there], ag_send, ag_recv.at[got])

    def publish(i):
        _, there = place(i, core)
        to(sibling, dw_out.at[there], dw_out.at[there], pub_send, pub_recv).start()

    lax.fori_loop(0, pieces, own_sum, 0)

    pl.semaphore_signal(free_sem, inc=1, device_id={axis: sibling}, device_id_type=pl.DeviceIdType.MESH)
    pl.semaphore_wait(free_sem, 1)

    def own_piece(s, _):
        publish(hops + s)
        return 0

    lax.fori_loop(0, pieces, own_piece, 0)
    gathered = packs.at[1 - core]
    pltpu.make_async_copy(gathered, gathered, share_recv).wait()

    def task(i):
        @pl.when(i < chips)
        def _():
            for ch in range(chunks):
                @pl.when(i == 0)
                def _():
                    arrived(3, ch)
                apply_top(0, ch, i)

        @pl.when((i >= chips) & (i < chips + units))
        def _():
            final_rows(i - chips)

        @pl.when(i < n)
        def _():
            low_degree(i)

    def ag_step(i, _):
        ag_copy(i, i).wait_recv()

        @pl.when(i + pieces < hops)
        def _():
            ag_copy(i, i + pieces).start()

        publish(i)
        task(i)
        return 0

    lax.fori_loop(0, hops, ag_step, 0)

    def rest(i, _):
        task(i)
        return 0

    lax.fori_loop(hops, max(hops, chips + units, n), rest, 0)

    wait_sent(3 * chunks - 1, 2)
    for ch in range(chunks):
        wait_sent(3 * chunks + ch, 3)
    sent = work.at[pl.ds(0, (chips - 1) * block_rows)]
    pltpu.make_async_copy(sent, sent, rs_send).wait()
    pltpu.make_async_copy(sent, sent, ag_send).wait()
    sent = packs.at[0, pl.ds(0, chips - 1)]
    pltpu.make_async_copy(sent, sent, pack_send).wait()
    pltpu.make_async_copy(packs.at[0], packs.at[0], share_send).wait()
    shared = dw_out.at[pl.ds(0, chips * block_rows)]
    pltpu.make_async_copy(shared, shared, pub_send).wait()
    pltpu.make_async_copy(shared, shared, pub_recv).wait()


def put_kernel(df_ref, dw_ref, df_hbm, dw_hbm, sems):
    copies = []
    for source, target, parts in ((df_ref, df_hbm, 3), (dw_ref, dw_hbm, 4)):
        size = source.shape[0] // parts
        for k in range(parts):
            part = pl.ds(k * size, size)
            copies.append(pltpu.make_async_copy(source.at[part], target.at[part], sems.at[len(copies)]))
    for copy in copies:
        copy.start()
    for copy in copies:
        copy.wait()


def solution(mesh):
    n = mesh.shape['lat']
    field_spec = P('member', None, 'lat', None)

    def local_step(field_loc, grad_loc, p_fwd, p_inv, w_mix):
        batch, chans, tl, lons = field_loc.shape
        degs, lats = p_fwd.shape[1:]
        ml = p_fwd.shape[0] // n
        nb = 4
        chunks = batch // nb
        rows = ml * 2 * nb
        pitch = rows + 1
        half = degs // n - 1
        pieces = 4 if half * 2 * chans % 32 == 0 else 1
        hops = (n // 2 - 1) * pieces
        per = 4
        held = n // 2 + 1
        packed = (3, chunks, held, 2 * nb, chans)
        tables = fourier_tables(n, ml, lons)
        anywhere = pl.BlockSpec(memory_space=pl.ANY)
        vmem = pl.BlockSpec(memory_space=pltpu.VMEM)
        grad_field, grad_w = pl.pallas_call(
            functools.partial(layer_kernel, 'lat', n, nb, pieces, per),
            name='layer',
            out_shape=(
                pltpu.VMEM((batch, tl, lons, chans), F32),
                pltpu.VMEM((degs * 2 * chans, chans), F32),
            ),
            in_specs=[anywhere] * 6,
            out_specs=(vmem, vmem),
            scratch_shapes=[
                pltpu.VMEM((2, chunks, n, tl, rows, chans), BF16),
                pltpu.VMEM((chunks + 1, n, tl, rows, chans), BF16),
                pltpu.VMEM((max(2 * lats * pitch, n // 2 * half * 2 * chans), chans), F32),
                pltpu.VMEM((lats, 2 * nb * chans), BF16),
                pltpu.VMEM((degs, chunks, rows, chans), BF16),
                pltpu.VMEM((degs, chunks, rows, chans), BF16),
                pltpu.VMEM((degs, 2 * chans, chans), BF16),
                pltpu.VMEM((2, max(per, half) * 2 * chans, chans), F32),
                pltpu.VMEM((2, nb, lons, chans), F32),
                pltpu.VMEM((n * rows, chans), F32),
                pltpu.VMEM((2, ml, degs, lats), F32),
                pltpu.VMEM((2, ml, degs, lats), BF16),
                pltpu.VMEM((2, n, n, lats), F32),
                pltpu.VMEM((2, n // 2, 16, 32), F32),
                pltpu.VMEM((32 * 2 * nb, chans), F32),
                pltpu.VMEM((2,) + packed, BF16),
                pltpu.VMEM(packed, BF16),
                pltpu.VMEM((2, n // 2) + packed, BF16),
                pltpu.VMEM((2, n, chunks, 2 * nb, chans), BF16),
                pltpu.VMEM(tables.shape, BF16),
                pltpu.SemaphoreType.DMA((4 * chunks,)),
                pltpu.SemaphoreType.DMA((4 * chunks,)),
                pltpu.SemaphoreType.DMA((2,)),
                pltpu.SemaphoreType.DMA((degs // per,)),
                pltpu.SemaphoreType.DMA((2,)),
                pltpu.SemaphoreType.DMA((2,)),
                pltpu.SemaphoreType.DMA((2,)),
                pltpu.SemaphoreType.DMA((n // 2,)),
                pltpu.SemaphoreType.DMA,
                pltpu.SemaphoreType.DMA((hops,)),
                pltpu.SemaphoreType.DMA,
                pltpu.SemaphoreType.DMA((hops,)),
                pltpu.SemaphoreType.REGULAR,
                pltpu.SemaphoreType.DMA,
                pltpu.SemaphoreType.DMA,
                pltpu.SemaphoreType.DMA,
                pltpu.SemaphoreType.DMA,
                pltpu.SemaphoreType.DMA,
                pltpu.SemaphoreType.DMA((n // 2 - 1,)),
                pltpu.SemaphoreType.DMA,
                pltpu.SemaphoreType.DMA,
                pltpu.SemaphoreType.DMA((2,)),
                pltpu.SemaphoreType.DMA,
                pltpu.SemaphoreType.DMA((chunks,)),
                pltpu.SemaphoreType.DMA((chunks,)),
                pltpu.SemaphoreType.DMA((chunks,)),
                pltpu.SemaphoreType.DMA((chunks,)),
            ],
            compiler_params=pltpu.CompilerParams(
                collective_id=0, has_side_effects=True, vmem_limit_bytes=42 * 1024 * 1024),
        )(
            field_loc.transpose(0, 2, 3, 1), grad_loc.transpose(0, 2, 3, 1),
            w_mix.transpose(0, 1, 3, 2).reshape(degs * 2 * chans, chans),
            p_fwd, p_inv, tables)
        grad_field, grad_w = pl.pallas_call(
            put_kernel,
            name='put',
            out_shape=(
                jax.ShapeDtypeStruct(grad_field.shape, F32),
                jax.ShapeDtypeStruct(grad_w.shape, F32),
            ),
            in_specs=[vmem] * 2,
            out_specs=(anywhere, anywhere),
            scratch_shapes=[pltpu.SemaphoreType.DMA((7,))],
            compiler_params=pltpu.CompilerParams(vmem_limit_bytes=1024 * 1024),
        )(grad_field, grad_w)
        return grad_field.transpose(0, 3, 1, 2), grad_w.reshape(degs, chans, 2, chans).transpose(0, 1, 3, 2)

    return jax.shard_map(
        local_step, mesh=mesh, in_specs=(field_spec, field_spec, P(), P(), P()),
        out_specs=(field_spec, P('member', None, None, None)), check_vma=False)
```

```python
import functools
import math

import jax
import jax.numpy as jnp
import numpy as np
from jax import lax
from jax.experimental import pallas as pl
from jax.experimental.pallas import tpu as pltpu
from jax.sharding import PartitionSpec as P

F32 = jnp.float32
BF16 = jnp.bfloat16


def split_const(matrix):
    head = matrix.astype(BF16)
    tail = (matrix - head.astype(np.float64)).astype(BF16)
    return [head, tail]


def fourier_tables(n, ml, lons):
    modes = n * ml
    device = np.arange(n)
    first = np.where(device % 2 == 0, device // 2, n - 1 - device // 2)
    order = (first[:, None] + n * np.arange(ml)[None, :]).reshape(-1)
    angle = 2.0 * np.pi * (np.outer(order, np.arange(lons)) % lons) / lons
    forward = np.stack([np.cos(angle), -np.sin(angle)], axis=1).reshape(2 * modes, lons) / math.sqrt(lons)
    gains = np.repeat(np.where(order == 0, 1.0, 2.0), 2)[:, None]
    doubled = forward * gains
    tables = split_const(forward) + split_const(doubled) + split_const(doubled.T) + split_const(forward.T)
    return jnp.stack([jnp.asarray(t) for t in tables])


def gelu_grad(values):
    cumulative = 0.5 * (1.0 + lax.erf(values * math.sqrt(0.5)))
    density = jnp.exp(-0.5 * values * values) / math.sqrt(2.0 * math.pi)
    return cumulative + values * density


def loop(stop, step, start=0, unroll=None):
    def one(i, carry):
        step(i)
        return carry

    lax.fori_loop(start, stop, one, 0, unroll=unroll)


def head(size):
    return pl.ds(0, size)


def dot(a, b, dims=((1,), (0,))):
    return lax.dot_general(a, b, (dims, ((), ())), preferred_element_type=F32)


def layer_kernel(
    axis, n, nb, pieces, per,
    f_hbm, dg_hbm, w_hbm, pf_hbm, pv_hbm, tab_hbm,
    df_out, dw_out,
    recv, send, work, xb, coef, dq, vmix, wbuf, inbuf, gather, pbuf, pmat, band, cmat, qs, own, other, packs, lowx, tab,
    topin, partial, mid, sums, sumin, joined,
    send_sem, recv_sem, in_sem, w_sem, p_sem, band_sem, pair_send, pair_recv, rs_send, rs_recv, ag_send, ag_recv,
    free_sem, pub_send, pub_recv, own_send, own_recv, pack_send, pack_recv, share_send, share_recv,
    tab_sem, top_send, near_recv, far_recv, swap_send, swap_recv,
    row_send, row_recv, mid_send, mid_recv, sum_send, sum_recv, join_send, join_recv,
):
    me = lax.axis_index(axis)
    batch, tl, lons, chans = f_hbm.shape
    ml, degs, lats = pmat.shape[1:]
    chunks = batch // nb
    tile = 2 * nb
    rows = ml * tile
    pitch = rows + 1
    modes2 = 2 * n * ml
    units = chunks * tl
    slots = chunks + 1
    fwd_h, fwd_l, dbl_h, dbl_l, syn_h, syn_l, adj_h, adj_l = (tab.at[k] for k in range(8))
    area = lats * pitch
    top = n * (ml - 1)
    held = n // 2 + 1
    chip, core = lax.div(me, 2), lax.rem(me, 2)
    chips = n // 2
    way = 1 - 2 * core
    sibling = me + way
    onward = 2 * lax.rem(chip + way + chips, chips) + core

    def first_mode(device):
        z = lax.div(device, 2)
        return jnp.where(lax.rem(device, 2) == 0, z, n - 1 - z)

    def to(device, src, dst, sent, got):
        return pltpu.make_async_remote_copy(
            src_ref=src, dst_ref=dst, send_sem=sent, recv_sem=got,
            device_id={axis: device}, device_id_type=pl.DeviceIdType.MESH)

    def unit_of(unit):
        return lax.div(unit, tl), lax.rem(unit, tl)

    def unit_in(src, unit):
        ch, t = unit_of(unit)
        slot = lax.rem(unit, 2)
        return pltpu.make_async_copy(src.at[pl.ds(ch * nb, nb), t], inbuf.at[slot], in_sem.at[slot])

    def step_in(src, unit):
        @pl.when(unit + 1 < units)
        def _():
            unit_in(src, unit + 1).start()
        unit_in(src, unit).wait()

    body, peak = head(rows - tile), pl.ds(rows - tile, tile)

    def ship(stage, ch, t0, nt):
        index = stage * chunks + ch
        slot = lax.rem(index, slots)
        part = pl.ds(t0, nt)

        def one(k):
            peer = lax.rem(me + k, n)
            to(peer, send.at[slot, peer, part, body], recv.at[stage % 2, ch, me, part, body],
               send_sem.at[index], recv_sem.at[index]).start()

        loop(n, one, 1)
        recv[stage % 2, ch, me, part, body] = send[slot, me, part, body]

    def arrived(stage, ch):
        others = recv.at[stage % 2, ch, head(n - 1), :, body]
        pltpu.make_async_copy(others, others, recv_sem.at[stage * chunks + ch]).wait()

    def peaks(count):
        return topin.at[0, 0, head(count)]

    def wait_sent(index, stage):
        others = send.at[lax.rem(index, slots), head(n - 1), :, body]
        pltpu.make_async_copy(others, others, send_sem.at[index]).wait()
        if stage % 2 == 0:
            ch = index - stage * chunks
            pltpu.make_async_copy(peaks(n - 3), peaks(n - 3), row_send.at[ch]).wait()

    def send_peak(stage, ch):
        slot = lax.rem(stage * chunks + ch, slots)
        far = chips // 2
        for same in (True, False):
            its_core = core if same else 1 - core
            for away in range(1 - far, far + 1):
                place = (away > 0) - (away < 0)
                hop, target = away - place, (0, 2, 1)[place]
                if away == far:
                    hop = jnp.where(its_core == 0, 1 - far, far - 1)
                    target = jnp.where(its_core == 0, 1, 2)
                owner = 2 * lax.rem(chip + away + chips, chips) + its_core
                source = send.at[slot, owner, :, peak]
                if same and away in (-1, 0, 1):
                    topin[ch, target, me] = source[...]
                else:
                    to(2 * lax.rem(chip + hop + chips, chips) + its_core, source, topin.at[ch, target, me],
                       row_send.at[ch], row_recv.at[ch]).start()

    def free_slot(stage, ch):
        index = stage * chunks + ch
        if stage >= 1:
            @pl.when(ch >= 1)
            def _():
                wait_sent(index - slots, stage - 1)
        if stage >= 2:
            @pl.when(ch == 0)
            def _():
                wait_sent(index - slots, stage - 2)
        return lax.rem(index, slots)

    def put_rows(slot, t):
        send[slot, :, t] = gather[...].reshape(n, rows, chans).astype(BF16)

    def transform(values, head, tail):
        high = values.astype(BF16)
        low = (values - high.astype(F32)).astype(BF16)
        return dot(head[...], high) + (dot(tail[...], high) + dot(head[...], low))

    unit_in(f_hbm, 0).start()
    first_tables = pltpu.make_async_copy(tab_hbm.at[head(2)], tab.at[head(2)], tab_sem.at[0])
    other_tables = pltpu.make_async_copy(tab_hbm.at[pl.ds(2, 6)], tab.at[pl.ds(2, 6)], tab_sem.at[1])
    first_tables.start()

    def clear(ch):
        topin[ch] = jnp.zeros(topin.shape[1:], BF16)

    loop(chunks, clear)
    barrier = pltpu.get_barrier_semaphore()

    def announce(k):
        pl.semaphore_signal(barrier, inc=1, device_id={axis: lax.rem(me + k, n)}, device_id_type=pl.DeviceIdType.MESH)

    loop(n, announce, 1)

    for which, source in enumerate((pf_hbm, pv_hbm)):
        for k in range(ml):
            pltpu.make_async_copy(source.at[first_mode(me) + n * k], pbuf.at[which, k], p_sem.at[which]).start()

    other_tables.start()

    def band_in(d):
        for which, source in enumerate((pf_hbm, pv_hbm)):
            pltpu.make_async_copy(
                source.at[top + first_mode(d), pl.ds(top, n)], band.at[which, d], band_sem.at[which]).start()

    loop(n, band_in)
    first_tables.wait()

    group = max(1, tl // 3)

    parts = degs // per
    depth = min(parts, work.shape[0] // (per * 2 * chans))

    def w_in(k):
        slot = lax.rem(k, depth)
        return pltpu.make_async_copy(
            w_hbm.at[pl.ds(k * per * 2 * chans, per * 2 * chans)],
            work.at[pl.ds(slot * per * 2 * chans, per * 2 * chans)], w_sem.at[slot])

    def step1_chunk(ch):
        slot = free_slot(0, ch)

        def row(t):
            unit = ch * tl + t
            step_in(f_hbm, unit)
            buf = lax.rem(unit, 2)
            for b in range(0, nb, 2):
                pair = jnp.concatenate([inbuf[buf, b], inbuf[buf, b + 1]], axis=1)
                spec = transform(pair, fwd_h, fwd_l)
                gather[pl.ds(b, modes2, stride=nb), :] = spec[:, :chans]
                gather[pl.ds(b + 1, modes2, stride=nb), :] = spec[:, chans:]
            put_rows(slot, t)

            @pl.when((ch == 0) & (t == group - 1))
            def _():
                pl.semaphore_wait(barrier, n - 1)
                ship(0, 0, 0, group)


        loop(tl, row)
        send_peak(0, ch)

        @pl.when(ch == 0)
        def _():
            ship(0, 0, group, tl - group)
            for k in range(depth):
                w_in(k).start()


    loop(chunks, step1_chunk)
    unit_in(dg_hbm, 0).start()
    for which in range(2):
        pltpu.make_async_copy(band.at[which], band.at[which], band_sem.at[which]).wait()
    qs[...] = jnp.zeros_like(qs)

    def pack(z, store):
        def one(index):
            half_at, row = lax.div(index, held), lax.rem(index, held)
            p = half_at * (held - 1) + row
            degree = jnp.where(core == 0, jnp.minimum(z + p, n - 1), jnp.maximum(p - 1, 0))
            store(half_at, row, degree, (p < n - z) == (core == 0))

        loop(2 * held, one)

    def project(which, ch, target, device):
        def body_of(src):
            gather[pl.ds(src * tl * tile, tl * tile), :] = topin[ch, target, src].reshape(tl * tile, chans).astype(F32)

        loop(n, body_of)
        for k in range(tile):
            xb[:, k * chans:(k + 1) * chans] = gather[pl.ds(k, lats, stride=tile), :].astype(BF16)
        out = dot(band[which, device].astype(BF16), xb[...])
        for k in range(tile):
            qs[pl.ds(k, n, stride=tile), :] = out[:, k * chans:(k + 1) * chans]

    def relay_peak(which, ch):
        pltpu.make_async_copy(peaks(n - 3), peaks(n - 3), row_recv.at[ch]).wait()
        targets = (lax.rem(chip - 1 + chips, chips), lax.rem(chip + 1, chips))
        for side, z in enumerate(targets):
            project(which, ch, side + 1, 2 * z + core)

            def keep(half_at, row, degree, ours):
                values = qs[pl.ds(pl.multiple_of(degree * tile, tile), tile), :]
                partial[half_at, side, row] = jnp.where(ours, values, jnp.zeros_like(values))

            pack(z, keep)
        swap = to(sibling, partial.at[1 - core], mid.at[ch], mid_send.at[ch], mid_recv.at[ch])
        swap.start()
        if which == 1:
            pltpu.make_async_copy(sums.at[ch], sums.at[ch], sum_send.at[ch]).wait()
        swap.wait()
        sums[ch] = partial[core] + mid[ch]
        for side, z in enumerate(targets):
            to(2 * z + core, sums.at[ch, side], sumin.at[ch, side], sum_send.at[ch], sum_recv.at[ch]).start()

    def finish_peak(which, ch):
        pltpu.make_async_copy(sumin.at[ch], sumin.at[ch], sum_recv.at[ch]).wait()
        joined[ch, core] = sumin[ch, 0] + sumin[ch, 1]
        swap = to(sibling, joined.at[ch, core], joined.at[ch, core], join_send.at[ch], join_recv.at[ch])
        swap.start()
        project(which, ch, 0, me)
        swap.wait()

        def one(degree):
            p = jnp.where(core == 0, degree - chip, degree + 1)
            ours = degree >= first_mode(me)
            p = jnp.maximum(p, 0)
            h = jnp.where(p > held - 1, 1, 0)
            come = joined[ch, h, p - h * (held - 1)]
            work[pl.ds(area + (top + degree) * pitch + rows - tile, tile), :] = qs[
                pl.ds(pl.multiple_of(degree * tile, tile), tile), :] + jnp.where(ours, come, jnp.zeros_like(come))

        loop(n, one)

    relay_peak(0, 0)

    def ship_rows(ch):
        ship(0, ch, 0, tl)

    loop(chunks - 1, ship_rows, 1)
    for which in range(2):
        pltpu.make_async_copy(pbuf.at[which], pbuf.at[which], p_sem.at[which]).wait()
    pmat[...] = pbuf[...].astype(BF16)
    other_tables.wait()

    def load_w(k):
        w_in(k).wait()
        base = lax.rem(k, depth) * per * 2 * chans
        for j in range(per):
            for part in range(2):
                vmix[k * per + j, pl.ds(part * chans, chans)] = work[
                    pl.ds(base + j * 2 * chans + part, chans, stride=2), :].astype(BF16)

        @pl.when(k + depth < parts)
        def _():
            w_in(k + depth).start()


    loop(parts, load_w)

    span = cmat.shape[3]
    mine_t = (lax.broadcasted_iota(jnp.int32, (8, lats), 1) == me * tl + lax.broadcasted_iota(jnp.int32, (8, lats), 0))
    mine_t &= lax.broadcasted_iota(jnp.int32, (8, lats), 0) < tl
    mine_t = jnp.where(mine_t, 1.0, 0.0).astype(BF16)

    def tabulate(d):
        z, of_core = lax.div(d, 2), lax.rem(d, 2)
        row = lax.broadcasted_iota(jnp.int32, (n, span), 0)
        p = jnp.where(of_core == 0, row - z, row + 1)
        target = jnp.where(p > held - 1, p + 1, p)
        moved = jnp.where(target == lax.broadcasted_iota(jnp.int32, (n, span), 1), 1.0, 0.0).astype(BF16)
        for which in range(2):
            picked = dot(mine_t, band[which, d].astype(BF16), ((1,), (1,))).astype(BF16)
            cmat[which, z, pl.ds(pl.multiple_of(of_core * 8, 8), 8), :] = dot(picked, moved)

    loop(n, tabulate)

    def no_degree(l):
        work[pl.ds(area + l * pitch + rows - tile, tile), :] = jnp.zeros((tile, chans), F32)

    loop(top, no_degree)

    def relay_first(ch):
        relay_peak(0, ch)

    loop(chunks, relay_first, 1)
    ship(0, chunks - 1, 0, tl)

    sign = jnp.where(lax.broadcasted_iota(jnp.int32, (tile, chans), 0) < nb, -1.0, 1.0).astype(F32)

    def turn(values):
        groups = values.reshape(-1, tile, chans)
        return (pltpu.roll(groups, nb, 1) * sign[None]).reshape(values.shape)

    def legendre(src, dst, which, over):
        def mode(m):
            for k in range(tile):
                xb[:, k * chans:(k + 1) * chans] = work[
                    pl.ds(src + m * tile + k, lats, stride=pitch), :].astype(BF16)
            out = dot(pmat[which, m], xb[...], ((over,), (0,)))
            for k in range(tile):
                work[pl.ds(dst + m * tile + k, degs, stride=pitch), :] = out[:, k * chans:(k + 1) * chans]

        loop(ml - 1, mode)

    def unload(stage, ch):
        def body(src):
            for t in range(tl):
                work[pl.ds((src * tl + t) * pitch, rows), :] = recv[stage % 2, ch, src, t].astype(F32)

        loop(n, body)

    def load(slot):
        def body(dev):
            for t in range(tl):
                send[slot, dev, t] = work[pl.ds(area + (dev * tl + t) * pitch, rows), :].astype(BF16)

        loop(n, body)

    def only(ours, values):
        values = values.astype(F32)
        return jnp.where(ours, values, jnp.zeros_like(values)).astype(BF16)

    def spectral(stage, ch, into, kept, mix):
        arrived(stage - 1, ch)
        unload(stage - 1, ch)
        legendre(0, area, into, 1)
        finish_peak(into, ch)

        def degree(l):
            x = work[pl.ds(area + l * pitch, rows), :].astype(BF16)
            kept[l, ch] = x
            work[pl.ds(l * pitch, rows), :] = mix(l, x)

        loop(degs, degree, unroll=2)

        def keep_top(half_at, row, degree, ours):
            own[half_at, 2, ch, row] = only(ours, work[pl.ds((top + degree) * pitch + rows - tile, tile), :])

        pack(chip, keep_top)
        if stage == 1:
            swap = to(sibling, own.at[1 - core, 2, ch], other.at[2, ch], swap_send.at[ch], swap_recv.at[ch])
            swap.start()
        legendre(0, area, 1 - into, 0)
        load(free_slot(stage, ch))
        if stage == 1:
            swap.wait()
            packs[core, chip, 2, ch] = (own[core, 2, ch].astype(F32) + other[2, ch].astype(F32)).astype(BF16)

            @pl.when(ch >= 2)
            def _():
                relay_top(ch - 2)

            for away in (2, -2):
                top_copy(0, away, ch, near_recv).start()
        else:
            @pl.when(ch == 0)
            def _():
                relay_peak(1, chunks - 1)

        ship(stage, ch, 0, tl)

    def top_copy(source, away, ch, got):
        block = packs.at[core, lax.rem(chip + source + chips, chips), 2, ch]
        return to(2 * lax.rem(chip + away + chips, chips) + core, block, block, top_send, got.at[ch])

    def top_blocks(count, ch):
        return packs.at[core, head(count), 2, ch]

    def relay_top(ch):
        pltpu.make_async_copy(top_blocks(2, ch), top_blocks(2, ch), near_recv.at[ch]).wait()
        for source in (2, -2):
            for away in (1, -1):
                top_copy(source, away, ch, far_recv).start()
        top_copy(-2 * way, 2 * way, ch, far_recv).start()

    def apply_top(which, ch, z):
        for h in range(2):
            qs[pl.ds(h * held * tile, held * tile), :] = packs[h, z, 2, ch].reshape(held * tile, chans).astype(F32)
        for k in range(tile):
            xb[0:span, k * chans:(k + 1) * chans] = qs[pl.ds(k, span, stride=tile), :].astype(BF16)
        out = dot(cmat[which, z].astype(BF16), xb[0:span, :])
        for k in range(tile):
            gather[pl.ds(k, 16, stride=tile), :] = out[:, k * chans:(k + 1) * chans]
        for c in range(2):
            for t in range(tl):
                recv[1, ch, 2 * z + c, t, pl.ds(rows - tile, tile)] = gather[
                    pl.ds((8 * c + t) * tile, tile), :].astype(BF16)

    def mix_forward(l, x):
        both = dot(x, vmix[l], ((1,), (1,)))
        return both[:, :chans] + turn(both[:, chans:])

    def mix_adjoint(l, x):
        real = dot(x, vmix[l, head(chans)])
        imag = dot(x, vmix[l, pl.ds(chans, chans)])
        return real - turn(imag)

    def step2_chunk(ch):
        spectral(1, ch, 0, coef, mix_forward)

    loop(chunks, step2_chunk)
    relay_top(chunks - 2)

    def fetch_rows(stage, ch, t):
        for src in range(n):
            gather[pl.ds(src * rows, rows), :] = recv[stage % 2, ch, src, t].astype(F32)

    def fetch_pair(b):
        return jnp.concatenate(
            [gather[pl.ds(b, modes2, stride=nb), :], gather[pl.ds(b + 1, modes2, stride=nb), :]], axis=1).astype(BF16)

    def step3_chunk(ch):
        arrived(1, ch)
        pltpu.make_async_copy(top_blocks(5, ch), top_blocks(5, ch), far_recv.at[ch]).wait()
        swap = to(sibling, top_blocks(chips, ch), top_blocks(chips, ch), swap_send.at[ch], swap_recv.at[ch])
        swap.start()

        @pl.when(ch == 0)
        def _():
            relay_top(chunks - 1)

        swap.wait()

        @pl.when(ch == chunks - 1)
        def _():
            all_sent = packs.at[0, head(7), 2]
            pltpu.make_async_copy(all_sent, all_sent, top_send).wait()

        def apply(z):
            apply_top(1, ch, z)

        loop(chips, apply)

        @pl.when(ch == 1)
        def _():
            relay_peak(1, 0)

        slot = free_slot(2, ch)

        def row(t):
            unit = ch * tl + t
            step_in(dg_hbm, unit)
            buf = lax.rem(unit, 2)
            fetch_rows(1, ch, t)
            for b in range(0, nb, 2):
                g = fetch_pair(b)
                hidden = dot(syn_h[...], g) + dot(syn_l[...], g)
                pair = jnp.concatenate([inbuf[buf, b], inbuf[buf, b + 1]], axis=1)
                spec = transform(pair * gelu_grad(hidden), dbl_h, dbl_l)
                gather[pl.ds(b, modes2, stride=nb), :] = spec[:, :chans]
                gather[pl.ds(b + 1, modes2, stride=nb), :] = spec[:, chans:]
            put_rows(slot, t)

        loop(tl, row)
        send_peak(2, ch)

        @pl.when(ch < chunks - 1)
        def _():
            ship(2, ch, 0, tl)


    loop(chunks, step3_chunk)

    def relay_second(ch):
        relay_peak(1, ch)

    loop(chunks - 1, relay_second, 1)
    ship(2, chunks - 1, 0, tl)
    unit_in(dg_hbm, 0).start()

    def step4_chunk(ch):
        spectral(3, ch, 1, dq, mix_adjoint)

    loop(chunks, step4_chunk)

    for which, kept in enumerate((coef, dq)):
        def keep_low(half_at, row, degree, ours):
            own[half_at, which, :, row] = only(ours, kept[degree, :, head(tile)])

        pack(chip, keep_low)
    own_copy = to(sibling, own.at[1 - core], other, own_send, own_recv)
    own_copy.start()

    def pack_block(k):
        return packs.at[core, lax.rem(chip - way * k + chips, chips)]

    def pack_copy(k):
        return to(onward, pack_block(k), pack_block(k), pack_send, pack_recv.at[k])

    def share(k):
        to(sibling, pack_block(k), pack_block(k), share_send, share_recv).start()

    half = degs // n - 1
    wide = 2 * chans
    block_rows = half * wide
    piece = block_rows // pieces
    hops = (chips - 1) * pieces

    def block_at(k, direction):
        return lax.rem(chip - direction * (1 + k) + 2 * chips, chips)

    def outer(dst, row, pairs):
        real = jnp.zeros((chans, chans), F32)
        imag = jnp.zeros((chans, chans), F32)
        for y, x in pairs:
            real += dot(y, x, ((0,), (0,)))
            imag -= dot(turn(y.astype(F32)).astype(BF16), x, ((0,), (0,)))
        dst[pl.ds(row, chans, stride=2), :] = real
        dst[pl.ds(row + 1, chans, stride=2), :] = imag

    def first_degree(block, of_core):
        return n + (2 * block + of_core) * half

    def weight_grad(dst, degree):
        def one(j):
            outer(dst, j * wide, [(dq[degree + j, ch], coef[degree + j, ch]) for ch in range(chunks)])

        loop(half, one)

    def pair_copy(k):
        slot = lax.rem(k, 2)
        rows_there = pl.ds(first_degree(block_at(k, -way), core) * wide, block_rows)
        return to(sibling, wbuf.at[slot, head(block_rows)], dw_out.at[rows_there],
                  pair_send.at[slot], pair_recv.at[k])

    def weight_block(k):
        @pl.when(k >= 2)
        def _():
            pair_copy(k - 2).wait_send()
        weight_grad(wbuf.at[lax.rem(k, 2)], first_degree(block_at(k, -way), 1 - core))
        pair_copy(k).start()
        block = block_at(k, way)
        weight_grad(work.at[pl.ds(block * block_rows, block_rows)], first_degree(block, core))

    loop(chips, weight_block)
    pair_copy(chips - 2).wait_send()
    pair_copy(chips - 1).wait_send()
    own_copy.wait()
    packs[core, chip] = (own[core].astype(F32) + other[...].astype(F32)).astype(BF16)

    def low_degree(l):
        def one(z):
            for c in range(2):
                p = l - z if c == 0 else l + 1
                ours = p >= 0 if c == 0 else p >= n - z
                p = jnp.maximum(p, 0)
                h = jnp.where(p > held - 1, 1, 0)
                for which in range(2):
                    lowx[which, 2 * z + c] = only(ours, packs[h, z, which, :, p - h * (held - 1)])

        loop(chips, one)
        outer(wbuf.at[0], 0, [(lowx[1].reshape(-1, chans), lowx[0].reshape(-1, chans))])
        dw_out[pl.ds(l * wide, wide)] = wbuf[0, head(wide)]

    def final_rows(unit):
        ch, t = unit_of(unit)

        step_in(dg_hbm, unit)
        buf = lax.rem(unit, 2)

        fetch_rows(3, ch, t)
        for b in range(0, nb, 2):
            g = fetch_pair(b)
            change = dot(adj_h[...], g) + dot(adj_l[...], g)
            df_out[ch * nb + b, t] = inbuf[buf, b] + change[:, :chans]
            df_out[ch * nb + b + 1, t] = inbuf[buf, b + 1] + change[:, chans:]

    def place(i, of_core):
        block = block_at(lax.div(i, pieces), way)
        start = lax.rem(i, pieces) * piece
        return pl.ds(block * block_rows + start, piece), pl.ds(first_degree(block, of_core) * wide + start, piece)

    def rs_copy(i):
        here, there = place(i, core)
        return to(onward, work.at[here], dw_out.at[there], rs_send, rs_recv.at[i])

    def add_pair(i):
        here, passed = place(i, 1 - core)

        @pl.when(lax.rem(i, pieces) == 0)
        def _():
            pair_copy(lax.div(i, pieces)).wait_recv()

        work[here] += dw_out[passed]

    def rs_step(i):
        add_pair(i)

        @pl.when(i >= pieces)
        def _():
            rs_copy(i - pieces).wait_recv()
            here, there = place(i, core)
            work[here] += dw_out[there]

        rs_copy(i).start()

        @pl.when(lax.rem(i, pieces) == 0)
        def _():
            k = lax.div(i, pieces)

            @pl.when(k > 0)
            def _():
                pack_copy(k - 1).wait_recv()

            pack_copy(k).start()
            share(k)


    loop(hops, rs_step)
    pack_copy(chips - 2).wait_recv()
    share(chips - 1)

    def own_sum(s):
        i = hops + s
        add_pair(i)
        rs_copy(i - pieces).wait_recv()
        here, there = place(i, core)
        dw_out[there] += work[here]
        ag_copy(i, s).start()

    def ag_copy(i, got):
        _, there = place(i, core)
        return to(onward, dw_out.at[there], dw_out.at[there], ag_send, ag_recv.at[got])

    def publish(i):
        _, there = place(i, core)
        to(sibling, dw_out.at[there], dw_out.at[there], pub_send, pub_recv).start()

    loop(pieces, own_sum)

    pl.semaphore_signal(free_sem, inc=1, device_id={axis: sibling}, device_id_type=pl.DeviceIdType.MESH)
    pl.semaphore_wait(free_sem, 1)

    def own_piece(s):
        publish(hops + s)

    loop(pieces, own_piece)
    gathered = packs.at[1 - core]
    pltpu.make_async_copy(gathered, gathered, share_recv).wait()

    def task(i):
        @pl.when(i < chips)
        def _():
            for ch in range(chunks):
                @pl.when(i == 0)
                def _():
                    arrived(3, ch)
                apply_top(0, ch, i)

        @pl.when((i >= chips) & (i < chips + units))
        def _():
            final_rows(i - chips)

        @pl.when(i < n)
        def _():
            low_degree(i)

    def ag_step(i):
        ag_copy(i, i).wait_recv()

        @pl.when(i + pieces < hops)
        def _():
            ag_copy(i, i + pieces).start()

        publish(i)
        task(i)

    loop(hops, ag_step)

    def rest(i):
        task(i)

    loop(max(hops, chips + units, n), rest, hops)

    wait_sent(3 * chunks - 1, 2)
    for ch in range(chunks):
        wait_sent(3 * chunks + ch, 3)
    for ch in range(chunks):
        pltpu.make_async_copy(sums.at[ch], sums.at[ch], sum_send.at[ch]).wait()
    sent = work.at[head((chips - 1) * block_rows)]
    pltpu.make_async_copy(sent, sent, rs_send).wait()
    pltpu.make_async_copy(sent, sent, ag_send).wait()
    sent = packs.at[0, head(chips - 1)]
    pltpu.make_async_copy(sent, sent, pack_send).wait()
    pltpu.make_async_copy(packs.at[0], packs.at[0], share_send).wait()
    shared = dw_out.at[head(chips * block_rows)]
    pltpu.make_async_copy(shared, shared, pub_send).wait()
    pltpu.make_async_copy(shared, shared, pub_recv).wait()


def put_kernel(df_ref, dw_ref, df_hbm, dw_hbm, sems):
    copies = []
    for source, target, parts in ((df_ref, df_hbm, 3), (dw_ref, dw_hbm, 4)):
        size = source.shape[0] // parts
        for k in range(parts):
            part = pl.ds(k * size, size)
            copies.append(pltpu.make_async_copy(source.at[part], target.at[part], sems.at[len(copies)]))
    for copy in copies:
        copy.start()
    for copy in copies:
        copy.wait()


def solution(mesh):
    n = mesh.shape['lat']
    field_spec = P('member', None, 'lat', None)

    def local_step(field_loc, grad_loc, p_fwd, p_inv, w_mix):
        batch, chans, tl, lons = field_loc.shape
        degs, lats = p_fwd.shape[1:]
        ml = p_fwd.shape[0] // n
        nb = 4
        chunks = batch // nb
        rows = ml * 2 * nb
        pitch = rows + 1
        half = degs // n - 1
        pieces = 4 if half * 2 * chans % 32 == 0 else 1
        hops = (n // 2 - 1) * pieces
        per = 4
        held = n // 2 + 1
        packed = (3, chunks, held, 2 * nb, chans)
        tables = fourier_tables(n, ml, lons)
        anywhere = pl.BlockSpec(memory_space=pl.ANY)
        vmem = pl.BlockSpec(memory_space=pltpu.VMEM)
        grad_field, grad_w = pl.pallas_call(
            functools.partial(layer_kernel, 'lat', n, nb, pieces, per),
            name='layer',
            out_shape=(
                pltpu.VMEM((batch, tl, lons, chans), F32),
                pltpu.VMEM((degs * 2 * chans, chans), F32),
            ),
            in_specs=[anywhere] * 6,
            out_specs=(vmem, vmem),
            scratch_shapes=[
                pltpu.VMEM((2, chunks, n, tl, rows, chans), BF16),
                pltpu.VMEM((chunks + 1, n, tl, rows, chans), BF16),
                pltpu.VMEM((max(2 * lats * pitch, n // 2 * half * 2 * chans), chans), F32),
                pltpu.VMEM((lats, 2 * nb * chans), BF16),
                pltpu.VMEM((degs, chunks, rows, chans), BF16),
                pltpu.VMEM((degs, chunks, rows, chans), BF16),
                pltpu.VMEM((degs, 2 * chans, chans), BF16),
                pltpu.VMEM((2, max(per, half) * 2 * chans, chans), F32),
                pltpu.VMEM((2, nb, lons, chans), F32),
                pltpu.VMEM((n * rows, chans), F32),
                pltpu.VMEM((2, ml, degs, lats), F32),
                pltpu.VMEM((2, ml, degs, lats), BF16),
                pltpu.VMEM((2, n, n, lats), F32),
                pltpu.VMEM((2, n // 2, 16, 32), F32),
                pltpu.VMEM((32 * 2 * nb, chans), F32),
                pltpu.VMEM((2,) + packed, BF16),
                pltpu.VMEM(packed, BF16),
                pltpu.VMEM((2, n // 2) + packed, BF16),
                pltpu.VMEM((2, n, chunks, 2 * nb, chans), BF16),
                pltpu.VMEM(tables.shape, BF16),
                pltpu.VMEM((chunks, 3, n, tl, 2 * nb, chans), BF16),
                pltpu.VMEM((2, 2, held, 2 * nb, chans), F32),
                pltpu.VMEM((chunks, 2, held, 2 * nb, chans), F32),
                pltpu.VMEM((chunks, 2, held, 2 * nb, chans), F32),
                pltpu.VMEM((chunks, 2, held, 2 * nb, chans), F32),
                pltpu.VMEM((chunks, 2, held, 2 * nb, chans), F32),
                pltpu.SemaphoreType.DMA((4 * chunks,)),
                pltpu.SemaphoreType.DMA((4 * chunks,)),
                pltpu.SemaphoreType.DMA((2,)),
                pltpu.SemaphoreType.DMA((degs // per,)),
                pltpu.SemaphoreType.DMA((2,)),
                pltpu.SemaphoreType.DMA((2,)),
                pltpu.SemaphoreType.DMA((2,)),
                pltpu.SemaphoreType.DMA((n // 2,)),
                pltpu.SemaphoreType.DMA,
                pltpu.SemaphoreType.DMA((hops,)),
                pltpu.SemaphoreType.DMA,
                pltpu.SemaphoreType.DMA((hops,)),
                pltpu.SemaphoreType.REGULAR,
                pltpu.SemaphoreType.DMA,
                pltpu.SemaphoreType.DMA,
                pltpu.SemaphoreType.DMA,
                pltpu.SemaphoreType.DMA,
                pltpu.SemaphoreType.DMA,
                pltpu.SemaphoreType.DMA((n // 2 - 1,)),
                pltpu.SemaphoreType.DMA,
                pltpu.SemaphoreType.DMA,
                pltpu.SemaphoreType.DMA((2,)),
                pltpu.SemaphoreType.DMA,
                pltpu.SemaphoreType.DMA((chunks,)),
                pltpu.SemaphoreType.DMA((chunks,)),
                pltpu.SemaphoreType.DMA((chunks,)),
                pltpu.SemaphoreType.DMA((chunks,)),
                pltpu.SemaphoreType.DMA((chunks,)),
                pltpu.SemaphoreType.DMA((chunks,)),
                pltpu.SemaphoreType.DMA((chunks,)),
                pltpu.SemaphoreType.DMA((chunks,)),
                pltpu.SemaphoreType.DMA((chunks,)),
                pltpu.SemaphoreType.DMA((chunks,)),
                pltpu.SemaphoreType.DMA((chunks,)),
                pltpu.SemaphoreType.DMA((chunks,)),
            ],
            compiler_params=pltpu.CompilerParams(
                collective_id=0, has_side_effects=True, vmem_limit_bytes=43 * 1024 * 1024),
        )(
            field_loc.transpose(0, 2, 3, 1), grad_loc.transpose(0, 2, 3, 1),
            w_mix.transpose(0, 1, 3, 2).reshape(degs * 2 * chans, chans),
            p_fwd, p_inv, tables)
        grad_field, grad_w = pl.pallas_call(
            put_kernel,
            name='put',
            out_shape=(
                jax.ShapeDtypeStruct(grad_field.shape, F32),
                jax.ShapeDtypeStruct(grad_w.shape, F32),
            ),
            in_specs=[vmem] * 2,
            out_specs=(anywhere, anywhere),
            scratch_shapes=[pltpu.SemaphoreType.DMA((7,))],
            compiler_params=pltpu.CompilerParams(vmem_limit_bytes=1024 * 1024),
        )(grad_field, grad_w)
        return grad_field.transpose(0, 3, 1, 2), grad_w.reshape(degs, chans, 2, chans).transpose(0, 1, 3, 2)

    return jax.shard_map(
        local_step, mesh=mesh, in_specs=(field_spec, field_spec, P(), P(), P()),
        out_specs=(field_spec, P('member', None, None, None)), check_vma=False)
```

```python
import functools
import math

import jax
import jax.numpy as jnp
import numpy as np
from jax import lax
from jax.experimental import pallas as pl
from jax.experimental.pallas import tpu as pltpu
from jax.sharding import PartitionSpec as P

F32 = jnp.float32
BF16 = jnp.bfloat16


def split_const(matrix):
    head = matrix.astype(BF16)
    tail = (matrix - head.astype(np.float64)).astype(BF16)
    return [head, tail]


def fourier_tables(n, ml, lons):
    modes = n * ml
    device = np.arange(n)
    first = np.where(device % 2 == 0, device // 2, n - 1 - device // 2)
    order = (first[:, None] + n * np.arange(ml)[None, :]).reshape(-1)
    angle = 2.0 * np.pi * (np.outer(order, np.arange(lons)) % lons) / lons
    forward = np.stack([np.cos(angle), -np.sin(angle)], axis=1).reshape(2 * modes, lons) / math.sqrt(lons)
    gains = np.repeat(np.where(order == 0, 1.0, 2.0), 2)[:, None]
    doubled = forward * gains
    tables = split_const(forward) + split_const(doubled) + split_const(doubled.T) + split_const(forward.T)
    return jnp.stack([jnp.asarray(t) for t in tables])


def gelu_grad(values):
    cumulative = 0.5 * (1.0 + lax.erf(values * math.sqrt(0.5)))
    density = jnp.exp(-0.5 * values * values) / math.sqrt(2.0 * math.pi)
    return cumulative + values * density


def loop(stop, step, start=0, unroll=None):
    def one(i, carry):
        step(i)
        return carry

    lax.fori_loop(start, stop, one, 0, unroll=unroll)


def head(size):
    return pl.ds(0, size)


def dot(a, b, dims=((1,), (0,))):
    return lax.dot_general(a, b, (dims, ((), ())), preferred_element_type=F32)


def layer_kernel(
    axis, n, nb, pieces, per,
    f_hbm, dg_hbm, w_hbm, pf_hbm, pv_hbm, tab_hbm,
    df_out, dw_out,
    recv, send, work, xb, coef, dq, vmix, wbuf, inbuf, gather, pbuf, pmat, band, cmat, qs, own, other, packs, lowx, tab,
    topin, partial, mid, sums, sumin, joined, second,
    send_sem, recv_sem, in_sem, w_sem, p_sem, band_sem, pair_send, pair_recv, rs_send, rs_recv, ag_send, ag_recv,
    free_sem, pub_send, pub_recv, own_send, own_recv, pack_send, pack_recv, share_send, share_recv,
    tab_sem, top_send, near_recv, far_recv, swap_send, swap_recv,
    row_send, row_recv, mid_send, mid_recv, sum_send, sum_recv, join_send, join_recv,
    always_send, always_recv, some_send, some_recv,
):
    me = lax.axis_index(axis)
    batch, tl, lons, chans = f_hbm.shape
    ml, degs, lats = pmat.shape[1:]
    chunks = batch // nb
    tile = 2 * nb
    rows = ml * tile
    pitch = rows + 1
    modes2 = 2 * n * ml
    units = chunks * tl
    final = chunks - 1
    slots = chunks + 1
    fwd_h, fwd_l, dbl_h, dbl_l, syn_h, syn_l, adj_h, adj_l = (tab.at[k] for k in range(8))
    area = lats * pitch
    top = n * (ml - 1)
    held = n // 2 + 1
    chip, core = lax.div(me, 2), lax.rem(me, 2)
    chips = n // 2
    last = chips - 1
    way = 1 - 2 * core
    sibling = me + way
    onward = 2 * lax.rem(chip + way + chips, chips) + core

    def first_mode(device):
        z = lax.div(device, 2)
        return jnp.where(lax.rem(device, 2) == 0, z, n - 1 - z)

    def to(device, src, dst, sent, got):
        return pltpu.make_async_remote_copy(
            src_ref=src, dst_ref=dst, send_sem=sent, recv_sem=got,
            device_id={axis: device}, device_id_type=pl.DeviceIdType.MESH)

    def unit_of(unit):
        return lax.div(unit, tl), lax.rem(unit, tl)

    def unit_in(src, unit):
        ch, t = unit_of(unit)
        slot = lax.rem(unit, 2)
        return pltpu.make_async_copy(src.at[pl.ds(ch * nb, nb), t], inbuf.at[slot], in_sem.at[slot])

    def step_in(src, unit):
        @pl.when(unit + 1 < units)
        def _():
            unit_in(src, unit + 1).start()
        unit_in(src, unit).wait()

    body, peak = head(rows - tile), pl.ds(rows - tile, tile)

    def ship(stage, ch, t0, nt):
        index = stage * chunks + ch
        slot = lax.rem(index, slots)
        part = pl.ds(t0, nt)

        def one(k):
            peer = lax.rem(me + k, n)
            to(peer, send.at[slot, peer, part, body], recv.at[stage % 2, ch, me, part, body],
               send_sem.at[index], recv_sem.at[index]).start()

        loop(n, one, 1)
        recv[stage % 2, ch, me, part, body] = send[slot, me, part, body]

    def arrived(stage, ch):
        others = recv.at[stage % 2, ch, head(n - 1), :, body]
        pltpu.make_async_copy(others, others, recv_sem.at[stage * chunks + ch]).wait()

    def peaks(count):
        return topin.at[0, 0, head(count)]

    def wait_sent(index, stage):
        others = send.at[lax.rem(index, slots), head(n - 1), :, body]
        pltpu.make_async_copy(others, others, send_sem.at[index]).wait()
        if stage % 2 == 0:
            ch = index - stage * chunks
            pltpu.make_async_copy(peaks(n - 3), peaks(n - 3), row_send.at[ch]).wait()

    def send_peak(stage, ch):
        slot = lax.rem(stage * chunks + ch, slots)
        far = chips // 2
        for same in (True, False):
            its_core = core if same else 1 - core
            for away in range(1 - far, far + 1):
                place = (away > 0) - (away < 0)
                hop, target = away - place, (0, 2, 1)[place]
                if away == far:
                    hop = jnp.where(its_core == 0, 1 - far, far - 1)
                    target = jnp.where(its_core == 0, 1, 2)
                owner = 2 * lax.rem(chip + away + chips, chips) + its_core
                source = send.at[slot, owner, :, peak]
                if same and away in (-1, 0, 1):
                    topin[ch, target, me] = source[...]
                else:
                    to(2 * lax.rem(chip + hop + chips, chips) + its_core, source, topin.at[ch, target, me],
                       row_send.at[ch], row_recv.at[ch]).start()

    def free_slot(stage, ch):
        index = stage * chunks + ch
        if stage >= 1:
            @pl.when(ch >= 1)
            def _():
                wait_sent(index - slots, stage - 1)
        if stage >= 2:
            @pl.when(ch == 0)
            def _():
                wait_sent(index - slots, stage - 2)
        return lax.rem(index, slots)

    def put_rows(slot, t):
        send[slot, :, t] = gather[...].reshape(n, rows, chans).astype(BF16)

    def transform(values, head, tail):
        high = values.astype(BF16)
        low = (values - high.astype(F32)).astype(BF16)
        return dot(head[...], high) + (dot(tail[...], high) + dot(head[...], low))

    unit_in(f_hbm, 0).start()
    first_tables = pltpu.make_async_copy(tab_hbm.at[head(2)], tab.at[head(2)], tab_sem.at[0])
    other_tables = pltpu.make_async_copy(tab_hbm.at[pl.ds(2, 6)], tab.at[pl.ds(2, 6)], tab_sem.at[1])
    first_tables.start()
    barrier = pltpu.get_barrier_semaphore()

    def announce(k):
        pl.semaphore_signal(barrier, inc=1, device_id={axis: lax.rem(me + k, n)}, device_id_type=pl.DeviceIdType.MESH)

    loop(n, announce, 1)

    for which, source in enumerate((pf_hbm, pv_hbm)):
        for k in range(ml):
            pltpu.make_async_copy(source.at[first_mode(me) + n * k], pbuf.at[which, k], p_sem.at[which]).start()

    other_tables.start()

    def band_in(d):
        for which, source in enumerate((pf_hbm, pv_hbm)):
            pltpu.make_async_copy(
                source.at[top + first_mode(d), pl.ds(top, n)], band.at[which, d], band_sem.at[which]).start()

    loop(n, band_in)
    first_tables.wait()

    group = max(1, tl // 3)

    parts = degs // per
    depth = min(parts, work.shape[0] // (per * 2 * chans))

    def w_in(k):
        slot = lax.rem(k, depth)
        return pltpu.make_async_copy(
            w_hbm.at[pl.ds(k * per * 2 * chans, per * 2 * chans)],
            work.at[pl.ds(slot * per * 2 * chans, per * 2 * chans)], w_sem.at[slot])

    def step1_chunk(ch):
        slot = free_slot(0, ch)

        def row(t):
            unit = ch * tl + t
            step_in(f_hbm, unit)
            buf = lax.rem(unit, 2)
            for b in range(0, nb, 2):
                pair = jnp.concatenate([inbuf[buf, b], inbuf[buf, b + 1]], axis=1)
                spec = transform(pair, fwd_h, fwd_l)
                gather[pl.ds(b, modes2, stride=nb), :] = spec[:, :chans]
                gather[pl.ds(b + 1, modes2, stride=nb), :] = spec[:, chans:]
            put_rows(slot, t)

            @pl.when((ch == 0) & (t == group - 1))
            def _():
                pl.semaphore_wait(barrier, n - 1)
                ship(0, 0, 0, group)


        loop(tl, row)
        send_peak(0, ch)

        @pl.when(ch == 0)
        def _():
            ship(0, 0, group, tl - group)
            for k in range(depth):
                w_in(k).start()


    loop(chunks, step1_chunk)

    def clear(src):
        away = lax.rem(lax.div(src, 2) - chip + chips, chips)
        back = lax.rem(chips - away, chips)
        reach = chips // 2 - 1
        own_chip = away == 0
        above = (away < reach) | ((away == reach) & (core == 0))
        below = (back < reach) | ((back == reach) & (core == 1))
        for target, used in enumerate((own_chip, above, below)):
            @pl.when(jnp.logical_not(used))
            def _():
                for ch in range(chunks):
                    topin[ch, target, src] = jnp.zeros(topin.shape[3:], BF16)

    loop(n, clear)
    unit_in(dg_hbm, 0).start()
    for which in range(2):
        pltpu.make_async_copy(band.at[which], band.at[which], band_sem.at[which]).wait()
    qs[...] = jnp.zeros_like(qs)

    def pack(z, store):
        def one(index):
            half_at, row = lax.div(index, held), lax.rem(index, held)
            p = half_at * (held - 1) + row
            degree = jnp.where(core == 0, jnp.minimum(z + p, n - 1), jnp.maximum(p - 1, 0))
            store(half_at, row, degree, (p < n - z) == (core == 0))

        loop(2 * held, one)

    def project(which, ch, target, device):
        def body_of(src):
            gather[pl.ds(src * tl * tile, tl * tile), :] = topin[ch, target, src].reshape(tl * tile, chans).astype(F32)

        loop(n, body_of)
        for k in range(tile):
            xb[:, k * chans:(k + 1) * chans] = gather[pl.ds(k, lats, stride=tile), :].astype(BF16)
        out = dot(band[which, device].astype(BF16), xb[...])
        for k in range(tile):
            qs[pl.ds(k, n, stride=tile), :] = out[:, k * chans:(k + 1) * chans]

    def relay_peak(which, ch):
        pltpu.make_async_copy(peaks(n - 3), peaks(n - 3), row_recv.at[ch]).wait()
        targets = (lax.rem(chip + last, chips), lax.rem(chip + 1, chips))
        for side, z in enumerate(targets):
            project(which, ch, side + 1, 2 * z + core)

            def keep(half_at, row, degree, ours):
                values = qs[pl.ds(pl.multiple_of(degree * tile, tile), tile), :]
                partial[half_at, side, row] = jnp.where(ours, values, jnp.zeros_like(values))

            pack(z, keep)
        swap = to(sibling, partial.at[1 - core], mid.at[ch], mid_send.at[ch], mid_recv.at[ch])
        swap.start()
        if which == 1:
            pltpu.make_async_copy(sums.at[ch], sums.at[ch], sum_send.at[ch]).wait()
        swap.wait()
        sums[ch] = partial[core] + mid[ch]
        for side, z in enumerate(targets):
            to(2 * z + core, sums.at[ch, side], sumin.at[ch, side], sum_send.at[ch], sum_recv.at[ch]).start()

    def finish_peak(which, ch):
        pltpu.make_async_copy(sumin.at[ch], sumin.at[ch], sum_recv.at[ch]).wait()
        joined[ch, core] = sumin[ch, 0] + sumin[ch, 1]
        swap = to(sibling, joined.at[ch, core], joined.at[ch, core], join_send.at[ch], join_recv.at[ch])
        swap.start()
        project(which, ch, 0, me)
        swap.wait()

        def one(degree):
            p = jnp.where(core == 0, degree - chip, degree + 1)
            ours = degree >= first_mode(me)
            p = jnp.maximum(p, 0)
            h = jnp.where(p > held - 1, 1, 0)
            come = joined[ch, h, p - h * (held - 1)]
            work[pl.ds(area + (top + degree) * pitch + rows - tile, tile), :] = qs[
                pl.ds(pl.multiple_of(degree * tile, tile), tile), :] + jnp.where(ours, come, jnp.zeros_like(come))

        loop(n, one)

    relay_peak(0, 0)

    def ship_rows(ch):
        ship(0, ch, 0, tl)

    loop(final, ship_rows, 1)
    for which in range(2):
        pltpu.make_async_copy(pbuf.at[which], pbuf.at[which], p_sem.at[which]).wait()
    pmat[...] = pbuf[...].astype(BF16)
    other_tables.wait()

    def load_w(k):
        w_in(k).wait()
        base = lax.rem(k, depth) * per * 2 * chans
        for j in range(per):
            for part in range(2):
                vmix[k * per + j, pl.ds(part * chans, chans)] = work[
                    pl.ds(base + j * 2 * chans + part, chans, stride=2), :].astype(BF16)

        @pl.when(k + depth < parts)
        def _():
            w_in(k + depth).start()


    loop(parts, load_w)

    span = cmat.shape[3]
    mine_t = (lax.broadcasted_iota(jnp.int32, (8, lats), 1) == me * tl + lax.broadcasted_iota(jnp.int32, (8, lats), 0))
    mine_t &= lax.broadcasted_iota(jnp.int32, (8, lats), 0) < tl
    mine_t = jnp.where(mine_t, 1.0, 0.0).astype(BF16)

    def tabulate(d):
        z, of_core = lax.div(d, 2), lax.rem(d, 2)
        row = lax.broadcasted_iota(jnp.int32, (n, span), 0)
        p = jnp.where(of_core == 0, row - z, row + 1)
        target = jnp.where(p > held - 1, p + 1, p)
        moved = jnp.where(target == lax.broadcasted_iota(jnp.int32, (n, span), 1), 1.0, 0.0).astype(BF16)
        for which in range(2):
            picked = dot(mine_t, band[which, d].astype(BF16), ((1,), (1,))).astype(BF16)
            cmat[which, z, pl.ds(pl.multiple_of(of_core * 8, 8), 8), :] = dot(picked, moved)

    loop(n, tabulate)

    def no_degree(l):
        work[pl.ds(area + l * pitch + rows - tile, tile), :] = jnp.zeros((tile, chans), F32)

    loop(top, no_degree)

    def relay_first(ch):
        relay_peak(0, ch)

    loop(chunks, relay_first, 1)
    ship(0, final, 0, tl)

    sign = jnp.where(lax.broadcasted_iota(jnp.int32, (tile, chans), 0) < nb, -1.0, 1.0).astype(F32)

    def turn(values):
        groups = values.reshape(-1, tile, chans)
        return (pltpu.roll(groups, nb, 1) * sign[None]).reshape(values.shape)

    def legendre(src, dst, which, over):
        def mode(m):
            for k in range(tile):
                xb[:, k * chans:(k + 1) * chans] = work[
                    pl.ds(src + m * tile + k, lats, stride=pitch), :].astype(BF16)
            out = dot(pmat[which, m], xb[...], ((over,), (0,)))
            for k in range(tile):
                work[pl.ds(dst + m * tile + k, degs, stride=pitch), :] = out[:, k * chans:(k + 1) * chans]

        loop(ml - 1, mode)

    def unload(stage, ch):
        def body(src):
            for t in range(tl):
                work[pl.ds((src * tl + t) * pitch, rows), :] = recv[stage % 2, ch, src, t].astype(F32)

        loop(n, body)

    def load(slot):
        def body(dev):
            for t in range(tl):
                send[slot, dev, t] = work[pl.ds(area + (dev * tl + t) * pitch, rows), :].astype(BF16)

        loop(n, body)

    def only(ours, values):
        values = values.astype(F32)
        return jnp.where(ours, values, jnp.zeros_like(values)).astype(BF16)

    def spectral(stage, ch, into, kept, mix):
        arrived(stage - 1, ch)
        unload(stage - 1, ch)
        legendre(0, area, into, 1)
        finish_peak(into, ch)

        def degree(l):
            x = work[pl.ds(area + l * pitch, rows), :].astype(BF16)
            kept[l, ch] = x
            work[pl.ds(l * pitch, rows), :] = mix(l, x)

        loop(degs, degree, unroll=2)

        def keep_top(half_at, row, degree, ours):
            own[half_at, 2, ch, row] = only(ours, work[pl.ds((top + degree) * pitch + rows - tile, tile), :])

        pack(chip, keep_top)
        if stage == 1:
            swap = to(sibling, own.at[1 - core, 2, ch], other.at[2, ch], swap_send.at[ch], swap_recv.at[ch])
            swap.start()
        legendre(0, area, 1 - into, 0)
        load(free_slot(stage, ch))
        if stage == 1:
            swap.wait()
            packs[core, chip, 2, ch] = (own[core, 2, ch].astype(F32) + other[2, ch].astype(F32)).astype(BF16)

            @pl.when(ch >= 2)
            def _():
                relay_top(ch - 2)

            for away in (2, -2):
                top_copy(0, away, ch, near_recv).start()
        else:
            @pl.when(ch == 0)
            def _():
                relay_peak(1, final)

        ship(stage, ch, 0, tl)

    def top_copy(source, away, ch, got):
        block = packs.at[core, lax.rem(chip + source + chips, chips), 2, ch]
        return to(2 * lax.rem(chip + away + chips, chips) + core, block, block, top_send, got.at[ch])

    def top_blocks(count, ch):
        return packs.at[core, head(count), 2, ch]

    def relay_top(ch):
        pltpu.make_async_copy(top_blocks(2, ch), top_blocks(2, ch), near_recv.at[ch]).wait()
        for source in (2, -2):
            for away in (1, -1):
                top_copy(source, away, ch, far_recv).start()
        top_copy(-2 * way, 2 * way, ch, far_recv).start()

    def apply_top(which, ch, z):
        for h in range(2):
            qs[pl.ds(h * held * tile, held * tile), :] = packs[h, z, 2, ch].reshape(held * tile, chans).astype(F32)
        for k in range(tile):
            xb[0:span, k * chans:(k + 1) * chans] = qs[pl.ds(k, span, stride=tile), :].astype(BF16)
        out = dot(cmat[which, z].astype(BF16), xb[0:span, :])
        for k in range(tile):
            gather[pl.ds(k, 16, stride=tile), :] = out[:, k * chans:(k + 1) * chans]
        for c in range(2):
            for t in range(tl):
                recv[1, ch, 2 * z + c, t, pl.ds(rows - tile, tile)] = gather[
                    pl.ds((8 * c + t) * tile, tile), :].astype(BF16)

    def mix_forward(l, x):
        both = dot(x, vmix[l], ((1,), (1,)))
        return both[:, :chans] + turn(both[:, chans:])

    def mix_adjoint(l, x):
        real = dot(x, vmix[l, head(chans)])
        imag = dot(x, vmix[l, pl.ds(chans, chans)])
        return real - turn(imag)

    def step2_chunk(ch):
        spectral(1, ch, 0, coef, mix_forward)

    loop(chunks, step2_chunk)
    relay_top(chunks - 2)

    def fetch_rows(stage, ch, t):
        for src in range(n):
            gather[pl.ds(src * rows, rows), :] = recv[stage % 2, ch, src, t].astype(F32)

    def fetch_pair(b):
        return jnp.concatenate(
            [gather[pl.ds(b, modes2, stride=nb), :], gather[pl.ds(b + 1, modes2, stride=nb), :]], axis=1).astype(BF16)

    def step3_chunk(ch):
        arrived(1, ch)
        pltpu.make_async_copy(top_blocks(5, ch), top_blocks(5, ch), far_recv.at[ch]).wait()
        swap = to(sibling, top_blocks(chips, ch), top_blocks(chips, ch), swap_send.at[ch], swap_recv.at[ch])
        swap.start()

        @pl.when(ch == 0)
        def _():
            relay_top(final)

        swap.wait()

        @pl.when(ch == final)
        def _():
            all_sent = packs.at[0, head(7), 2]
            pltpu.make_async_copy(all_sent, all_sent, top_send).wait()

        def apply(z):
            apply_top(1, ch, z)

        loop(chips, apply)

        @pl.when(ch == 1)
        def _():
            relay_peak(1, 0)

        slot = free_slot(2, ch)

        def row(t):
            unit = ch * tl + t
            step_in(dg_hbm, unit)
            buf = lax.rem(unit, 2)
            fetch_rows(1, ch, t)
            for b in range(0, nb, 2):
                g = fetch_pair(b)
                hidden = dot(syn_h[...], g) + dot(syn_l[...], g)
                pair = jnp.concatenate([inbuf[buf, b], inbuf[buf, b + 1]], axis=1)
                spec = transform(pair * gelu_grad(hidden), dbl_h, dbl_l)
                gather[pl.ds(b, modes2, stride=nb), :] = spec[:, :chans]
                gather[pl.ds(b + 1, modes2, stride=nb), :] = spec[:, chans:]
            put_rows(slot, t)

        loop(tl, row)
        send_peak(2, ch)

        @pl.when(ch < final)
        def _():
            ship(2, ch, 0, tl)


    loop(chunks, step3_chunk)

    def relay_second(ch):
        relay_peak(1, ch)

    loop(final, relay_second, 1)
    ship(2, final, 0, tl)
    unit_in(dg_hbm, 0).start()

    def step4_chunk(ch):
        spectral(3, ch, 1, dq, mix_adjoint)

    loop(chunks, step4_chunk)

    for which, kept in enumerate((coef, dq)):
        def keep_low(half_at, row, degree, ours):
            own[half_at, which, :, row] = only(ours, kept[degree, :, head(tile)])

        pack(chip, keep_low)

    def both_parts(peer, action):
        degree = n + peer
        for which, kept in enumerate((coef, dq)):
            action(to(peer, kept.at[degree, :, head(tile)], second.at[which, me, :, head(tile)],
                      always_send, always_recv))

            @pl.when(first_mode(me) <= peer)
            def _():
                more = pl.ds(tile, tile)
                action(to(peer, kept.at[degree, :, more], second.at[which, me, :, more],
                          some_send.at[peer], some_recv.at[me]))

    def send_second(k):
        both_parts(lax.rem(me + k, n), lambda copy: copy.start())

    loop(n, send_second, 1)
    for which, kept in enumerate((coef, dq)):
        second[which, me] = kept[n + me, :, head(2 * tile)]

    def clear_second(src):
        @pl.when(first_mode(src) > me)
        def _():
            for which in range(2):
                second[which, src, :, pl.ds(tile, tile)] = jnp.zeros((chunks, tile, chans), BF16)

    loop(n, clear_second)
    own_copy = to(sibling, own.at[1 - core], other, own_send, own_recv)
    own_copy.start()

    def pack_block(k):
        return packs.at[core, lax.rem(chip - way * k + chips, chips)]

    def pack_copy(k):
        return to(onward, pack_block(k), pack_block(k), pack_send, pack_recv.at[k])

    def share(k):
        to(sibling, pack_block(k), pack_block(k), share_send, share_recv).start()

    half = degs // n - 2
    wide = 2 * chans
    block_rows = half * wide
    piece = block_rows // pieces
    hops = (last) * pieces

    def block_at(k, direction):
        return lax.rem(chip - direction * (1 + k) + 2 * chips, chips)

    def outer(dst, row, pairs):
        real = jnp.zeros((chans, chans), F32)
        imag = jnp.zeros((chans, chans), F32)
        for y, x in pairs:
            real += dot(y, x, ((0,), (0,)))
            imag -= dot(turn(y.astype(F32)).astype(BF16), x, ((0,), (0,)))
        dst[pl.ds(row, chans, stride=2), :] = real
        dst[pl.ds(row + 1, chans, stride=2), :] = imag

    def first_degree(block, of_core):
        return 2 * n + (2 * block + of_core) * half

    def weight_grad(dst, degree):
        def one(j):
            outer(dst, j * wide, [(dq[degree + j, ch], coef[degree + j, ch]) for ch in range(chunks)])

        loop(half, one)

    def pair_copy(k):
        slot = lax.rem(k, 2)
        rows_there = pl.ds(first_degree(block_at(k, -way), core) * wide, block_rows)
        return to(sibling, wbuf.at[slot, head(block_rows)], dw_out.at[rows_there],
                  pair_send.at[slot], pair_recv.at[k])

    def weight_block(k):
        @pl.when(k >= 2)
        def _():
            pair_copy(k - 2).wait_send()
        weight_grad(wbuf.at[lax.rem(k, 2)], first_degree(block_at(k, -way), 1 - core))
        pair_copy(k).start()
        block = block_at(k, way)
        weight_grad(work.at[pl.ds(block * block_rows, block_rows)], first_degree(block, core))

    loop(chips, weight_block)
    pair_copy(chips - 2).wait_send()
    pair_copy(last).wait_send()
    own_copy.wait()
    packs[core, chip] = (own[core].astype(F32) + other[...].astype(F32)).astype(BF16)

    def low_degree(l):
        def one(z):
            for c in range(2):
                p = l - z if c == 0 else l + 1
                ours = p >= 0 if c == 0 else p >= n - z
                p = jnp.maximum(p, 0)
                h = jnp.where(p > held - 1, 1, 0)
                for which in range(2):
                    lowx[which, 2 * z + c] = only(ours, packs[h, z, which, :, p - h * (held - 1)])

        loop(chips, one)
        outer(wbuf.at[0], 0, [(lowx[1].reshape(-1, chans), lowx[0].reshape(-1, chans))])
        dw_out[pl.ds(l * wide, wide)] = wbuf[0, head(wide)]

    def final_rows(unit):
        ch, t = unit_of(unit)

        step_in(dg_hbm, unit)
        buf = lax.rem(unit, 2)

        fetch_rows(3, ch, t)
        for b in range(0, nb, 2):
            g = fetch_pair(b)
            change = dot(adj_h[...], g) + dot(adj_l[...], g)
            df_out[ch * nb + b, t] = inbuf[buf, b] + change[:, :chans]
            df_out[ch * nb + b + 1, t] = inbuf[buf, b + 1] + change[:, chans:]

    def place(i, of_core):
        block = block_at(lax.div(i, pieces), way)
        start = lax.rem(i, pieces) * piece
        return pl.ds(block * block_rows + start, piece), pl.ds(first_degree(block, of_core) * wide + start, piece)

    def rs_copy(i):
        here, there = place(i, core)
        return to(onward, work.at[here], dw_out.at[there], rs_send, rs_recv.at[i])

    def add_pair(i):
        here, passed = place(i, 1 - core)

        @pl.when(lax.rem(i, pieces) == 0)
        def _():
            pair_copy(lax.div(i, pieces)).wait_recv()

        work[here] += dw_out[passed]

    def rs_step(i):
        add_pair(i)

        @pl.when(i >= pieces)
        def _():
            rs_copy(i - pieces).wait_recv()
            here, there = place(i, core)
            work[here] += dw_out[there]

        rs_copy(i).start()

        @pl.when(lax.rem(i, pieces) == 0)
        def _():
            k = lax.div(i, pieces)

            @pl.when(k > 0)
            def _():
                pack_copy(k - 1).wait_recv()

            pack_copy(k).start()
            share(k)


    loop(hops, rs_step)
    pack_copy(chips - 2).wait_recv()
    share(last)

    def own_sum(s):
        i = hops + s
        add_pair(i)
        rs_copy(i - pieces).wait_recv()
        here, there = place(i, core)
        dw_out[there] += work[here]
        ag_copy(i, s).start()

    def second_spot(k):
        return pl.ds((n + 2 * block_at(k, way) + core) * wide, wide)

    def second_copy(k, got):
        spot = dw_out.at[second_spot(k)]
        return to(onward, spot, spot, ag_send, ag_recv.at[hops + got])

    def second_publish(k):
        spot = dw_out.at[second_spot(k)]
        to(sibling, spot, spot, pub_send, pub_recv).start()

    def ag_copy(i, got):
        _, there = place(i, core)
        return to(onward, dw_out.at[there], dw_out.at[there], ag_send, ag_recv.at[got])

    def publish(i):
        _, there = place(i, core)
        to(sibling, dw_out.at[there], dw_out.at[there], pub_send, pub_recv).start()

    firsts = second.at[:, head(n - 1), :, head(tile)]
    pltpu.make_async_copy(firsts, firsts, always_recv).wait()

    def wait_second(src):
        @pl.when((first_mode(src) <= me) & (src != me))
        def _():
            part = second.at[:, src, :, pl.ds(tile, tile)]
            pltpu.make_async_copy(part, part, some_recv.at[src]).wait()

    loop(n, wait_second)
    outer(wbuf.at[0], 0, [(second[1].reshape(-1, chans), second[0].reshape(-1, chans))])
    dw_out[second_spot(last)] = wbuf[0, head(wide)]
    loop(pieces, own_sum)
    second_copy(last, 0).start()

    pl.semaphore_signal(free_sem, inc=1, device_id={axis: sibling}, device_id_type=pl.DeviceIdType.MESH)
    pl.semaphore_wait(free_sem, 1)

    def own_piece(s):
        publish(hops + s)

    loop(pieces, own_piece)
    second_publish(last)
    gathered = packs.at[1 - core]
    pltpu.make_async_copy(gathered, gathered, share_recv).wait()

    def task(i):
        @pl.when(i < chips)
        def _():
            for ch in range(chunks):
                @pl.when(i == 0)
                def _():
                    arrived(3, ch)
                apply_top(0, ch, i)

        @pl.when((i >= chips) & (i < chips + units))
        def _():
            final_rows(i - chips)

        @pl.when(i < n)
        def _():
            low_degree(i)

    def ag_step(i):
        ag_copy(i, i).wait_recv()

        @pl.when(i + pieces < hops)
        def _():
            ag_copy(i, i + pieces).start()

        publish(i)

        @pl.when(lax.rem(i, pieces) == pieces - 1)
        def _():
            k = lax.div(i, pieces)
            second_copy(k, k).wait_recv()

            @pl.when(k < chips - 2)
            def _():
                second_copy(k, k + 1).start()

            second_publish(k)

        task(i)

    loop(hops, ag_step)

    def rest(i):
        task(i)

    loop(max(hops, chips + units, n), rest, hops)

    wait_sent(2 * chunks + final, 2)
    for ch in range(chunks):
        wait_sent(3 * chunks + ch, 3)
    for ch in range(chunks):
        pltpu.make_async_copy(sums.at[ch], sums.at[ch], sum_send.at[ch]).wait()
    sent = work.at[head((last) * block_rows)]
    pltpu.make_async_copy(sent, sent, rs_send).wait()
    sent = dw_out.at[head((last) * (block_rows + wide))]
    pltpu.make_async_copy(sent, sent, ag_send).wait()
    pltpu.make_async_copy(firsts, firsts, always_send).wait()

    def wait_some(peer):
        @pl.when((first_mode(me) <= peer) & (peer != me))
        def _():
            part = second.at[:, peer, :, pl.ds(tile, tile)]
            pltpu.make_async_copy(part, part, some_send.at[peer]).wait()

    loop(n, wait_some)
    sent = packs.at[0, head(last)]
    pltpu.make_async_copy(sent, sent, pack_send).wait()
    pltpu.make_async_copy(packs.at[0], packs.at[0], share_send).wait()
    shared = dw_out.at[head(chips * (block_rows + wide))]
    pltpu.make_async_copy(shared, shared, pub_send).wait()
    pltpu.make_async_copy(shared, shared, pub_recv).wait()


def put_kernel(df_ref, dw_ref, df_hbm, dw_hbm, sems):
    copies = []
    for source, target, parts in ((df_ref, df_hbm, 3), (dw_ref, dw_hbm, 4)):
        size = source.shape[0] // parts
        for k in range(parts):
            part = pl.ds(k * size, size)
            copies.append(pltpu.make_async_copy(source.at[part], target.at[part], sems.at[len(copies)]))
    for copy in copies:
        copy.start()
    for copy in copies:
        copy.wait()


def solution(mesh):
    n = mesh.shape['lat']
    field_spec = P('member', None, 'lat', None)

    def local_step(field_loc, grad_loc, p_fwd, p_inv, w_mix):
        batch, chans, tl, lons = field_loc.shape
        degs, lats = p_fwd.shape[1:]
        ml = p_fwd.shape[0] // n
        nb = 4
        chunks = batch // nb
        rows = ml * 2 * nb
        pitch = rows + 1
        half = degs // n - 2
        pieces = 4 if half * 2 * chans % 32 == 0 else 1
        hops = (n // 2 - 1) * pieces
        per = 4
        held = n // 2 + 1
        packed = (3, chunks, held, 2 * nb, chans)
        tables = fourier_tables(n, ml, lons)
        anywhere = pl.BlockSpec(memory_space=pl.ANY)
        vmem = pl.BlockSpec(memory_space=pltpu.VMEM)
        grad_field, grad_w = pl.pallas_call(
            functools.partial(layer_kernel, 'lat', n, nb, pieces, per),
            name='layer',
            out_shape=(
                pltpu.VMEM((batch, tl, lons, chans), F32),
                pltpu.VMEM((degs * 2 * chans, chans), F32),
            ),
            in_specs=[anywhere] * 6,
            out_specs=(vmem, vmem),
            scratch_shapes=[
                pltpu.VMEM((2, chunks, n, tl, rows, chans), BF16),
                pltpu.VMEM((chunks + 1, n, tl, rows, chans), BF16),
                pltpu.VMEM((max(2 * lats * pitch, n // 2 * half * 2 * chans), chans), F32),
                pltpu.VMEM((lats, 2 * nb * chans), BF16),
                pltpu.VMEM((degs, chunks, rows, chans), BF16),
                pltpu.VMEM((degs, chunks, rows, chans), BF16),
                pltpu.VMEM((degs, 2 * chans, chans), BF16),
                pltpu.VMEM((2, max(per, half) * 2 * chans, chans), F32),
                pltpu.VMEM((2, nb, lons, chans), F32),
                pltpu.VMEM((n * rows, chans), F32),
                pltpu.VMEM((2, ml, degs, lats), F32),
                pltpu.VMEM((2, ml, degs, lats), BF16),
                pltpu.VMEM((2, n, n, lats), F32),
                pltpu.VMEM((2, n // 2, 16, 32), F32),
                pltpu.VMEM((32 * 2 * nb, chans), F32),
                pltpu.VMEM((2,) + packed, BF16),
                pltpu.VMEM(packed, BF16),
                pltpu.VMEM((2, n // 2) + packed, BF16),
                pltpu.VMEM((2, n, chunks, 2 * nb, chans), BF16),
                pltpu.VMEM(tables.shape, BF16),
                pltpu.VMEM((chunks, 3, n, tl, 2 * nb, chans), BF16),
                pltpu.VMEM((2, 2, held, 2 * nb, chans), F32),
                pltpu.VMEM((chunks, 2, held, 2 * nb, chans), F32),
                pltpu.VMEM((chunks, 2, held, 2 * nb, chans), F32),
                pltpu.VMEM((chunks, 2, held, 2 * nb, chans), F32),
                pltpu.VMEM((chunks, 2, held, 2 * nb, chans), F32),
                pltpu.VMEM((2, n, chunks, 4 * nb, chans), BF16),
                pltpu.SemaphoreType.DMA((4 * chunks,)),
                pltpu.SemaphoreType.DMA((4 * chunks,)),
                pltpu.SemaphoreType.DMA((2,)),
                pltpu.SemaphoreType.DMA((degs // per,)),
                pltpu.SemaphoreType.DMA((2,)),
                pltpu.SemaphoreType.DMA((2,)),
                pltpu.SemaphoreType.DMA((2,)),
                pltpu.SemaphoreType.DMA((n // 2,)),
                pltpu.SemaphoreType.DMA,
                pltpu.SemaphoreType.DMA((hops,)),
                pltpu.SemaphoreType.DMA,
                pltpu.SemaphoreType.DMA((hops + n // 2 - 1,)),
                pltpu.SemaphoreType.REGULAR,
                pltpu.SemaphoreType.DMA,
                pltpu.SemaphoreType.DMA,
                pltpu.SemaphoreType.DMA,
                pltpu.SemaphoreType.DMA,
                pltpu.SemaphoreType.DMA,
                pltpu.SemaphoreType.DMA((n // 2 - 1,)),
                pltpu.SemaphoreType.DMA,
                pltpu.SemaphoreType.DMA,
                pltpu.SemaphoreType.DMA((2,)),
                pltpu.SemaphoreType.DMA,
                pltpu.SemaphoreType.DMA((chunks,)),
                pltpu.SemaphoreType.DMA((chunks,)),
                pltpu.SemaphoreType.DMA((chunks,)),
                pltpu.SemaphoreType.DMA((chunks,)),
                pltpu.SemaphoreType.DMA((chunks,)),
                pltpu.SemaphoreType.DMA((chunks,)),
                pltpu.SemaphoreType.DMA((chunks,)),
                pltpu.SemaphoreType.DMA((chunks,)),
                pltpu.SemaphoreType.DMA((chunks,)),
                pltpu.SemaphoreType.DMA((chunks,)),
                pltpu.SemaphoreType.DMA((chunks,)),
                pltpu.SemaphoreType.DMA((chunks,)),
                pltpu.SemaphoreType.DMA,
                pltpu.SemaphoreType.DMA,
                pltpu.SemaphoreType.DMA((n,)),
                pltpu.SemaphoreType.DMA((n,)),
            ],
            compiler_params=pltpu.CompilerParams(
                collective_id=0, has_side_effects=True, vmem_limit_bytes=43 * 1024 * 1024),
        )(
            field_loc.transpose(0, 2, 3, 1), grad_loc.transpose(0, 2, 3, 1),
            w_mix.transpose(0, 1, 3, 2).reshape(degs * 2 * chans, chans),
            p_fwd, p_inv, tables)
        grad_field, grad_w = pl.pallas_call(
            put_kernel,
            name='put',
            out_shape=(
                jax.ShapeDtypeStruct(grad_field.shape, F32),
                jax.ShapeDtypeStruct(grad_w.shape, F32),
            ),
            in_specs=[vmem] * 2,
            out_specs=(anywhere, anywhere),
            scratch_shapes=[pltpu.SemaphoreType.DMA((7,))],
            compiler_params=pltpu.CompilerParams(vmem_limit_bytes=1024 * 1024),
        )(grad_field, grad_w)
        return grad_field.transpose(0, 3, 1, 2), grad_w.reshape(degs, chans, 2, chans).transpose(0, 1, 3, 2)

    return jax.shard_map(
        local_step, mesh=mesh, in_specs=(field_spec, field_spec, P(), P(), P()),
        out_specs=(field_spec, P('member', None, None, None)), check_vma=False)
```

```python
import functools
import math

import jax
import jax.numpy as jnp
import numpy as np
from jax import lax
from jax.experimental import pallas as pl
from jax.experimental.pallas import tpu as pltpu
from jax.sharding import PartitionSpec as P

F32 = jnp.float32
BF16 = jnp.bfloat16


def split_const(matrix):
    head = matrix.astype(BF16)
    tail = (matrix - head.astype(np.float64)).astype(BF16)
    return [head, tail]


def fourier_tables(n, ml, lons):
    modes = n * ml
    device = np.arange(n)
    first = np.where(device % 2 == 0, device // 2, n - 1 - device // 2)
    order = (first[:, None] + n * np.arange(ml)[None, :]).reshape(-1)
    angle = 2.0 * np.pi * (np.outer(order, np.arange(lons)) % lons) / lons
    forward = np.stack([np.cos(angle), -np.sin(angle)], axis=1).reshape(2 * modes, lons) / math.sqrt(lons)
    gains = np.repeat(np.where(order == 0, 1.0, 2.0), 2)[:, None]
    doubled = forward * gains
    tables = split_const(forward) + split_const(doubled) + split_const(doubled.T) + split_const(forward.T)
    return jnp.stack([jnp.asarray(t) for t in tables])


def gelu_grad(values):
    cumulative = 0.5 * (1.0 + lax.erf(values * math.sqrt(0.5)))
    density = jnp.exp(-0.5 * values * values) / math.sqrt(2.0 * math.pi)
    return cumulative + values * density


def loop(stop, step, start=0, unroll=None):
    def one(i, carry):
        step(i)
        return carry

    lax.fori_loop(start, stop, one, 0, unroll=unroll)


def head(size):
    return pl.ds(0, size)


def dot(a, b, dims=((1,), (0,))):
    return lax.dot_general(a, b, (dims, ((), ())), preferred_element_type=F32)


def layer_kernel(
    axis, n, nb, pieces, per,
    f_hbm, dg_hbm, w_hbm, pf_hbm, pv_hbm, tab_hbm,
    df_out, dw_out,
    recv, send, work, xb, coef, dq, vmix, wbuf, inbuf, gather, pbuf, pmat, band, cmat, qs, own, other, packs, lowx, tab,
    topin, partial, mid, sums, sumin, joined, handed, second,
    send_sem, recv_sem, in_sem, w_sem, p_sem, band_sem, pair_send, pair_recv, rs_send, rs_recv, ag_send, ag_recv,
    free_sem, pub_send, pub_recv, own_send, own_recv, pack_send, pack_recv, share_send, share_recv,
    tab_sem, top_send, near_recv, far_recv, swap_send, swap_recv,
    row_send, row_recv, mid_send, mid_recv, sum_send, sum_recv, join_send, join_recv,
    always_send, always_recv, some_send, some_recv, hand_recv,
):
    me = lax.axis_index(axis)
    batch, tl, lons, chans = f_hbm.shape
    ml, degs, lats = pmat.shape[1:]
    chunks = batch // nb
    tile = 2 * nb
    rows = ml * tile
    pitch = rows + 1
    modes2 = 2 * n * ml
    units = chunks * tl
    final = chunks - 1
    slots = chunks + 1
    fwd_h, fwd_l, dbl_h, dbl_l, syn_h, syn_l, adj_h, adj_l = (tab.at[k] for k in range(8))
    area = lats * pitch
    top = n * (ml - 1)
    held = n // 2 + 1
    chip, core = lax.div(me, 2), lax.rem(me, 2)
    other_core = 1 - core
    chips = n // 2
    last = chips - 1
    way = 1 - 2 * core
    sibling = me + way

    def chip_at(away):
        return lax.rem(chip + away + chips, chips)

    def across(away, its_core):
        return 2 * chip_at(away) + its_core

    onward = across(way, core)

    def first_mode(device):
        z = lax.div(device, 2)
        return jnp.where(lax.rem(device, 2) == 0, z, n - 1 - z)

    def to(device, src, dst, sent, got):
        return pltpu.make_async_remote_copy(
            src_ref=src, dst_ref=dst, send_sem=sent, recv_sem=got,
            device_id={axis: device}, device_id_type=pl.DeviceIdType.MESH)

    def unit_of(unit):
        return lax.div(unit, tl), lax.rem(unit, tl)

    def unit_in(src, unit):
        ch, t = unit_of(unit)
        slot = lax.rem(unit, 2)
        return pltpu.make_async_copy(src.at[pl.ds(ch * nb, nb), t], inbuf.at[slot], in_sem.at[slot])

    def step_in(src, unit):
        @pl.when(unit + 1 < units)
        def _():
            unit_in(src, unit + 1).start()
        unit_in(src, unit).wait()

    body, peak = head(rows - tile), pl.ds(rows - tile, tile)

    def ship(stage, ch, t0, nt):
        index = stage * chunks + ch
        slot = lax.rem(index, slots)
        part = pl.ds(t0, nt)

        def one(k):
            peer = lax.rem(me + k, n)
            to(peer, send.at[slot, peer, part, body], recv.at[stage % 2, ch, me, part, body],
               send_sem.at[index], recv_sem.at[index]).start()

        loop(n, one, 1)
        recv[stage % 2, ch, me, part, body] = send[slot, me, part, body]

    def arrived(stage, ch):
        others = recv.at[stage % 2, ch, head(n - 1), :, body]
        pltpu.make_async_copy(others, others, recv_sem.at[stage * chunks + ch]).wait()

    def peaks():
        return send.at[0, head(n - 5), :, peak]

    def wait_sent(index, stage):
        others = send.at[lax.rem(index, slots), head(n - 1), :, body]
        pltpu.make_async_copy(others, others, send_sem.at[index]).wait()
        if stage % 2 == 0:
            ch = index - stage * chunks
            pltpu.make_async_copy(peaks(), peaks(), row_send.at[ch]).wait()

    def send_peak(stage, ch):
        slot = lax.rem(stage * chunks + ch, slots)
        far = chips // 2
        for same in (True, False):
            its_core = core if same else other_core
            for away in range(1 - far, far + 1):
                near = max(-2, min(2, away))
                hop, target, apart = away - near, (0, 2, 4, 3, 1)[near], abs(away - near)
                if away == far:
                    hop = jnp.where(its_core == 0, 2 - far, far - 2)
                    target = jnp.where(its_core == 0, 3, 4)
                source = send.at[slot, across(away, its_core), :, peak]
                place = topin.at[ch, target, 2 * apart + core]
                if same and not apart:
                    place[...] = source[...]
                else:
                    to(across(hop, its_core), source, place,
                       row_send.at[ch], row_recv.at[ch]).start()

    def free_slot(stage, ch):
        index = stage * chunks + ch
        if stage >= 1:
            @pl.when(ch >= 1)
            def _():
                wait_sent(index - slots, stage - 1)
        if stage >= 2:
            @pl.when(ch == 0)
            def _():
                wait_sent(index - slots, stage - 2)
        return lax.rem(index, slots)

    def put_rows(slot, t):
        send[slot, :, t] = gather[...].reshape(n, rows, chans).astype(BF16)

    def transform(values, head, tail):
        high = values.astype(BF16)
        low = (values - high.astype(F32)).astype(BF16)
        return dot(head[...], high) + (dot(tail[...], high) + dot(head[...], low))

    unit_in(f_hbm, 0).start()
    first_tables = pltpu.make_async_copy(tab_hbm.at[head(2)], tab.at[head(2)], tab_sem.at[0])
    other_tables = pltpu.make_async_copy(tab_hbm.at[pl.ds(2, 6)], tab.at[pl.ds(2, 6)], tab_sem.at[1])
    first_tables.start()
    barrier = pltpu.get_barrier_semaphore()

    def announce(k):
        pl.semaphore_signal(barrier, inc=1, device_id={axis: lax.rem(me + k, n)}, device_id_type=pl.DeviceIdType.MESH)

    loop(n, announce, 1)

    for which, source in enumerate((pf_hbm, pv_hbm)):
        for k in range(ml):
            pltpu.make_async_copy(source.at[first_mode(me) + n * k], pbuf.at[which, k], p_sem.at[which]).start()

    other_tables.start()

    def band_in(d):
        for which, source in enumerate((pf_hbm, pv_hbm)):
            pltpu.make_async_copy(
                source.at[top + first_mode(d), pl.ds(top, n)], band.at[which, d], band_sem.at[which]).start()

    loop(n, band_in)
    first_tables.wait()

    group = max(1, tl // 3)

    parts = degs // per
    depth = min(parts, work.shape[0] // (per * 2 * chans))

    def w_in(k):
        slot = lax.rem(k, depth)
        return pltpu.make_async_copy(
            w_hbm.at[pl.ds(k * per * 2 * chans, per * 2 * chans)],
            work.at[pl.ds(slot * per * 2 * chans, per * 2 * chans)], w_sem.at[slot])

    def step1_chunk(ch):
        slot = free_slot(0, ch)

        def row(t):
            unit = ch * tl + t
            step_in(f_hbm, unit)
            buf = lax.rem(unit, 2)
            for b in range(0, nb, 2):
                pair = jnp.concatenate([inbuf[buf, b], inbuf[buf, b + 1]], axis=1)
                spec = transform(pair, fwd_h, fwd_l)
                gather[pl.ds(b, modes2, stride=nb), :] = spec[:, :chans]
                gather[pl.ds(b + 1, modes2, stride=nb), :] = spec[:, chans:]
            put_rows(slot, t)

            @pl.when((ch == 0) & (t == group - 1))
            def _():
                pl.semaphore_wait(barrier, n - 1)
                ship(0, 0, 0, group)


        loop(tl, row)
        send_peak(0, ch)

        @pl.when(ch == 0)
        def _():
            ship(0, 0, group, tl - group)
            for k in range(depth):
                w_in(k).start()


    loop(chunks, step1_chunk)

    unit_in(dg_hbm, 0).start()
    for which in range(2):
        pltpu.make_async_copy(band.at[which], band.at[which], band_sem.at[which]).wait()
    qs[...] = jnp.zeros_like(qs)

    def pack(z, store):
        def one(index):
            half_at, row = lax.div(index, held), lax.rem(index, held)
            p = half_at * (held - 1) + row
            degree = jnp.where(core == 0, jnp.minimum(z + p, n - 1), jnp.maximum(p - 1, 0))
            store(half_at, row, degree, (p < n - z) == (core == 0))

        loop(2 * held, one)

    def project(which, ch, target, device):
        gather[...] = jnp.zeros_like(gather)
        side = 1 if target == 3 else -1

        def place_rows(apart):
            for c in range(2):
                src = across(side * apart, c)
                gather[pl.ds(pl.multiple_of(src * tl * tile, tile), tl * tile), :] = topin[
                    ch, target, 2 * apart + c].reshape(tl * tile, chans).astype(F32)

        place_rows(0)
        if target > 2:
            place_rows(1)

            @pl.when(core == target - 3)
            def _():
                place_rows(2)

        for k in range(tile):
            xb[:, k * chans:(k + 1) * chans] = gather[pl.ds(k, lats, stride=tile), :].astype(BF16)
        out = dot(band[which, device].astype(BF16), xb[...])
        for k in range(tile):
            qs[pl.ds(k, n, stride=tile), :] = out[:, k * chans:(k + 1) * chans]

    def sum_rows(which, ch):
        pltpu.make_async_copy(peaks(), peaks(), row_recv.at[ch]).wait()
        for target, away in enumerate((-1, 1, -2, 2)):
            project(which, ch, target + 1, across(away, core))

            def keep(half_at, row, degree, ours):
                values = qs[pl.ds(pl.multiple_of(degree * tile, tile), tile), :]
                partial[half_at, target, row] = jnp.where(ours, values, jnp.zeros_like(values))

            pack(chip_at(away), keep)
        swap = to(sibling, partial.at[other_core], mid.at[ch], mid_send.at[ch], mid_recv.at[ch])
        swap.start()
        if which == 1:
            pltpu.make_async_copy(sums.at[ch], sums.at[ch], sum_send.at[ch]).wait()
        swap.wait()
        sums[ch] = partial[core] + mid[ch]
        for side, away in enumerate((-1, 1)):
            to(across(away, core), sums.at[ch, 2 + side], handed.at[ch, side],
               sum_send.at[ch], hand_recv.at[ch]).start()

    def pass_sums(ch):
        pltpu.make_async_copy(handed.at[ch], handed.at[ch], hand_recv.at[ch]).wait()
        for side, away in enumerate((-1, 1)):
            sums[ch, side] += handed[ch, side]
            to(across(away, core), sums.at[ch, side], sumin.at[ch, side],
               sum_send.at[ch], sum_recv.at[ch]).start()

    def finish_peak(which, ch):
        pltpu.make_async_copy(sumin.at[ch], sumin.at[ch], sum_recv.at[ch]).wait()
        joined[ch, core] = sumin[ch, 0] + sumin[ch, 1]
        swap = to(sibling, joined.at[ch, core], joined.at[ch, core], join_send.at[ch], join_recv.at[ch])
        swap.start()
        project(which, ch, 0, me)
        swap.wait()

        def one(degree):
            p = jnp.where(core == 0, degree - chip, degree + 1)
            ours = degree >= first_mode(me)
            p = jnp.maximum(p, 0)
            h = jnp.where(p > held - 1, 1, 0)
            come = joined[ch, h, p - h * (held - 1)]
            work[pl.ds(area + (top + degree) * pitch + rows - tile, tile), :] = qs[
                pl.ds(pl.multiple_of(degree * tile, tile), tile), :] + jnp.where(ours, come, jnp.zeros_like(come))

        loop(n, one)

    sum_rows(0, 0)

    def ship_rows(ch):
        ship(0, ch, 0, tl)

    loop(final, ship_rows, 1)
    for which in range(2):
        pltpu.make_async_copy(pbuf.at[which], pbuf.at[which], p_sem.at[which]).wait()
    pmat[...] = pbuf[...].astype(BF16)
    other_tables.wait()

    def load_w(k):
        w_in(k).wait()
        base = lax.rem(k, depth) * per * 2 * chans
        for j in range(per):
            for part in range(2):
                vmix[k * per + j, pl.ds(part * chans, chans)] = work[
                    pl.ds(base + j * 2 * chans + part, chans, stride=2), :].astype(BF16)

        @pl.when(k + depth < parts)
        def _():
            w_in(k + depth).start()


    loop(parts, load_w)

    span = cmat.shape[3]
    mine_t = (lax.broadcasted_iota(jnp.int32, (8, lats), 1) == me * tl + lax.broadcasted_iota(jnp.int32, (8, lats), 0))
    mine_t &= lax.broadcasted_iota(jnp.int32, (8, lats), 0) < tl
    mine_t = jnp.where(mine_t, 1.0, 0.0).astype(BF16)

    def tabulate(d):
        z, of_core = lax.div(d, 2), lax.rem(d, 2)
        row = lax.broadcasted_iota(jnp.int32, (n, span), 0)
        p = jnp.where(of_core == 0, row - z, row + 1)
        target = jnp.where(p > held - 1, p + 1, p)
        moved = jnp.where(target == lax.broadcasted_iota(jnp.int32, (n, span), 1), 1.0, 0.0).astype(BF16)
        for which in range(2):
            picked = dot(mine_t, band[which, d].astype(BF16), ((1,), (1,))).astype(BF16)
            cmat[which, z, pl.ds(pl.multiple_of(of_core * 8, 8), 8), :] = dot(picked, moved)

    loop(n, tabulate)

    def no_degree(l):
        work[pl.ds(area + l * pitch + rows - tile, tile), :] = jnp.zeros((tile, chans), F32)

    loop(top, no_degree)

    pass_sums(0)

    def sum_first(ch):
        sum_rows(0, ch)

    loop(chunks, sum_first, 1)
    ship(0, final, 0, tl)
    loop(chunks, pass_sums, 1)

    sign = jnp.where(lax.broadcasted_iota(jnp.int32, (tile, chans), 0) < nb, -1.0, 1.0).astype(F32)

    def turn(values):
        groups = values.reshape(-1, tile, chans)
        return (pltpu.roll(groups, nb, 1) * sign[None]).reshape(values.shape)

    def legendre(src, dst, which, over):
        def mode(m):
            for k in range(tile):
                xb[:, k * chans:(k + 1) * chans] = work[
                    pl.ds(src + m * tile + k, lats, stride=pitch), :].astype(BF16)
            out = dot(pmat[which, m], xb[...], ((over,), (0,)))
            for k in range(tile):
                work[pl.ds(dst + m * tile + k, degs, stride=pitch), :] = out[:, k * chans:(k + 1) * chans]

        loop(ml - 1, mode)

    def unload(stage, ch):
        def body(src):
            for t in range(tl):
                work[pl.ds((src * tl + t) * pitch, rows), :] = recv[stage % 2, ch, src, t].astype(F32)

        loop(n, body)

    def load(slot):
        def body(dev):
            for t in range(tl):
                send[slot, dev, t] = work[pl.ds(area + (dev * tl + t) * pitch, rows), :].astype(BF16)

        loop(n, body)

    def only(ours, values):
        values = values.astype(F32)
        return jnp.where(ours, values, jnp.zeros_like(values)).astype(BF16)

    def spectral(stage, ch, into, kept, mix):
        arrived(stage - 1, ch)
        unload(stage - 1, ch)
        legendre(0, area, into, 1)
        finish_peak(into, ch)

        def degree(l):
            x = work[pl.ds(area + l * pitch, rows), :].astype(BF16)
            kept[l, ch] = x
            work[pl.ds(l * pitch, rows), :] = mix(l, x)

        loop(degs, degree, unroll=2)

        def keep_top(half_at, row, degree, ours):
            own[half_at, 2, ch, row] = only(ours, work[pl.ds((top + degree) * pitch + rows - tile, tile), :])

        pack(chip, keep_top)
        if stage == 1:
            swap = to(sibling, own.at[other_core, 2, ch], other.at[2, ch], swap_send.at[ch], swap_recv.at[ch])
            swap.start()
        legendre(0, area, 1 - into, 0)
        load(free_slot(stage, ch))
        if stage == 1:
            swap.wait()
            packs[core, chip, 2, ch] = (own[core, 2, ch].astype(F32) + other[2, ch].astype(F32)).astype(BF16)

            @pl.when(ch >= 2)
            def _():
                relay_top(ch - 2)

            for away in (2, -2):
                top_copy(0, away, ch, near_recv).start()
        else:
            @pl.when(ch == 0)
            def _():
                pass_sums(final - 1)
                sum_rows(1, final)

            @pl.when(ch == 1)
            def _():
                pass_sums(final)

        ship(stage, ch, 0, tl)

    def top_copy(source, away, ch, got):
        block = packs.at[core, chip_at(source), 2, ch]
        return to(across(away, core), block, block, top_send, got.at[ch])

    def top_blocks(count, ch):
        return packs.at[core, head(count), 2, ch]

    def relay_top(ch):
        pltpu.make_async_copy(top_blocks(2, ch), top_blocks(2, ch), near_recv.at[ch]).wait()
        for source in (2, -2):
            for away in (1, -1):
                top_copy(source, away, ch, far_recv).start()
        top_copy(-2 * way, 2 * way, ch, far_recv).start()

    def apply_top(which, ch, z):
        for h in range(2):
            qs[pl.ds(h * held * tile, held * tile), :] = packs[h, z, 2, ch].reshape(held * tile, chans).astype(F32)
        for k in range(tile):
            xb[0:span, k * chans:(k + 1) * chans] = qs[pl.ds(k, span, stride=tile), :].astype(BF16)
        out = dot(cmat[which, z].astype(BF16), xb[0:span, :])
        for k in range(tile):
            gather[pl.ds(k, 16, stride=tile), :] = out[:, k * chans:(k + 1) * chans]
        for c in range(2):
            for t in range(tl):
                recv[1, ch, 2 * z + c, t, pl.ds(rows - tile, tile)] = gather[
                    pl.ds((8 * c + t) * tile, tile), :].astype(BF16)

    def mix_forward(l, x):
        both = dot(x, vmix[l], ((1,), (1,)))
        return both[:, :chans] + turn(both[:, chans:])

    def mix_adjoint(l, x):
        real = dot(x, vmix[l, head(chans)])
        imag = dot(x, vmix[l, pl.ds(chans, chans)])
        return real - turn(imag)

    def step2_chunk(ch):
        spectral(1, ch, 0, coef, mix_forward)

    loop(chunks, step2_chunk)
    relay_top(chunks - 2)

    def fetch_rows(stage, ch, t):
        for src in range(n):
            gather[pl.ds(src * rows, rows), :] = recv[stage % 2, ch, src, t].astype(F32)

    def fetch_pair(b):
        return jnp.concatenate(
            [gather[pl.ds(b, modes2, stride=nb), :], gather[pl.ds(b + 1, modes2, stride=nb), :]], axis=1).astype(BF16)

    def step3_chunk(ch):
        arrived(1, ch)
        pltpu.make_async_copy(top_blocks(5, ch), top_blocks(5, ch), far_recv.at[ch]).wait()
        swap = to(sibling, top_blocks(chips, ch), top_blocks(chips, ch), swap_send.at[ch], swap_recv.at[ch])
        swap.start()

        @pl.when(ch == 0)
        def _():
            relay_top(final)

        swap.wait()

        @pl.when(ch == final)
        def _():
            all_sent = packs.at[0, head(7), 2]
            pltpu.make_async_copy(all_sent, all_sent, top_send).wait()

        def apply(z):
            apply_top(1, ch, z)

        loop(chips, apply)

        @pl.when(ch == 1)
        def _():
            sum_rows(1, 0)

        slot = free_slot(2, ch)

        def row(t):
            unit = ch * tl + t
            step_in(dg_hbm, unit)
            buf = lax.rem(unit, 2)
            fetch_rows(1, ch, t)
            for b in range(0, nb, 2):
                g = fetch_pair(b)
                hidden = dot(syn_h[...], g) + dot(syn_l[...], g)
                pair = jnp.concatenate([inbuf[buf, b], inbuf[buf, b + 1]], axis=1)
                spec = transform(pair * gelu_grad(hidden), dbl_h, dbl_l)
                gather[pl.ds(b, modes2, stride=nb), :] = spec[:, :chans]
                gather[pl.ds(b + 1, modes2, stride=nb), :] = spec[:, chans:]
            put_rows(slot, t)

        loop(tl, row)
        send_peak(2, ch)

        @pl.when(ch < final)
        def _():
            ship(2, ch, 0, tl)


    loop(chunks, step3_chunk)

    def sum_second(ch):
        pass_sums(ch - 1)
        sum_rows(1, ch)

    loop(final, sum_second, 1)
    ship(2, final, 0, tl)
    unit_in(dg_hbm, 0).start()

    def step4_chunk(ch):
        spectral(3, ch, 1, dq, mix_adjoint)

    loop(chunks, step4_chunk)

    for which, kept in enumerate((coef, dq)):
        def keep_low(half_at, row, degree, ours):
            own[half_at, which, :, row] = only(ours, kept[degree, :, head(tile)])

        pack(chip, keep_low)

    def both_parts(peer, action):
        degree = n + peer
        for which, kept in enumerate((coef, dq)):
            action(to(peer, kept.at[degree, :, head(tile)], second.at[which, me, :, head(tile)],
                      always_send, always_recv))

            @pl.when(first_mode(me) <= peer)
            def _():
                more = pl.ds(tile, tile)
                action(to(peer, kept.at[degree, :, more], second.at[which, me, :, more],
                          some_send.at[peer], some_recv.at[me]))

    def send_second(k):
        both_parts(lax.rem(me + k, n), lambda copy: copy.start())

    loop(n, send_second, 1)
    for which, kept in enumerate((coef, dq)):
        second[which, me] = kept[n + me, :, head(2 * tile)]

    def clear_second(src):
        @pl.when(first_mode(src) > me)
        def _():
            for which in range(2):
                second[which, src, :, pl.ds(tile, tile)] = jnp.zeros((chunks, tile, chans), BF16)

    loop(n, clear_second)
    own_copy = to(sibling, own.at[other_core], other, own_send, own_recv)
    own_copy.start()

    def pack_block(k):
        return packs.at[core, chip_at(-way * k)]

    def pack_copy(k):
        return to(onward, pack_block(k), pack_block(k), pack_send, pack_recv.at[k])

    def share(k):
        to(sibling, pack_block(k), pack_block(k), share_send, share_recv).start()

    half = degs // n - 2
    wide = 2 * chans
    block_rows = half * wide
    piece = block_rows // pieces
    hops = (last) * pieces

    def block_at(k, direction):
        return lax.rem(chip - direction * (1 + k) + 2 * chips, chips)

    def outer(dst, row, pairs):
        real = jnp.zeros((chans, chans), F32)
        imag = jnp.zeros((chans, chans), F32)
        for y, x in pairs:
            real += dot(y, x, ((0,), (0,)))
            imag -= dot(turn(y.astype(F32)).astype(BF16), x, ((0,), (0,)))
        dst[pl.ds(row, chans, stride=2), :] = real
        dst[pl.ds(row + 1, chans, stride=2), :] = imag

    def first_degree(block, of_core):
        return 2 * n + (2 * block + of_core) * half

    def weight_grad(dst, degree):
        def one(j):
            outer(dst, j * wide, [(dq[degree + j, ch], coef[degree + j, ch]) for ch in range(chunks)])

        loop(half, one)

    def pair_copy(k):
        slot = lax.rem(k, 2)
        rows_there = pl.ds(first_degree(block_at(k, -way), core) * wide, block_rows)
        return to(sibling, wbuf.at[slot, head(block_rows)], dw_out.at[rows_there],
                  pair_send.at[slot], pair_recv.at[k])

    def weight_block(k):
        @pl.when(k >= 2)
        def _():
            pair_copy(k - 2).wait_send()
        weight_grad(wbuf.at[lax.rem(k, 2)], first_degree(block_at(k, -way), other_core))
        pair_copy(k).start()
        block = block_at(k, way)
        weight_grad(work.at[pl.ds(block * block_rows, block_rows)], first_degree(block, core))

    loop(chips, weight_block)
    pair_copy(chips - 2).wait_send()
    pair_copy(last).wait_send()
    own_copy.wait()
    packs[core, chip] = (own[core].astype(F32) + other[...].astype(F32)).astype(BF16)

    def low_degree(l):
        def one(z):
            for c in range(2):
                p = l - z if c == 0 else l + 1
                ours = p >= 0 if c == 0 else p >= n - z
                p = jnp.maximum(p, 0)
                h = jnp.where(p > held - 1, 1, 0)
                for which in range(2):
                    lowx[which, 2 * z + c] = only(ours, packs[h, z, which, :, p - h * (held - 1)])

        loop(chips, one)
        outer(wbuf.at[0], 0, [(lowx[1].reshape(-1, chans), lowx[0].reshape(-1, chans))])
        dw_out[pl.ds(l * wide, wide)] = wbuf[0, head(wide)]

    def final_rows(unit):
        ch, t = unit_of(unit)

        step_in(dg_hbm, unit)
        buf = lax.rem(unit, 2)

        fetch_rows(3, ch, t)
        for b in range(0, nb, 2):
            g = fetch_pair(b)
            change = dot(adj_h[...], g) + dot(adj_l[...], g)
            df_out[ch * nb + b, t] = inbuf[buf, b] + change[:, :chans]
            df_out[ch * nb + b + 1, t] = inbuf[buf, b + 1] + change[:, chans:]

    def place(i, of_core):
        block = block_at(lax.div(i, pieces), way)
        start = lax.rem(i, pieces) * piece
        return pl.ds(block * block_rows + start, piece), pl.ds(first_degree(block, of_core) * wide + start, piece)

    def rs_copy(i):
        here, there = place(i, core)
        return to(onward, work.at[here], dw_out.at[there], rs_send, rs_recv.at[i])

    def add_pair(i):
        here, passed = place(i, other_core)

        @pl.when(lax.rem(i, pieces) == 0)
        def _():
            pair_copy(lax.div(i, pieces)).wait_recv()

        work[here] += dw_out[passed]

    def rs_step(i):
        add_pair(i)

        @pl.when(i >= pieces)
        def _():
            rs_copy(i - pieces).wait_recv()
            here, there = place(i, core)
            work[here] += dw_out[there]

        rs_copy(i).start()

        @pl.when(lax.rem(i, pieces) == 0)
        def _():
            k = lax.div(i, pieces)

            @pl.when(k > 0)
            def _():
                pack_copy(k - 1).wait_recv()

            pack_copy(k).start()
            share(k)


    loop(hops, rs_step)
    pack_copy(chips - 2).wait_recv()
    share(last)

    def own_sum(s):
        i = hops + s
        add_pair(i)
        rs_copy(i - pieces).wait_recv()
        here, there = place(i, core)
        dw_out[there] += work[here]
        ag_copy(i, s).start()

    def second_spot(k):
        return pl.ds((n + 2 * block_at(k, way) + core) * wide, wide)

    def second_copy(k, got):
        spot = dw_out.at[second_spot(k)]
        return to(onward, spot, spot, ag_send, ag_recv.at[hops + got])

    def second_publish(k):
        spot = dw_out.at[second_spot(k)]
        to(sibling, spot, spot, pub_send, pub_recv).start()

    def ag_copy(i, got):
        _, there = place(i, core)
        return to(onward, dw_out.at[there], dw_out.at[there], ag_send, ag_recv.at[got])

    def publish(i):
        _, there = place(i, core)
        to(sibling, dw_out.at[there], dw_out.at[there], pub_send, pub_recv).start()

    firsts = second.at[:, head(n - 1), :, head(tile)]
    pltpu.make_async_copy(firsts, firsts, always_recv).wait()

    def wait_second(src):
        @pl.when((first_mode(src) <= me) & (src != me))
        def _():
            part = second.at[:, src, :, pl.ds(tile, tile)]
            pltpu.make_async_copy(part, part, some_recv.at[src]).wait()

    loop(n, wait_second)
    outer(wbuf.at[0], 0, [(second[1].reshape(-1, chans), second[0].reshape(-1, chans))])
    dw_out[second_spot(last)] = wbuf[0, head(wide)]
    loop(pieces, own_sum)
    second_copy(last, 0).start()

    pl.semaphore_signal(free_sem, inc=1, device_id={axis: sibling}, device_id_type=pl.DeviceIdType.MESH)
    pl.semaphore_wait(free_sem, 1)

    def own_piece(s):
        publish(hops + s)

    loop(pieces, own_piece)
    second_publish(last)
    gathered = packs.at[other_core]
    pltpu.make_async_copy(gathered, gathered, share_recv).wait()

    def task(i):
        @pl.when(i < chips)
        def _():
            for ch in range(chunks):
                @pl.when(i == 0)
                def _():
                    arrived(3, ch)
                apply_top(0, ch, i)

        @pl.when((i >= chips) & (i < chips + units))
        def _():
            final_rows(i - chips)

        @pl.when(i < n)
        def _():
            low_degree(i)

    def ag_step(i):
        ag_copy(i, i).wait_recv()

        @pl.when(i + pieces < hops)
        def _():
            ag_copy(i, i + pieces).start()

        publish(i)

        @pl.when(lax.rem(i, pieces) == pieces - 1)
        def _():
            k = lax.div(i, pieces)
            second_copy(k, k).wait_recv()

            @pl.when(k < chips - 2)
            def _():
                second_copy(k, k + 1).start()

            second_publish(k)

        task(i)

    loop(hops, ag_step)

    def rest(i):
        task(i)

    loop(max(hops, chips + units, n), rest, hops)

    wait_sent(2 * chunks + final, 2)
    for ch in range(chunks):
        wait_sent(3 * chunks + ch, 3)
    for ch in range(chunks):
        pltpu.make_async_copy(sums.at[ch], sums.at[ch], sum_send.at[ch]).wait()
    sent = work.at[head((last) * block_rows)]
    pltpu.make_async_copy(sent, sent, rs_send).wait()
    sent = dw_out.at[head((last) * (block_rows + wide))]
    pltpu.make_async_copy(sent, sent, ag_send).wait()
    pltpu.make_async_copy(firsts, firsts, always_send).wait()

    def wait_some(peer):
        @pl.when((first_mode(me) <= peer) & (peer != me))
        def _():
            part = second.at[:, peer, :, pl.ds(tile, tile)]
            pltpu.make_async_copy(part, part, some_send.at[peer]).wait()

    loop(n, wait_some)
    sent = packs.at[0, head(last)]
    pltpu.make_async_copy(sent, sent, pack_send).wait()
    pltpu.make_async_copy(packs.at[0], packs.at[0], share_send).wait()
    shared = dw_out.at[head(chips * (block_rows + wide))]
    pltpu.make_async_copy(shared, shared, pub_send).wait()
    pltpu.make_async_copy(shared, shared, pub_recv).wait()


def put_kernel(df_ref, dw_ref, df_hbm, dw_hbm, sems):
    copies = []
    for source, target, parts in ((df_ref, df_hbm, 6), (dw_ref, dw_hbm, 12)):
        size = source.shape[0] // parts
        for k in range(parts):
            part = pl.ds(k * size, size)
            copies.append(pltpu.make_async_copy(source.at[part], target.at[part], sems.at[len(copies)]))
    for copy in copies:
        copy.start()
    for copy in copies:
        copy.wait()


def solution(mesh):
    n = mesh.shape['lat']
    field_spec = P('member', None, 'lat', None)

    def local_step(field_loc, grad_loc, p_fwd, p_inv, w_mix):
        batch, chans, tl, lons = field_loc.shape
        degs, lats = p_fwd.shape[1:]
        ml = p_fwd.shape[0] // n
        nb = 4
        chunks = batch // nb
        rows = ml * 2 * nb
        pitch = rows + 1
        half = degs // n - 2
        pieces = 4 if half * 2 * chans % 32 == 0 else 1
        hops = (n // 2 - 1) * pieces
        per = 4
        held = n // 2 + 1
        packed = (3, chunks, held, 2 * nb, chans)
        tables = fourier_tables(n, ml, lons)
        anywhere = pl.BlockSpec(memory_space=pl.ANY)
        vmem = pl.BlockSpec(memory_space=pltpu.VMEM)
        grad_field, grad_w = pl.pallas_call(
            functools.partial(layer_kernel, 'lat', n, nb, pieces, per),
            name='layer',
            out_shape=(
                pltpu.VMEM((batch, tl, lons, chans), F32),
                pltpu.VMEM((degs * 2 * chans, chans), F32),
            ),
            in_specs=[anywhere] * 6,
            out_specs=(vmem, vmem),
            scratch_shapes=[
                pltpu.VMEM((2, chunks, n, tl, rows, chans), BF16),
                pltpu.VMEM((chunks + 1, n, tl, rows, chans), BF16),
                pltpu.VMEM((max(2 * lats * pitch, n // 2 * half * 2 * chans), chans), F32),
                pltpu.VMEM((lats, 2 * nb * chans), BF16),
                pltpu.VMEM((degs, chunks, rows, chans), BF16),
                pltpu.VMEM((degs, chunks, rows, chans), BF16),
                pltpu.VMEM((degs, 2 * chans, chans), BF16),
                pltpu.VMEM((2, max(per, half) * 2 * chans, chans), F32),
                pltpu.VMEM((2, nb, lons, chans), F32),
                pltpu.VMEM((n * rows, chans), F32),
                pltpu.VMEM((2, ml, degs, lats), F32),
                pltpu.VMEM((2, ml, degs, lats), BF16),
                pltpu.VMEM((2, n, n, lats), F32),
                pltpu.VMEM((2, n // 2, 16, 32), F32),
                pltpu.VMEM((32 * 2 * nb, chans), F32),
                pltpu.VMEM((2,) + packed, BF16),
                pltpu.VMEM(packed, BF16),
                pltpu.VMEM((2, n // 2) + packed, BF16),
                pltpu.VMEM((2, n, chunks, 2 * nb, chans), BF16),
                pltpu.VMEM(tables.shape, BF16),
                pltpu.VMEM((chunks, 5, 6, tl, 2 * nb, chans), BF16),
                pltpu.VMEM((2, 4, held, 2 * nb, chans), F32),
                pltpu.VMEM((chunks, 4, held, 2 * nb, chans), F32),
                pltpu.VMEM((chunks, 4, held, 2 * nb, chans), F32),
                pltpu.VMEM((chunks, 2, held, 2 * nb, chans), F32),
                pltpu.VMEM((chunks, 2, held, 2 * nb, chans), F32),
                pltpu.VMEM((chunks, 2, held, 2 * nb, chans), F32),
                pltpu.VMEM((2, n, chunks, 4 * nb, chans), BF16),
                pltpu.SemaphoreType.DMA((4 * chunks,)),
                pltpu.SemaphoreType.DMA((4 * chunks,)),
                pltpu.SemaphoreType.DMA((2,)),
                pltpu.SemaphoreType.DMA((degs // per,)),
                pltpu.SemaphoreType.DMA((2,)),
                pltpu.SemaphoreType.DMA((2,)),
                pltpu.SemaphoreType.DMA((2,)),
                pltpu.SemaphoreType.DMA((n // 2,)),
                pltpu.SemaphoreType.DMA,
                pltpu.SemaphoreType.DMA((hops,)),
                pltpu.SemaphoreType.DMA,
                pltpu.SemaphoreType.DMA((hops + n // 2 - 1,)),
                pltpu.SemaphoreType.REGULAR,
                pltpu.SemaphoreType.DMA,
                pltpu.SemaphoreType.DMA,
                pltpu.SemaphoreType.DMA,
                pltpu.SemaphoreType.DMA,
                pltpu.SemaphoreType.DMA,
                pltpu.SemaphoreType.DMA((n // 2 - 1,)),
                pltpu.SemaphoreType.DMA,
                pltpu.SemaphoreType.DMA,
                pltpu.SemaphoreType.DMA((2,)),
                pltpu.SemaphoreType.DMA,
                pltpu.SemaphoreType.DMA((chunks,)),
                pltpu.SemaphoreType.DMA((chunks,)),
                pltpu.SemaphoreType.DMA((chunks,)),
                pltpu.SemaphoreType.DMA((chunks,)),
                pltpu.SemaphoreType.DMA((chunks,)),
                pltpu.SemaphoreType.DMA((chunks,)),
                pltpu.SemaphoreType.DMA((chunks,)),
                pltpu.SemaphoreType.DMA((chunks,)),
                pltpu.SemaphoreType.DMA((chunks,)),
                pltpu.SemaphoreType.DMA((chunks,)),
                pltpu.SemaphoreType.DMA((chunks,)),
                pltpu.SemaphoreType.DMA((chunks,)),
                pltpu.SemaphoreType.DMA,
                pltpu.SemaphoreType.DMA,
                pltpu.SemaphoreType.DMA((n,)),
                pltpu.SemaphoreType.DMA((n,)),
                pltpu.SemaphoreType.DMA((chunks,)),
            ],
            compiler_params=pltpu.CompilerParams(
                collective_id=0, has_side_effects=True, vmem_limit_bytes=43 * 1024 * 1024),
        )(
            field_loc.transpose(0, 2, 3, 1), grad_loc.transpose(0, 2, 3, 1),
            w_mix.transpose(0, 1, 3, 2).reshape(degs * 2 * chans, chans),
            p_fwd, p_inv, tables)
        grad_field, grad_w = pl.pallas_call(
            put_kernel,
            name='put',
            out_shape=(
                jax.ShapeDtypeStruct(grad_field.shape, F32),
                jax.ShapeDtypeStruct(grad_w.shape, F32),
            ),
            in_specs=[vmem] * 2,
            out_specs=(anywhere, anywhere),
            scratch_shapes=[pltpu.SemaphoreType.DMA((18,))],
            compiler_params=pltpu.CompilerParams(vmem_limit_bytes=1024 * 1024),
        )(grad_field, grad_w)
        return grad_field.transpose(0, 3, 1, 2), grad_w.reshape(degs, chans, 2, chans).transpose(0, 1, 3, 2)

    return jax.shard_map(
        local_step, mesh=mesh, in_specs=(field_spec, field_spec, P(), P(), P()),
        out_specs=(field_spec, P('member', None, None, None)), check_vma=False)
```

```python
import functools
import math

import jax
import jax.numpy as jnp
import numpy as np
from jax import lax
from jax.experimental import pallas as pl
from jax.experimental.pallas import tpu as pltpu
from jax.sharding import PartitionSpec as P

F32 = jnp.float32
BF16 = jnp.bfloat16


def split_const(matrix):
    head = matrix.astype(BF16)
    tail = (matrix - head.astype(np.float64)).astype(BF16)
    return [head, tail]


def fourier_tables(n, ml, lons):
    modes = n * ml
    device = np.arange(n)
    first = np.where(device % 2 == 0, device // 2, n - 1 - device // 2)
    order = (first[:, None] + n * np.arange(ml)[None, :]).reshape(-1)
    angle = 2.0 * np.pi * (np.outer(order, np.arange(lons)) % lons) / lons
    forward = np.stack([np.cos(angle), -np.sin(angle)], axis=1).reshape(2 * modes, lons) / math.sqrt(lons)
    gains = np.repeat(np.where(order == 0, 1.0, 2.0), 2)[:, None]
    doubled = forward * gains
    tables = split_const(forward) + split_const(doubled) + split_const(doubled.T) + split_const(forward.T)
    return jnp.stack([jnp.asarray(t) for t in tables])


def gelu_grad(values):
    cumulative = 0.5 * (1.0 + lax.erf(values * math.sqrt(0.5)))
    density = jnp.exp(-0.5 * values * values) / math.sqrt(2.0 * math.pi)
    return cumulative + values * density


def loop(stop, step, start=0, unroll=None):
    def one(i, carry):
        step(i)
        return carry

    lax.fori_loop(start, stop, one, 0, unroll=unroll)


def head(size):
    return pl.ds(0, size)


def dot(a, b, dims=((1,), (0,))):
    return lax.dot_general(a, b, (dims, ((), ())), preferred_element_type=F32)


def layer_kernel(
    axis, n, nb, pieces, per,
    f_hbm, dg_hbm, w_hbm, pf_hbm, pv_hbm, tab_hbm,
    df_out, dw_out,
    recv, send, work, xb, coef, dq, vmix, wbuf, inbuf, gather, pbuf, pmat, band, cmat, qs, own, other, packs, lowx, tab,
    topin, partial, mid, sums, sumin, joined, handed, second,
    send_sem, recv_sem, in_sem, w_sem, p_sem, band_sem, pair_send, pair_recv, rs_send, rs_recv, ag_send, ag_recv,
    free_sem, pub_send, pub_recv, own_send, own_recv, pack_send, pack_recv, share_send, share_recv,
    tab_sem, top_send, near_recv, far_recv, swap_send, swap_recv,
    row_send, row_recv, mid_send, mid_recv, sum_send, sum_recv, join_send, join_recv,
    always_send, always_recv, some_send, some_recv, hand_recv,
):
    me = lax.axis_index(axis)
    batch, tl, lons, chans = f_hbm.shape
    ml, degs, lats = pmat.shape[1:]
    chunks = batch // nb
    tile = 2 * nb
    rows = ml * tile
    pitch = rows + 1
    modes2 = 2 * n * ml
    units = chunks * tl
    final = chunks - 1
    slots = chunks + 1
    fwd_h, fwd_l, dbl_h, dbl_l, syn_h, syn_l, adj_h, adj_l = (tab.at[k] for k in range(8))
    area = lats * pitch
    top = n * (ml - 1)
    held = n // 2 + 1
    chip, core = lax.div(me, 2), lax.rem(me, 2)
    other_core = 1 - core
    chips = n // 2
    last = chips - 1
    way = 1 - 2 * core
    sibling = me + way

    def chip_at(away):
        return lax.rem(chip + away + chips, chips)

    def across(away, its_core):
        return 2 * chip_at(away) + its_core

    onward = across(way, core)

    def first_mode(device):
        z = lax.div(device, 2)
        return jnp.where(lax.rem(device, 2) == 0, z, n - 1 - z)

    def to(device, src, dst, sent, got):
        return pltpu.make_async_remote_copy(
            src_ref=src, dst_ref=dst, send_sem=sent, recv_sem=got,
            device_id={axis: device}, device_id_type=pl.DeviceIdType.MESH)

    def unit_of(unit):
        return lax.div(unit, tl), lax.rem(unit, tl)

    def unit_in(src, unit):
        ch, t = unit_of(unit)
        slot = lax.rem(unit, 2)
        return pltpu.make_async_copy(src.at[pl.ds(ch * nb, nb), t], inbuf.at[slot], in_sem.at[slot])

    def step_in(src, unit):
        @pl.when(unit + 1 < units)
        def _():
            unit_in(src, unit + 1).start()
        unit_in(src, unit).wait()

    body, peak = head(rows - tile), pl.ds(rows - tile, tile)

    def ship(stage, ch, t0, nt):
        index = stage * chunks + ch
        slot = lax.rem(index, slots)
        part = pl.ds(t0, nt)

        def one(k):
            peer = lax.rem(me + k, n)
            to(peer, send.at[slot, peer, part, body], recv.at[stage % 2, ch, me, part, body],
               send_sem.at[index], recv_sem.at[index]).start()

        loop(n, one, 1)
        recv[stage % 2, ch, me, part, body] = send[slot, me, part, body]

    def arrived(stage, ch):
        others = recv.at[stage % 2, ch, head(n - 1), :, body]
        pltpu.make_async_copy(others, others, recv_sem.at[stage * chunks + ch]).wait()

    def peaks():
        return send.at[0, head(n - 5), :, peak]

    def wait_sent(index, stage):
        others = send.at[lax.rem(index, slots), head(n - 1), :, body]
        pltpu.make_async_copy(others, others, send_sem.at[index]).wait()
        if stage % 2 == 0:
            ch = index - stage * chunks
            pltpu.make_async_copy(peaks(), peaks(), row_send.at[ch]).wait()

    def send_peak(stage, ch):
        slot = lax.rem(stage * chunks + ch, slots)
        far = chips // 2
        for same in (True, False):
            its_core = core if same else other_core
            for away in range(1 - far, far + 1):
                near = max(-2, min(2, away))
                hop, target, apart = away - near, (0, 2, 4, 3, 1)[near], abs(away - near)
                if away == far:
                    hop = jnp.where(its_core == 0, 2 - far, far - 2)
                    target = jnp.where(its_core == 0, 3, 4)
                source = send.at[slot, across(away, its_core), :, peak]
                place = topin.at[ch, target, 2 * apart + core]
                if same and not apart:
                    place[...] = source[...]
                else:
                    to(across(hop, its_core), source, place,
                       row_send.at[ch], row_recv.at[ch]).start()

    def free_slot(stage, ch):
        index = stage * chunks + ch
        if stage >= 1:
            @pl.when(ch >= 1)
            def _():
                wait_sent(index - slots, stage - 1)
        if stage >= 2:
            @pl.when(ch == 0)
            def _():
                wait_sent(index - slots, stage - 2)
        return lax.rem(index, slots)

    def put_rows(slot, t):
        send[slot, :, t] = gather[...].reshape(n, rows, chans).astype(BF16)

    def transform(values, head, tail):
        high = values.astype(BF16)
        low = (values - high.astype(F32)).astype(BF16)
        return dot(head[...], high) + (dot(tail[...], high) + dot(head[...], low))

    unit_in(f_hbm, 0).start()
    first_tables = pltpu.make_async_copy(tab_hbm.at[head(2)], tab.at[head(2)], tab_sem.at[0])
    other_tables = pltpu.make_async_copy(tab_hbm.at[pl.ds(2, 6)], tab.at[pl.ds(2, 6)], tab_sem.at[1])
    first_tables.start()
    barrier = pltpu.get_barrier_semaphore()

    def announce(k):
        pl.semaphore_signal(barrier, inc=1, device_id={axis: lax.rem(me + k, n)}, device_id_type=pl.DeviceIdType.MESH)

    loop(n, announce, 1)

    for which, source in enumerate((pf_hbm, pv_hbm)):
        for k in range(ml):
            pltpu.make_async_copy(source.at[first_mode(me) + n * k], pbuf.at[which, k], p_sem.at[which]).start()

    other_tables.start()

    def band_in(d):
        for which, source in enumerate((pf_hbm, pv_hbm)):
            pltpu.make_async_copy(
                source.at[top + first_mode(d), pl.ds(top, n)], band.at[which, d], band_sem.at[which]).start()

    loop(n, band_in)
    first_tables.wait()

    group = max(1, tl // 3)

    parts = degs // per
    depth = min(parts, work.shape[0] // (per * 2 * chans))

    def w_in(k):
        slot = lax.rem(k, depth)
        return pltpu.make_async_copy(
            w_hbm.at[pl.ds(k * per * 2 * chans, per * 2 * chans)],
            work.at[pl.ds(slot * per * 2 * chans, per * 2 * chans)], w_sem.at[slot])

    def step1_chunk(ch):
        slot = free_slot(0, ch)

        def row(t):
            unit = ch * tl + t
            step_in(f_hbm, unit)
            buf = lax.rem(unit, 2)
            for b in range(0, nb, 2):
                pair = jnp.concatenate([inbuf[buf, b], inbuf[buf, b + 1]], axis=1)
                spec = transform(pair, fwd_h, fwd_l)
                gather[pl.ds(b, modes2, stride=nb), :] = spec[:, :chans]
                gather[pl.ds(b + 1, modes2, stride=nb), :] = spec[:, chans:]
            put_rows(slot, t)

            @pl.when((ch == 0) & (t == group - 1))
            def _():
                pl.semaphore_wait(barrier, n - 1)
                ship(0, 0, 0, group)


        loop(tl, row)
        send_peak(0, ch)

        @pl.when(ch == 0)
        def _():
            ship(0, 0, group, tl - group)
            for k in range(depth):
                w_in(k).start()


    loop(chunks, step1_chunk)

    unit_in(dg_hbm, 0).start()
    for which in range(2):
        pltpu.make_async_copy(band.at[which], band.at[which], band_sem.at[which]).wait()
    qs[...] = jnp.zeros_like(qs)

    def pack(z, store):
        def one(index):
            half_at, row = lax.div(index, held), lax.rem(index, held)
            p = half_at * (held - 1) + row
            degree = jnp.where(core == 0, jnp.minimum(z + p, n - 1), jnp.maximum(p - 1, 0))
            store(half_at, row, degree, (p < n - z) == (core == 0))

        loop(2 * held, one)

    def project(which, ch, target, device):
        gather[...] = jnp.zeros_like(gather)
        side = 1 if target == 3 else -1

        def place_rows(apart):
            for c in range(2):
                src = across(side * apart, c)
                gather[pl.ds(pl.multiple_of(src * tl * tile, tile), tl * tile), :] = topin[
                    ch, target, 2 * apart + c].reshape(tl * tile, chans).astype(F32)

        place_rows(0)
        if target > 2:
            place_rows(1)

            @pl.when(core == target - 3)
            def _():
                place_rows(2)

        for k in range(tile):
            xb[:, k * chans:(k + 1) * chans] = gather[pl.ds(k, lats, stride=tile), :].astype(BF16)
        out = dot(band[which, device].astype(BF16), xb[...])
        for k in range(tile):
            qs[pl.ds(k, n, stride=tile), :] = out[:, k * chans:(k + 1) * chans]

    def sum_rows(which, ch):
        pltpu.make_async_copy(peaks(), peaks(), row_recv.at[ch]).wait()
        for target, away in enumerate((-1, 1, -2, 2)):
            project(which, ch, target + 1, across(away, core))

            def keep(half_at, row, degree, ours):
                values = qs[pl.ds(pl.multiple_of(degree * tile, tile), tile), :]
                partial[half_at, target, row] = jnp.where(ours, values, jnp.zeros_like(values))

            pack(chip_at(away), keep)
        swap = to(sibling, partial.at[other_core], mid.at[ch], mid_send.at[ch], mid_recv.at[ch])
        swap.start()
        if which == 1:
            pltpu.make_async_copy(sums.at[ch], sums.at[ch], sum_send.at[ch]).wait()
        swap.wait()
        sums[ch] = partial[core] + mid[ch]
        for side, away in enumerate((-1, 1)):
            to(across(away, core), sums.at[ch, 2 + side], handed.at[ch, side],
               sum_send.at[ch], hand_recv.at[ch]).start()

    def pass_sums(ch):
        pltpu.make_async_copy(handed.at[ch], handed.at[ch], hand_recv.at[ch]).wait()
        for side, away in enumerate((-1, 1)):
            sums[ch, side] += handed[ch, side]
            to(across(away, core), sums.at[ch, side], sumin.at[ch, side],
               sum_send.at[ch], sum_recv.at[ch]).start()

    def finish_peak(which, ch):
        pltpu.make_async_copy(sumin.at[ch], sumin.at[ch], sum_recv.at[ch]).wait()
        joined[ch, core] = sumin[ch, 0] + sumin[ch, 1]
        swap = to(sibling, joined.at[ch, core], joined.at[ch, core], join_send.at[ch], join_recv.at[ch])
        swap.start()
        project(which, ch, 0, me)
        swap.wait()

        def one(degree):
            p = jnp.where(core == 0, degree - chip, degree + 1)
            ours = degree >= first_mode(me)
            p = jnp.maximum(p, 0)
            h = jnp.where(p > held - 1, 1, 0)
            come = joined[ch, h, p - h * (held - 1)]
            work[pl.ds(area + (top + degree) * pitch + rows - tile, tile), :] = qs[
                pl.ds(pl.multiple_of(degree * tile, tile), tile), :] + jnp.where(ours, come, jnp.zeros_like(come))

        loop(n, one)

    sum_rows(0, 0)

    def ship_rows(ch):
        ship(0, ch, 0, tl)

    loop(final, ship_rows, 1)
    for which in range(2):
        pltpu.make_async_copy(pbuf.at[which], pbuf.at[which], p_sem.at[which]).wait()
    pmat[...] = pbuf[...].astype(BF16)
    other_tables.wait()

    def load_w(k):
        w_in(k).wait()
        base = lax.rem(k, depth) * per * 2 * chans
        for j in range(per):
            for part in range(2):
                vmix[k * per + j, pl.ds(part * chans, chans)] = work[
                    pl.ds(base + j * 2 * chans + part, chans, stride=2), :].astype(BF16)

        @pl.when(k + depth < parts)
        def _():
            w_in(k + depth).start()


    loop(parts, load_w)

    span = cmat.shape[3]
    mine_t = (lax.broadcasted_iota(jnp.int32, (8, lats), 1) == me * tl + lax.broadcasted_iota(jnp.int32, (8, lats), 0))
    mine_t &= lax.broadcasted_iota(jnp.int32, (8, lats), 0) < tl
    mine_t = jnp.where(mine_t, 1.0, 0.0).astype(BF16)

    def tabulate(d):
        z, of_core = lax.div(d, 2), lax.rem(d, 2)
        row = lax.broadcasted_iota(jnp.int32, (n, span), 0)
        p = jnp.where(of_core == 0, row - z, row + 1)
        target = jnp.where(p > held - 1, p + 1, p)
        moved = jnp.where(target == lax.broadcasted_iota(jnp.int32, (n, span), 1), 1.0, 0.0).astype(BF16)
        for which in range(2):
            picked = dot(mine_t, band[which, d].astype(BF16), ((1,), (1,))).astype(BF16)
            cmat[which, z, pl.ds(pl.multiple_of(of_core * 8, 8), 8), :] = dot(picked, moved)

    loop(n, tabulate)

    def no_degree(l):
        work[pl.ds(area + l * pitch + rows - tile, tile), :] = jnp.zeros((tile, chans), F32)

    loop(top, no_degree)

    pass_sums(0)

    def sum_first(ch):
        sum_rows(0, ch)

    loop(chunks, sum_first, 1)
    ship(0, final, 0, tl)
    loop(chunks, pass_sums, 1)

    sign = jnp.where(lax.broadcasted_iota(jnp.int32, (tile, chans), 0) < nb, -1.0, 1.0).astype(F32)

    def turn(values):
        groups = values.reshape(-1, tile, chans)
        return (pltpu.roll(groups, nb, 1) * sign[None]).reshape(values.shape)

    def legendre(src, dst, which, over):
        def mode(m):
            for k in range(tile):
                xb[:, k * chans:(k + 1) * chans] = work[
                    pl.ds(src + m * tile + k, lats, stride=pitch), :].astype(BF16)
            out = dot(pmat[which, m], xb[...], ((over,), (0,)))
            for k in range(tile):
                work[pl.ds(dst + m * tile + k, degs, stride=pitch), :] = out[:, k * chans:(k + 1) * chans]

        loop(ml - 1, mode)

    def unload(stage, ch):
        def body(src):
            for t in range(tl):
                work[pl.ds((src * tl + t) * pitch, rows), :] = recv[stage % 2, ch, src, t].astype(F32)

        loop(n, body)

    def load(slot):
        def body(dev):
            for t in range(tl):
                send[slot, dev, t] = work[pl.ds(area + (dev * tl + t) * pitch, rows), :].astype(BF16)

        loop(n, body)

    def only(ours, values):
        values = values.astype(F32)
        return jnp.where(ours, values, jnp.zeros_like(values)).astype(BF16)

    def spectral(stage, ch, into, kept, mix):
        arrived(stage - 1, ch)
        unload(stage - 1, ch)
        legendre(0, area, into, 1)
        finish_peak(into, ch)

        def degree(l):
            x = work[pl.ds(area + l * pitch, rows), :].astype(BF16)
            kept[l, ch] = x
            work[pl.ds(l * pitch, rows), :] = mix(l, x)

        loop(degs, degree, unroll=8)

        def keep_top(half_at, row, degree, ours):
            own[half_at, 2, ch, row] = only(ours, work[pl.ds((top + degree) * pitch + rows - tile, tile), :])

        pack(chip, keep_top)
        if stage == 1:
            swap = to(sibling, own.at[other_core, 2, ch], other.at[2, ch], swap_send.at[ch], swap_recv.at[ch])
            swap.start()
        legendre(0, area, 1 - into, 0)
        load(free_slot(stage, ch))
        if stage == 1:
            swap.wait()
            packs[core, chip, 2, ch] = (own[core, 2, ch].astype(F32) + other[2, ch].astype(F32)).astype(BF16)

            @pl.when(ch >= 2)
            def _():
                relay_top(ch - 2)

            for away in (2, -2):
                top_copy(0, away, ch, near_recv).start()
        else:
            @pl.when(ch == 0)
            def _():
                pass_sums(final - 1)
                sum_rows(1, final)

            @pl.when(ch == 1)
            def _():
                pass_sums(final)

        ship(stage, ch, 0, tl)

    def top_copy(source, away, ch, got):
        block = packs.at[core, chip_at(source), 2, ch]
        return to(across(away, core), block, block, top_send, got.at[ch])

    def top_blocks(count, ch):
        return packs.at[core, head(count), 2, ch]

    def relay_top(ch):
        pltpu.make_async_copy(top_blocks(2, ch), top_blocks(2, ch), near_recv.at[ch]).wait()
        for source in (2, -2):
            for away in (1, -1):
                top_copy(source, away, ch, far_recv).start()
        top_copy(-2 * way, 2 * way, ch, far_recv).start()

    def apply_top(which, ch, z):
        for h in range(2):
            qs[pl.ds(h * held * tile, held * tile), :] = packs[h, z, 2, ch].reshape(held * tile, chans).astype(F32)
        for k in range(tile):
            xb[0:span, k * chans:(k + 1) * chans] = qs[pl.ds(k, span, stride=tile), :].astype(BF16)
        out = dot(cmat[which, z].astype(BF16), xb[0:span, :])
        for k in range(tile):
            gather[pl.ds(k, 16, stride=tile), :] = out[:, k * chans:(k + 1) * chans]
        for c in range(2):
            for t in range(tl):
                recv[1, ch, 2 * z + c, t, pl.ds(rows - tile, tile)] = gather[
                    pl.ds((8 * c + t) * tile, tile), :].astype(BF16)

    def mix_forward(l, x):
        both = dot(x, vmix[l], ((1,), (1,)))
        return both[:, :chans] + turn(both[:, chans:])

    def mix_adjoint(l, x):
        both = dot(x, jnp.concatenate([vmix[l, head(chans)], vmix[l, pl.ds(chans, chans)]], axis=1))
        return both[:, :chans] - turn(both[:, chans:])

    def step2_chunk(ch):
        spectral(1, ch, 0, coef, mix_forward)

    loop(chunks, step2_chunk)
    relay_top(chunks - 2)

    def fetch_rows(stage, ch, t):
        for src in range(n):
            gather[pl.ds(src * rows, rows), :] = recv[stage % 2, ch, src, t].astype(F32)

    def fetch_pair(b):
        return jnp.concatenate(
            [gather[pl.ds(b, modes2, stride=nb), :], gather[pl.ds(b + 1, modes2, stride=nb), :]], axis=1).astype(BF16)

    def step3_chunk(ch):
        arrived(1, ch)
        pltpu.make_async_copy(top_blocks(5, ch), top_blocks(5, ch), far_recv.at[ch]).wait()
        swap = to(sibling, top_blocks(chips, ch), top_blocks(chips, ch), swap_send.at[ch], swap_recv.at[ch])
        swap.start()

        @pl.when(ch == 0)
        def _():
            relay_top(final)

        swap.wait()

        @pl.when(ch == final)
        def _():
            all_sent = packs.at[0, head(7), 2]
            pltpu.make_async_copy(all_sent, all_sent, top_send).wait()

        def apply(z):
            apply_top(1, ch, z)

        loop(chips, apply)

        @pl.when(ch == 1)
        def _():
            sum_rows(1, 0)

        slot = free_slot(2, ch)

        def row(t):
            unit = ch * tl + t
            step_in(dg_hbm, unit)
            buf = lax.rem(unit, 2)
            fetch_rows(1, ch, t)
            for b in range(0, nb, 2):
                g = fetch_pair(b)
                hidden = dot(syn_h[...], g) + dot(syn_l[...], g)
                pair = jnp.concatenate([inbuf[buf, b], inbuf[buf, b + 1]], axis=1)
                spec = transform(pair * gelu_grad(hidden), dbl_h, dbl_l)
                gather[pl.ds(b, modes2, stride=nb), :] = spec[:, :chans]
                gather[pl.ds(b + 1, modes2, stride=nb), :] = spec[:, chans:]
            put_rows(slot, t)

        loop(tl, row)
        send_peak(2, ch)

        @pl.when(ch < final)
        def _():
            ship(2, ch, 0, tl)


    loop(chunks, step3_chunk)

    def sum_second(ch):
        pass_sums(ch - 1)
        sum_rows(1, ch)

    loop(final, sum_second, 1)
    ship(2, final, 0, tl)
    unit_in(dg_hbm, 0).start()

    def step4_chunk(ch):
        spectral(3, ch, 1, dq, mix_adjoint)

    loop(chunks, step4_chunk)

    for which, kept in enumerate((coef, dq)):
        def keep_low(half_at, row, degree, ours):
            own[half_at, which, :, row] = only(ours, kept[degree, :, head(tile)])

        pack(chip, keep_low)

    def both_parts(peer, action):
        degree = n + peer
        for which, kept in enumerate((coef, dq)):
            action(to(peer, kept.at[degree, :, head(tile)], second.at[which, me, :, head(tile)],
                      always_send, always_recv))

            @pl.when(first_mode(me) <= peer)
            def _():
                more = pl.ds(tile, tile)
                action(to(peer, kept.at[degree, :, more], second.at[which, me, :, more],
                          some_send.at[peer], some_recv.at[me]))

    def send_second(k):
        both_parts(lax.rem(me + k, n), lambda copy: copy.start())

    loop(n, send_second, 1)
    for which, kept in enumerate((coef, dq)):
        second[which, me] = kept[n + me, :, head(2 * tile)]

    def clear_second(src):
        @pl.when(first_mode(src) > me)
        def _():
            for which in range(2):
                second[which, src, :, pl.ds(tile, tile)] = jnp.zeros((chunks, tile, chans), BF16)

    loop(n, clear_second)
    own_copy = to(sibling, own.at[other_core], other, own_send, own_recv)
    own_copy.start()

    def pack_block(k):
        return packs.at[core, chip_at(-way * k)]

    def pack_copy(k):
        return to(onward, pack_block(k), pack_block(k), pack_send, pack_recv.at[k])

    def share(k):
        to(sibling, pack_block(k), pack_block(k), share_send, share_recv).start()

    half = degs // n - 2
    wide = 2 * chans
    block_rows = half * wide
    piece = block_rows // pieces
    hops = (last) * pieces

    def block_at(k, direction):
        return lax.rem(chip - direction * (1 + k) + 2 * chips, chips)

    def outer(dst, row, pairs):
        real = jnp.zeros((chans, chans), F32)
        imag = jnp.zeros((chans, chans), F32)
        for y, x in pairs:
            real += dot(y, x, ((0,), (0,)))
            imag -= dot(turn(y.astype(F32)).astype(BF16), x, ((0,), (0,)))
        dst[pl.ds(row, chans, stride=2), :] = real
        dst[pl.ds(row + 1, chans, stride=2), :] = imag

    def first_degree(block, of_core):
        return 2 * n + (2 * block + of_core) * half

    def weight_grad(dst, degree):
        def one(j):
            outer(dst, j * wide, [(dq[degree + j, ch], coef[degree + j, ch]) for ch in range(chunks)])

        loop(half, one)

    def pair_copy(k):
        slot = lax.rem(k, 2)
        rows_there = pl.ds(first_degree(block_at(k, -way), core) * wide, block_rows)
        return to(sibling, wbuf.at[slot, head(block_rows)], dw_out.at[rows_there],
                  pair_send.at[slot], pair_recv.at[k])

    def weight_block(k):
        @pl.when(k >= 2)
        def _():
            pair_copy(k - 2).wait_send()
        weight_grad(wbuf.at[lax.rem(k, 2)], first_degree(block_at(k, -way), other_core))
        pair_copy(k).start()
        block = block_at(k, way)
        weight_grad(work.at[pl.ds(block * block_rows, block_rows)], first_degree(block, core))

    loop(chips, weight_block)
    pair_copy(chips - 2).wait_send()
    pair_copy(last).wait_send()
    own_copy.wait()
    packs[core, chip] = (own[core].astype(F32) + other[...].astype(F32)).astype(BF16)

    def low_degree(l):
        def one(z):
            for c in range(2):
                p = l - z if c == 0 else l + 1
                ours = p >= 0 if c == 0 else p >= n - z
                p = jnp.maximum(p, 0)
                h = jnp.where(p > held - 1, 1, 0)
                for which in range(2):
                    lowx[which, 2 * z + c] = only(ours, packs[h, z, which, :, p - h * (held - 1)])

        loop(chips, one)
        outer(wbuf.at[0], 0, [(lowx[1].reshape(-1, chans), lowx[0].reshape(-1, chans))])
        dw_out[pl.ds(l * wide, wide)] = wbuf[0, head(wide)]

    def final_rows(unit):
        ch, t = unit_of(unit)

        step_in(dg_hbm, unit)
        buf = lax.rem(unit, 2)

        fetch_rows(3, ch, t)
        for b in range(0, nb, 2):
            g = fetch_pair(b)
            change = dot(adj_h[...], g) + dot(adj_l[...], g)
            df_out[ch * nb + b, t] = inbuf[buf, b] + change[:, :chans]
            df_out[ch * nb + b + 1, t] = inbuf[buf, b + 1] + change[:, chans:]

    def place(i, of_core):
        block = block_at(lax.div(i, pieces), way)
        start = lax.rem(i, pieces) * piece
        return pl.ds(block * block_rows + start, piece), pl.ds(first_degree(block, of_core) * wide + start, piece)

    def rs_copy(i):
        here, there = place(i, core)
        return to(onward, work.at[here], dw_out.at[there], rs_send, rs_recv.at[i])

    def add_pair(i):
        here, passed = place(i, other_core)

        @pl.when(lax.rem(i, pieces) == 0)
        def _():
            pair_copy(lax.div(i, pieces)).wait_recv()

        work[here] += dw_out[passed]

    def rs_step(i):
        add_pair(i)

        @pl.when(i >= pieces)
        def _():
            rs_copy(i - pieces).wait_recv()
            here, there = place(i, core)
            work[here] += dw_out[there]

        rs_copy(i).start()

        @pl.when(lax.rem(i, pieces) == 0)
        def _():
            k = lax.div(i, pieces)

            @pl.when(k > 0)
            def _():
                pack_copy(k - 1).wait_recv()

            pack_copy(k).start()
            share(k)


    loop(hops, rs_step)
    pack_copy(chips - 2).wait_recv()
    share(last)

    def own_sum(s):
        i = hops + s
        add_pair(i)
        rs_copy(i - pieces).wait_recv()
        here, there = place(i, core)
        dw_out[there] += work[here]
        ag_copy(i, s).start()

    def second_spot(k):
        return pl.ds((n + 2 * block_at(k, way) + core) * wide, wide)

    def second_copy(k, got):
        spot = dw_out.at[second_spot(k)]
        return to(onward, spot, spot, ag_send, ag_recv.at[hops + got])

    def second_publish(k):
        spot = dw_out.at[second_spot(k)]
        to(sibling, spot, spot, pub_send, pub_recv).start()

    def ag_copy(i, got):
        _, there = place(i, core)
        return to(onward, dw_out.at[there], dw_out.at[there], ag_send, ag_recv.at[got])

    def publish(i):
        _, there = place(i, core)
        to(sibling, dw_out.at[there], dw_out.at[there], pub_send, pub_recv).start()

    firsts = second.at[:, head(n - 1), :, head(tile)]
    pltpu.make_async_copy(firsts, firsts, always_recv).wait()

    def wait_second(src):
        @pl.when((first_mode(src) <= me) & (src != me))
        def _():
            part = second.at[:, src, :, pl.ds(tile, tile)]
            pltpu.make_async_copy(part, part, some_recv.at[src]).wait()

    loop(n, wait_second)
    outer(wbuf.at[0], 0, [(second[1].reshape(-1, chans), second[0].reshape(-1, chans))])
    dw_out[second_spot(last)] = wbuf[0, head(wide)]
    loop(pieces, own_sum)
    second_copy(last, 0).start()

    pl.semaphore_signal(free_sem, inc=1, device_id={axis: sibling}, device_id_type=pl.DeviceIdType.MESH)
    pl.semaphore_wait(free_sem, 1)

    def own_piece(s):
        publish(hops + s)

    loop(pieces, own_piece)
    second_publish(last)
    gathered = packs.at[other_core]
    pltpu.make_async_copy(gathered, gathered, share_recv).wait()

    def task(i):
        @pl.when(i < chips)
        def _():
            for ch in range(chunks):
                @pl.when(i == 0)
                def _():
                    arrived(3, ch)
                apply_top(0, ch, i)

        @pl.when((i >= chips) & (i < chips + units))
        def _():
            final_rows(i - chips)

        @pl.when(i < n)
        def _():
            low_degree(i)

    def ag_step(i):
        ag_copy(i, i).wait_recv()

        @pl.when(i + pieces < hops)
        def _():
            ag_copy(i, i + pieces).start()

        publish(i)

        @pl.when(lax.rem(i, pieces) == pieces - 1)
        def _():
            k = lax.div(i, pieces)
            second_copy(k, k).wait_recv()

            @pl.when(k < chips - 2)
            def _():
                second_copy(k, k + 1).start()

            second_publish(k)

        task(i)

    loop(hops, ag_step)

    def rest(i):
        task(i)

    loop(max(hops, chips + units, n), rest, hops)

    wait_sent(2 * chunks + final, 2)
    for ch in range(chunks):
        wait_sent(3 * chunks + ch, 3)
    for ch in range(chunks):
        pltpu.make_async_copy(sums.at[ch], sums.at[ch], sum_send.at[ch]).wait()
    sent = work.at[head((last) * block_rows)]
    pltpu.make_async_copy(sent, sent, rs_send).wait()
    sent = dw_out.at[head((last) * (block_rows + wide))]
    pltpu.make_async_copy(sent, sent, ag_send).wait()
    pltpu.make_async_copy(firsts, firsts, always_send).wait()

    def wait_some(peer):
        @pl.when((first_mode(me) <= peer) & (peer != me))
        def _():
            part = second.at[:, peer, :, pl.ds(tile, tile)]
            pltpu.make_async_copy(part, part, some_send.at[peer]).wait()

    loop(n, wait_some)
    sent = packs.at[0, head(last)]
    pltpu.make_async_copy(sent, sent, pack_send).wait()
    pltpu.make_async_copy(packs.at[0], packs.at[0], share_send).wait()
    shared = dw_out.at[head(chips * (block_rows + wide))]
    pltpu.make_async_copy(shared, shared, pub_send).wait()
    pltpu.make_async_copy(shared, shared, pub_recv).wait()


def put_kernel(df_ref, dw_ref, df_hbm, dw_hbm, sems):
    copies = []
    for source, target, parts in ((df_ref, df_hbm, 6), (dw_ref, dw_hbm, 12)):
        size = source.shape[0] // parts
        for k in range(parts):
            part = pl.ds(k * size, size)
            copies.append(pltpu.make_async_copy(source.at[part], target.at[part], sems.at[len(copies)]))
    for copy in copies:
        copy.start()
    for copy in copies:
        copy.wait()


def solution(mesh):
    n = mesh.shape['lat']
    field_spec = P('member', None, 'lat', None)

    def local_step(field_loc, grad_loc, p_fwd, p_inv, w_mix):
        batch, chans, tl, lons = field_loc.shape
        degs, lats = p_fwd.shape[1:]
        ml = p_fwd.shape[0] // n
        nb = 4
        chunks = batch // nb
        rows = ml * 2 * nb
        pitch = rows + 1
        half = degs // n - 2
        pieces = 4 if half * 2 * chans % 32 == 0 else 1
        hops = (n // 2 - 1) * pieces
        per = 4
        held = n // 2 + 1
        packed = (3, chunks, held, 2 * nb, chans)
        tables = fourier_tables(n, ml, lons)
        anywhere = pl.BlockSpec(memory_space=pl.ANY)
        vmem = pl.BlockSpec(memory_space=pltpu.VMEM)
        grad_field, grad_w = pl.pallas_call(
            functools.partial(layer_kernel, 'lat', n, nb, pieces, per),
            name='layer',
            out_shape=(
                pltpu.VMEM((batch, tl, lons, chans), F32),
                pltpu.VMEM((degs * 2 * chans, chans), F32),
            ),
            in_specs=[anywhere] * 6,
            out_specs=(vmem, vmem),
            scratch_shapes=[
                pltpu.VMEM((2, chunks, n, tl, rows, chans), BF16),
                pltpu.VMEM((chunks + 1, n, tl, rows, chans), BF16),
                pltpu.VMEM((max(2 * lats * pitch, n // 2 * half * 2 * chans), chans), F32),
                pltpu.VMEM((lats, 2 * nb * chans), BF16),
                pltpu.VMEM((degs, chunks, rows, chans), BF16),
                pltpu.VMEM((degs, chunks, rows, chans), BF16),
                pltpu.VMEM((degs, 2 * chans, chans), BF16),
                pltpu.VMEM((2, max(per, half) * 2 * chans, chans), F32),
                pltpu.VMEM((2, nb, lons, chans), F32),
                pltpu.VMEM((n * rows, chans), F32),
                pltpu.VMEM((2, ml, degs, lats), F32),
                pltpu.VMEM((2, ml, degs, lats), BF16),
                pltpu.VMEM((2, n, n, lats), F32),
                pltpu.VMEM((2, n // 2, 16, 32), F32),
                pltpu.VMEM((32 * 2 * nb, chans), F32),
                pltpu.VMEM((2,) + packed, BF16),
                pltpu.VMEM(packed, BF16),
                pltpu.VMEM((2, n // 2) + packed, BF16),
                pltpu.VMEM((2, n, chunks, 2 * nb, chans), BF16),
                pltpu.VMEM(tables.shape, BF16),
                pltpu.VMEM((chunks, 5, 6, tl, 2 * nb, chans), BF16),
                pltpu.VMEM((2, 4, held, 2 * nb, chans), F32),
                pltpu.VMEM((chunks, 4, held, 2 * nb, chans), F32),
                pltpu.VMEM((chunks, 4, held, 2 * nb, chans), F32),
                pltpu.VMEM((chunks, 2, held, 2 * nb, chans), F32),
                pltpu.VMEM((chunks, 2, held, 2 * nb, chans), F32),
                pltpu.VMEM((chunks, 2, held, 2 * nb, chans), F32),
                pltpu.VMEM((2, n, chunks, 4 * nb, chans), BF16),
                pltpu.SemaphoreType.DMA((4 * chunks,)),
                pltpu.SemaphoreType.DMA((4 * chunks,)),
                pltpu.SemaphoreType.DMA((2,)),
                pltpu.SemaphoreType.DMA((degs // per,)),
                pltpu.SemaphoreType.DMA((2,)),
                pltpu.SemaphoreType.DMA((2,)),
                pltpu.SemaphoreType.DMA((2,)),
                pltpu.SemaphoreType.DMA((n // 2,)),
                pltpu.SemaphoreType.DMA,
                pltpu.SemaphoreType.DMA((hops,)),
                pltpu.SemaphoreType.DMA,
                pltpu.SemaphoreType.DMA((hops + n // 2 - 1,)),
                pltpu.SemaphoreType.REGULAR,
                pltpu.SemaphoreType.DMA,
                pltpu.SemaphoreType.DMA,
                pltpu.SemaphoreType.DMA,
                pltpu.SemaphoreType.DMA,
                pltpu.SemaphoreType.DMA,
                pltpu.SemaphoreType.DMA((n // 2 - 1,)),
                pltpu.SemaphoreType.DMA,
                pltpu.SemaphoreType.DMA,
                pltpu.SemaphoreType.DMA((2,)),
                pltpu.SemaphoreType.DMA,
                pltpu.SemaphoreType.DMA((chunks,)),
                pltpu.SemaphoreType.DMA((chunks,)),
                pltpu.SemaphoreType.DMA((chunks,)),
                pltpu.SemaphoreType.DMA((chunks,)),
                pltpu.SemaphoreType.DMA((chunks,)),
                pltpu.SemaphoreType.DMA((chunks,)),
                pltpu.SemaphoreType.DMA((chunks,)),
                pltpu.SemaphoreType.DMA((chunks,)),
                pltpu.SemaphoreType.DMA((chunks,)),
                pltpu.SemaphoreType.DMA((chunks,)),
                pltpu.SemaphoreType.DMA((chunks,)),
                pltpu.SemaphoreType.DMA((chunks,)),
                pltpu.SemaphoreType.DMA,
                pltpu.SemaphoreType.DMA,
                pltpu.SemaphoreType.DMA((n,)),
                pltpu.SemaphoreType.DMA((n,)),
                pltpu.SemaphoreType.DMA((chunks,)),
            ],
            compiler_params=pltpu.CompilerParams(
                collective_id=0, has_side_effects=True, vmem_limit_bytes=43 * 1024 * 1024),
        )(
            field_loc.transpose(0, 2, 3, 1), grad_loc.transpose(0, 2, 3, 1),
            w_mix.transpose(0, 1, 3, 2).reshape(degs * 2 * chans, chans),
            p_fwd, p_inv, tables)
        grad_field, grad_w = pl.pallas_call(
            put_kernel,
            name='put',
            out_shape=(
                jax.ShapeDtypeStruct(grad_field.shape, F32),
                jax.ShapeDtypeStruct(grad_w.shape, F32),
            ),
            in_specs=[vmem] * 2,
            out_specs=(anywhere, anywhere),
            scratch_shapes=[pltpu.SemaphoreType.DMA((18,))],
            compiler_params=pltpu.CompilerParams(vmem_limit_bytes=1024 * 1024),
        )(grad_field, grad_w)
        return grad_field.transpose(0, 3, 1, 2), grad_w.reshape(degs, chans, 2, chans).transpose(0, 1, 3, 2)

    return jax.shard_map(
        local_step, mesh=mesh, in_specs=(field_spec, field_spec, P(), P(), P()),
        out_specs=(field_spec, P('member', None, None, None)), check_vma=False)
```

```python
import functools
import math

import jax
import jax.numpy as jnp
import numpy as np
from jax import lax
from jax.experimental import pallas as pl
from jax.experimental.pallas import tpu as pltpu
from jax.sharding import PartitionSpec as P

F32 = jnp.float32
BF16 = jnp.bfloat16


def split_const(matrix):
    head = matrix.astype(BF16)
    tail = (matrix - head.astype(np.float64)).astype(BF16)
    return [head, tail]


def fourier_tables(n, ml, lons):
    modes = n * ml
    device = np.arange(n)
    first = np.where(device % 2 == 0, device // 2, n - 1 - device // 2)
    order = (first[:, None] + n * np.arange(ml)[None, :]).reshape(-1)
    angle = 2.0 * np.pi * (np.outer(order, np.arange(lons)) % lons) / lons
    forward = np.stack([np.cos(angle), -np.sin(angle)], axis=1).reshape(2 * modes, lons) / math.sqrt(lons)
    gains = np.repeat(np.where(order == 0, 1.0, 2.0), 2)[:, None]
    doubled = forward * gains
    tables = split_const(forward) + split_const(doubled) + split_const(doubled.T) + split_const(forward.T)
    return jnp.stack([jnp.asarray(t) for t in tables])


def gelu_grad(values):
    cumulative = 0.5 * (1.0 + lax.erf(values * math.sqrt(0.5)))
    density = jnp.exp(-0.5 * values * values) / math.sqrt(2.0 * math.pi)
    return cumulative + values * density


def loop(stop, step, start=0, unroll=None):
    def one(i, carry):
        step(i)
        return carry

    lax.fori_loop(start, stop, one, 0, unroll=unroll)


def head(size):
    return pl.ds(0, size)


def dot(a, b, dims=((1,), (0,))):
    return lax.dot_general(a, b, (dims, ((), ())), preferred_element_type=F32)


def layer_kernel(
    axis, n, nb, pieces, per, depth,
    f_hbm, dg_hbm, w_hbm, pf_hbm, pv_hbm, tab_hbm,
    df_out, dw_out,
    recv, send, work, xb, coef, dq, vmix, wbuf, inbuf, gather, pbuf, pmat, band, cmat, qs, own, other, packs, lowx, tab,
    topin, partial, mid, sums, sumin, joined, handed, second,
    send_sem, recv_sem, in_sem, w_sem, p_sem, band_sem, pair_send, pair_recv, rs_send, rs_recv, ag_send, ag_recv,
    free_sem, pub_send, pub_recv, own_send, own_recv, pack_send, pack_recv, share_send, share_recv,
    tab_sem, top_send, near_recv, far_recv, swap_send, swap_recv,
    row_send, row_recv, mid_send, mid_recv, sum_send, sum_recv, join_send, join_recv,
    always_send, always_recv, some_send, some_recv, hand_recv,
):
    me = lax.axis_index(axis)
    batch, tl, lons, chans = f_hbm.shape
    ml, degs, lats = pmat.shape[1:]
    chunks = batch // nb
    tile = 2 * nb
    rows = ml * tile
    pitch = rows + 1
    modes2 = 2 * n * ml
    units = chunks * tl
    final = chunks - 1
    slots = chunks + 1
    fwd_h, fwd_l, dbl_h, dbl_l, syn_h, syn_l, adj_h, adj_l = (tab.at[k] for k in range(8))
    area = lats * pitch
    top = n * (ml - 1)
    held = n // 2 + 1
    chip, core = lax.div(me, 2), lax.rem(me, 2)
    other_core = 1 - core
    chips = n // 2
    last = chips - 1
    way = 1 - 2 * core
    sibling = me + way

    def chip_at(away):
        return lax.rem(chip + away + chips, chips)

    def across(away, its_core):
        return 2 * chip_at(away) + its_core

    onward = across(way, core)

    def first_mode(device):
        z = lax.div(device, 2)
        return jnp.where(lax.rem(device, 2) == 0, z, n - 1 - z)

    def to(device, src, dst, sent, got):
        return pltpu.make_async_remote_copy(
            src_ref=src, dst_ref=dst, send_sem=sent, recv_sem=got,
            device_id={axis: device}, device_id_type=pl.DeviceIdType.MESH)

    def unit_of(unit):
        return lax.div(unit, tl), lax.rem(unit, tl)

    def unit_in(src, unit):
        ch, t = unit_of(unit)
        slot = lax.rem(unit, 2)
        return pltpu.make_async_copy(src.at[pl.ds(ch * nb, nb), t], inbuf.at[slot], in_sem.at[slot])

    def step_in(src, unit):
        @pl.when(unit + 1 < units)
        def _():
            unit_in(src, unit + 1).start()
        unit_in(src, unit).wait()

    body, peak = head(rows - tile), pl.ds(rows - tile, tile)

    def ship(stage, ch, t0, nt):
        index = stage * chunks + ch
        slot = lax.rem(index, slots)
        part = pl.ds(t0, nt)

        def one(k):
            peer = lax.rem(me + k, n)
            to(peer, send.at[slot, peer, part, body], recv.at[stage % 2, ch, me, part, body],
               send_sem.at[index], recv_sem.at[index]).start()

        loop(n, one, 1)
        recv[stage % 2, ch, me, part, body] = send[slot, me, part, body]

    def arrived(stage, ch):
        others = recv.at[stage % 2, ch, head(n - 1), :, body]
        pltpu.make_async_copy(others, others, recv_sem.at[stage * chunks + ch]).wait()

    def peaks():
        return send.at[0, head(n - 5), :, peak]

    def wait_sent(index, stage):
        others = send.at[lax.rem(index, slots), head(n - 1), :, body]
        pltpu.make_async_copy(others, others, send_sem.at[index]).wait()
        if stage % 2 == 0:
            ch = index - stage * chunks
            pltpu.make_async_copy(peaks(), peaks(), row_send.at[ch]).wait()

    def send_peak(stage, ch):
        slot = lax.rem(stage * chunks + ch, slots)
        far = chips // 2
        for same in (True, False):
            its_core = core if same else other_core
            for away in range(1 - far, far + 1):
                near = max(-2, min(2, away))
                hop, target, apart = away - near, (0, 2, 4, 3, 1)[near], abs(away - near)
                if away == far:
                    hop = jnp.where(its_core == 0, 2 - far, far - 2)
                    target = jnp.where(its_core == 0, 3, 4)
                source = send.at[slot, across(away, its_core), :, peak]
                place = topin.at[ch, target, 2 * apart + core]
                if same and not apart:
                    place[...] = source[...]
                else:
                    to(across(hop, its_core), source, place,
                       row_send.at[ch], row_recv.at[ch]).start()

    def free_slot(stage, ch):
        index = stage * chunks + ch
        if stage >= 1:
            @pl.when(ch >= 1)
            def _():
                wait_sent(index - slots, stage - 1)
        if stage >= 2:
            @pl.when(ch == 0)
            def _():
                wait_sent(index - slots, stage - 2)
        return lax.rem(index, slots)

    def put_rows(slot, t):
        send[slot, :, t] = gather[...].reshape(n, rows, chans).astype(BF16)

    def transform(values, head, tail):
        high = values.astype(BF16)
        low = (values - high.astype(F32)).astype(BF16)
        return dot(head[...], high) + (dot(tail[...], high) + dot(head[...], low))

    unit_in(f_hbm, 0).start()
    first_tables = pltpu.make_async_copy(tab_hbm.at[head(2)], tab.at[head(2)], tab_sem.at[0])
    other_tables = pltpu.make_async_copy(tab_hbm.at[pl.ds(2, 6)], tab.at[pl.ds(2, 6)], tab_sem.at[1])
    first_tables.start()
    barrier = pltpu.get_barrier_semaphore()

    def announce(k):
        pl.semaphore_signal(barrier, inc=1, device_id={axis: lax.rem(me + k, n)}, device_id_type=pl.DeviceIdType.MESH)

    loop(n, announce, 1)

    first_tables.wait()

    group = max(1, tl // 3)

    parts = degs // per

    def w_in(k):
        slot = lax.rem(k, depth)
        return pltpu.make_async_copy(
            w_hbm.at[pl.ds(k * per * 2 * chans, per * 2 * chans)],
            work.at[pl.ds(slot * per * 2 * chans, per * 2 * chans)], w_sem.at[slot])

    def band_in(d):
        for which, source in enumerate((pf_hbm, pv_hbm)):
            pltpu.make_async_copy(
                source.at[top + first_mode(d), pl.ds(top, n)], band.at[which, d], band_sem.at[which]).start()

    def step1_chunk(ch):
        slot = free_slot(0, ch)

        def row(t):
            unit = ch * tl + t
            step_in(f_hbm, unit)
            buf = lax.rem(unit, 2)
            for b in range(0, nb, 2):
                pair = jnp.concatenate([inbuf[buf, b], inbuf[buf, b + 1]], axis=1)
                spec = transform(pair, fwd_h, fwd_l)
                gather[pl.ds(b, modes2, stride=nb), :] = spec[:, :chans]
                gather[pl.ds(b + 1, modes2, stride=nb), :] = spec[:, chans:]
            put_rows(slot, t)

            @pl.when((ch == 0) & (t == group - 1))
            def _():
                pl.semaphore_wait(barrier, n - 1)
                ship(0, 0, 0, group)


        loop(tl, row)
        send_peak(0, ch)

        @pl.when(ch == 0)
        def _():
            ship(0, 0, group, tl - group)
            other_tables.start()
            for which, source in enumerate((pf_hbm, pv_hbm)):
                for k in range(ml):
                    pltpu.make_async_copy(
                        source.at[first_mode(me) + n * k], pbuf.at[which, k], p_sem.at[which]).start()
            loop(n, band_in)
            for k in range(depth):
                w_in(k).start()


    loop(chunks, step1_chunk)

    unit_in(dg_hbm, 0).start()
    for which in range(2):
        pltpu.make_async_copy(band.at[which], band.at[which], band_sem.at[which]).wait()
    qs[...] = jnp.zeros_like(qs)

    def pack(z, store):
        def one(index):
            half_at, row = lax.div(index, held), lax.rem(index, held)
            p = half_at * (held - 1) + row
            degree = jnp.where(core == 0, jnp.minimum(z + p, n - 1), jnp.maximum(p - 1, 0))
            store(half_at, row, degree, (p < n - z) == (core == 0))

        loop(2 * held, one)

    def project(which, ch, target, device):
        gather[...] = jnp.zeros_like(gather)
        side = 1 if target == 3 else -1

        def place_rows(apart):
            for c in range(2):
                src = across(side * apart, c)
                gather[pl.ds(pl.multiple_of(src * tl * tile, tile), tl * tile), :] = topin[
                    ch, target, 2 * apart + c].reshape(tl * tile, chans).astype(F32)

        place_rows(0)
        if target > 2:
            place_rows(1)

            @pl.when(core == target - 3)
            def _():
                place_rows(2)

        for k in range(tile):
            xb[:, k * chans:(k + 1) * chans] = gather[pl.ds(k, lats, stride=tile), :].astype(BF16)
        out = dot(band[which, device].astype(BF16), xb[...])
        for k in range(tile):
            qs[pl.ds(k, n, stride=tile), :] = out[:, k * chans:(k + 1) * chans]

    def sum_rows(which, ch):
        pltpu.make_async_copy(peaks(), peaks(), row_recv.at[ch]).wait()
        for target, away in enumerate((-1, 1, -2, 2)):
            project(which, ch, target + 1, across(away, core))

            def keep(half_at, row, degree, ours):
                values = qs[pl.ds(pl.multiple_of(degree * tile, tile), tile), :]
                partial[half_at, target, row] = jnp.where(ours, values, jnp.zeros_like(values))

            pack(chip_at(away), keep)
        swap = to(sibling, partial.at[other_core], mid.at[ch], mid_send.at[ch], mid_recv.at[ch])
        swap.start()
        if which == 1:
            pltpu.make_async_copy(sums.at[ch], sums.at[ch], sum_send.at[ch]).wait()
        swap.wait()
        sums[ch] = partial[core] + mid[ch]
        for side, away in enumerate((-1, 1)):
            to(across(away, core), sums.at[ch, 2 + side], handed.at[ch, side],
               sum_send.at[ch], hand_recv.at[ch]).start()

    def pass_sums(ch):
        pltpu.make_async_copy(handed.at[ch], handed.at[ch], hand_recv.at[ch]).wait()
        for side, away in enumerate((-1, 1)):
            sums[ch, side] += handed[ch, side]
            to(across(away, core), sums.at[ch, side], sumin.at[ch, side],
               sum_send.at[ch], sum_recv.at[ch]).start()

    def finish_peak(which, ch):
        pltpu.make_async_copy(sumin.at[ch], sumin.at[ch], sum_recv.at[ch]).wait()
        joined[ch, core] = sumin[ch, 0] + sumin[ch, 1]
        swap = to(sibling, joined.at[ch, core], joined.at[ch, core], join_send.at[ch], join_recv.at[ch])
        swap.start()
        project(which, ch, 0, me)
        swap.wait()

        def one(degree):
            p = jnp.where(core == 0, degree - chip, degree + 1)
            ours = degree >= first_mode(me)
            p = jnp.maximum(p, 0)
            h = jnp.where(p > held - 1, 1, 0)
            come = joined[ch, h, p - h * (held - 1)]
            work[pl.ds(area + (top + degree) * pitch + rows - tile, tile), :] = qs[
                pl.ds(pl.multiple_of(degree * tile, tile), tile), :] + jnp.where(ours, come, jnp.zeros_like(come))

        loop(n, one)

    sum_rows(0, 0)

    def ship_rows(ch):
        ship(0, ch, 0, tl)

    loop(final, ship_rows, 1)
    for which in range(2):
        pltpu.make_async_copy(pbuf.at[which], pbuf.at[which], p_sem.at[which]).wait()
    pmat[...] = pbuf[...].astype(BF16)
    other_tables.wait()

    def load_w(k):
        w_in(k).wait()
        base = lax.rem(k, depth) * per * 2 * chans
        for j in range(per):
            for part in range(2):
                vmix[k * per + j, pl.ds(part * chans, chans)] = work[
                    pl.ds(base + j * 2 * chans + part, chans, stride=2), :].astype(BF16)

        @pl.when(k + depth < parts)
        def _():
            w_in(k + depth).start()


    loop(parts, load_w)

    span = cmat.shape[3]
    mine_t = (lax.broadcasted_iota(jnp.int32, (8, lats), 1) == me * tl + lax.broadcasted_iota(jnp.int32, (8, lats), 0))
    mine_t &= lax.broadcasted_iota(jnp.int32, (8, lats), 0) < tl
    mine_t = jnp.where(mine_t, 1.0, 0.0).astype(BF16)

    def tabulate(d):
        z, of_core = lax.div(d, 2), lax.rem(d, 2)
        row = lax.broadcasted_iota(jnp.int32, (n, span), 0)
        p = jnp.where(of_core == 0, row - z, row + 1)
        target = jnp.where(p > held - 1, p + 1, p)
        moved = jnp.where(target == lax.broadcasted_iota(jnp.int32, (n, span), 1), 1.0, 0.0).astype(BF16)
        for which in range(2):
            picked = dot(mine_t, band[which, d].astype(BF16), ((1,), (1,))).astype(BF16)
            cmat[which, z, pl.ds(pl.multiple_of(of_core * 8, 8), 8), :] = dot(picked, moved)

    loop(n, tabulate)

    def no_degree(l):
        work[pl.ds(area + l * pitch + rows - tile, tile), :] = jnp.zeros((tile, chans), F32)

    loop(top, no_degree)

    pass_sums(0)

    def sum_first(ch):
        sum_rows(0, ch)

    loop(chunks, sum_first, 1)
    ship(0, final, 0, tl)
    loop(chunks, pass_sums, 1)

    sign = jnp.where(lax.broadcasted_iota(jnp.int32, (tile, chans), 0) < nb, -1.0, 1.0).astype(F32)

    def turn(values):
        groups = values.reshape(-1, tile, chans)
        return (pltpu.roll(groups, nb, 1) * sign[None]).reshape(values.shape)

    def legendre(src, dst, which, over):
        def mode(m):
            for k in range(tile):
                xb[:, k * chans:(k + 1) * chans] = work[
                    pl.ds(src + m * tile + k, lats, stride=pitch), :].astype(BF16)
            out = dot(pmat[which, m], xb[...], ((over,), (0,)))
            for k in range(tile):
                work[pl.ds(dst + m * tile + k, degs, stride=pitch), :] = out[:, k * chans:(k + 1) * chans]

        loop(ml - 1, mode)

    def unload(stage, ch):
        def body(src):
            for t in range(tl):
                work[pl.ds((src * tl + t) * pitch, rows), :] = recv[stage % 2, ch, src, t].astype(F32)

        loop(n, body)

    def load(slot):
        def body(dev):
            for t in range(tl):
                send[slot, dev, t] = work[pl.ds(area + (dev * tl + t) * pitch, rows), :].astype(BF16)

        loop(n, body)

    def only(ours, values):
        values = values.astype(F32)
        return jnp.where(ours, values, jnp.zeros_like(values)).astype(BF16)

    def spectral(stage, ch, into, kept, mix):
        arrived(stage - 1, ch)
        unload(stage - 1, ch)
        legendre(0, area, into, 1)
        finish_peak(into, ch)

        def degree(l):
            x = work[pl.ds(area + l * pitch, rows), :].astype(BF16)
            kept[l, ch] = x
            work[pl.ds(l * pitch, rows), :] = mix(l, x)

        loop(degs, degree, unroll=8)

        def keep_top(half_at, row, degree, ours):
            own[half_at, 2, ch, row] = only(ours, work[pl.ds((top + degree) * pitch + rows - tile, tile), :])

        pack(chip, keep_top)
        if stage == 1:
            swap = to(sibling, own.at[other_core, 2, ch], other.at[2, ch], swap_send.at[ch], swap_recv.at[ch])
            swap.start()
        legendre(0, area, 1 - into, 0)
        load(free_slot(stage, ch))
        if stage == 1:
            swap.wait()
            packs[core, chip, 2, ch] = (own[core, 2, ch].astype(F32) + other[2, ch].astype(F32)).astype(BF16)

            @pl.when(ch >= 2)
            def _():
                relay_top(ch - 2)

            for away in (2, -2):
                top_copy(0, away, ch, near_recv).start()
        else:
            @pl.when(ch == 0)
            def _():
                pass_sums(final - 1)
                sum_rows(1, final)

            @pl.when(ch == 1)
            def _():
                pass_sums(final)

        ship(stage, ch, 0, tl)

    def top_copy(source, away, ch, got):
        block = packs.at[core, chip_at(source), 2, ch]
        return to(across(away, core), block, block, top_send, got.at[ch])

    def top_blocks(count, ch):
        return packs.at[core, head(count), 2, ch]

    def relay_top(ch):
        pltpu.make_async_copy(top_blocks(2, ch), top_blocks(2, ch), near_recv.at[ch]).wait()
        for source in (2, -2):
            for away in (1, -1):
                top_copy(source, away, ch, far_recv).start()
        top_copy(-2 * way, 2 * way, ch, far_recv).start()

    def apply_top(which, ch, z):
        for h in range(2):
            qs[pl.ds(h * held * tile, held * tile), :] = packs[h, z, 2, ch].reshape(held * tile, chans).astype(F32)
        for k in range(tile):
            xb[0:span, k * chans:(k + 1) * chans] = qs[pl.ds(k, span, stride=tile), :].astype(BF16)
        out = dot(cmat[which, z].astype(BF16), xb[0:span, :])
        for k in range(tile):
            gather[pl.ds(k, 16, stride=tile), :] = out[:, k * chans:(k + 1) * chans]
        for c in range(2):
            for t in range(tl):
                recv[1, ch, 2 * z + c, t, pl.ds(rows - tile, tile)] = gather[
                    pl.ds((8 * c + t) * tile, tile), :].astype(BF16)

    def mix_forward(l, x):
        both = dot(x, vmix[l], ((1,), (1,)))
        return both[:, :chans] + turn(both[:, chans:])

    def mix_adjoint(l, x):
        both = dot(x, jnp.concatenate([vmix[l, head(chans)], vmix[l, pl.ds(chans, chans)]], axis=1))
        return both[:, :chans] - turn(both[:, chans:])

    def step2_chunk(ch):
        spectral(1, ch, 0, coef, mix_forward)

    loop(chunks, step2_chunk)
    relay_top(chunks - 2)

    def fetch_rows(stage, ch, t):
        for src in range(n):
            gather[pl.ds(src * rows, rows), :] = recv[stage % 2, ch, src, t].astype(F32)

    def fetch_pair(b):
        return jnp.concatenate(
            [gather[pl.ds(b, modes2, stride=nb), :], gather[pl.ds(b + 1, modes2, stride=nb), :]], axis=1).astype(BF16)

    def step3_chunk(ch):
        arrived(1, ch)
        pltpu.make_async_copy(top_blocks(5, ch), top_blocks(5, ch), far_recv.at[ch]).wait()
        swap = to(sibling, top_blocks(chips, ch), top_blocks(chips, ch), swap_send.at[ch], swap_recv.at[ch])
        swap.start()

        @pl.when(ch == 0)
        def _():
            relay_top(final)

        swap.wait()

        @pl.when(ch == final)
        def _():
            all_sent = packs.at[0, head(7), 2]
            pltpu.make_async_copy(all_sent, all_sent, top_send).wait()

        def apply(z):
            apply_top(1, ch, z)

        loop(chips, apply)

        @pl.when(ch == 1)
        def _():
            sum_rows(1, 0)

        slot = free_slot(2, ch)

        def row(t):
            unit = ch * tl + t
            step_in(dg_hbm, unit)
            buf = lax.rem(unit, 2)
            fetch_rows(1, ch, t)
            for b in range(0, nb, 2):
                g = fetch_pair(b)
                hidden = dot(syn_h[...], g) + dot(syn_l[...], g)
                pair = jnp.concatenate([inbuf[buf, b], inbuf[buf, b + 1]], axis=1)
                spec = transform(pair * gelu_grad(hidden), dbl_h, dbl_l)
                gather[pl.ds(b, modes2, stride=nb), :] = spec[:, :chans]
                gather[pl.ds(b + 1, modes2, stride=nb), :] = spec[:, chans:]
            put_rows(slot, t)

        loop(tl, row)
        send_peak(2, ch)

        @pl.when(ch < final)
        def _():
            ship(2, ch, 0, tl)


    loop(chunks, step3_chunk)

    def sum_second(ch):
        pass_sums(ch - 1)
        sum_rows(1, ch)

    loop(final, sum_second, 1)
    ship(2, final, 0, tl)
    unit_in(dg_hbm, 0).start()

    def step4_chunk(ch):
        spectral(3, ch, 1, dq, mix_adjoint)

    loop(chunks, step4_chunk)

    for which, kept in enumerate((coef, dq)):
        def keep_low(half_at, row, degree, ours):
            own[half_at, which, :, row] = only(ours, kept[degree, :, head(tile)])

        pack(chip, keep_low)

    def both_parts(peer, action):
        degree = n + peer
        for which, kept in enumerate((coef, dq)):
            action(to(peer, kept.at[degree, :, head(tile)], second.at[which, me, :, head(tile)],
                      always_send, always_recv))

            @pl.when(first_mode(me) <= peer)
            def _():
                more = pl.ds(tile, tile)
                action(to(peer, kept.at[degree, :, more], second.at[which, me, :, more],
                          some_send, some_recv))

    def send_second(k):
        both_parts(lax.rem(me + k, n), lambda copy: copy.start())

    loop(n, send_second, 1)
    for which, kept in enumerate((coef, dq)):
        second[which, me] = kept[n + me, :, head(2 * tile)]

    def clear_second(src):
        @pl.when(first_mode(src) > me)
        def _():
            for which in range(2):
                second[which, src, :, pl.ds(tile, tile)] = jnp.zeros((chunks, tile, chans), BF16)

    loop(n, clear_second)
    own_copy = to(sibling, own.at[other_core], other, own_send, own_recv)
    own_copy.start()

    def pack_block(k):
        return packs.at[core, chip_at(-way * k)]

    def pack_copy(k):
        return to(onward, pack_block(k), pack_block(k), pack_send, pack_recv.at[k])

    def share(k):
        to(sibling, pack_block(k), pack_block(k), share_send, share_recv).start()

    half = degs // n - 2
    wide = 2 * chans
    block_rows = half * wide
    piece = block_rows // pieces
    hops = (last) * pieces

    def block_at(k, direction):
        return lax.rem(chip - direction * (1 + k) + 2 * chips, chips)

    def outer(dst, row, pairs):
        real = jnp.zeros((chans, chans), F32)
        imag = jnp.zeros((chans, chans), F32)
        for y, x in pairs:
            real += dot(y, x, ((0,), (0,)))
            imag -= dot(turn(y.astype(F32)).astype(BF16), x, ((0,), (0,)))
        dst[pl.ds(row, chans, stride=2), :] = real
        dst[pl.ds(row + 1, chans, stride=2), :] = imag

    def first_degree(block, of_core):
        return 2 * n + (2 * block + of_core) * half

    def weight_grad(dst, degree):
        def one(j):
            outer(dst, j * wide, [(dq[degree + j, ch], coef[degree + j, ch]) for ch in range(chunks)])

        loop(half, one)

    def pair_copy(k):
        slot = lax.rem(k, 2)
        rows_there = pl.ds(first_degree(block_at(k, -way), core) * wide, block_rows)
        return to(sibling, wbuf.at[slot, head(block_rows)], dw_out.at[rows_there],
                  pair_send.at[slot], pair_recv.at[k])

    def weight_block(k):
        @pl.when(k >= 2)
        def _():
            pair_copy(k - 2).wait_send()
        weight_grad(wbuf.at[lax.rem(k, 2)], first_degree(block_at(k, -way), other_core))
        pair_copy(k).start()
        block = block_at(k, way)
        weight_grad(work.at[pl.ds(block * block_rows, block_rows)], first_degree(block, core))

    loop(chips, weight_block)
    pair_copy(chips - 2).wait_send()
    pair_copy(last).wait_send()
    own_copy.wait()
    packs[core, chip] = (own[core].astype(F32) + other[...].astype(F32)).astype(BF16)

    def low_degree(l):
        def one(z):
            for c in range(2):
                p = l - z if c == 0 else l + 1
                ours = p >= 0 if c == 0 else p >= n - z
                p = jnp.maximum(p, 0)
                h = jnp.where(p > held - 1, 1, 0)
                for which in range(2):
                    lowx[which, 2 * z + c] = only(ours, packs[h, z, which, :, p - h * (held - 1)])

        loop(chips, one)
        outer(wbuf.at[0], 0, [(lowx[1].reshape(-1, chans), lowx[0].reshape(-1, chans))])
        dw_out[pl.ds(l * wide, wide)] = wbuf[0, head(wide)]

    def final_rows(unit):
        ch, t = unit_of(unit)

        step_in(dg_hbm, unit)
        buf = lax.rem(unit, 2)

        fetch_rows(3, ch, t)
        for b in range(0, nb, 2):
            g = fetch_pair(b)
            change = dot(adj_h[...], g) + dot(adj_l[...], g)
            df_out[ch * nb + b, t] = inbuf[buf, b] + change[:, :chans]
            df_out[ch * nb + b + 1, t] = inbuf[buf, b + 1] + change[:, chans:]

    def place(i, of_core):
        block = block_at(lax.div(i, pieces), way)
        start = lax.rem(i, pieces) * piece
        return pl.ds(block * block_rows + start, piece), pl.ds(first_degree(block, of_core) * wide + start, piece)

    def rs_copy(i):
        here, there = place(i, core)
        return to(onward, work.at[here], dw_out.at[there], rs_send, rs_recv.at[i])

    def add_pair(i):
        here, passed = place(i, other_core)

        @pl.when(lax.rem(i, pieces) == 0)
        def _():
            pair_copy(lax.div(i, pieces)).wait_recv()

        work[here] += dw_out[passed]

    def rs_step(i):
        add_pair(i)

        @pl.when(i >= pieces)
        def _():
            rs_copy(i - pieces).wait_recv()
            here, there = place(i, core)
            work[here] += dw_out[there]

        rs_copy(i).start()

        @pl.when(lax.rem(i, pieces) == 0)
        def _():
            k = lax.div(i, pieces)

            @pl.when(k > 0)
            def _():
                pack_copy(k - 1).wait_recv()

            pack_copy(k).start()
            share(k)


    loop(hops, rs_step)
    pack_copy(chips - 2).wait_recv()
    share(last)

    def own_sum(s):
        i = hops + s
        add_pair(i)
        rs_copy(i - pieces).wait_recv()
        here, there = place(i, core)
        dw_out[there] += work[here]
        ag_copy(i, s).start()

    def second_spot(k):
        return pl.ds((n + 2 * block_at(k, way) + core) * wide, wide)

    def second_copy(k, got):
        spot = dw_out.at[second_spot(k)]
        return to(onward, spot, spot, ag_send, ag_recv.at[hops + got])

    def second_publish(k):
        spot = dw_out.at[second_spot(k)]
        to(sibling, spot, spot, pub_send, pub_recv).start()

    def ag_copy(i, got):
        _, there = place(i, core)
        return to(onward, dw_out.at[there], dw_out.at[there], ag_send, ag_recv.at[got])

    def publish(i):
        _, there = place(i, core)
        to(sibling, dw_out.at[there], dw_out.at[there], pub_send, pub_recv).start()

    firsts = second.at[:, head(n - 1), :, head(tile)]
    pltpu.make_async_copy(firsts, firsts, always_recv).wait()

    self_too = (first_mode(me) <= me).astype(jnp.int32)
    comes, goes = me + 1 - self_too, n - first_mode(me) - self_too

    def wait_some(count, sem):
        for k in range(1, n):
            @pl.when(count == k)
            def _():
                part = second.at[:, head(k), :, pl.ds(tile, tile)]
                pltpu.make_async_copy(part, part, sem).wait()

    wait_some(comes, some_recv)
    outer(wbuf.at[0], 0, [(second[1].reshape(-1, chans), second[0].reshape(-1, chans))])
    dw_out[second_spot(last)] = wbuf[0, head(wide)]
    loop(pieces, own_sum)
    second_copy(last, 0).start()

    pl.semaphore_signal(free_sem, inc=1, device_id={axis: sibling}, device_id_type=pl.DeviceIdType.MESH)
    pl.semaphore_wait(free_sem, 1)

    def own_piece(s):
        publish(hops + s)

    loop(pieces, own_piece)
    second_publish(last)
    gathered = packs.at[other_core]
    pltpu.make_async_copy(gathered, gathered, share_recv).wait()

    def task(i):
        @pl.when(i < chips)
        def _():
            for ch in range(chunks):
                @pl.when(i == 0)
                def _():
                    arrived(3, ch)
                apply_top(0, ch, i)

        @pl.when((i >= chips) & (i < chips + units))
        def _():
            final_rows(i - chips)

        @pl.when(i < n)
        def _():
            low_degree(i)

    def ag_step(i):
        ag_copy(i, i).wait_recv()

        @pl.when(i + pieces < hops)
        def _():
            ag_copy(i, i + pieces).start()

        publish(i)

        @pl.when(lax.rem(i, pieces) == pieces - 1)
        def _():
            k = lax.div(i, pieces)
            second_copy(k, k).wait_recv()

            @pl.when(k < chips - 2)
            def _():
                second_copy(k, k + 1).start()

            second_publish(k)

        task(i)

    loop(hops, ag_step)

    def rest(i):
        task(i)

    loop(max(hops, chips + units, n), rest, hops)

    wait_sent(2 * chunks + final, 2)
    for ch in range(chunks):
        wait_sent(3 * chunks + ch, 3)
    for ch in range(chunks):
        pltpu.make_async_copy(sums.at[ch], sums.at[ch], sum_send.at[ch]).wait()
    sent = work.at[head((last) * block_rows)]
    pltpu.make_async_copy(sent, sent, rs_send).wait()
    sent = dw_out.at[head((last) * (block_rows + wide))]
    pltpu.make_async_copy(sent, sent, ag_send).wait()
    pltpu.make_async_copy(firsts, firsts, always_send).wait()

    wait_some(goes, some_send)
    sent = packs.at[0, head(last)]
    pltpu.make_async_copy(sent, sent, pack_send).wait()
    pltpu.make_async_copy(packs.at[0], packs.at[0], share_send).wait()
    shared = dw_out.at[head(chips * (block_rows + wide))]
    pltpu.make_async_copy(shared, shared, pub_send).wait()
    pltpu.make_async_copy(shared, shared, pub_recv).wait()


def put_kernel(df_ref, dw_ref, df_hbm, dw_hbm, sems):
    copies = []
    for source, target, parts in ((df_ref, df_hbm, 6), (dw_ref, dw_hbm, 12)):
        size = source.shape[0] // parts
        for k in range(parts):
            part = pl.ds(k * size, size)
            copies.append(pltpu.make_async_copy(source.at[part], target.at[part], sems.at[len(copies)]))
    for copy in copies:
        copy.start()
    for copy in copies:
        copy.wait()


def solution(mesh):
    n = mesh.shape['lat']
    field_spec = P('member', None, 'lat', None)

    def local_step(field_loc, grad_loc, p_fwd, p_inv, w_mix):
        batch, chans, tl, lons = field_loc.shape
        degs, lats = p_fwd.shape[1:]
        ml = p_fwd.shape[0] // n
        nb = 4
        chunks = batch // nb
        rows = ml * 2 * nb
        pitch = rows + 1
        half = degs // n - 2
        pieces = 4 if half * 2 * chans % 32 == 0 else 1
        hops = (n // 2 - 1) * pieces
        per = 4
        area = max(2 * lats * pitch, n // 2 * half * 2 * chans)
        depth = min(degs // per, area // (per * 2 * chans))
        held = n // 2 + 1
        packed = (3, chunks, held, 2 * nb, chans)
        tables = fourier_tables(n, ml, lons)
        anywhere = pl.BlockSpec(memory_space=pl.ANY)
        vmem = pl.BlockSpec(memory_space=pltpu.VMEM)
        grad_field, grad_w = pl.pallas_call(
            functools.partial(layer_kernel, 'lat', n, nb, pieces, per, depth),
            name='layer',
            out_shape=(
                pltpu.VMEM((batch, tl, lons, chans), F32),
                pltpu.VMEM((degs * 2 * chans, chans), F32),
            ),
            in_specs=[anywhere] * 6,
            out_specs=(vmem, vmem),
            scratch_shapes=[
                pltpu.VMEM((2, chunks, n, tl, rows, chans), BF16),
                pltpu.VMEM((chunks + 1, n, tl, rows, chans), BF16),
                pltpu.VMEM((area, chans), F32),
                pltpu.VMEM((lats, 2 * nb * chans), BF16),
                pltpu.VMEM((degs, chunks, rows, chans), BF16),
                pltpu.VMEM((degs, chunks, rows, chans), BF16),
                pltpu.VMEM((degs, 2 * chans, chans), BF16),
                pltpu.VMEM((2, max(per, half) * 2 * chans, chans), F32),
                pltpu.VMEM((2, nb, lons, chans), F32),
                pltpu.VMEM((n * rows, chans), F32),
                pltpu.VMEM((2, ml, degs, lats), F32),
                pltpu.VMEM((2, ml, degs, lats), BF16),
                pltpu.VMEM((2, n, n, lats), F32),
                pltpu.VMEM((2, n // 2, 16, 32), F32),
                pltpu.VMEM((32 * 2 * nb, chans), F32),
                pltpu.VMEM((2,) + packed, BF16),
                pltpu.VMEM(packed, BF16),
                pltpu.VMEM((2, n // 2) + packed, BF16),
                pltpu.VMEM((2, n, chunks, 2 * nb, chans), BF16),
                pltpu.VMEM(tables.shape, BF16),
                pltpu.VMEM((chunks, 5, 6, tl, 2 * nb, chans), BF16),
                pltpu.VMEM((2, 4, held, 2 * nb, chans), F32),
                pltpu.VMEM((chunks, 4, held, 2 * nb, chans), F32),
                pltpu.VMEM((chunks, 4, held, 2 * nb, chans), F32),
                pltpu.VMEM((chunks, 2, held, 2 * nb, chans), F32),
                pltpu.VMEM((chunks, 2, held, 2 * nb, chans), F32),
                pltpu.VMEM((chunks, 2, held, 2 * nb, chans), F32),
                pltpu.VMEM((2, n, chunks, 4 * nb, chans), BF16),
                pltpu.SemaphoreType.DMA((4 * chunks,)),
                pltpu.SemaphoreType.DMA((4 * chunks,)),
                pltpu.SemaphoreType.DMA((2,)),
                pltpu.SemaphoreType.DMA((depth,)),
                pltpu.SemaphoreType.DMA((2,)),
                pltpu.SemaphoreType.DMA((2,)),
                pltpu.SemaphoreType.DMA((2,)),
                pltpu.SemaphoreType.DMA((n // 2,)),
                pltpu.SemaphoreType.DMA,
                pltpu.SemaphoreType.DMA((hops,)),
                pltpu.SemaphoreType.DMA,
                pltpu.SemaphoreType.DMA((hops + n // 2 - 1,)),
                pltpu.SemaphoreType.REGULAR,
                pltpu.SemaphoreType.DMA,
                pltpu.SemaphoreType.DMA,
                pltpu.SemaphoreType.DMA,
                pltpu.SemaphoreType.DMA,
                pltpu.SemaphoreType.DMA,
                pltpu.SemaphoreType.DMA((n // 2 - 1,)),
                pltpu.SemaphoreType.DMA,
                pltpu.SemaphoreType.DMA,
                pltpu.SemaphoreType.DMA((2,)),
                pltpu.SemaphoreType.DMA,
                pltpu.SemaphoreType.DMA((chunks,)),
                pltpu.SemaphoreType.DMA((chunks,)),
                pltpu.SemaphoreType.DMA((chunks,)),
                pltpu.SemaphoreType.DMA((chunks,)),
                pltpu.SemaphoreType.DMA((chunks,)),
                pltpu.SemaphoreType.DMA((chunks,)),
                pltpu.SemaphoreType.DMA((chunks,)),
                pltpu.SemaphoreType.DMA((chunks,)),
                pltpu.SemaphoreType.DMA((chunks,)),
                pltpu.SemaphoreType.DMA((chunks,)),
                pltpu.SemaphoreType.DMA((chunks,)),
                pltpu.SemaphoreType.DMA((chunks,)),
                pltpu.SemaphoreType.DMA,
                pltpu.SemaphoreType.DMA,
                pltpu.SemaphoreType.DMA,
                pltpu.SemaphoreType.DMA,
                pltpu.SemaphoreType.DMA((chunks,)),
            ],
            compiler_params=pltpu.CompilerParams(
                collective_id=0, has_side_effects=True, vmem_limit_bytes=43 * 1024 * 1024),
        )(
            field_loc.transpose(0, 2, 3, 1), grad_loc.transpose(0, 2, 3, 1),
            w_mix.transpose(0, 1, 3, 2).reshape(degs * 2 * chans, chans),
            p_fwd, p_inv, tables)
        grad_field, grad_w = pl.pallas_call(
            put_kernel,
            name='put',
            out_shape=(
                jax.ShapeDtypeStruct(grad_field.shape, F32),
                jax.ShapeDtypeStruct(grad_w.shape, F32),
            ),
            in_specs=[vmem] * 2,
            out_specs=(anywhere, anywhere),
            scratch_shapes=[pltpu.SemaphoreType.DMA((18,))],
            compiler_params=pltpu.CompilerParams(vmem_limit_bytes=1024 * 1024),
        )(grad_field, grad_w)
        return grad_field.transpose(0, 3, 1, 2), grad_w.reshape(degs, chans, 2, chans).transpose(0, 1, 3, 2)

    return jax.shard_map(
        local_step, mesh=mesh, in_specs=(field_spec, field_spec, P(), P(), P()),
        out_specs=(field_spec, P('member', None, None, None)), check_vma=False)
```

```python
import functools
import math

import jax
import jax.numpy as jnp
import numpy as np
from jax import lax
from jax.experimental import pallas as pl
from jax.experimental.pallas import tpu as pltpu
from jax.sharding import PartitionSpec as P

F32 = jnp.float32
BF16 = jnp.bfloat16


def split_const(matrix):
    head = matrix.astype(BF16)
    tail = (matrix - head.astype(np.float64)).astype(BF16)
    return [head, tail]


def fourier_tables(n, ml, lons):
    modes = n * ml
    device = np.arange(n)
    first = np.where(device % 2 == 0, device // 2, n - 1 - device // 2)
    order = (first[:, None] + n * np.arange(ml)[None, :]).reshape(-1)
    angle = 2.0 * np.pi * (np.outer(order, np.arange(lons)) % lons) / lons
    forward = np.stack([np.cos(angle), -np.sin(angle)], axis=1).reshape(2 * modes, lons) / math.sqrt(lons)
    gains = np.repeat(np.where(order == 0, 1.0, 2.0), 2)[:, None]
    doubled = forward * gains
    tables = split_const(forward) + split_const(doubled) + split_const(doubled.T) + split_const(forward.T)
    return jnp.stack([jnp.asarray(t) for t in tables])


def gelu_grad(values):
    cumulative = 0.5 * (1.0 + lax.erf(values * math.sqrt(0.5)))
    density = jnp.exp(-0.5 * values * values) / math.sqrt(2.0 * math.pi)
    return cumulative + values * density


def loop(stop, step, start=0, unroll=None):
    def one(i, carry):
        step(i)
        return carry

    lax.fori_loop(start, stop, one, 0, unroll=unroll)


def head(size):
    return pl.ds(0, size)


def dot(a, b, dims=((1,), (0,))):
    return lax.dot_general(a, b, (dims, ((), ())), preferred_element_type=F32)


def layer_kernel(
    axis, n, nb, pieces, per, depth,
    f_hbm, dg_hbm, w_hbm, pf_hbm, pv_hbm, tab_hbm,
    df_out, dw_out,
    recv, send, work, xb, coef, dq, vmix, wbuf, inbuf, gather, pbuf, pmat, band, cmat, qs, own, other, packs, lowx, tab,
    topin, partial, mid, sums, sumin, joined, handed, second,
    send_sem, recv_sem, in_sem, w_sem, p_sem, band_sem, pair_send, pair_recv, rs_send, rs_recv, ag_send, ag_recv,
    free_sem, pub_send, pub_recv, own_send, own_recv, pack_send, pack_recv, share_send, share_recv,
    tab_sem, top_send, near_recv, far_recv, swap_send, swap_recv,
    row_send, row_recv, mid_send, mid_recv, sum_send, sum_recv, join_send, join_recv,
    always_send, always_recv, some_send, some_recv, hand_recv,
):
    me = lax.axis_index(axis)
    batch, tl, lons, chans = f_hbm.shape
    ml, degs, lats = pmat.shape[1:]
    chunks = batch // nb
    tile = 2 * nb
    rows = ml * tile
    pitch = rows + 1
    modes2 = 2 * n * ml
    units = chunks * tl
    final = chunks - 1
    slots = chunks + 1
    fwd_h, fwd_l, dbl_h, dbl_l, syn_h, syn_l, adj_h, adj_l = (tab.at[k] for k in range(8))
    area = lats * pitch
    top = n * (ml - 1)
    held = n // 2 + 1
    chip, core = lax.div(me, 2), lax.rem(me, 2)
    other_core = 1 - core
    chips = n // 2
    last = chips - 1
    way = 1 - 2 * core
    sibling = me + way

    def chip_at(away):
        return lax.rem(chip + away + chips, chips)

    def across(away, its_core):
        return 2 * chip_at(away) + its_core

    onward = across(way, core)

    def first_mode(device):
        z = lax.div(device, 2)
        return jnp.where(lax.rem(device, 2) == 0, z, n - 1 - z)

    def to(device, src, dst, sent, got):
        return pltpu.make_async_remote_copy(
            src_ref=src, dst_ref=dst, send_sem=sent, recv_sem=got,
            device_id={axis: device}, device_id_type=pl.DeviceIdType.MESH)

    def unit_of(unit):
        return lax.div(unit, tl), lax.rem(unit, tl)

    def unit_in(src, unit):
        ch, t = unit_of(unit)
        slot = lax.rem(unit, 2)
        return pltpu.make_async_copy(src.at[pl.ds(ch * nb, nb), t], inbuf.at[slot], in_sem.at[slot])

    def step_in(src, unit):
        @pl.when(unit + 1 < units)
        def _():
            unit_in(src, unit + 1).start()
        unit_in(src, unit).wait()

    body, peak = head(rows - tile), pl.ds(rows - tile, tile)

    def ship(stage, ch, t0, nt):
        index = stage * chunks + ch
        slot = lax.rem(index, slots)
        part = pl.ds(t0, nt)

        def one(k):
            peer = lax.rem(me + k, n)
            to(peer, send.at[slot, peer, part, body], recv.at[stage % 2, ch, me, part, body],
               send_sem.at[index], recv_sem.at[index]).start()

        loop(n, one, 1)
        recv[stage % 2, ch, me, part, body] = send[slot, me, part, body]

    def arrived(stage, ch):
        others = recv.at[stage % 2, ch, head(n - 1), :, body]
        pltpu.make_async_copy(others, others, recv_sem.at[stage * chunks + ch]).wait()

    def peaks():
        return send.at[0, head(n - 5), :, peak]

    def wait_sent(index, stage):
        others = send.at[lax.rem(index, slots), head(n - 1), :, body]
        pltpu.make_async_copy(others, others, send_sem.at[index]).wait()
        if stage % 2 == 0:
            ch = index - stage * chunks
            pltpu.make_async_copy(peaks(), peaks(), row_send.at[ch]).wait()

    def send_peak(stage, ch):
        slot = lax.rem(stage * chunks + ch, slots)
        far = chips // 2
        for same in (True, False):
            its_core = core if same else other_core
            for away in range(1 - far, far + 1):
                near = max(-2, min(2, away))
                hop, target, apart = away - near, (0, 2, 4, 3, 1)[near], abs(away - near)
                if away == far:
                    hop = jnp.where(its_core == 0, 2 - far, far - 2)
                    target = jnp.where(its_core == 0, 3, 4)
                source = send.at[slot, across(away, its_core), :, peak]
                place = topin.at[ch, target, 2 * apart + core]
                if same and not apart:
                    place[...] = source[...]
                else:
                    to(across(hop, its_core), source, place,
                       row_send.at[ch], row_recv.at[ch]).start()

    def free_slot(stage, ch):
        index = stage * chunks + ch
        if stage >= 1:
            @pl.when(ch >= 1)
            def _():
                wait_sent(index - slots, stage - 1)
        if stage >= 2:
            @pl.when(ch == 0)
            def _():
                wait_sent(index - slots, stage - 2)
        return lax.rem(index, slots)

    def put_rows(slot, t):
        send[slot, :, t] = gather[...].reshape(n, rows, chans).astype(BF16)

    def transform(values, head, tail):
        high = values.astype(BF16)
        low = (values - high.astype(F32)).astype(BF16)
        return dot(head[...], high) + (dot(tail[...], high) + dot(head[...], low))

    unit_in(f_hbm, 0).start()
    first_tables = pltpu.make_async_copy(tab_hbm.at[head(2)], tab.at[head(2)], tab_sem.at[0])
    other_tables = pltpu.make_async_copy(tab_hbm.at[pl.ds(2, 6)], tab.at[pl.ds(2, 6)], tab_sem.at[1])
    first_tables.start()
    barrier = pltpu.get_barrier_semaphore()

    def announce(k):
        pl.semaphore_signal(barrier, inc=1, device_id={axis: lax.rem(me + k, n)}, device_id_type=pl.DeviceIdType.MESH)

    loop(n, announce, 1)

    first_tables.wait()

    group = max(1, tl // 3)

    parts = degs // per

    def w_in(k):
        slot = lax.rem(k, depth)
        return pltpu.make_async_copy(
            w_hbm.at[pl.ds(k * per * 2 * chans, per * 2 * chans)],
            work.at[pl.ds(slot * per * 2 * chans, per * 2 * chans)], w_sem.at[slot])

    def band_in(d):
        for which, source in enumerate((pf_hbm, pv_hbm)):
            pltpu.make_async_copy(
                source.at[top + first_mode(d), pl.ds(top, n)], band.at[which, d], band_sem.at[which]).start()

    def step1_chunk(ch):
        slot = free_slot(0, ch)

        def row(t):
            unit = ch * tl + t
            step_in(f_hbm, unit)
            buf = lax.rem(unit, 2)
            for b in range(0, nb, 2):
                pair = jnp.concatenate([inbuf[buf, b], inbuf[buf, b + 1]], axis=1)
                spec = transform(pair, fwd_h, fwd_l)
                gather[pl.ds(b, modes2, stride=nb), :] = spec[:, :chans]
                gather[pl.ds(b + 1, modes2, stride=nb), :] = spec[:, chans:]
            put_rows(slot, t)

            @pl.when((ch == 0) & (t == group - 1))
            def _():
                pl.semaphore_wait(barrier, n - 1)
                ship(0, 0, 0, group)


        loop(tl, row)
        send_peak(0, ch)

        @pl.when(ch == 0)
        def _():
            ship(0, 0, group, tl - group)
            other_tables.start()
            for which, source in enumerate((pf_hbm, pv_hbm)):
                for k in range(ml):
                    pltpu.make_async_copy(
                        source.at[first_mode(me) + n * k], pbuf.at[which, k], p_sem.at[which]).start()
            loop(n, band_in)
            for k in range(depth):
                w_in(k).start()


    loop(chunks, step1_chunk)

    unit_in(dg_hbm, 0).start()
    for which in range(2):
        pltpu.make_async_copy(band.at[which], band.at[which], band_sem.at[which]).wait()
    qs[...] = jnp.zeros_like(qs)

    def pack(z, store):
        def one(index):
            half_at, row = lax.div(index, held), lax.rem(index, held)
            p = half_at * (held - 1) + row
            degree = jnp.where(core == 0, jnp.minimum(z + p, n - 1), jnp.maximum(p - 1, 0))
            store(half_at, row, degree, (p < n - z) == (core == 0))

        loop(2 * held, one)

    def project(which, ch, target, device):
        gather[...] = jnp.zeros_like(gather)
        side = 1 if target == 3 else -1

        def place_rows(apart):
            for c in range(2):
                src = across(side * apart, c)
                gather[pl.ds(pl.multiple_of(src * tl * tile, tile), tl * tile), :] = topin[
                    ch, target, 2 * apart + c].reshape(tl * tile, chans).astype(F32)

        place_rows(0)
        if target > 2:
            place_rows(1)

            @pl.when(core == target - 3)
            def _():
                place_rows(2)

        for k in range(tile):
            xb[:, k * chans:(k + 1) * chans] = gather[pl.ds(k, lats, stride=tile), :].astype(BF16)
        out = dot(band[which, device].astype(BF16), xb[...])
        for k in range(tile):
            qs[pl.ds(k, n, stride=tile), :] = out[:, k * chans:(k + 1) * chans]

    def sum_rows(which, ch):
        pltpu.make_async_copy(peaks(), peaks(), row_recv.at[ch]).wait()
        for target, away in enumerate((-1, 1, -2, 2)):
            project(which, ch, target + 1, across(away, core))

            def keep(half_at, row, degree, ours):
                values = qs[pl.ds(pl.multiple_of(degree * tile, tile), tile), :]
                partial[half_at, target, row] = jnp.where(ours, values, jnp.zeros_like(values))

            pack(chip_at(away), keep)
        swap = to(sibling, partial.at[other_core], mid.at[ch], mid_send.at[ch], mid_recv.at[ch])
        swap.start()
        if which == 1:
            pltpu.make_async_copy(sums.at[ch], sums.at[ch], sum_send.at[ch]).wait()
        swap.wait()
        sums[ch] = partial[core] + mid[ch]
        for side, away in enumerate((-1, 1)):
            to(across(away, core), sums.at[ch, 2 + side], handed.at[ch, side],
               sum_send.at[ch], hand_recv.at[ch]).start()

    def pass_sums(ch):
        pltpu.make_async_copy(handed.at[ch], handed.at[ch], hand_recv.at[ch]).wait()
        for side, away in enumerate((-1, 1)):
            sums[ch, side] += handed[ch, side]
            to(across(away, core), sums.at[ch, side], sumin.at[ch, side],
               sum_send.at[ch], sum_recv.at[ch]).start()

    def finish_peak(which, ch):
        pltpu.make_async_copy(sumin.at[ch], sumin.at[ch], sum_recv.at[ch]).wait()
        joined[ch, core] = sumin[ch, 0] + sumin[ch, 1]
        swap = to(sibling, joined.at[ch, core], joined.at[ch, core], join_send.at[ch], join_recv.at[ch])
        swap.start()
        project(which, ch, 0, me)
        swap.wait()

        def one(degree):
            p = jnp.where(core == 0, degree - chip, degree + 1)
            ours = degree >= first_mode(me)
            p = jnp.maximum(p, 0)
            h = jnp.where(p > held - 1, 1, 0)
            come = joined[ch, h, p - h * (held - 1)]
            work[pl.ds(area + (top + degree) * pitch + rows - tile, tile), :] = qs[
                pl.ds(pl.multiple_of(degree * tile, tile), tile), :] + jnp.where(ours, come, jnp.zeros_like(come))

        loop(n, one)

    sum_rows(0, 0)

    def ship_rows(ch):
        ship(0, ch, 0, tl)

    loop(final, ship_rows, 1)
    for which in range(2):
        pltpu.make_async_copy(pbuf.at[which], pbuf.at[which], p_sem.at[which]).wait()
    pmat[...] = pbuf[...].astype(BF16)
    other_tables.wait()

    def load_w(k):
        w_in(k).wait()
        base = lax.rem(k, depth) * per * 2 * chans
        for j in range(per):
            for part in range(2):
                vmix[k * per + j, pl.ds(part * chans, chans)] = work[
                    pl.ds(base + j * 2 * chans + part, chans, stride=2), :].astype(BF16)

        @pl.when(k + depth < parts)
        def _():
            w_in(k + depth).start()


    loop(parts, load_w)

    span = cmat.shape[3]
    mine_t = (lax.broadcasted_iota(jnp.int32, (8, lats), 1) == me * tl + lax.broadcasted_iota(jnp.int32, (8, lats), 0))
    mine_t &= lax.broadcasted_iota(jnp.int32, (8, lats), 0) < tl
    mine_t = jnp.where(mine_t, 1.0, 0.0).astype(BF16)

    def tabulate(d):
        z, of_core = lax.div(d, 2), lax.rem(d, 2)
        row = lax.broadcasted_iota(jnp.int32, (n, span), 0)
        p = jnp.where(of_core == 0, row - z, row + 1)
        target = jnp.where(p > held - 1, p + 1, p)
        moved = jnp.where(target == lax.broadcasted_iota(jnp.int32, (n, span), 1), 1.0, 0.0).astype(BF16)
        for which in range(2):
            picked = dot(mine_t, band[which, d].astype(BF16), ((1,), (1,))).astype(BF16)
            cmat[which, z, pl.ds(pl.multiple_of(of_core * 8, 8), 8), :] = dot(picked, moved)

    loop(n, tabulate)

    def no_degree(l):
        work[pl.ds(area + l * pitch + rows - tile, tile), :] = jnp.zeros((tile, chans), F32)

    loop(top, no_degree)

    pass_sums(0)

    def sum_first(ch):
        sum_rows(0, ch)

    loop(chunks, sum_first, 1)
    ship(0, final, 0, tl)
    loop(chunks, pass_sums, 1)

    sign = jnp.where(lax.broadcasted_iota(jnp.int32, (tile, chans), 0) < nb, -1.0, 1.0).astype(F32)

    def turn(values):
        groups = values.reshape(-1, tile, chans)
        return (pltpu.roll(groups, nb, 1) * sign[None]).reshape(values.shape)

    def legendre(src, dst, which, over):
        def mode(m):
            for k in range(tile):
                xb[:, k * chans:(k + 1) * chans] = work[
                    pl.ds(src + m * tile + k, lats, stride=pitch), :].astype(BF16)
            out = dot(pmat[which, m], xb[...], ((over,), (0,)))
            for k in range(tile):
                work[pl.ds(dst + m * tile + k, degs, stride=pitch), :] = out[:, k * chans:(k + 1) * chans]

        loop(ml - 1, mode)

    def unload(stage, ch):
        def body(src):
            for t in range(tl):
                work[pl.ds((src * tl + t) * pitch, rows), :] = recv[stage % 2, ch, src, t].astype(F32)

        loop(n, body)

    def load(slot):
        def body(dev):
            for t in range(tl):
                send[slot, dev, t] = work[pl.ds(area + (dev * tl + t) * pitch, rows), :].astype(BF16)

        loop(n, body)

    def only(ours, values):
        values = values.astype(F32)
        return jnp.where(ours, values, jnp.zeros_like(values)).astype(BF16)

    def spectral(stage, ch, into, kept, mix):
        arrived(stage - 1, ch)
        unload(stage - 1, ch)
        legendre(0, area, into, 1)
        finish_peak(into, ch)

        def degree(l):
            x = work[pl.ds(area + l * pitch, rows), :].astype(BF16)
            kept[l, ch] = x
            work[pl.ds(l * pitch, rows), :] = mix(l, x)

        loop(degs, degree, unroll=8)

        def keep_top(half_at, row, degree, ours):
            own[half_at, 2, ch, row] = only(ours, work[pl.ds((top + degree) * pitch + rows - tile, tile), :])

        pack(chip, keep_top)
        if stage == 1:
            swap = to(sibling, own.at[other_core, 2, ch], other.at[2, ch], swap_send.at[ch], swap_recv.at[ch])
            swap.start()
        legendre(0, area, 1 - into, 0)
        load(free_slot(stage, ch))
        if stage == 1:
            swap.wait()
            packs[core, chip, 2, ch] = (own[core, 2, ch].astype(F32) + other[2, ch].astype(F32)).astype(BF16)

            @pl.when(ch >= 2)
            def _():
                relay_top(ch - 2)

            for away in (2, -2):
                top_copy(0, away, ch, near_recv).start()
        else:
            @pl.when(ch == 0)
            def _():
                pass_sums(final - 1)
                sum_rows(1, final)

            @pl.when(ch == 1)
            def _():
                pass_sums(final)

        ship(stage, ch, 0, tl)

    def top_copy(source, away, ch, got):
        block = packs.at[core, chip_at(source), 2, ch]
        return to(across(away, core), block, block, top_send, got.at[ch])

    def top_blocks(count, ch):
        return packs.at[core, head(count), 2, ch]

    def relay_top(ch):
        pltpu.make_async_copy(top_blocks(2, ch), top_blocks(2, ch), near_recv.at[ch]).wait()
        for source in (2, -2):
            for away in (1, -1):
                top_copy(source, away, ch, far_recv).start()
        top_copy(-2 * way, 2 * way, ch, far_recv).start()

    def apply_top(which, ch, z):
        for h in range(2):
            qs[pl.ds(h * held * tile, held * tile), :] = packs[h, z, 2, ch].reshape(held * tile, chans).astype(F32)
        for k in range(tile):
            xb[0:span, k * chans:(k + 1) * chans] = qs[pl.ds(k, span, stride=tile), :].astype(BF16)
        out = dot(cmat[which, z].astype(BF16), xb[0:span, :])
        for k in range(tile):
            gather[pl.ds(k, 16, stride=tile), :] = out[:, k * chans:(k + 1) * chans]
        for c in range(2):
            for t in range(tl):
                recv[1, ch, 2 * z + c, t, pl.ds(rows - tile, tile)] = gather[
                    pl.ds((8 * c + t) * tile, tile), :].astype(BF16)

    def mix_forward(l, x):
        both = dot(x, vmix[l], ((1,), (1,)))
        return both[:, :chans] + turn(both[:, chans:])

    def mix_adjoint(l, x):
        both = dot(x, jnp.concatenate([vmix[l, head(chans)], vmix[l, pl.ds(chans, chans)]], axis=1))
        return both[:, :chans] - turn(both[:, chans:])

    def step2_chunk(ch):
        spectral(1, ch, 0, coef, mix_forward)

    loop(chunks, step2_chunk)
    relay_top(chunks - 2)

    def fetch_rows(stage, ch, t):
        for src in range(n):
            gather[pl.ds(src * rows, rows), :] = recv[stage % 2, ch, src, t].astype(F32)

    def fetch_pair(b):
        return jnp.concatenate(
            [gather[pl.ds(b, modes2, stride=nb), :], gather[pl.ds(b + 1, modes2, stride=nb), :]], axis=1).astype(BF16)

    def step3_chunk(ch):
        arrived(1, ch)
        pltpu.make_async_copy(top_blocks(5, ch), top_blocks(5, ch), far_recv.at[ch]).wait()
        swap = to(sibling, top_blocks(chips, ch), top_blocks(chips, ch), swap_send.at[ch], swap_recv.at[ch])
        swap.start()

        @pl.when(ch == 0)
        def _():
            relay_top(final)

        swap.wait()

        @pl.when(ch == final)
        def _():
            all_sent = packs.at[0, head(7), 2]
            pltpu.make_async_copy(all_sent, all_sent, top_send).wait()

        def apply(z):
            apply_top(1, ch, z)

        loop(chips, apply)

        @pl.when(ch == 1)
        def _():
            sum_rows(1, 0)

        slot = free_slot(2, ch)

        def row(t):
            unit = ch * tl + t
            step_in(dg_hbm, unit)
            buf = lax.rem(unit, 2)
            fetch_rows(1, ch, t)
            for b in range(0, nb, 2):
                g = fetch_pair(b)
                hidden = dot(syn_h[...], g) + dot(syn_l[...], g)
                pair = jnp.concatenate([inbuf[buf, b], inbuf[buf, b + 1]], axis=1)
                spec = transform(pair * gelu_grad(hidden), dbl_h, dbl_l)
                gather[pl.ds(b, modes2, stride=nb), :] = spec[:, :chans]
                gather[pl.ds(b + 1, modes2, stride=nb), :] = spec[:, chans:]
            put_rows(slot, t)

        loop(tl, row)
        send_peak(2, ch)

        @pl.when(ch < final)
        def _():
            ship(2, ch, 0, tl)


    loop(chunks, step3_chunk)

    def sum_second(ch):
        pass_sums(ch - 1)
        sum_rows(1, ch)

    loop(final, sum_second, 1)
    ship(2, final, 0, tl)
    unit_in(dg_hbm, 0).start()

    def step4_chunk(ch):
        spectral(3, ch, 1, dq, mix_adjoint)

    loop(chunks, step4_chunk)

    for which, kept in enumerate((coef, dq)):
        def keep_low(half_at, row, degree, ours):
            own[half_at, which, :, row] = only(ours, kept[degree, :, head(tile)])

        pack(chip, keep_low)

    def both_parts(peer, action):
        degree = n + first_mode(peer)
        for which, kept in enumerate((coef, dq)):
            action(to(peer, kept.at[degree, :, head(tile)], second.at[which, me, :, head(tile)],
                      always_send, always_recv))

            @pl.when(first_mode(me) <= first_mode(peer))
            def _():
                more = pl.ds(tile, tile)
                action(to(peer, kept.at[degree, :, more], second.at[which, me, :, more],
                          some_send, some_recv))

    def send_second(k):
        both_parts(lax.rem(me + k, n), lambda copy: copy.start())

    loop(n, send_second, 1)
    for which, kept in enumerate((coef, dq)):
        second[which, me] = kept[n + first_mode(me), :, head(2 * tile)]

    def clear_second(src):
        @pl.when(first_mode(src) > first_mode(me))
        def _():
            for which in range(2):
                second[which, src, :, pl.ds(tile, tile)] = jnp.zeros((chunks, tile, chans), BF16)

    loop(n, clear_second)
    own_copy = to(sibling, own.at[other_core], other, own_send, own_recv)
    own_copy.start()

    def pack_block(k):
        return packs.at[core, chip_at(-way * k)]

    def pack_copy(k):
        return to(onward, pack_block(k), pack_block(k), pack_send, pack_recv.at[k])

    def share(k):
        to(sibling, pack_block(k), pack_block(k), share_send, share_recv).start()

    half = degs // n - 2
    wide = 2 * chans
    block_rows = half * wide
    piece = block_rows // pieces
    hops = (last) * pieces

    def block_at(k, direction):
        return lax.rem(chip - direction * (1 + k) + 2 * chips, chips)

    def outer(dst, row, pairs):
        real = jnp.zeros((chans, chans), F32)
        imag = jnp.zeros((chans, chans), F32)
        for y, x in pairs:
            real += dot(y, x, ((0,), (0,)))
            imag -= dot(turn(y.astype(F32)).astype(BF16), x, ((0,), (0,)))
        dst[pl.ds(row, chans, stride=2), :] = real
        dst[pl.ds(row + 1, chans, stride=2), :] = imag

    def first_degree(block, of_core):
        return 2 * n + (2 * block + of_core) * half

    def weight_grad(dst, degree):
        def one(j):
            outer(dst, j * wide, [(dq[degree + j, ch], coef[degree + j, ch]) for ch in range(chunks)])

        loop(half, one)

    def pair_copy(k):
        slot = lax.rem(k, 2)
        rows_there = pl.ds(first_degree(block_at(k, -way), core) * wide, block_rows)
        return to(sibling, wbuf.at[slot, head(block_rows)], dw_out.at[rows_there],
                  pair_send.at[slot], pair_recv.at[k])

    def weight_block(k):
        @pl.when(k >= 2)
        def _():
            pair_copy(k - 2).wait_send()
        weight_grad(wbuf.at[lax.rem(k, 2)], first_degree(block_at(k, -way), other_core))
        pair_copy(k).start()
        block = block_at(k, way)
        weight_grad(work.at[pl.ds(block * block_rows, block_rows)], first_degree(block, core))

    loop(chips, weight_block)
    pair_copy(chips - 2).wait_send()
    pair_copy(last).wait_send()
    own_copy.wait()
    packs[core, chip] = (own[core].astype(F32) + other[...].astype(F32)).astype(BF16)

    def low_degree(l):
        def one(z):
            for c in range(2):
                p = l - z if c == 0 else l + 1
                ours = p >= 0 if c == 0 else p >= n - z
                p = jnp.maximum(p, 0)
                h = jnp.where(p > held - 1, 1, 0)
                for which in range(2):
                    lowx[which, 2 * z + c] = only(ours, packs[h, z, which, :, p - h * (held - 1)])

        loop(chips, one)
        outer(wbuf.at[0], 0, [(lowx[1].reshape(-1, chans), lowx[0].reshape(-1, chans))])
        dw_out[pl.ds(l * wide, wide)] = wbuf[0, head(wide)]

    def final_rows(unit):
        ch, t = unit_of(unit)

        step_in(dg_hbm, unit)
        buf = lax.rem(unit, 2)

        fetch_rows(3, ch, t)
        for b in range(0, nb, 2):
            g = fetch_pair(b)
            change = dot(adj_h[...], g) + dot(adj_l[...], g)
            df_out[ch * nb + b, t] = inbuf[buf, b] + change[:, :chans]
            df_out[ch * nb + b + 1, t] = inbuf[buf, b + 1] + change[:, chans:]

    def place(i, of_core):
        block = block_at(lax.div(i, pieces), way)
        start = lax.rem(i, pieces) * piece
        return pl.ds(block * block_rows + start, piece), pl.ds(first_degree(block, of_core) * wide + start, piece)

    def rs_copy(i):
        here, there = place(i, core)
        return to(onward, work.at[here], dw_out.at[there], rs_send, rs_recv.at[i])

    def add_pair(i):
        here, passed = place(i, other_core)

        @pl.when(lax.rem(i, pieces) == 0)
        def _():
            pair_copy(lax.div(i, pieces)).wait_recv()

        work[here] += dw_out[passed]

    def rs_step(i):
        add_pair(i)

        @pl.when(i >= pieces)
        def _():
            rs_copy(i - pieces).wait_recv()
            here, there = place(i, core)
            work[here] += dw_out[there]

        rs_copy(i).start()

        @pl.when(lax.rem(i, pieces) == 0)
        def _():
            k = lax.div(i, pieces)

            @pl.when(k > 0)
            def _():
                pack_copy(k - 1).wait_recv()

            pack_copy(k).start()
            share(k)


    loop(hops, rs_step)
    pack_copy(chips - 2).wait_recv()
    share(last)

    def own_sum(s):
        i = hops + s
        add_pair(i)
        rs_copy(i - pieces).wait_recv()
        here, there = place(i, core)
        dw_out[there] += work[here]
        ag_copy(i, s).start()

    def second_spot(k):
        return pl.ds((n + first_mode(2 * block_at(k, way) + core)) * wide, wide)

    def second_copy(k, got):
        spot = dw_out.at[second_spot(k)]
        return to(onward, spot, spot, ag_send, ag_recv.at[hops + got])

    def second_publish(k):
        spot = dw_out.at[second_spot(k)]
        to(sibling, spot, spot, pub_send, pub_recv).start()

    def ag_copy(i, got):
        _, there = place(i, core)
        return to(onward, dw_out.at[there], dw_out.at[there], ag_send, ag_recv.at[got])

    def publish(i):
        _, there = place(i, core)
        to(sibling, dw_out.at[there], dw_out.at[there], pub_send, pub_recv).start()

    firsts = second.at[:, head(n - 1), :, head(tile)]
    pltpu.make_async_copy(firsts, firsts, always_recv).wait()

    comes, goes = first_mode(me), n - 1 - first_mode(me)

    def wait_some(count, sem):
        for k in range(1, n):
            @pl.when(count == k)
            def _():
                part = second.at[:, head(k), :, pl.ds(tile, tile)]
                pltpu.make_async_copy(part, part, sem).wait()

    wait_some(comes, some_recv)
    outer(wbuf.at[0], 0, [(second[1].reshape(-1, chans), second[0].reshape(-1, chans))])
    dw_out[second_spot(last)] = wbuf[0, head(wide)]
    loop(pieces, own_sum)
    second_copy(last, 0).start()

    pl.semaphore_signal(free_sem, inc=1, device_id={axis: sibling}, device_id_type=pl.DeviceIdType.MESH)
    pl.semaphore_wait(free_sem, 1)

    def own_piece(s):
        publish(hops + s)

    loop(pieces, own_piece)
    second_publish(last)
    gathered = packs.at[other_core]
    pltpu.make_async_copy(gathered, gathered, share_recv).wait()

    def task(i):
        @pl.when(i < chips)
        def _():
            for ch in range(chunks):
                @pl.when(i == 0)
                def _():
                    arrived(3, ch)
                apply_top(0, ch, i)

        @pl.when((i >= chips) & (i < chips + units))
        def _():
            final_rows(i - chips)

        @pl.when(i < n)
        def _():
            low_degree(i)

    def ag_step(i):
        ag_copy(i, i).wait_recv()

        @pl.when(i + pieces < hops)
        def _():
            ag_copy(i, i + pieces).start()

        publish(i)

        @pl.when(lax.rem(i, pieces) == pieces - 1)
        def _():
            k = lax.div(i, pieces)
            second_copy(k, k).wait_recv()

            @pl.when(k < chips - 2)
            def _():
                second_copy(k, k + 1).start()

            second_publish(k)

        task(i)

    loop(hops, ag_step)

    def rest(i):
        task(i)

    loop(max(hops, chips + units, n), rest, hops)

    wait_sent(2 * chunks + final, 2)
    for ch in range(chunks):
        wait_sent(3 * chunks + ch, 3)
    for ch in range(chunks):
        pltpu.make_async_copy(sums.at[ch], sums.at[ch], sum_send.at[ch]).wait()
    sent = work.at[head((last) * block_rows)]
    pltpu.make_async_copy(sent, sent, rs_send).wait()
    sent = dw_out.at[head((last) * (block_rows + wide))]
    pltpu.make_async_copy(sent, sent, ag_send).wait()
    pltpu.make_async_copy(firsts, firsts, always_send).wait()

    wait_some(goes, some_send)
    sent = packs.at[0, head(last)]
    pltpu.make_async_copy(sent, sent, pack_send).wait()
    pltpu.make_async_copy(packs.at[0], packs.at[0], share_send).wait()
    shared = dw_out.at[head(chips * (block_rows + wide))]
    pltpu.make_async_copy(shared, shared, pub_send).wait()
    pltpu.make_async_copy(shared, shared, pub_recv).wait()


def put_kernel(df_ref, dw_ref, df_hbm, dw_hbm, sems):
    copies = []
    for source, target, parts in ((df_ref, df_hbm, 6), (dw_ref, dw_hbm, 12)):
        size = source.shape[0] // parts
        for k in range(parts):
            part = pl.ds(k * size, size)
            copies.append(pltpu.make_async_copy(source.at[part], target.at[part], sems.at[len(copies)]))
    for copy in copies:
        copy.start()
    for copy in copies:
        copy.wait()


def solution(mesh):
    n = mesh.shape['lat']
    field_spec = P('member', None, 'lat', None)

    def local_step(field_loc, grad_loc, p_fwd, p_inv, w_mix):
        batch, chans, tl, lons = field_loc.shape
        degs, lats = p_fwd.shape[1:]
        ml = p_fwd.shape[0] // n
        nb = 4
        chunks = batch // nb
        rows = ml * 2 * nb
        pitch = rows + 1
        half = degs // n - 2
        pieces = 4 if half * 2 * chans % 32 == 0 else 1
        hops = (n // 2 - 1) * pieces
        per = 4
        area = max(2 * lats * pitch, n // 2 * half * 2 * chans)
        depth = min(degs // per, area // (per * 2 * chans))
        held = n // 2 + 1
        packed = (3, chunks, held, 2 * nb, chans)
        tables = fourier_tables(n, ml, lons)
        anywhere = pl.BlockSpec(memory_space=pl.ANY)
        vmem = pl.BlockSpec(memory_space=pltpu.VMEM)
        grad_field, grad_w = pl.pallas_call(
            functools.partial(layer_kernel, 'lat', n, nb, pieces, per, depth),
            name='layer',
            out_shape=(
                pltpu.VMEM((batch, tl, lons, chans), F32),
                pltpu.VMEM((degs * 2 * chans, chans), F32),
            ),
            in_specs=[anywhere] * 6,
            out_specs=(vmem, vmem),
            scratch_shapes=[
                pltpu.VMEM((2, chunks, n, tl, rows, chans), BF16),
                pltpu.VMEM((chunks + 1, n, tl, rows, chans), BF16),
                pltpu.VMEM((area, chans), F32),
                pltpu.VMEM((lats, 2 * nb * chans), BF16),
                pltpu.VMEM((degs, chunks, rows, chans), BF16),
                pltpu.VMEM((degs, chunks, rows, chans), BF16),
                pltpu.VMEM((degs, 2 * chans, chans), BF16),
                pltpu.VMEM((2, max(per, half) * 2 * chans, chans), F32),
                pltpu.VMEM((2, nb, lons, chans), F32),
                pltpu.VMEM((n * rows, chans), F32),
                pltpu.VMEM((2, ml, degs, lats), F32),
                pltpu.VMEM((2, ml, degs, lats), BF16),
                pltpu.VMEM((2, n, n, lats), F32),
                pltpu.VMEM((2, n // 2, 16, 32), F32),
                pltpu.VMEM((32 * 2 * nb, chans), F32),
                pltpu.VMEM((2,) + packed, BF16),
                pltpu.VMEM(packed, BF16),
                pltpu.VMEM((2, n // 2) + packed, BF16),
                pltpu.VMEM((2, n, chunks, 2 * nb, chans), BF16),
                pltpu.VMEM(tables.shape, BF16),
                pltpu.VMEM((chunks, 5, 6, tl, 2 * nb, chans), BF16),
                pltpu.VMEM((2, 4, held, 2 * nb, chans), F32),
                pltpu.VMEM((chunks, 4, held, 2 * nb, chans), F32),
                pltpu.VMEM((chunks, 4, held, 2 * nb, chans), F32),
                pltpu.VMEM((chunks, 2, held, 2 * nb, chans), F32),
                pltpu.VMEM((chunks, 2, held, 2 * nb, chans), F32),
                pltpu.VMEM((chunks, 2, held, 2 * nb, chans), F32),
                pltpu.VMEM((2, n, chunks, 4 * nb, chans), BF16),
                pltpu.SemaphoreType.DMA((4 * chunks,)),
                pltpu.SemaphoreType.DMA((4 * chunks,)),
                pltpu.SemaphoreType.DMA((2,)),
                pltpu.SemaphoreType.DMA((depth,)),
                pltpu.SemaphoreType.DMA((2,)),
                pltpu.SemaphoreType.DMA((2,)),
                pltpu.SemaphoreType.DMA((2,)),
                pltpu.SemaphoreType.DMA((n // 2,)),
                pltpu.SemaphoreType.DMA,
                pltpu.SemaphoreType.DMA((hops,)),
                pltpu.SemaphoreType.DMA,
                pltpu.SemaphoreType.DMA((hops + n // 2 - 1,)),
                pltpu.SemaphoreType.REGULAR,
                pltpu.SemaphoreType.DMA,
                pltpu.SemaphoreType.DMA,
                pltpu.SemaphoreType.DMA,
                pltpu.SemaphoreType.DMA,
                pltpu.SemaphoreType.DMA,
                pltpu.SemaphoreType.DMA((n // 2 - 1,)),
                pltpu.SemaphoreType.DMA,
                pltpu.SemaphoreType.DMA,
                pltpu.SemaphoreType.DMA((2,)),
                pltpu.SemaphoreType.DMA,
                pltpu.SemaphoreType.DMA((chunks,)),
                pltpu.SemaphoreType.DMA((chunks,)),
                pltpu.SemaphoreType.DMA((chunks,)),
                pltpu.SemaphoreType.DMA((chunks,)),
                pltpu.SemaphoreType.DMA((chunks,)),
                pltpu.SemaphoreType.DMA((chunks,)),
                pltpu.SemaphoreType.DMA((chunks,)),
                pltpu.SemaphoreType.DMA((chunks,)),
                pltpu.SemaphoreType.DMA((chunks,)),
                pltpu.SemaphoreType.DMA((chunks,)),
                pltpu.SemaphoreType.DMA((chunks,)),
                pltpu.SemaphoreType.DMA((chunks,)),
                pltpu.SemaphoreType.DMA,
                pltpu.SemaphoreType.DMA,
                pltpu.SemaphoreType.DMA,
                pltpu.SemaphoreType.DMA,
                pltpu.SemaphoreType.DMA((chunks,)),
            ],
            compiler_params=pltpu.CompilerParams(
                collective_id=0, has_side_effects=True, vmem_limit_bytes=43 * 1024 * 1024),
        )(
            field_loc.transpose(0, 2, 3, 1), grad_loc.transpose(0, 2, 3, 1),
            w_mix.transpose(0, 1, 3, 2).reshape(degs * 2 * chans, chans),
            p_fwd, p_inv, tables)
        grad_field, grad_w = pl.pallas_call(
            put_kernel,
            name='put',
            out_shape=(
                jax.ShapeDtypeStruct(grad_field.shape, F32),
                jax.ShapeDtypeStruct(grad_w.shape, F32),
            ),
            in_specs=[vmem] * 2,
            out_specs=(anywhere, anywhere),
            scratch_shapes=[pltpu.SemaphoreType.DMA((18,))],
            compiler_params=pltpu.CompilerParams(vmem_limit_bytes=1024 * 1024),
        )(grad_field, grad_w)
        return grad_field.transpose(0, 3, 1, 2), grad_w.reshape(degs, chans, 2, chans).transpose(0, 1, 3, 2)

    return jax.shard_map(
        local_step, mesh=mesh, in_specs=(field_spec, field_spec, P(), P(), P()),
        out_specs=(field_spec, P('member', None, None, None)), check_vma=False)
```

```python
import functools
import math

import jax
import jax.numpy as jnp
import numpy as np
from jax import lax
from jax.experimental import pallas as pl
from jax.experimental.pallas import tpu as pltpu
from jax.sharding import PartitionSpec as P

F32 = jnp.float32
BF16 = jnp.bfloat16


def split_const(matrix):
    head = matrix.astype(BF16)
    tail = (matrix - head.astype(np.float64)).astype(BF16)
    return [head, tail]


def fourier_tables(n, ml, lons):
    modes = n * ml
    device = np.arange(n)
    first = np.where(device % 2 == 0, device // 2, n - 1 - device // 2)
    order = (first[:, None] + n * np.arange(ml)[None, :]).reshape(-1)
    angle = 2.0 * np.pi * (np.outer(order, np.arange(lons)) % lons) / lons
    forward = np.stack([np.cos(angle), -np.sin(angle)], axis=1).reshape(2 * modes, lons) / math.sqrt(lons)
    gains = np.repeat(np.where(order == 0, 1.0, 2.0), 2)[:, None]
    doubled = forward * gains
    tables = split_const(forward) + split_const(doubled) + split_const(doubled.T) + split_const(forward.T)
    return jnp.stack([jnp.asarray(t) for t in tables])


def gelu_grad(values):
    cumulative = 0.5 * (1.0 + lax.erf(values * math.sqrt(0.5)))
    density = jnp.exp(-0.5 * values * values) / math.sqrt(2.0 * math.pi)
    return cumulative + values * density


def loop(stop, step, start=0, unroll=None):
    def one(i, carry):
        step(i)
        return carry

    lax.fori_loop(start, stop, one, 0, unroll=unroll)


def head(size):
    return pl.ds(0, size)


def dot(a, b, dims=((1,), (0,))):
    return lax.dot_general(a, b, (dims, ((), ())), preferred_element_type=F32)


def layer_kernel(
    axis, n, nb, pieces, per, depth,
    f_hbm, dg_hbm, w_hbm, pf_hbm, pv_hbm, tab_hbm,
    df_out, dw_out,
    recv, send, work, xb, coef, dq, vmix, wbuf, inbuf, gather, pbuf, pmat, band, cmat, qs, own, other, packs, lowx, tab,
    topin, partial, mid, sums, sumin, joined, handed, second,
    send_sem, recv_sem, in_sem, w_sem, p_sem, band_sem, pair_send, pair_recv, rs_send, rs_recv, ag_send, ag_recv,
    free_sem, pub_send, pub_recv, own_send, own_recv, pack_send, pack_recv, share_send, share_recv,
    tab_sem, top_send, near_recv, far_recv, swap_send, swap_recv,
    row_send, row_recv, mid_send, mid_recv, sum_send, sum_recv, join_send, join_recv,
    always_send, always_recv, some_send, some_recv, hand_recv,
):
    me = lax.axis_index(axis)
    batch, tl, lons, chans = f_hbm.shape
    ml, degs, lats = pmat.shape[1:]
    chunks = batch // nb
    tile = 2 * nb
    rows = ml * tile
    pitch = rows + 1
    modes2 = 2 * n * ml
    units = chunks * tl
    final = chunks - 1
    slots = chunks + 1
    fwd_h, fwd_l, dbl_h, dbl_l, syn_h, syn_l, adj_h, adj_l = (tab.at[k] for k in range(8))
    area = lats * pitch
    top = n * (ml - 1)
    held = n // 2 + 1
    chip, core = lax.div(me, 2), lax.rem(me, 2)
    other_core = 1 - core
    chips = n // 2
    last = chips - 1
    way = 1 - 2 * core
    sibling = me + way

    def chip_at(away):
        return lax.rem(chip + away + chips, chips)

    def across(away, its_core):
        return 2 * chip_at(away) + its_core

    onward = across(way, core)

    def first_mode(device):
        z = lax.div(device, 2)
        return jnp.where(lax.rem(device, 2) == 0, z, n - 1 - z)

    def to(device, src, dst, sent, got):
        return pltpu.make_async_remote_copy(
            src_ref=src, dst_ref=dst, send_sem=sent, recv_sem=got,
            device_id={axis: device}, device_id_type=pl.DeviceIdType.MESH)

    def unit_of(unit):
        return lax.div(unit, tl), lax.rem(unit, tl)

    ahead = inbuf.shape[0] - 1

    def unit_in(src, unit):
        ch, t = unit_of(unit)
        slot = in_slot(unit)
        return pltpu.make_async_copy(src.at[pl.ds(ch * nb, nb), t], inbuf.at[slot], in_sem.at[slot])

    def in_slot(unit):
        return lax.rem(unit, ahead + 1)

    def start_in(src, first=0):
        for unit in range(first, ahead):
            unit_in(src, unit).start()

    def step_in(src, unit):
        @pl.when(unit + ahead < units)
        def _():
            unit_in(src, unit + ahead).start()
        unit_in(src, unit).wait()

    body, peak = head(rows - tile), pl.ds(rows - tile, tile)

    def ship(stage, ch, t0, nt):
        index = stage * chunks + ch
        slot = lax.rem(index, slots)
        part = pl.ds(t0, nt)

        def one(k):
            peer = lax.rem(me + k, n)
            to(peer, send.at[slot, peer, part, body], recv.at[stage % 2, ch, me, part, body],
               send_sem.at[index], recv_sem.at[index]).start()

        loop(n, one, 1)
        recv[stage % 2, ch, me, part, body] = send[slot, me, part, body]

    def arrived(stage, ch):
        others = recv.at[stage % 2, ch, head(n - 1), :, body]
        pltpu.make_async_copy(others, others, recv_sem.at[stage * chunks + ch]).wait()

    def peaks():
        return send.at[0, head(n - 5), :, peak]

    def wait_sent(index, stage):
        others = send.at[lax.rem(index, slots), head(n - 1), :, body]
        pltpu.make_async_copy(others, others, send_sem.at[index]).wait()
        if stage % 2 == 0:
            ch = index - stage * chunks
            pltpu.make_async_copy(peaks(), peaks(), row_send.at[ch]).wait()

    def send_peak(stage, ch):
        slot = lax.rem(stage * chunks + ch, slots)
        far = chips // 2
        for same in (True, False):
            its_core = core if same else other_core
            for away in range(1 - far, far + 1):
                near = max(-2, min(2, away))
                hop, target, apart = away - near, (0, 2, 4, 3, 1)[near], abs(away - near)
                if away == far:
                    hop = jnp.where(its_core == 0, 2 - far, far - 2)
                    target = jnp.where(its_core == 0, 3, 4)
                source = send.at[slot, across(away, its_core), :, peak]
                place = topin.at[ch, target, 2 * apart + core]
                if same and not apart:
                    place[...] = source[...]
                else:
                    to(across(hop, its_core), source, place,
                       row_send.at[ch], row_recv.at[ch]).start()

    def free_slot(stage, ch):
        index = stage * chunks + ch
        if stage >= 1:
            @pl.when(ch >= 1)
            def _():
                wait_sent(index - slots, stage - 1)
        if stage >= 2:
            @pl.when(ch == 0)
            def _():
                wait_sent(index - slots, stage - 2)
        return lax.rem(index, slots)

    def put_rows(slot, t):
        send[slot, :, t] = gather[...].reshape(n, rows, chans).astype(BF16)

    def transform(values, head, tail):
        high = values.astype(BF16)
        low = (values - high.astype(F32)).astype(BF16)
        return dot(head[...], high) + (dot(tail[...], high) + dot(head[...], low))

    unit_in(f_hbm, 0).start()
    first_tables = pltpu.make_async_copy(tab_hbm.at[head(2)], tab.at[head(2)], tab_sem.at[0])
    other_tables = pltpu.make_async_copy(tab_hbm.at[pl.ds(2, 6)], tab.at[pl.ds(2, 6)], tab_sem.at[1])
    first_tables.start()
    start_in(f_hbm, 1)
    barrier = pltpu.get_barrier_semaphore()

    def announce(k):
        pl.semaphore_signal(barrier, inc=1, device_id={axis: lax.rem(me + k, n)}, device_id_type=pl.DeviceIdType.MESH)

    loop(n, announce, 1)

    first_tables.wait()

    group = max(1, tl // 3)

    parts = degs // per

    def w_in(k):
        slot = lax.rem(k, depth)
        return pltpu.make_async_copy(
            w_hbm.at[pl.ds(k * per * 2 * chans, per * 2 * chans)],
            work.at[pl.ds(slot * per * 2 * chans, per * 2 * chans)], w_sem.at[slot])

    def band_in(d):
        for which, source in enumerate((pf_hbm, pv_hbm)):
            pltpu.make_async_copy(
                source.at[top + first_mode(d), pl.ds(top, n)], band.at[which, d], band_sem.at[which]).start()

    def step1_chunk(ch):
        slot = free_slot(0, ch)

        def row(t):
            unit = ch * tl + t
            step_in(f_hbm, unit)
            buf = in_slot(unit)
            for b in range(0, nb, 2):
                pair = jnp.concatenate([inbuf[buf, b], inbuf[buf, b + 1]], axis=1)
                spec = transform(pair, fwd_h, fwd_l)
                gather[pl.ds(b, modes2, stride=nb), :] = spec[:, :chans]
                gather[pl.ds(b + 1, modes2, stride=nb), :] = spec[:, chans:]
            put_rows(slot, t)

            @pl.when((ch == 0) & (t == group - 1))
            def _():
                pl.semaphore_wait(barrier, n - 1)
                ship(0, 0, 0, group)


        loop(tl, row)
        send_peak(0, ch)

        @pl.when(ch == 0)
        def _():
            ship(0, 0, group, tl - group)
            other_tables.start()
            for which, source in enumerate((pf_hbm, pv_hbm)):
                for k in range(ml):
                    pltpu.make_async_copy(
                        source.at[first_mode(me) + n * k], pbuf.at[which, k], p_sem.at[which]).start()
            loop(n, band_in)
            for k in range(depth):
                w_in(k).start()


    loop(chunks, step1_chunk)

    start_in(dg_hbm)
    for which in range(2):
        pltpu.make_async_copy(band.at[which], band.at[which], band_sem.at[which]).wait()
    qs[...] = jnp.zeros_like(qs)

    def pack(z, store):
        def one(index):
            half_at, row = lax.div(index, held), lax.rem(index, held)
            p = half_at * (held - 1) + row
            degree = jnp.where(core == 0, jnp.minimum(z + p, n - 1), jnp.maximum(p - 1, 0))
            store(half_at, row, degree, (p < n - z) == (core == 0))

        loop(2 * held, one)

    def project(which, ch, target, device):
        gather[...] = jnp.zeros_like(gather)
        side = 1 if target == 3 else -1

        def place_rows(apart):
            for c in range(2):
                src = across(side * apart, c)
                gather[pl.ds(pl.multiple_of(src * tl * tile, tile), tl * tile), :] = topin[
                    ch, target, 2 * apart + c].reshape(tl * tile, chans).astype(F32)

        place_rows(0)
        if target > 2:
            place_rows(1)

            @pl.when(core == target - 3)
            def _():
                place_rows(2)

        for k in range(tile):
            xb[:, k * chans:(k + 1) * chans] = gather[pl.ds(k, lats, stride=tile), :].astype(BF16)
        out = dot(band[which, device].astype(BF16), xb[...])
        for k in range(tile):
            qs[pl.ds(k, n, stride=tile), :] = out[:, k * chans:(k + 1) * chans]

    def sum_rows(which, ch):
        pltpu.make_async_copy(peaks(), peaks(), row_recv.at[ch]).wait()
        for target, away in enumerate((-1, 1, -2, 2)):
            project(which, ch, target + 1, across(away, core))

            def keep(half_at, row, degree, ours):
                values = qs[pl.ds(pl.multiple_of(degree * tile, tile), tile), :]
                partial[half_at, target, row] = jnp.where(ours, values, jnp.zeros_like(values))

            pack(chip_at(away), keep)
        swap = to(sibling, partial.at[other_core], mid.at[ch], mid_send.at[ch], mid_recv.at[ch])
        swap.start()
        if which == 1:
            pltpu.make_async_copy(sums.at[ch], sums.at[ch], sum_send.at[ch]).wait()
        swap.wait()
        sums[ch] = partial[core] + mid[ch]
        for side, away in enumerate((-1, 1)):
            to(across(away, core), sums.at[ch, 2 + side], handed.at[ch, side],
               sum_send.at[ch], hand_recv.at[ch]).start()

    def pass_sums(ch):
        pltpu.make_async_copy(handed.at[ch], handed.at[ch], hand_recv.at[ch]).wait()
        for side, away in enumerate((-1, 1)):
            sums[ch, side] += handed[ch, side]
            to(across(away, core), sums.at[ch, side], sumin.at[ch, side],
               sum_send.at[ch], sum_recv.at[ch]).start()

    def finish_peak(which, ch):
        pltpu.make_async_copy(sumin.at[ch], sumin.at[ch], sum_recv.at[ch]).wait()
        joined[ch, core] = sumin[ch, 0] + sumin[ch, 1]
        swap = to(sibling, joined.at[ch, core], joined.at[ch, core], join_send.at[ch], join_recv.at[ch])
        swap.start()
        project(which, ch, 0, me)
        swap.wait()

        def one(degree):
            p = jnp.where(core == 0, degree - chip, degree + 1)
            ours = degree >= first_mode(me)
            p = jnp.maximum(p, 0)
            h = jnp.where(p > held - 1, 1, 0)
            come = joined[ch, h, p - h * (held - 1)]
            work[pl.ds(area + (top + degree) * pitch + rows - tile, tile), :] = qs[
                pl.ds(pl.multiple_of(degree * tile, tile), tile), :] + jnp.where(ours, come, jnp.zeros_like(come))

        loop(n, one)

    sum_rows(0, 0)

    def ship_rows(ch):
        ship(0, ch, 0, tl)

    loop(final, ship_rows, 1)
    for which in range(2):
        pltpu.make_async_copy(pbuf.at[which], pbuf.at[which], p_sem.at[which]).wait()
    pmat[...] = pbuf[...].astype(BF16)
    other_tables.wait()

    def load_w(k):
        w_in(k).wait()
        base = lax.rem(k, depth) * per * 2 * chans
        for j in range(per):
            for part in range(2):
                vmix[k * per + j, pl.ds(part * chans, chans)] = work[
                    pl.ds(base + j * 2 * chans + part, chans, stride=2), :].astype(BF16)

        @pl.when(k + depth < parts)
        def _():
            w_in(k + depth).start()


    loop(parts, load_w)

    span = cmat.shape[3]
    mine_t = (lax.broadcasted_iota(jnp.int32, (8, lats), 1) == me * tl + lax.broadcasted_iota(jnp.int32, (8, lats), 0))
    mine_t &= lax.broadcasted_iota(jnp.int32, (8, lats), 0) < tl
    mine_t = jnp.where(mine_t, 1.0, 0.0).astype(BF16)

    def tabulate(d):
        z, of_core = lax.div(d, 2), lax.rem(d, 2)
        row = lax.broadcasted_iota(jnp.int32, (n, span), 0)
        p = jnp.where(of_core == 0, row - z, row + 1)
        target = jnp.where(p > held - 1, p + 1, p)
        moved = jnp.where(target == lax.broadcasted_iota(jnp.int32, (n, span), 1), 1.0, 0.0).astype(BF16)
        for which in range(2):
            picked = dot(mine_t, band[which, d].astype(BF16), ((1,), (1,))).astype(BF16)
            cmat[which, z, pl.ds(pl.multiple_of(of_core * 8, 8), 8), :] = dot(picked, moved)

    loop(n, tabulate)

    def no_degree(l):
        work[pl.ds(area + l * pitch + rows - tile, tile), :] = jnp.zeros((tile, chans), F32)

    loop(top, no_degree)

    pass_sums(0)

    def sum_first(ch):
        sum_rows(0, ch)

    loop(chunks, sum_first, 1)
    ship(0, final, 0, tl)
    loop(chunks, pass_sums, 1)

    sign = jnp.where(lax.broadcasted_iota(jnp.int32, (tile, chans), 0) < nb, -1.0, 1.0).astype(F32)

    def turn(values):
        groups = values.reshape(-1, tile, chans)
        return (pltpu.roll(groups, nb, 1) * sign[None]).reshape(values.shape)

    def legendre(src, dst, which, over):
        def mode(m):
            for k in range(tile):
                xb[:, k * chans:(k + 1) * chans] = work[
                    pl.ds(src + m * tile + k, lats, stride=pitch), :].astype(BF16)
            out = dot(pmat[which, m], xb[...], ((over,), (0,)))
            for k in range(tile):
                work[pl.ds(dst + m * tile + k, degs, stride=pitch), :] = out[:, k * chans:(k + 1) * chans]

        loop(ml - 1, mode)

    def unload(stage, ch):
        def body(src):
            for t in range(tl):
                work[pl.ds((src * tl + t) * pitch, rows), :] = recv[stage % 2, ch, src, t].astype(F32)

        loop(n, body)

    def load(slot):
        def body(dev):
            for t in range(tl):
                send[slot, dev, t] = work[pl.ds(area + (dev * tl + t) * pitch, rows), :].astype(BF16)

        loop(n, body)

    def only(ours, values):
        values = values.astype(F32)
        return jnp.where(ours, values, jnp.zeros_like(values)).astype(BF16)

    def spectral(stage, ch, into, kept, mix):
        arrived(stage - 1, ch)
        unload(stage - 1, ch)
        legendre(0, area, into, 1)
        finish_peak(into, ch)

        def degree(l):
            x = work[pl.ds(area + l * pitch, rows), :].astype(BF16)
            kept[l, ch] = x
            work[pl.ds(l * pitch, rows), :] = mix(l, x)

        loop(degs, degree, unroll=8)

        def keep_top(half_at, row, degree, ours):
            own[half_at, 2, ch, row] = only(ours, work[pl.ds((top + degree) * pitch + rows - tile, tile), :])

        pack(chip, keep_top)
        if stage == 1:
            swap = to(sibling, own.at[other_core, 2, ch], other.at[2, ch], swap_send.at[ch], swap_recv.at[ch])
            swap.start()
        legendre(0, area, 1 - into, 0)
        load(free_slot(stage, ch))
        if stage == 1:
            swap.wait()
            packs[core, chip, 2, ch] = (own[core, 2, ch].astype(F32) + other[2, ch].astype(F32)).astype(BF16)

            @pl.when(ch >= 2)
            def _():
                relay_top(ch - 2)

            for away in (2, -2):
                top_copy(0, away, ch, near_recv).start()
        else:
            @pl.when(ch == 0)
            def _():
                pass_sums(final - 1)
                sum_rows(1, final)

            @pl.when(ch == 1)
            def _():
                pass_sums(final)

        ship(stage, ch, 0, tl)

    def top_copy(source, away, ch, got):
        block = packs.at[core, chip_at(source), 2, ch]
        return to(across(away, core), block, block, top_send, got.at[ch])

    def top_blocks(count, ch):
        return packs.at[core, head(count), 2, ch]

    def relay_top(ch):
        pltpu.make_async_copy(top_blocks(2, ch), top_blocks(2, ch), near_recv.at[ch]).wait()
        for source in (2, -2):
            for away in (1, -1):
                top_copy(source, away, ch, far_recv).start()
        top_copy(-2 * way, 2 * way, ch, far_recv).start()

    def apply_top(which, ch, z):
        for h in range(2):
            qs[pl.ds(h * held * tile, held * tile), :] = packs[h, z, 2, ch].reshape(held * tile, chans).astype(F32)
        for k in range(tile):
            xb[0:span, k * chans:(k + 1) * chans] = qs[pl.ds(k, span, stride=tile), :].astype(BF16)
        out = dot(cmat[which, z].astype(BF16), xb[0:span, :])
        for k in range(tile):
            gather[pl.ds(k, 16, stride=tile), :] = out[:, k * chans:(k + 1) * chans]
        for c in range(2):
            for t in range(tl):
                recv[1, ch, 2 * z + c, t, pl.ds(rows - tile, tile)] = gather[
                    pl.ds((8 * c + t) * tile, tile), :].astype(BF16)

    def mix_forward(l, x):
        both = dot(x, vmix[l], ((1,), (1,)))
        return both[:, :chans] + turn(both[:, chans:])

    def mix_adjoint(l, x):
        both = dot(x, jnp.concatenate([vmix[l, head(chans)], vmix[l, pl.ds(chans, chans)]], axis=1))
        return both[:, :chans] - turn(both[:, chans:])

    def step2_chunk(ch):
        spectral(1, ch, 0, coef, mix_forward)

    loop(chunks, step2_chunk)
    relay_top(chunks - 2)

    def fetch_rows(stage, ch, t):
        for src in range(n):
            gather[pl.ds(src * rows, rows), :] = recv[stage % 2, ch, src, t].astype(F32)

    def fetch_pair(b):
        return jnp.concatenate(
            [gather[pl.ds(b, modes2, stride=nb), :], gather[pl.ds(b + 1, modes2, stride=nb), :]], axis=1).astype(BF16)

    def step3_chunk(ch):
        arrived(1, ch)
        pltpu.make_async_copy(top_blocks(5, ch), top_blocks(5, ch), far_recv.at[ch]).wait()
        swap = to(sibling, top_blocks(chips, ch), top_blocks(chips, ch), swap_send.at[ch], swap_recv.at[ch])
        swap.start()

        @pl.when(ch == 0)
        def _():
            relay_top(final)

        swap.wait()

        @pl.when(ch == final)
        def _():
            all_sent = packs.at[0, head(7), 2]
            pltpu.make_async_copy(all_sent, all_sent, top_send).wait()

        def apply(z):
            apply_top(1, ch, z)

        loop(chips, apply)

        @pl.when(ch == 1)
        def _():
            sum_rows(1, 0)

        slot = free_slot(2, ch)

        def row(t):
            unit = ch * tl + t
            step_in(dg_hbm, unit)
            buf = in_slot(unit)
            fetch_rows(1, ch, t)
            for b in range(0, nb, 2):
                g = fetch_pair(b)
                hidden = dot(syn_h[...], g) + dot(syn_l[...], g)
                pair = jnp.concatenate([inbuf[buf, b], inbuf[buf, b + 1]], axis=1)
                spec = transform(pair * gelu_grad(hidden), dbl_h, dbl_l)
                gather[pl.ds(b, modes2, stride=nb), :] = spec[:, :chans]
                gather[pl.ds(b + 1, modes2, stride=nb), :] = spec[:, chans:]
            put_rows(slot, t)

        loop(tl, row)
        send_peak(2, ch)

        @pl.when(ch < final)
        def _():
            ship(2, ch, 0, tl)


    loop(chunks, step3_chunk)

    def sum_second(ch):
        pass_sums(ch - 1)
        sum_rows(1, ch)

    loop(final, sum_second, 1)
    ship(2, final, 0, tl)
    start_in(dg_hbm)

    def step4_chunk(ch):
        spectral(3, ch, 1, dq, mix_adjoint)

    loop(chunks, step4_chunk)

    for which, kept in enumerate((coef, dq)):
        def keep_low(half_at, row, degree, ours):
            own[half_at, which, :, row] = only(ours, kept[degree, :, head(tile)])

        pack(chip, keep_low)

    def both_parts(peer, action):
        degree = n + first_mode(peer)
        for which, kept in enumerate((coef, dq)):
            action(to(peer, kept.at[degree, :, head(tile)], second.at[which, me, :, head(tile)],
                      always_send, always_recv))

            @pl.when(first_mode(me) <= first_mode(peer))
            def _():
                more = pl.ds(tile, tile)
                action(to(peer, kept.at[degree, :, more], second.at[which, me, :, more],
                          some_send, some_recv))

    def send_second(k):
        both_parts(lax.rem(me + k, n), lambda copy: copy.start())

    loop(n, send_second, 1)
    for which, kept in enumerate((coef, dq)):
        second[which, me] = kept[n + first_mode(me), :, head(2 * tile)]

    def clear_second(src):
        @pl.when(first_mode(src) > first_mode(me))
        def _():
            for which in range(2):
                second[which, src, :, pl.ds(tile, tile)] = jnp.zeros((chunks, tile, chans), BF16)

    loop(n, clear_second)
    own_copy = to(sibling, own.at[other_core], other, own_send, own_recv)
    own_copy.start()

    def pack_block(k):
        return packs.at[core, chip_at(-way * k)]

    def pack_copy(k):
        return to(onward, pack_block(k), pack_block(k), pack_send, pack_recv.at[k])

    def share(k):
        to(sibling, pack_block(k), pack_block(k), share_send, share_recv).start()

    half = degs // n - 2
    wide = 2 * chans
    block_rows = half * wide
    piece = block_rows // pieces
    hops = (last) * pieces

    def block_at(k, direction):
        return lax.rem(chip - direction * (1 + k) + 2 * chips, chips)

    def outer(dst, row, pairs):
        real = jnp.zeros((chans, chans), F32)
        imag = jnp.zeros((chans, chans), F32)
        for y, x in pairs:
            real += dot(y, x, ((0,), (0,)))
            imag -= dot(turn(y.astype(F32)).astype(BF16), x, ((0,), (0,)))
        dst[pl.ds(row, chans, stride=2), :] = real
        dst[pl.ds(row + 1, chans, stride=2), :] = imag

    def first_degree(block, of_core):
        return 2 * n + (2 * block + of_core) * half

    def weight_grad(dst, degree):
        def one(j):
            outer(dst, j * wide, [(dq[degree + j, ch], coef[degree + j, ch]) for ch in range(chunks)])

        loop(half, one)

    def pair_copy(k):
        slot = lax.rem(k, 2)
        rows_there = pl.ds(first_degree(block_at(k, -way), core) * wide, block_rows)
        return to(sibling, wbuf.at[slot, head(block_rows)], dw_out.at[rows_there],
                  pair_send.at[slot], pair_recv.at[k])

    def weight_block(k):
        @pl.when(k >= 2)
        def _():
            pair_copy(k - 2).wait_send()
        weight_grad(wbuf.at[lax.rem(k, 2)], first_degree(block_at(k, -way), other_core))
        pair_copy(k).start()
        block = block_at(k, way)
        weight_grad(work.at[pl.ds(block * block_rows, block_rows)], first_degree(block, core))

    loop(chips, weight_block)
    pair_copy(chips - 2).wait_send()
    pair_copy(last).wait_send()
    own_copy.wait()
    packs[core, chip] = (own[core].astype(F32) + other[...].astype(F32)).astype(BF16)

    def low_degree(l):
        def one(z):
            for c in range(2):
                p = l - z if c == 0 else l + 1
                ours = p >= 0 if c == 0 else p >= n - z
                p = jnp.maximum(p, 0)
                h = jnp.where(p > held - 1, 1, 0)
                for which in range(2):
                    lowx[which, 2 * z + c] = only(ours, packs[h, z, which, :, p - h * (held - 1)])

        loop(chips, one)
        outer(wbuf.at[0], 0, [(lowx[1].reshape(-1, chans), lowx[0].reshape(-1, chans))])
        dw_out[pl.ds(l * wide, wide)] = wbuf[0, head(wide)]

    def final_rows(unit):
        ch, t = unit_of(unit)

        step_in(dg_hbm, unit)
        buf = in_slot(unit)

        fetch_rows(3, ch, t)
        for b in range(0, nb, 2):
            g = fetch_pair(b)
            change = dot(adj_h[...], g) + dot(adj_l[...], g)
            df_out[ch * nb + b, t] = inbuf[buf, b] + change[:, :chans]
            df_out[ch * nb + b + 1, t] = inbuf[buf, b + 1] + change[:, chans:]

    def place(i, of_core):
        block = block_at(lax.div(i, pieces), way)
        start = lax.rem(i, pieces) * piece
        return pl.ds(block * block_rows + start, piece), pl.ds(first_degree(block, of_core) * wide + start, piece)

    def rs_copy(i):
        here, there = place(i, core)
        return to(onward, work.at[here], dw_out.at[there], rs_send, rs_recv.at[i])

    def add_pair(i):
        here, passed = place(i, other_core)

        @pl.when(lax.rem(i, pieces) == 0)
        def _():
            pair_copy(lax.div(i, pieces)).wait_recv()

        work[here] += dw_out[passed]

    def rs_step(i):
        add_pair(i)

        @pl.when(i >= pieces)
        def _():
            rs_copy(i - pieces).wait_recv()
            here, there = place(i, core)
            work[here] += dw_out[there]

        rs_copy(i).start()

        @pl.when(lax.rem(i, pieces) == 0)
        def _():
            k = lax.div(i, pieces)

            @pl.when(k > 0)
            def _():
                pack_copy(k - 1).wait_recv()

            pack_copy(k).start()
            share(k)


    loop(hops, rs_step)
    pack_copy(chips - 2).wait_recv()
    share(last)

    def own_sum(s):
        i = hops + s
        add_pair(i)
        rs_copy(i - pieces).wait_recv()
        here, there = place(i, core)
        dw_out[there] += work[here]
        ag_copy(i, s).start()

    def second_spot(k):
        return pl.ds((n + first_mode(2 * block_at(k, way) + core)) * wide, wide)

    def second_copy(k, got):
        spot = dw_out.at[second_spot(k)]
        return to(onward, spot, spot, ag_send, ag_recv.at[hops + got])

    def second_publish(k):
        spot = dw_out.at[second_spot(k)]
        to(sibling, spot, spot, pub_send, pub_recv).start()

    def ag_copy(i, got):
        _, there = place(i, core)
        return to(onward, dw_out.at[there], dw_out.at[there], ag_send, ag_recv.at[got])

    def publish(i):
        _, there = place(i, core)
        to(sibling, dw_out.at[there], dw_out.at[there], pub_send, pub_recv).start()

    firsts = second.at[:, head(n - 1), :, head(tile)]
    pltpu.make_async_copy(firsts, firsts, always_recv).wait()

    comes, goes = first_mode(me), n - 1 - first_mode(me)

    def wait_some(count, sem):
        for k in range(1, n):
            @pl.when(count == k)
            def _():
                part = second.at[:, head(k), :, pl.ds(tile, tile)]
                pltpu.make_async_copy(part, part, sem).wait()

    wait_some(comes, some_recv)
    outer(wbuf.at[0], 0, [(second[1].reshape(-1, chans), second[0].reshape(-1, chans))])
    dw_out[second_spot(last)] = wbuf[0, head(wide)]
    loop(pieces, own_sum)
    second_copy(last, 0).start()

    pl.semaphore_signal(free_sem, inc=1, device_id={axis: sibling}, device_id_type=pl.DeviceIdType.MESH)
    pl.semaphore_wait(free_sem, 1)

    def own_piece(s):
        publish(hops + s)

    loop(pieces, own_piece)
    second_publish(last)
    gathered = packs.at[other_core]
    pltpu.make_async_copy(gathered, gathered, share_recv).wait()

    def task(i):
        @pl.when(i < chips)
        def _():
            for ch in range(chunks):
                @pl.when(i == 0)
                def _():
                    arrived(3, ch)
                apply_top(0, ch, i)

        @pl.when((i >= chips) & (i < chips + units))
        def _():
            final_rows(i - chips)

        @pl.when(i < n)
        def _():
            low_degree(i)

    def ag_step(i):
        ag_copy(i, i).wait_recv()

        @pl.when(i + pieces < hops)
        def _():
            ag_copy(i, i + pieces).start()

        publish(i)

        @pl.when(lax.rem(i, pieces) == pieces - 1)
        def _():
            k = lax.div(i, pieces)
            second_copy(k, k).wait_recv()

            @pl.when(k < chips - 2)
            def _():
                second_copy(k, k + 1).start()

            second_publish(k)

        task(i)

    loop(hops, ag_step)

    def rest(i):
        task(i)

    loop(max(hops, chips + units, n), rest, hops)

    wait_sent(2 * chunks + final, 2)
    for ch in range(chunks):
        wait_sent(3 * chunks + ch, 3)
    for ch in range(chunks):
        pltpu.make_async_copy(sums.at[ch], sums.at[ch], sum_send.at[ch]).wait()
    sent = work.at[head((last) * block_rows)]
    pltpu.make_async_copy(sent, sent, rs_send).wait()
    sent = dw_out.at[head((last) * (block_rows + wide))]
    pltpu.make_async_copy(sent, sent, ag_send).wait()
    pltpu.make_async_copy(firsts, firsts, always_send).wait()

    wait_some(goes, some_send)
    sent = packs.at[0, head(last)]
    pltpu.make_async_copy(sent, sent, pack_send).wait()
    pltpu.make_async_copy(packs.at[0], packs.at[0], share_send).wait()
    shared = dw_out.at[head(chips * (block_rows + wide))]
    pltpu.make_async_copy(shared, shared, pub_send).wait()
    pltpu.make_async_copy(shared, shared, pub_recv).wait()


def put_kernel(df_ref, dw_ref, df_hbm, dw_hbm, sems):
    copies = []
    for source, target, parts in ((df_ref, df_hbm, 6), (dw_ref, dw_hbm, 12)):
        size = source.shape[0] // parts
        for k in range(parts):
            part = pl.ds(k * size, size)
            copies.append(pltpu.make_async_copy(source.at[part], target.at[part], sems.at[len(copies)]))
    for copy in copies:
        copy.start()
    for copy in copies:
        copy.wait()


def solution(mesh):
    n = mesh.shape['lat']
    field_spec = P('member', None, 'lat', None)

    def local_step(field_loc, grad_loc, p_fwd, p_inv, w_mix):
        batch, chans, tl, lons = field_loc.shape
        degs, lats = p_fwd.shape[1:]
        ml = p_fwd.shape[0] // n
        nb = 4
        chunks = batch // nb
        rows = ml * 2 * nb
        pitch = rows + 1
        half = degs // n - 2
        pieces = 4 if half * 2 * chans % 32 == 0 else 1
        hops = (n // 2 - 1) * pieces
        per = 4
        area = max(2 * lats * pitch, n // 2 * half * 2 * chans)
        depth = min(degs // per, area // (per * 2 * chans))
        held = n // 2 + 1
        packed = (3, chunks, held, 2 * nb, chans)
        tables = fourier_tables(n, ml, lons)
        anywhere = pl.BlockSpec(memory_space=pl.ANY)
        vmem = pl.BlockSpec(memory_space=pltpu.VMEM)
        grad_field, grad_w = pl.pallas_call(
            functools.partial(layer_kernel, 'lat', n, nb, pieces, per, depth),
            name='layer',
            out_shape=(
                pltpu.VMEM((batch, tl, lons, chans), F32),
                pltpu.VMEM((degs * 2 * chans, chans), F32),
            ),
            in_specs=[anywhere] * 6,
            out_specs=(vmem, vmem),
            scratch_shapes=[
                pltpu.VMEM((2, chunks, n, tl, rows, chans), BF16),
                pltpu.VMEM((chunks + 1, n, tl, rows, chans), BF16),
                pltpu.VMEM((area, chans), F32),
                pltpu.VMEM((lats, 2 * nb * chans), BF16),
                pltpu.VMEM((degs, chunks, rows, chans), BF16),
                pltpu.VMEM((degs, chunks, rows, chans), BF16),
                pltpu.VMEM((degs, 2 * chans, chans), BF16),
                pltpu.VMEM((2, max(per, half) * 2 * chans, chans), F32),
                pltpu.VMEM((4, nb, lons, chans), F32),
                pltpu.VMEM((n * rows, chans), F32),
                pltpu.VMEM((2, ml, degs, lats), F32),
                pltpu.VMEM((2, ml, degs, lats), BF16),
                pltpu.VMEM((2, n, n, lats), F32),
                pltpu.VMEM((2, n // 2, 16, 32), F32),
                pltpu.VMEM((32 * 2 * nb, chans), F32),
                pltpu.VMEM((2,) + packed, BF16),
                pltpu.VMEM(packed, BF16),
                pltpu.VMEM((2, n // 2) + packed, BF16),
                pltpu.VMEM((2, n, chunks, 2 * nb, chans), BF16),
                pltpu.VMEM(tables.shape, BF16),
                pltpu.VMEM((chunks, 5, 6, tl, 2 * nb, chans), BF16),
                pltpu.VMEM((2, 4, held, 2 * nb, chans), F32),
                pltpu.VMEM((chunks, 4, held, 2 * nb, chans), F32),
                pltpu.VMEM((chunks, 4, held, 2 * nb, chans), F32),
                pltpu.VMEM((chunks, 2, held, 2 * nb, chans), F32),
                pltpu.VMEM((chunks, 2, held, 2 * nb, chans), F32),
                pltpu.VMEM((chunks, 2, held, 2 * nb, chans), F32),
                pltpu.VMEM((2, n, chunks, 4 * nb, chans), BF16),
                pltpu.SemaphoreType.DMA((4 * chunks,)),
                pltpu.SemaphoreType.DMA((4 * chunks,)),
                pltpu.SemaphoreType.DMA((4,)),
                pltpu.SemaphoreType.DMA((depth,)),
                pltpu.SemaphoreType.DMA((2,)),
                pltpu.SemaphoreType.DMA((2,)),
                pltpu.SemaphoreType.DMA((2,)),
                pltpu.SemaphoreType.DMA((n // 2,)),
                pltpu.SemaphoreType.DMA,
                pltpu.SemaphoreType.DMA((hops,)),
                pltpu.SemaphoreType.DMA,
                pltpu.SemaphoreType.DMA((hops + n // 2 - 1,)),
                pltpu.SemaphoreType.REGULAR,
                pltpu.SemaphoreType.DMA,
                pltpu.SemaphoreType.DMA,
                pltpu.SemaphoreType.DMA,
                pltpu.SemaphoreType.DMA,
                pltpu.SemaphoreType.DMA,
                pltpu.SemaphoreType.DMA((n // 2 - 1,)),
                pltpu.SemaphoreType.DMA,
                pltpu.SemaphoreType.DMA,
                pltpu.SemaphoreType.DMA((2,)),
                pltpu.SemaphoreType.DMA,
                pltpu.SemaphoreType.DMA((chunks,)),
                pltpu.SemaphoreType.DMA((chunks,)),
                pltpu.SemaphoreType.DMA((chunks,)),
                pltpu.SemaphoreType.DMA((chunks,)),
                pltpu.SemaphoreType.DMA((chunks,)),
                pltpu.SemaphoreType.DMA((chunks,)),
                pltpu.SemaphoreType.DMA((chunks,)),
                pltpu.SemaphoreType.DMA((chunks,)),
                pltpu.SemaphoreType.DMA((chunks,)),
                pltpu.SemaphoreType.DMA((chunks,)),
                pltpu.SemaphoreType.DMA((chunks,)),
                pltpu.SemaphoreType.DMA((chunks,)),
                pltpu.SemaphoreType.DMA,
                pltpu.SemaphoreType.DMA,
                pltpu.SemaphoreType.DMA,
                pltpu.SemaphoreType.DMA,
                pltpu.SemaphoreType.DMA((chunks,)),
            ],
            compiler_params=pltpu.CompilerParams(
                collective_id=0, has_side_effects=True, vmem_limit_bytes=43 * 1024 * 1024),
        )(
            field_loc.transpose(0, 2, 3, 1), grad_loc.transpose(0, 2, 3, 1),
            w_mix.transpose(0, 1, 3, 2).reshape(degs * 2 * chans, chans),
            p_fwd, p_inv, tables)
        grad_field, grad_w = pl.pallas_call(
            put_kernel,
            name='put',
            out_shape=(
                jax.ShapeDtypeStruct(grad_field.shape, F32),
                jax.ShapeDtypeStruct(grad_w.shape, F32),
            ),
            in_specs=[vmem] * 2,
            out_specs=(anywhere, anywhere),
            scratch_shapes=[pltpu.SemaphoreType.DMA((18,))],
            compiler_params=pltpu.CompilerParams(vmem_limit_bytes=1024 * 1024),
        )(grad_field, grad_w)
        return grad_field.transpose(0, 3, 1, 2), grad_w.reshape(degs, chans, 2, chans).transpose(0, 1, 3, 2)

    return jax.shard_map(
        local_step, mesh=mesh, in_specs=(field_spec, field_spec, P(), P(), P()),
        out_specs=(field_spec, P('member', None, None, None)), check_vma=False)
```

```python
import functools
import math

import jax
import jax.numpy as jnp
import numpy as np
from jax import lax
from jax.experimental import pallas as pl
from jax.experimental.pallas import tpu as pltpu
from jax.sharding import PartitionSpec as P

F32 = jnp.float32
BF16 = jnp.bfloat16


def split_const(matrix):
    head = matrix.astype(BF16)
    tail = (matrix - head.astype(np.float64)).astype(BF16)
    return [head, tail]


def fourier_tables(n, ml, lons):
    modes = n * ml
    device = np.arange(n)
    first = np.where(device % 2 == 0, device // 2, n - 1 - device // 2)
    order = (first[:, None] + n * np.arange(ml)[None, :]).reshape(-1)
    angle = math.tau * (np.outer(order, np.arange(lons)) % lons) / lons
    forward = np.stack([np.cos(angle), -np.sin(angle)], axis=1).reshape(2 * modes, lons) / math.sqrt(lons)
    gains = np.repeat(2.0 - (order == 0), 2)[:, None]
    doubled = forward * gains
    tables = split_const(forward) + split_const(doubled) + split_const(doubled.T) + split_const(forward.T)
    return jnp.stack([jnp.asarray(t) for t in tables])


def gelu_grad(values):
    cumulative = 0.5 * (1.0 + lax.erf(values * math.sqrt(0.5)))
    density = jnp.exp(-0.5 * values * values) / math.sqrt(math.tau)
    return cumulative + values * density


def loop(stop, step, start=0, unroll=None):
    def one(i, carry):
        step(i)
        return carry

    lax.fori_loop(start, stop, one, 0, unroll=unroll)


def head(size):
    return pl.ds(0, size)


def dot(a, b, dims=((1,), (0,))):
    return lax.dot_general(a, b, (dims, ((), ())), preferred_element_type=F32)


def layer_kernel(
    axis, n, nb, pieces, per, depth,
    f_hbm, dg_hbm, w_hbm, pf_hbm, pv_hbm, tab_hbm,
    df_out, dw_out,
    recv, send, work, xb, coef, dq, vmix, wbuf, inbuf, gather, pbuf, pmat, band, cmat, qs, own, other, packs, lowx, tab,
    topin, partial, mid, sums, sumin, joined, handed, second,
    send_sem, recv_sem, in_sem, w_sem, p_sem, band_sem, pair_send, pair_recv, rs_send, rs_recv, ag_send, ag_recv,
    free_sem, pub_send, pub_recv, own_send, own_recv, pack_send, pack_recv, share_send, share_recv,
    tab_sem, top_send, near_recv, far_recv, swap_send, swap_recv,
    row_send, row_recv, mid_send, mid_recv, sum_send, sum_recv, join_send, join_recv,
    always_send, always_recv, some_send, some_recv, hand_recv,
):
    me = lax.axis_index(axis)
    batch, tl, lons, chans = f_hbm.shape
    ml, degs, lats = pmat.shape[1:]
    chunks = batch // nb
    tile = 2 * nb
    rows = ml * tile
    pitch = rows + 1
    modes2 = 2 * n * ml
    units = chunks * tl
    final = chunks - 1
    slots = chunks + 1
    fwd_h, fwd_l, dbl_h, dbl_l, syn_h, syn_l, adj_h, adj_l = (tab.at[k] for k in range(8))
    area = lats * pitch
    top = n * (ml - 1)
    held = n // 2 + 1
    chip, core = lax.div(me, 2), lax.rem(me, 2)
    other_core = 1 - core
    chips = n // 2
    last = chips - 1
    way = 1 - 2 * core
    sibling = me + way

    def chip_at(away):
        return lax.rem(chip + away + chips, chips)

    def across(away, its_core):
        return 2 * chip_at(away) + its_core

    onward = across(way, core)

    def around(k):
        far = chips // 2 - lax.div(k + 1, 2)
        return jnp.where(lax.rem(k, 2) == 0, far, -far)

    def first_mode(device):
        z = lax.div(device, 2)
        return jnp.where(lax.rem(device, 2) == 0, z, n - 1 - z)

    def to(device, src, dst, sent, got):
        return pltpu.make_async_remote_copy(
            src_ref=src, dst_ref=dst, send_sem=sent, recv_sem=got,
            device_id={axis: device}, device_id_type=pl.DeviceIdType.MESH)

    def unit_of(unit):
        return lax.div(unit, tl), lax.rem(unit, tl)

    def unit_in(src, unit):
        ch, t = unit_of(unit)
        slot = lax.rem(unit, 2)
        return pltpu.make_async_copy(src.at[pl.ds(ch * nb, nb), t], inbuf.at[slot], in_sem.at[slot])

    def step_in(src, unit):
        @pl.when(unit + 1 < units)
        def _():
            unit_in(src, unit + 1).start()
        unit_in(src, unit).wait()

    body, peak = head(rows - tile), pl.ds(rows - tile, tile)

    def ship(stage, ch, t0, nt):
        index = stage * chunks + ch
        slot = lax.rem(index, slots)
        part = pl.ds(t0, nt)

        def one(k):
            away = around(k)
            for its_core in (core, other_core):
                peer = across(away, its_core)
                to(peer, send.at[slot, peer, part, body], recv.at[stage % 2, ch, me, part, body],
                   send_sem.at[index], recv_sem.at[index]).start()

        loop(last, one)
        to(sibling, send.at[slot, sibling, part, body], recv.at[stage % 2, ch, me, part, body],
           send_sem.at[index], recv_sem.at[index]).start()
        recv[stage % 2, ch, me, part, body] = send[slot, me, part, body]

    def arrived(stage, ch):
        others = recv.at[stage % 2, ch, head(n - 1), :, body]
        pltpu.make_async_copy(others, others, recv_sem.at[stage * chunks + ch]).wait()

    def peaks():
        return send.at[0, head(n - 5), :, peak]

    def wait_sent(index, stage):
        others = send.at[lax.rem(index, slots), head(n - 1), :, body]
        pltpu.make_async_copy(others, others, send_sem.at[index]).wait()
        if stage % 2 == 0:
            ch = index - stage * chunks
            pltpu.make_async_copy(peaks(), peaks(), row_send.at[ch]).wait()

    def send_peak(stage, ch):
        slot = lax.rem(stage * chunks + ch, slots)
        far = chips // 2
        for same in (True, False):
            its_core = core if same else other_core
            for away in range(1 - far, far + 1):
                near = max(-2, min(2, away))
                hop, target, apart = away - near, (0, 2, 4, 3, 1)[near], abs(away - near)
                if away == far:
                    hop = jnp.where(its_core == 0, 2 - far, far - 2)
                    target = jnp.where(its_core == 0, 3, 4)
                source = send.at[slot, across(away, its_core), :, peak]
                place = topin.at[ch, target, 2 * apart + core]
                if same and not apart:
                    place[...] = source[...]
                else:
                    to(across(hop, its_core), source, place,
                       row_send.at[ch], row_recv.at[ch]).start()

    def free_slot(stage, ch):
        index = stage * chunks + ch
        if stage >= 1:
            @pl.when(ch >= 1)
            def _():
                wait_sent(index - slots, stage - 1)
        if stage >= 2:
            @pl.when(ch == 0)
            def _():
                wait_sent(index - slots, stage - 2)
        return lax.rem(index, slots)

    def put_rows(slot, t):
        send[slot, :, t] = gather[...].reshape(n, rows, chans).astype(BF16)

    def transform(values, head, tail):
        high = values.astype(BF16)
        low = (values - high.astype(F32)).astype(BF16)
        return dot(head[...], high) + (dot(tail[...], high) + dot(head[...], low))

    unit_in(f_hbm, 0).start()
    first_tables = pltpu.make_async_copy(tab_hbm.at[head(2)], tab.at[head(2)], tab_sem.at[0])
    other_tables = pltpu.make_async_copy(tab_hbm.at[pl.ds(2, 6)], tab.at[pl.ds(2, 6)], tab_sem.at[1])
    first_tables.start()
    barrier = pltpu.get_barrier_semaphore()

    def announce(k):
        pl.semaphore_signal(barrier, inc=1, device_id={axis: lax.rem(me + k, n)}, device_id_type=pl.DeviceIdType.MESH)

    loop(n, announce, 1)

    first_tables.wait()

    group = max(1, tl // 3)

    parts = degs // per

    def w_in(k):
        slot = lax.rem(k, depth)
        return pltpu.make_async_copy(
            w_hbm.at[pl.ds(k * per * 2 * chans, per * 2 * chans)],
            work.at[pl.ds(slot * per * 2 * chans, per * 2 * chans)], w_sem.at[slot])

    def band_in(d):
        for which, source in enumerate((pf_hbm, pv_hbm)):
            pltpu.make_async_copy(
                source.at[top + first_mode(d), pl.ds(top, n)], band.at[which, d], band_sem.at[which]).start()

    def step1_chunk(ch):
        slot = free_slot(0, ch)

        def row(t):
            unit = ch * tl + t
            step_in(f_hbm, unit)
            buf = lax.rem(unit, 2)
            for b in range(0, nb, 2):
                pair = jnp.concatenate([inbuf[buf, b], inbuf[buf, b + 1]], axis=1)
                spec = transform(pair, fwd_h, fwd_l)
                gather[pl.ds(b, modes2, stride=nb), :] = spec[:, :chans]
                gather[pl.ds(b + 1, modes2, stride=nb), :] = spec[:, chans:]
            put_rows(slot, t)

            @pl.when((ch == 0) & (t == group - 1))
            def _():
                pl.semaphore_wait(barrier, n - 1)
                ship(0, 0, 0, group)


        loop(tl, row)
        send_peak(0, ch)

        @pl.when(ch == 0)
        def _():
            ship(0, 0, group, tl - group)
            other_tables.start()
            for which, source in enumerate((pf_hbm, pv_hbm)):
                for k in range(ml):
                    pltpu.make_async_copy(
                        source.at[first_mode(me) + n * k], pbuf.at[which, k], p_sem.at[which]).start()
            loop(n, band_in)
            for k in range(depth):
                w_in(k).start()


    loop(chunks, step1_chunk)

    unit_in(dg_hbm, 0).start()
    for which in range(2):
        pltpu.make_async_copy(band.at[which], band.at[which], band_sem.at[which]).wait()
    qs[...] = jnp.zeros_like(qs)

    def pack(z, store):
        def one(index):
            half_at, row = lax.div(index, held), lax.rem(index, held)
            p = half_at * (held - 1) + row
            degree = jnp.where(core == 0, jnp.minimum(z + p, n - 1), jnp.maximum(p - 1, 0))
            store(half_at, row, degree, (p < n - z) == (core == 0))

        loop(2 * held, one)

    def project(which, ch, target, device):
        gather[...] = jnp.zeros_like(gather)
        side = 1 if target == 3 else -1

        def place_rows(apart):
            for c in range(2):
                src = across(side * apart, c)
                gather[pl.ds(pl.multiple_of(src * tl * tile, tile), tl * tile), :] = topin[
                    ch, target, 2 * apart + c].reshape(tl * tile, chans).astype(F32)

        place_rows(0)
        if target > 2:
            place_rows(1)

            @pl.when(core == target - 3)
            def _():
                place_rows(2)

        for k in range(tile):
            xb[:, k * chans:(k + 1) * chans] = gather[pl.ds(k, lats, stride=tile), :].astype(BF16)
        out = dot(band[which, device].astype(BF16), xb[...])
        for k in range(tile):
            qs[pl.ds(k, n, stride=tile), :] = out[:, k * chans:(k + 1) * chans]

    def sum_rows(which, ch):
        pltpu.make_async_copy(peaks(), peaks(), row_recv.at[ch]).wait()
        for target, away in enumerate((-1, 1, -2, 2)):
            project(which, ch, target + 1, across(away, core))

            def keep(half_at, row, degree, ours):
                values = qs[pl.ds(pl.multiple_of(degree * tile, tile), tile), :]
                partial[half_at, target, row] = jnp.where(ours, values, jnp.zeros_like(values))

            pack(chip_at(away), keep)
        swap = to(sibling, partial.at[other_core], mid.at[ch], mid_send.at[ch], mid_recv.at[ch])
        swap.start()
        if which == 1:
            pltpu.make_async_copy(sums.at[ch], sums.at[ch], sum_send.at[ch]).wait()
        swap.wait()
        sums[ch] = partial[core] + mid[ch]
        for side, away in enumerate((-1, 1)):
            to(across(away, core), sums.at[ch, 2 + side], handed.at[ch, side],
               sum_send.at[ch], hand_recv.at[ch]).start()

    def pass_sums(ch):
        pltpu.make_async_copy(handed.at[ch], handed.at[ch], hand_recv.at[ch]).wait()
        for side, away in enumerate((-1, 1)):
            sums[ch, side] += handed[ch, side]
            to(across(away, core), sums.at[ch, side], sumin.at[ch, side],
               sum_send.at[ch], sum_recv.at[ch]).start()

    def finish_peak(which, ch):
        pltpu.make_async_copy(sumin.at[ch], sumin.at[ch], sum_recv.at[ch]).wait()
        joined[ch, core] = sumin[ch, 0] + sumin[ch, 1]
        swap = to(sibling, joined.at[ch, core], joined.at[ch, core], join_send.at[ch], join_recv.at[ch])
        swap.start()
        project(which, ch, 0, me)
        swap.wait()

        def one(degree):
            p = jnp.where(core == 0, degree - chip, degree + 1)
            ours = degree >= first_mode(me)
            p = jnp.maximum(p, 0)
            h = jnp.where(p > held - 1, 1, 0)
            come = joined[ch, h, p - h * (held - 1)]
            work[pl.ds(area + (top + degree) * pitch + rows - tile, tile), :] = qs[
                pl.ds(pl.multiple_of(degree * tile, tile), tile), :] + jnp.where(ours, come, jnp.zeros_like(come))

        loop(n, one)

    sum_rows(0, 0)

    def ship_rows(ch):
        ship(0, ch, 0, tl)

    loop(final, ship_rows, 1)
    for which in range(2):
        pltpu.make_async_copy(pbuf.at[which], pbuf.at[which], p_sem.at[which]).wait()
    pmat[...] = pbuf[...].astype(BF16)
    other_tables.wait()

    def load_w(k):
        w_in(k).wait()
        base = lax.rem(k, depth) * per * 2 * chans
        for j in range(per):
            for part in range(2):
                vmix[k * per + j, pl.ds(part * chans, chans)] = work[
                    pl.ds(base + j * 2 * chans + part, chans, stride=2), :].astype(BF16)

        @pl.when(k + depth < parts)
        def _():
            w_in(k + depth).start()


    loop(parts, load_w)

    span = cmat.shape[3]
    mine_t = (lax.broadcasted_iota(jnp.int32, (8, lats), 1) == me * tl + lax.broadcasted_iota(jnp.int32, (8, lats), 0))
    mine_t &= lax.broadcasted_iota(jnp.int32, (8, lats), 0) < tl
    mine_t = jnp.where(mine_t, 1.0, 0.0).astype(BF16)

    def tabulate(d):
        z, of_core = lax.div(d, 2), lax.rem(d, 2)
        row = lax.broadcasted_iota(jnp.int32, (n, span), 0)
        p = jnp.where(of_core == 0, row - z, row + 1)
        target = jnp.where(p > held - 1, p + 1, p)
        moved = jnp.where(target == lax.broadcasted_iota(jnp.int32, (n, span), 1), 1.0, 0.0).astype(BF16)
        for which in range(2):
            picked = dot(mine_t, band[which, d].astype(BF16), ((1,), (1,))).astype(BF16)
            cmat[which, z, pl.ds(pl.multiple_of(of_core * 8, 8), 8), :] = dot(picked, moved)

    loop(n, tabulate)

    def no_degree(l):
        work[pl.ds(area + l * pitch + rows - tile, tile), :] = jnp.zeros((tile, chans), F32)

    loop(top, no_degree)

    pass_sums(0)

    def sum_first(ch):
        sum_rows(0, ch)

    loop(chunks, sum_first, 1)
    ship(0, final, 0, tl)
    loop(chunks, pass_sums, 1)

    sign = jnp.where(lax.broadcasted_iota(jnp.int32, (tile, chans), 0) < nb, -1.0, 1.0).astype(F32)

    def turn(values):
        groups = values.reshape(-1, tile, chans)
        return (pltpu.roll(groups, nb, 1) * sign[None]).reshape(values.shape)

    def legendre(src, dst, which, over):
        def mode(m):
            for k in range(tile):
                xb[:, k * chans:(k + 1) * chans] = work[
                    pl.ds(src + m * tile + k, lats, stride=pitch), :].astype(BF16)
            out = dot(pmat[which, m], xb[...], ((over,), (0,)))
            for k in range(tile):
                work[pl.ds(dst + m * tile + k, degs, stride=pitch), :] = out[:, k * chans:(k + 1) * chans]

        loop(ml - 1, mode)

    def unload(stage, ch):
        def body(src):
            for t in range(tl):
                work[pl.ds((src * tl + t) * pitch, rows), :] = recv[stage % 2, ch, src, t].astype(F32)

        loop(n, body)

    def load(slot):
        def body(dev):
            for t in range(tl):
                send[slot, dev, t] = work[pl.ds(area + (dev * tl + t) * pitch, rows), :].astype(BF16)

        loop(n, body)

    def only(ours, values):
        values = values.astype(F32)
        return jnp.where(ours, values, jnp.zeros_like(values)).astype(BF16)

    def spectral(stage, ch, into, kept, mix):
        arrived(stage - 1, ch)
        unload(stage - 1, ch)
        legendre(0, area, into, 1)
        finish_peak(into, ch)

        def degree(l):
            x = work[pl.ds(area + l * pitch, rows), :].astype(BF16)
            kept[l, ch] = x
            work[pl.ds(l * pitch, rows), :] = mix(l, x)

        loop(degs, degree, unroll=8)

        def keep_top(half_at, row, degree, ours):
            own[half_at, 2, ch, row] = only(ours, work[pl.ds((top + degree) * pitch + rows - tile, tile), :])

        pack(chip, keep_top)
        if stage == 1:
            swap = to(sibling, own.at[other_core, 2, ch], other.at[2, ch], swap_send.at[ch], swap_recv.at[ch])
            swap.start()
        legendre(0, area, 1 - into, 0)
        load(free_slot(stage, ch))
        if stage == 1:
            swap.wait()
            packs[core, chip, 2, ch] = (own[core, 2, ch].astype(F32) + other[2, ch].astype(F32)).astype(BF16)

            @pl.when(ch >= 2)
            def _():
                relay_top(ch - 2)

            for away in (2, -2):
                top_copy(0, away, ch, near_recv).start()
        else:
            @pl.when(ch == 0)
            def _():
                pass_sums(final - 1)
                sum_rows(1, final)

            @pl.when(ch == 1)
            def _():
                pass_sums(final)

        ship(stage, ch, 0, tl)

    def top_copy(source, away, ch, got):
        block = packs.at[core, chip_at(source), 2, ch]
        return to(across(away, core), block, block, top_send, got.at[ch])

    def top_blocks(count, ch):
        return packs.at[core, head(count), 2, ch]

    def relay_top(ch):
        pltpu.make_async_copy(top_blocks(2, ch), top_blocks(2, ch), near_recv.at[ch]).wait()
        for source in (2, -2):
            for away in (1, -1):
                top_copy(source, away, ch, far_recv).start()
        top_copy(-2 * way, 2 * way, ch, far_recv).start()

    def apply_top(which, ch, z):
        for h in range(2):
            qs[pl.ds(h * held * tile, held * tile), :] = packs[h, z, 2, ch].reshape(held * tile, chans).astype(F32)
        for k in range(tile):
            xb[0:span, k * chans:(k + 1) * chans] = qs[pl.ds(k, span, stride=tile), :].astype(BF16)
        out = dot(cmat[which, z].astype(BF16), xb[0:span, :])
        for k in range(tile):
            gather[pl.ds(k, 16, stride=tile), :] = out[:, k * chans:(k + 1) * chans]
        for c in range(2):
            for t in range(tl):
                recv[1, ch, 2 * z + c, t, pl.ds(rows - tile, tile)] = gather[
                    pl.ds((8 * c + t) * tile, tile), :].astype(BF16)

    def mix_forward(l, x):
        both = dot(x, vmix[l], ((1,), (1,)))
        return both[:, :chans] + turn(both[:, chans:])

    def mix_adjoint(l, x):
        both = dot(x, jnp.concatenate([vmix[l, head(chans)], vmix[l, pl.ds(chans, chans)]], axis=1))
        return both[:, :chans] - turn(both[:, chans:])

    def step2_chunk(ch):
        spectral(1, ch, 0, coef, mix_forward)

    loop(chunks, step2_chunk)
    relay_top(chunks - 2)

    def fetch_rows(stage, ch, t):
        for src in range(n):
            gather[pl.ds(src * rows, rows), :] = recv[stage % 2, ch, src, t].astype(F32)

    def fetch_pair(b):
        return jnp.concatenate(
            [gather[pl.ds(b, modes2, stride=nb), :], gather[pl.ds(b + 1, modes2, stride=nb), :]], axis=1).astype(BF16)

    def step3_chunk(ch):
        arrived(1, ch)
        pltpu.make_async_copy(top_blocks(5, ch), top_blocks(5, ch), far_recv.at[ch]).wait()
        swap = to(sibling, top_blocks(chips, ch), top_blocks(chips, ch), swap_send.at[ch], swap_recv.at[ch])
        swap.start()

        @pl.when(ch == 0)
        def _():
            relay_top(final)

        swap.wait()

        @pl.when(ch == final)
        def _():
            all_sent = packs.at[0, head(7), 2]
            pltpu.make_async_copy(all_sent, all_sent, top_send).wait()

        def apply(z):
            apply_top(1, ch, z)

        loop(chips, apply)

        @pl.when(ch == 1)
        def _():
            sum_rows(1, 0)

        slot = free_slot(2, ch)

        def row(t):
            unit = ch * tl + t
            step_in(dg_hbm, unit)
            buf = lax.rem(unit, 2)
            fetch_rows(1, ch, t)
            for b in range(0, nb, 2):
                g = fetch_pair(b)
                hidden = dot(syn_h[...], g) + dot(syn_l[...], g)
                pair = jnp.concatenate([inbuf[buf, b], inbuf[buf, b + 1]], axis=1)
                spec = transform(pair * gelu_grad(hidden), dbl_h, dbl_l)
                gather[pl.ds(b, modes2, stride=nb), :] = spec[:, :chans]
                gather[pl.ds(b + 1, modes2, stride=nb), :] = spec[:, chans:]
            put_rows(slot, t)

        loop(tl, row)
        send_peak(2, ch)

        @pl.when(ch < final)
        def _():
            ship(2, ch, 0, tl)


    loop(chunks, step3_chunk)

    def sum_second(ch):
        pass_sums(ch - 1)
        sum_rows(1, ch)

    loop(final, sum_second, 1)
    ship(2, final, 0, tl)
    unit_in(dg_hbm, 0).start()

    def step4_chunk(ch):
        spectral(3, ch, 1, dq, mix_adjoint)

    loop(chunks, step4_chunk)

    for which, kept in enumerate((coef, dq)):
        def keep_low(half_at, row, degree, ours):
            own[half_at, which, :, row] = only(ours, kept[degree, :, head(tile)])

        pack(chip, keep_low)

    def both_parts(peer, action):
        degree = n + first_mode(peer)
        for which, kept in enumerate((coef, dq)):
            action(to(peer, kept.at[degree, :, head(tile)], second.at[which, me, :, head(tile)],
                      always_send, always_recv))

            @pl.when(first_mode(me) <= first_mode(peer))
            def _():
                more = pl.ds(tile, tile)
                action(to(peer, kept.at[degree, :, more], second.at[which, me, :, more],
                          some_send, some_recv))

    def send_second(k):
        both_parts(lax.rem(me + k, n), lambda copy: copy.start())

    loop(n, send_second, 1)
    for which, kept in enumerate((coef, dq)):
        second[which, me] = kept[n + first_mode(me), :, head(2 * tile)]

    def clear_second(src):
        @pl.when(first_mode(src) > first_mode(me))
        def _():
            for which in range(2):
                second[which, src, :, pl.ds(tile, tile)] = jnp.zeros((chunks, tile, chans), BF16)

    loop(n, clear_second)
    own_copy = to(sibling, own.at[other_core], other, own_send, own_recv)
    own_copy.start()

    def pack_block(k):
        return packs.at[core, chip_at(-way * k)]

    def pack_copy(k):
        return to(onward, pack_block(k), pack_block(k), pack_send, pack_recv.at[k])

    def share(k):
        to(sibling, pack_block(k), pack_block(k), share_send, share_recv).start()

    half = degs // n - 2
    wide = 2 * chans
    block_rows = half * wide
    piece = block_rows // pieces
    hops = (last) * pieces

    def block_at(k, direction):
        return lax.rem(chip - direction * (1 + k) + 2 * chips, chips)

    def outer(dst, row, pairs):
        real = jnp.zeros((chans, chans), F32)
        imag = jnp.zeros((chans, chans), F32)
        for y, x in pairs:
            real += dot(y, x, ((0,), (0,)))
            imag -= dot(turn(y.astype(F32)).astype(BF16), x, ((0,), (0,)))
        dst[pl.ds(row, chans, stride=2), :] = real
        dst[pl.ds(row + 1, chans, stride=2), :] = imag

    def first_degree(block, of_core):
        return 2 * n + (2 * block + of_core) * half

    def weight_grad(dst, degree):
        def one(j):
            outer(dst, j * wide, [(dq[degree + j, ch], coef[degree + j, ch]) for ch in range(chunks)])

        loop(half, one)

    def pair_copy(k):
        slot = lax.rem(k, 2)
        rows_there = pl.ds(first_degree(block_at(k, -way), core) * wide, block_rows)
        return to(sibling, wbuf.at[slot, head(block_rows)], dw_out.at[rows_there],
                  pair_send.at[slot], pair_recv.at[k])

    def weight_block(k):
        @pl.when(k >= 2)
        def _():
            pair_copy(k - 2).wait_send()
        weight_grad(wbuf.at[lax.rem(k, 2)], first_degree(block_at(k, -way), other_core))
        pair_copy(k).start()
        block = block_at(k, way)
        weight_grad(work.at[pl.ds(block * block_rows, block_rows)], first_degree(block, core))

    loop(chips, weight_block)
    pair_copy(chips - 2).wait_send()
    pair_copy(last).wait_send()
    own_copy.wait()
    packs[core, chip] = (own[core].astype(F32) + other[...].astype(F32)).astype(BF16)

    def low_degree(l):
        def one(z):
            for c in range(2):
                p = l - z if c == 0 else l + 1
                ours = p >= 0 if c == 0 else p >= n - z
                p = jnp.maximum(p, 0)
                h = jnp.where(p > held - 1, 1, 0)
                for which in range(2):
                    lowx[which, 2 * z + c] = only(ours, packs[h, z, which, :, p - h * (held - 1)])

        loop(chips, one)
        outer(wbuf.at[0], 0, [(lowx[1].reshape(-1, chans), lowx[0].reshape(-1, chans))])
        dw_out[pl.ds(l * wide, wide)] = wbuf[0, head(wide)]

    def final_rows(unit):
        ch, t = unit_of(unit)

        step_in(dg_hbm, unit)
        buf = lax.rem(unit, 2)

        fetch_rows(3, ch, t)
        for b in range(0, nb, 2):
            g = fetch_pair(b)
            change = dot(adj_h[...], g) + dot(adj_l[...], g)
            df_out[ch * nb + b, t] = inbuf[buf, b] + change[:, :chans]
            df_out[ch * nb + b + 1, t] = inbuf[buf, b + 1] + change[:, chans:]

    def place(i, of_core):
        block = block_at(lax.div(i, pieces), way)
        start = lax.rem(i, pieces) * piece
        return pl.ds(block * block_rows + start, piece), pl.ds(first_degree(block, of_core) * wide + start, piece)

    def rs_copy(i):
        here, there = place(i, core)
        return to(onward, work.at[here], dw_out.at[there], rs_send, rs_recv.at[i])

    def add_pair(i):
        here, passed = place(i, other_core)

        @pl.when(lax.rem(i, pieces) == 0)
        def _():
            pair_copy(lax.div(i, pieces)).wait_recv()

        work[here] += dw_out[passed]

    def rs_step(i):
        add_pair(i)

        @pl.when(i >= pieces)
        def _():
            rs_copy(i - pieces).wait_recv()
            here, there = place(i, core)
            work[here] += dw_out[there]

        rs_copy(i).start()

        @pl.when(lax.rem(i, pieces) == 0)
        def _():
            k = lax.div(i, pieces)

            @pl.when(k > 0)
            def _():
                pack_copy(k - 1).wait_recv()

            pack_copy(k).start()
            share(k)


    loop(hops, rs_step)
    pack_copy(chips - 2).wait_recv()
    share(last)

    def own_sum(s):
        i = hops + s
        add_pair(i)
        rs_copy(i - pieces).wait_recv()
        here, there = place(i, core)
        dw_out[there] += work[here]
        ag_copy(i, s).start()

    def second_spot(k):
        return pl.ds((n + first_mode(2 * block_at(k, way) + core)) * wide, wide)

    def second_copy(k, got):
        spot = dw_out.at[second_spot(k)]
        return to(onward, spot, spot, ag_send, ag_recv.at[hops + got])

    def second_publish(k):
        spot = dw_out.at[second_spot(k)]
        to(sibling, spot, spot, pub_send, pub_recv).start()

    def ag_copy(i, got):
        _, there = place(i, core)
        return to(onward, dw_out.at[there], dw_out.at[there], ag_send, ag_recv.at[got])

    def publish(i):
        _, there = place(i, core)
        to(sibling, dw_out.at[there], dw_out.at[there], pub_send, pub_recv).start()

    firsts = second.at[:, head(n - 1), :, head(tile)]
    pltpu.make_async_copy(firsts, firsts, always_recv).wait()

    comes, goes = first_mode(me), n - 1 - first_mode(me)

    def wait_some(count, sem):
        for k in range(1, n):
            @pl.when(count == k)
            def _():
                part = second.at[:, head(k), :, pl.ds(tile, tile)]
                pltpu.make_async_copy(part, part, sem).wait()

    wait_some(comes, some_recv)
    outer(wbuf.at[0], 0, [(second[1].reshape(-1, chans), second[0].reshape(-1, chans))])
    dw_out[second_spot(last)] = wbuf[0, head(wide)]
    loop(pieces, own_sum)
    second_copy(last, 0).start()

    pl.semaphore_signal(free_sem, inc=1, device_id={axis: sibling}, device_id_type=pl.DeviceIdType.MESH)
    pl.semaphore_wait(free_sem, 1)

    def own_piece(s):
        publish(hops + s)

    loop(pieces, own_piece)
    second_publish(last)
    gathered = packs.at[other_core]
    pltpu.make_async_copy(gathered, gathered, share_recv).wait()

    def task(i):
        @pl.when(i < chips)
        def _():
            for ch in range(chunks):
                @pl.when(i == 0)
                def _():
                    arrived(3, ch)
                apply_top(0, ch, i)

        @pl.when((i >= chips) & (i < chips + units))
        def _():
            final_rows(i - chips)

        @pl.when(i < n)
        def _():
            low_degree(i)

    def ag_step(i):
        ag_copy(i, i).wait_recv()

        @pl.when(i + pieces < hops)
        def _():
            ag_copy(i, i + pieces).start()

        publish(i)

        @pl.when(lax.rem(i, pieces) == pieces - 1)
        def _():
            k = lax.div(i, pieces)
            second_copy(k, k).wait_recv()

            @pl.when(k < chips - 2)
            def _():
                second_copy(k, k + 1).start()

            second_publish(k)

        task(i)

    loop(hops, ag_step)

    def rest(i):
        task(i)

    loop(max(hops, chips + units, n), rest, hops)

    wait_sent(2 * chunks + final, 2)
    for ch in range(chunks):
        wait_sent(3 * chunks + ch, 3)
    for ch in range(chunks):
        pltpu.make_async_copy(sums.at[ch], sums.at[ch], sum_send.at[ch]).wait()
    sent = work.at[head((last) * block_rows)]
    pltpu.make_async_copy(sent, sent, rs_send).wait()
    sent = dw_out.at[head((last) * (block_rows + wide))]
    pltpu.make_async_copy(sent, sent, ag_send).wait()
    pltpu.make_async_copy(firsts, firsts, always_send).wait()

    wait_some(goes, some_send)
    sent = packs.at[0, head(last)]
    pltpu.make_async_copy(sent, sent, pack_send).wait()
    pltpu.make_async_copy(packs.at[0], packs.at[0], share_send).wait()
    shared = dw_out.at[head(chips * (block_rows + wide))]
    pltpu.make_async_copy(shared, shared, pub_send).wait()
    pltpu.make_async_copy(shared, shared, pub_recv).wait()


def put_kernel(df_ref, dw_ref, df_hbm, dw_hbm, sems):
    copies = []
    for source, target, parts in ((df_ref, df_hbm, 6), (dw_ref, dw_hbm, 12)):
        size = source.shape[0] // parts
        for k in range(parts):
            part = pl.ds(k * size, size)
            copies.append(pltpu.make_async_copy(source.at[part], target.at[part], sems.at[len(copies)]))
    for copy in copies:
        copy.start()
    for copy in copies:
        copy.wait()


def solution(mesh):
    n = mesh.shape['lat']
    field_spec = P('member', None, 'lat', None)

    def local_step(field_loc, grad_loc, p_fwd, p_inv, w_mix):
        batch, chans, tl, lons = field_loc.shape
        degs, lats = p_fwd.shape[1:]
        ml = p_fwd.shape[0] // n
        nb = 4
        chunks = batch // nb
        rows = ml * 2 * nb
        pitch = rows + 1
        half = degs // n - 2
        pieces = 4 if half * 2 * chans % 32 == 0 else 1
        hops = (n // 2 - 1) * pieces
        per = 4
        area = max(2 * lats * pitch, n // 2 * half * 2 * chans)
        depth = min(degs // per, area // (per * 2 * chans))
        held = n // 2 + 1
        packed = (3, chunks, held, 2 * nb, chans)
        tables = fourier_tables(n, ml, lons)
        anywhere = pl.BlockSpec(memory_space=pl.ANY)
        vmem = pl.BlockSpec(memory_space=pltpu.VMEM)
        grad_field, grad_w = pl.pallas_call(
            functools.partial(layer_kernel, 'lat', n, nb, pieces, per, depth),
            name='layer',
            out_shape=(
                pltpu.VMEM((batch, tl, lons, chans), F32),
                pltpu.VMEM((degs * 2 * chans, chans), F32),
            ),
            in_specs=[anywhere] * 6,
            out_specs=(vmem, vmem),
            scratch_shapes=[
                pltpu.VMEM((2, chunks, n, tl, rows, chans), BF16),
                pltpu.VMEM((chunks + 1, n, tl, rows, chans), BF16),
                pltpu.VMEM((area, chans), F32),
                pltpu.VMEM((lats, 2 * nb * chans), BF16),
                pltpu.VMEM((degs, chunks, rows, chans), BF16),
                pltpu.VMEM((degs, chunks, rows, chans), BF16),
                pltpu.VMEM((degs, 2 * chans, chans), BF16),
                pltpu.VMEM((2, max(per, half) * 2 * chans, chans), F32),
                pltpu.VMEM((2, nb, lons, chans), F32),
                pltpu.VMEM((n * rows, chans), F32),
                pltpu.VMEM((2, ml, degs, lats), F32),
                pltpu.VMEM((2, ml, degs, lats), BF16),
                pltpu.VMEM((2, n, n, lats), F32),
                pltpu.VMEM((2, n // 2, 16, 32), F32),
                pltpu.VMEM((32 * 2 * nb, chans), F32),
                pltpu.VMEM((2,) + packed, BF16),
                pltpu.VMEM(packed, BF16),
                pltpu.VMEM((2, n // 2) + packed, BF16),
                pltpu.VMEM((2, n, chunks, 2 * nb, chans), BF16),
                pltpu.VMEM(tables.shape, BF16),
                pltpu.VMEM((chunks, 5, 6, tl, 2 * nb, chans), BF16),
                pltpu.VMEM((2, 4, held, 2 * nb, chans), F32),
                pltpu.VMEM((chunks, 4, held, 2 * nb, chans), F32),
                pltpu.VMEM((chunks, 4, held, 2 * nb, chans), F32),
                pltpu.VMEM((chunks, 2, held, 2 * nb, chans), F32),
                pltpu.VMEM((chunks, 2, held, 2 * nb, chans), F32),
                pltpu.VMEM((chunks, 2, held, 2 * nb, chans), F32),
                pltpu.VMEM((2, n, chunks, 4 * nb, chans), BF16),
                pltpu.SemaphoreType.DMA((4 * chunks,)),
                pltpu.SemaphoreType.DMA((4 * chunks,)),
                pltpu.SemaphoreType.DMA((2,)),
                pltpu.SemaphoreType.DMA((depth,)),
                pltpu.SemaphoreType.DMA((2,)),
                pltpu.SemaphoreType.DMA((2,)),
                pltpu.SemaphoreType.DMA((2,)),
                pltpu.SemaphoreType.DMA((n // 2,)),
                pltpu.SemaphoreType.DMA,
                pltpu.SemaphoreType.DMA((hops,)),
                pltpu.SemaphoreType.DMA,
                pltpu.SemaphoreType.DMA((hops + n // 2 - 1,)),
                pltpu.SemaphoreType.REGULAR,
                pltpu.SemaphoreType.DMA,
                pltpu.SemaphoreType.DMA,
                pltpu.SemaphoreType.DMA,
                pltpu.SemaphoreType.DMA,
                pltpu.SemaphoreType.DMA,
                pltpu.SemaphoreType.DMA((n // 2 - 1,)),
                pltpu.SemaphoreType.DMA,
                pltpu.SemaphoreType.DMA,
                pltpu.SemaphoreType.DMA((2,)),
                pltpu.SemaphoreType.DMA,
                pltpu.SemaphoreType.DMA((chunks,)),
                pltpu.SemaphoreType.DMA((chunks,)),
                pltpu.SemaphoreType.DMA((chunks,)),
                pltpu.SemaphoreType.DMA((chunks,)),
                pltpu.SemaphoreType.DMA((chunks,)),
                pltpu.SemaphoreType.DMA((chunks,)),
                pltpu.SemaphoreType.DMA((chunks,)),
                pltpu.SemaphoreType.DMA((chunks,)),
                pltpu.SemaphoreType.DMA((chunks,)),
                pltpu.SemaphoreType.DMA((chunks,)),
                pltpu.SemaphoreType.DMA((chunks,)),
                pltpu.SemaphoreType.DMA((chunks,)),
                pltpu.SemaphoreType.DMA,
                pltpu.SemaphoreType.DMA,
                pltpu.SemaphoreType.DMA,
                pltpu.SemaphoreType.DMA,
                pltpu.SemaphoreType.DMA((chunks,)),
            ],
            compiler_params=pltpu.CompilerParams(
                collective_id=0, has_side_effects=True, vmem_limit_bytes=43 << 20),
        )(
            field_loc.transpose(0, 2, 3, 1), grad_loc.transpose(0, 2, 3, 1),
            w_mix.transpose(0, 1, 3, 2).reshape(degs * 2 * chans, chans),
            p_fwd, p_inv, tables)
        grad_field, grad_w = pl.pallas_call(
            put_kernel,
            name='put',
            out_shape=(
                jax.ShapeDtypeStruct(grad_field.shape, F32),
                jax.ShapeDtypeStruct(grad_w.shape, F32),
            ),
            in_specs=[vmem] * 2,
            out_specs=(anywhere, anywhere),
            scratch_shapes=[pltpu.SemaphoreType.DMA((18,))],
            compiler_params=pltpu.CompilerParams(vmem_limit_bytes=1 << 20),
        )(grad_field, grad_w)
        return grad_field.transpose(0, 3, 1, 2), grad_w.reshape(degs, chans, 2, chans).transpose(0, 1, 3, 2)

    return jax.shard_map(
        local_step, mesh=mesh, in_specs=(field_spec, field_spec, P(), P(), P()),
        out_specs=(field_spec, P('member', None, None, None)), check_vma=False)
```

```python
import functools
import math

import jax
import jax.numpy as jnp
import numpy as np
from jax import lax
from jax.experimental import pallas as pl
from jax.experimental.pallas import tpu as pltpu
from jax.sharding import PartitionSpec as P

F32 = jnp.float32
BF16 = jnp.bfloat16


def split_const(matrix):
    head = matrix.astype(BF16)
    tail = (matrix - head.astype(np.float64)).astype(BF16)
    return [head, tail]


def fourier_tables(n, ml, lons):
    modes = n * ml
    device = np.arange(n)
    first = np.where(device % 2 == 0, device // 2, n - 1 - device // 2)
    order = (first[:, None] + n * np.arange(ml)[None, :]).reshape(-1)
    angle = math.tau * (np.outer(order, np.arange(lons)) % lons) / lons
    forward = np.stack([np.cos(angle), -np.sin(angle)], axis=1).reshape(2 * modes, lons) / math.sqrt(lons)
    gains = np.repeat(2.0 - (order == 0), 2)[:, None]
    doubled = forward * gains
    tables = split_const(forward) + split_const(doubled) + split_const(doubled.T) + split_const(forward.T)
    return jnp.stack([jnp.asarray(t) for t in tables])


def gelu_grad(values):
    cumulative = 0.5 * (1.0 + lax.erf(values * math.sqrt(0.5)))
    density = jnp.exp(-0.5 * values * values) / math.sqrt(math.tau)
    return cumulative + values * density


def loop(stop, step, start=0, **options):
    def one(i, carry):
        step(i)
        return carry

    lax.fori_loop(start, stop, one, 0, **options)


def head(size):
    return pl.ds(0, size)


def dot(a, b, dims=((1,), (0,))):
    return lax.dot_general(a, b, (dims, ((), ())), preferred_element_type=F32)


def layer_kernel(
    axis, n, nb, pieces, per, depth,
    f_hbm, dg_hbm, w_hbm, pf_hbm, pv_hbm, tab_hbm,
    df_out, dw_out,
    recv, send, work, xb, coef, dq, vmix, wbuf, inbuf, gather, pbuf, pmat, band, cmat, qs, own, other, packs, lowx, tab,
    topin, partial, mid, sums, sumin, joined, handed, second,
    send_sem, recv_sem, in_sem, w_sem, p_sem, band_sem, pair_send, pair_recv, rs_send, rs_recv, ag_send, ag_recv,
    free_sem, pub_send, pub_recv, own_send, own_recv, pack_send, pack_recv, share_send, share_recv,
    tab_sem, top_send, near_recv, far_recv, next_recv, swap_send, swap_recv,
    row_send, row_recv, mid_send, mid_recv, sum_send, sum_recv, join_send, join_recv,
    always_send, always_recv, some_send, some_recv, hand_recv,
):
    me = lax.axis_index(axis)
    batch, tl, lons, chans = f_hbm.shape
    ml, degs, lats = pmat.shape[1:]
    chunks = batch // nb
    tile = 2 * nb
    rows = ml * tile
    pitch = rows + 1
    modes2 = 2 * n * ml
    units = chunks * tl
    final = chunks - 1
    slots = chunks + 1
    fwd_h, fwd_l, dbl_h, dbl_l, syn_h, syn_l, adj_h, adj_l = (tab.at[k] for k in range(8))
    area = lats * pitch
    top = n * (ml - 1)
    held = n // 2 + 1
    chip, core = lax.div(me, 2), lax.rem(me, 2)
    other_core = 1 - core
    chips = n // 2
    last = chips - 1
    way = 1 - 2 * core
    sides = (-1, 1)
    sibling = me + way

    def chip_at(away):
        return lax.rem(chip + away + chips, chips)

    def across(away, its_core):
        return 2 * chip_at(away) + its_core

    onward = across(way, core)

    def around(k):
        far = chips // 2 - lax.div(k + 1, 2)
        return jnp.where(lax.rem(k, 2) == 0, far, -far)

    def first_mode(device):
        z = lax.div(device, 2)
        return jnp.where(lax.rem(device, 2) == 0, z, n - 1 - z)

    def to(device, src, dst, sent, got):
        return pltpu.make_async_remote_copy(
            src_ref=src, dst_ref=dst, send_sem=sent, recv_sem=got,
            device_id={axis: device}, device_id_type=pl.DeviceIdType.MESH)

    def unit_of(unit):
        return lax.div(unit, tl), lax.rem(unit, tl)

    def unit_in(src, unit):
        ch, t = unit_of(unit)
        slot = lax.rem(unit, 2)
        return pltpu.make_async_copy(src.at[pl.ds(ch * nb, nb), t], inbuf.at[slot], in_sem.at[slot])

    def step_in(src, unit):
        @pl.when(unit + 1 < units)
        def _():
            unit_in(src, unit + 1).start()
        unit_in(src, unit).wait()

    body, peak = head(rows - tile), pl.ds(rows - tile, tile)

    def ship(stage, ch, t0, nt):
        index = stage * chunks + ch
        slot = lax.rem(index, slots)
        part = pl.ds(t0, nt)

        def one(k):
            away = around(k)
            for its_core in (core, other_core):
                peer = across(away, its_core)
                to(peer, send.at[slot, peer, part, body], recv.at[stage % 2, ch, me, part, body],
                   send_sem.at[index], recv_sem.at[index]).start()

        loop(last, one)
        to(sibling, send.at[slot, sibling, part, body], recv.at[stage % 2, ch, me, part, body],
           send_sem.at[index], recv_sem.at[index]).start()
        recv[stage % 2, ch, me, part, body] = send[slot, me, part, body]

    def arrived(stage, ch):
        others = recv.at[stage % 2, ch, head(n - 1), :, body]
        pltpu.make_async_copy(others, others, recv_sem.at[stage * chunks + ch]).wait()

    def peaks():
        return send.at[0, head(n - 5), :, peak]

    def wait_sent(index, stage):
        others = send.at[lax.rem(index, slots), head(n - 1), :, body]
        pltpu.make_async_copy(others, others, send_sem.at[index]).wait()
        if stage % 2 == 0:
            ch = index - stage * chunks
            pltpu.make_async_copy(peaks(), peaks(), row_send.at[ch]).wait()

    def send_peak(stage, ch):
        slot = lax.rem(stage * chunks + ch, slots)
        far = chips // 2
        for same in (True, False):
            its_core = core if same else other_core
            for away in range(1 - far, far + 1):
                near = max(-2, min(2, away))
                hop, target, apart = away - near, (0, 2, 4, 3, 1)[near], abs(away - near)
                if away == far:
                    hop = jnp.where(its_core == 0, 2 - far, far - 2)
                    target = jnp.where(its_core == 0, 3, 4)
                source = send.at[slot, across(away, its_core), :, peak]
                place = topin.at[ch, target, 2 * apart + core]
                if same and not apart:
                    place[...] = source[...]
                else:
                    to(across(hop, its_core), source, place,
                       row_send.at[ch], row_recv.at[ch]).start()

    def free_slot(stage, ch):
        index = stage * chunks + ch
        if stage >= 1:
            @pl.when(ch >= 1)
            def _():
                wait_sent(index - slots, stage - 1)
        if stage >= 2:
            @pl.when(ch == 0)
            def _():
                wait_sent(index - slots, stage - 2)
        return lax.rem(index, slots)

    def put_rows(slot, t):
        send[slot, :, t] = gather[...].reshape(n, rows, chans).astype(BF16)

    def transform(values, head, tail):
        high = values.astype(BF16)
        low = (values - high.astype(F32)).astype(BF16)
        return dot(head[...], high) + (dot(tail[...], high) + dot(head[...], low))

    unit_in(f_hbm, 0).start()
    first_tables = pltpu.make_async_copy(tab_hbm.at[head(2)], tab.at[head(2)], tab_sem.at[0])
    other_tables = pltpu.make_async_copy(tab_hbm.at[pl.ds(2, 6)], tab.at[pl.ds(2, 6)], tab_sem.at[1])
    first_tables.start()
    barrier = pltpu.get_barrier_semaphore()

    def announce(k):
        pl.semaphore_signal(barrier, inc=1, device_id={axis: lax.rem(me + k, n)}, device_id_type=pl.DeviceIdType.MESH)

    loop(n, announce, 1)

    first_tables.wait()

    group = max(1, tl // 3)

    parts = degs // per

    def w_in(k):
        slot = lax.rem(k, depth)
        return pltpu.make_async_copy(
            w_hbm.at[pl.ds(k * per * 2 * chans, per * 2 * chans)],
            work.at[pl.ds(slot * per * 2 * chans, per * 2 * chans)], w_sem.at[slot])

    def band_in(d):
        for which, source in enumerate((pf_hbm, pv_hbm)):
            pltpu.make_async_copy(
                source.at[top + first_mode(d), pl.ds(top, n)], band.at[which, d], band_sem.at[which]).start()

    def step1_chunk(ch):
        slot = free_slot(0, ch)

        def row(t):
            unit = ch * tl + t
            step_in(f_hbm, unit)
            buf = lax.rem(unit, 2)
            for b in range(0, nb, 2):
                pair = jnp.concatenate([inbuf[buf, b], inbuf[buf, b + 1]], axis=1)
                spec = transform(pair, fwd_h, fwd_l)
                gather[pl.ds(b, modes2, stride=nb), :] = spec[:, :chans]
                gather[pl.ds(b + 1, modes2, stride=nb), :] = spec[:, chans:]
            put_rows(slot, t)

            @pl.when((ch == 0) & (t == group - 1))
            def _():
                pl.semaphore_wait(barrier, n - 1)
                ship(0, 0, 0, group)


        loop(tl, row)
        send_peak(0, ch)

        @pl.when(ch == 0)
        def _():
            ship(0, 0, group, tl - group)
            other_tables.start()
            for which, source in enumerate((pf_hbm, pv_hbm)):
                for k in range(ml):
                    pltpu.make_async_copy(
                        source.at[first_mode(me) + n * k], pbuf.at[which, k], p_sem.at[which]).start()
            loop(n, band_in)
            for k in range(depth):
                w_in(k).start()


    loop(chunks, step1_chunk)

    unit_in(dg_hbm, 0).start()
    for which in range(2):
        pltpu.make_async_copy(band.at[which], band.at[which], band_sem.at[which]).wait()
    qs[...] = jnp.zeros_like(qs)

    def pack(z, store):
        def one(index):
            half_at, row = lax.div(index, held), lax.rem(index, held)
            p = half_at * (held - 1) + row
            degree = jnp.where(core == 0, jnp.minimum(z + p, n - 1), jnp.maximum(p - 1, 0))
            store(half_at, row, degree, (p < n - z) == (core == 0))

        loop(2 * held, one)

    def project(which, ch, target, device):
        gather[...] = jnp.zeros_like(gather)
        side = 1 if target == 3 else -1

        def place_rows(apart):
            for c in range(2):
                src = across(side * apart, c)
                gather[pl.ds(pl.multiple_of(src * tl * tile, tile), tl * tile), :] = topin[
                    ch, target, 2 * apart + c].reshape(tl * tile, chans).astype(F32)

        place_rows(0)
        if target > 2:
            place_rows(1)

            @pl.when(core == target - 3)
            def _():
                place_rows(2)

        for k in range(tile):
            xb[:, k * chans:(k + 1) * chans] = gather[pl.ds(k, lats, stride=tile), :].astype(BF16)
        out = dot(band[which, device].astype(BF16), xb[...])
        for k in range(tile):
            qs[pl.ds(k, n, stride=tile), :] = out[:, k * chans:(k + 1) * chans]

    def sum_rows(which, ch):
        pltpu.make_async_copy(peaks(), peaks(), row_recv.at[ch]).wait()
        for target, away in enumerate((-1, 1, -2, 2)):
            project(which, ch, target + 1, across(away, core))

            def keep(half_at, row, degree, ours):
                values = qs[pl.ds(pl.multiple_of(degree * tile, tile), tile), :]
                partial[half_at, target, row] = jnp.where(ours, values, jnp.zeros_like(values))

            pack(chip_at(away), keep)
        swap = to(sibling, partial.at[other_core], mid.at[ch], mid_send.at[ch], mid_recv.at[ch])
        swap.start()
        if which == 1:
            pltpu.make_async_copy(sums.at[ch], sums.at[ch], sum_send.at[ch]).wait()
        swap.wait()
        sums[ch] = partial[core] + mid[ch]
        for side, away in enumerate(sides):
            to(across(away, core), sums.at[ch, 2 + side], handed.at[ch, side],
               sum_send.at[ch], hand_recv.at[ch]).start()

    def pass_sums(ch):
        pltpu.make_async_copy(handed.at[ch], handed.at[ch], hand_recv.at[ch]).wait()
        for side, away in enumerate(sides):
            sums[ch, side] += handed[ch, side]
            to(across(away, core), sums.at[ch, side], sumin.at[ch, side],
               sum_send.at[ch], sum_recv.at[ch]).start()

    def finish_peak(which, ch):
        pltpu.make_async_copy(sumin.at[ch], sumin.at[ch], sum_recv.at[ch]).wait()
        joined[ch, core] = sumin[ch, 0] + sumin[ch, 1]
        swap = to(sibling, joined.at[ch, core], joined.at[ch, core], join_send.at[ch], join_recv.at[ch])
        swap.start()
        project(which, ch, 0, me)
        swap.wait()

        def one(degree):
            p = jnp.where(core == 0, degree - chip, degree + 1)
            ours = degree >= first_mode(me)
            p = jnp.maximum(p, 0)
            h = jnp.where(p > held - 1, 1, 0)
            come = joined[ch, h, p - h * (held - 1)]
            work[pl.ds(area + (top + degree) * pitch + rows - tile, tile), :] = qs[
                pl.ds(pl.multiple_of(degree * tile, tile), tile), :] + jnp.where(ours, come, jnp.zeros_like(come))

        loop(n, one)

    sum_rows(0, 0)

    def ship_rows(ch):
        ship(0, ch, 0, tl)

    loop(final, ship_rows, 1)
    for which in range(2):
        pltpu.make_async_copy(pbuf.at[which], pbuf.at[which], p_sem.at[which]).wait()
    pmat[...] = pbuf[...].astype(BF16)
    other_tables.wait()

    def load_w(k):
        w_in(k).wait()
        base = lax.rem(k, depth) * per * 2 * chans
        for j in range(per):
            for part in range(2):
                vmix[k * per + j, pl.ds(part * chans, chans)] = work[
                    pl.ds(base + j * 2 * chans + part, chans, stride=2), :].astype(BF16)

        @pl.when(k + depth < parts)
        def _():
            w_in(k + depth).start()


    loop(parts, load_w)

    span = cmat.shape[3]
    mine_t = (lax.broadcasted_iota(jnp.int32, (8, lats), 1) == me * tl + lax.broadcasted_iota(jnp.int32, (8, lats), 0))
    mine_t &= lax.broadcasted_iota(jnp.int32, (8, lats), 0) < tl
    mine_t = jnp.where(mine_t, 1.0, 0.0).astype(BF16)

    def tabulate(d):
        z, of_core = lax.div(d, 2), lax.rem(d, 2)
        row = lax.broadcasted_iota(jnp.int32, (n, span), 0)
        p = jnp.where(of_core == 0, row - z, row + 1)
        target = jnp.where(p > held - 1, p + 1, p)
        moved = jnp.where(target == lax.broadcasted_iota(jnp.int32, (n, span), 1), 1.0, 0.0).astype(BF16)
        for which in range(2):
            picked = dot(mine_t, band[which, d].astype(BF16), ((1,), (1,))).astype(BF16)
            cmat[which, z, pl.ds(pl.multiple_of(of_core * 8, 8), 8), :] = dot(picked, moved)

    loop(n, tabulate)

    def no_degree(l):
        work[pl.ds(area + l * pitch + rows - tile, tile), :] = jnp.zeros((tile, chans), F32)

    loop(top, no_degree)

    pass_sums(0)

    def sum_first(ch):
        sum_rows(0, ch)

    loop(chunks, sum_first, 1)
    ship(0, final, 0, tl)
    loop(chunks, pass_sums, 1)

    sign = jnp.where(lax.broadcasted_iota(jnp.int32, (tile, chans), 0) < nb, -1.0, 1.0).astype(F32)

    def turn(values):
        groups = values.reshape(-1, tile, chans)
        return (pltpu.roll(groups, nb, 1) * sign[None]).reshape(values.shape)

    def legendre(src, dst, which, over):
        def mode(m):
            for k in range(tile):
                xb[:, k * chans:(k + 1) * chans] = work[
                    pl.ds(src + m * tile + k, lats, stride=pitch), :].astype(BF16)
            out = dot(pmat[which, m], xb[...], ((over,), (0,)))
            for k in range(tile):
                work[pl.ds(dst + m * tile + k, degs, stride=pitch), :] = out[:, k * chans:(k + 1) * chans]

        loop(ml - 1, mode)

    def unload(stage, ch):
        def body(src):
            for t in range(tl):
                work[pl.ds((src * tl + t) * pitch, rows), :] = recv[stage % 2, ch, src, t].astype(F32)

        loop(n, body)

    def load(slot):
        def body(dev):
            for t in range(tl):
                send[slot, dev, t] = work[pl.ds(area + (dev * tl + t) * pitch, rows), :].astype(BF16)

        loop(n, body)

    def only(ours, values):
        values = values.astype(F32)
        return jnp.where(ours, values, jnp.zeros_like(values)).astype(BF16)

    def spectral(stage, ch, into, kept, mix):
        arrived(stage - 1, ch)
        unload(stage - 1, ch)
        legendre(0, area, into, 1)
        finish_peak(into, ch)

        def degree(l):
            x = work[pl.ds(area + l * pitch, rows), :].astype(BF16)
            kept[l, ch] = x
            work[pl.ds(l * pitch, rows), :] = mix(l, x)

        loop(degs, degree, unroll=8)

        def keep_top(half_at, row, degree, ours):
            own[half_at, 2, ch, row] = only(ours, work[pl.ds((top + degree) * pitch + rows - tile, tile), :])

        pack(chip, keep_top)
        if stage == 1:
            swap = to(sibling, own.at[other_core, 2, ch], other.at[2, ch], swap_send.at[ch], swap_recv.at[ch])
            swap.start()
        legendre(0, area, 1 - into, 0)
        load(free_slot(stage, ch))
        if stage == 1:
            swap.wait()
            packs[core, chip, 2, ch] = (own[core, 2, ch].astype(F32) + other[2, ch].astype(F32)).astype(BF16)

            @pl.when(ch == final - 1)
            def _():
                relay_near(ch - 1)

            for away in sides:
                top_copy(0, away, ch, near_recv).start()
        else:
            @pl.when(ch == 0)
            def _():
                pass_sums(final - 1)
                sum_rows(1, final)

            @pl.when(ch == 1)
            def _():
                pass_sums(final)

        if stage == 1:
            @pl.when(ch < final)
            def _():
                ship(stage, ch, 0, tl)
        else:
            ship(stage, ch, 0, tl)

    def top_copy(source, away, ch, got):
        block = packs.at[core, chip_at(source), 2, ch]
        return to(across(away, core), block, block, top_send, got.at[ch])

    def top_blocks(count, ch):
        return packs.at[core, head(count), 2, ch]

    def relay_near(ch):
        pltpu.make_async_copy(top_blocks(2, ch), top_blocks(2, ch), near_recv.at[ch]).wait()
        for side in sides:
            top_copy(-side, side, ch, next_recv).start()

    def relay_next(ch):
        pltpu.make_async_copy(top_blocks(2, ch), top_blocks(2, ch), next_recv.at[ch]).wait()
        for side in sides:
            top_copy(-2 * side, side, ch, far_recv).start()
        top_copy(-2 * way, 2 * way, ch, far_recv).start()

    def apply_top(which, ch, z):
        for h in range(2):
            qs[pl.ds(h * held * tile, held * tile), :] = packs[h, z, 2, ch].reshape(held * tile, chans).astype(F32)
        for k in range(tile):
            xb[0:span, k * chans:(k + 1) * chans] = qs[pl.ds(k, span, stride=tile), :].astype(BF16)
        out = dot(cmat[which, z].astype(BF16), xb[0:span, :])
        for k in range(tile):
            gather[pl.ds(k, 16, stride=tile), :] = out[:, k * chans:(k + 1) * chans]
        for c in range(2):
            for t in range(tl):
                recv[1, ch, 2 * z + c, t, pl.ds(rows - tile, tile)] = gather[
                    pl.ds((8 * c + t) * tile, tile), :].astype(BF16)

    def mix_forward(l, x):
        both = dot(x, vmix[l], ((1,), (1,)))
        return both[:, :chans] + turn(both[:, chans:])

    def mix_adjoint(l, x):
        both = dot(x, jnp.concatenate([vmix[l, head(chans)], vmix[l, pl.ds(chans, chans)]], axis=1))
        return both[:, :chans] - turn(both[:, chans:])

    def step2_chunk(ch):
        spectral(1, ch, 0, coef, mix_forward)

    loop(chunks, step2_chunk)
    relay_next(final - 2)
    relay_near(final - 1)
    ship(1, final, 0, tl)

    def fetch_rows(stage, ch, t):
        for src in range(n):
            gather[pl.ds(src * rows, rows), :] = recv[stage % 2, ch, src, t].astype(F32)

    def fetch_pair(b):
        return jnp.concatenate(
            [gather[pl.ds(b, modes2, stride=nb), :], gather[pl.ds(b + 1, modes2, stride=nb), :]], axis=1).astype(BF16)

    def step3_chunk(ch):
        arrived(1, ch)

        @pl.when(ch == 0)
        def _():
            relay_near(final)
            relay_next(final - 1)

        pltpu.make_async_copy(top_blocks(3, ch), top_blocks(3, ch), far_recv.at[ch]).wait()
        swap = to(sibling, top_blocks(chips, ch), top_blocks(chips, ch), swap_send.at[ch], swap_recv.at[ch])
        swap.start()

        @pl.when(ch == 1)
        def _():
            relay_next(final)

        swap.wait()

        @pl.when(ch == final)
        def _():
            all_sent = packs.at[0, head(7), 2]
            pltpu.make_async_copy(all_sent, all_sent, top_send).wait()

        def apply(z):
            apply_top(1, ch, z)

        loop(chips, apply)

        @pl.when(ch == 1)
        def _():
            sum_rows(1, 0)

        slot = free_slot(2, ch)

        def row(t):
            unit = ch * tl + t
            step_in(dg_hbm, unit)
            buf = lax.rem(unit, 2)
            fetch_rows(1, ch, t)
            for b in range(0, nb, 2):
                g = fetch_pair(b)
                hidden = dot(syn_h[...], g) + dot(syn_l[...], g)
                pair = jnp.concatenate([inbuf[buf, b], inbuf[buf, b + 1]], axis=1)
                spec = transform(pair * gelu_grad(hidden), dbl_h, dbl_l)
                gather[pl.ds(b, modes2, stride=nb), :] = spec[:, :chans]
                gather[pl.ds(b + 1, modes2, stride=nb), :] = spec[:, chans:]
            put_rows(slot, t)

        loop(tl, row)
        send_peak(2, ch)

        @pl.when(ch < final)
        def _():
            ship(2, ch, 0, tl)


    loop(chunks, step3_chunk)

    def sum_second(ch):
        pass_sums(ch - 1)
        sum_rows(1, ch)

    loop(final, sum_second, 1)
    ship(2, final, 0, tl)
    unit_in(dg_hbm, 0).start()

    def step4_chunk(ch):
        spectral(3, ch, 1, dq, mix_adjoint)

    loop(chunks, step4_chunk)

    for which, kept in enumerate((coef, dq)):
        def keep_low(half_at, row, degree, ours):
            own[half_at, which, :, row] = only(ours, kept[degree, :, head(tile)])

        pack(chip, keep_low)

    def both_parts(peer, action):
        degree = n + first_mode(peer)
        for which, kept in enumerate((coef, dq)):
            action(to(peer, kept.at[degree, :, head(tile)], second.at[which, me, :, head(tile)],
                      always_send, always_recv))

            @pl.when(first_mode(me) <= first_mode(peer))
            def _():
                more = pl.ds(tile, tile)
                action(to(peer, kept.at[degree, :, more], second.at[which, me, :, more],
                          some_send, some_recv))

    def send_second(k):
        both_parts(lax.rem(me + k, n), lambda copy: copy.start())

    loop(n, send_second, 1)
    for which, kept in enumerate((coef, dq)):
        second[which, me] = kept[n + first_mode(me), :, head(2 * tile)]

    def clear_second(src):
        @pl.when(first_mode(src) > first_mode(me))
        def _():
            for which in range(2):
                second[which, src, :, pl.ds(tile, tile)] = jnp.zeros((chunks, tile, chans), BF16)

    loop(n, clear_second)
    own_copy = to(sibling, own.at[other_core], other, own_send, own_recv)
    own_copy.start()

    def pack_block(k):
        return packs.at[core, chip_at(-way * k)]

    def pack_copy(k):
        return to(onward, pack_block(k), pack_block(k), pack_send, pack_recv.at[k])

    def share(k):
        to(sibling, pack_block(k), pack_block(k), share_send, share_recv).start()

    half = degs // n - 2
    wide = 2 * chans
    block_rows = half * wide
    piece = block_rows // pieces
    hops = (last) * pieces

    def block_at(k, direction):
        return lax.rem(chip - direction * (1 + k) + 2 * chips, chips)

    def outer(dst, row, pairs):
        real = jnp.zeros((chans, chans), F32)
        imag = jnp.zeros((chans, chans), F32)
        for y, x in pairs:
            real += dot(y, x, ((0,), (0,)))
            imag -= dot(turn(y.astype(F32)).astype(BF16), x, ((0,), (0,)))
        dst[pl.ds(row, chans, stride=2), :] = real
        dst[pl.ds(row + 1, chans, stride=2), :] = imag

    def first_degree(block, of_core):
        return 2 * n + (2 * block + of_core) * half

    def weight_grad(dst, degree):
        def one(j):
            outer(dst, j * wide, [(dq[degree + j, ch], coef[degree + j, ch]) for ch in range(chunks)])

        loop(half, one)

    def pair_copy(k):
        slot = lax.rem(k, 2)
        rows_there = pl.ds(first_degree(block_at(k, -way), core) * wide, block_rows)
        return to(sibling, wbuf.at[slot, head(block_rows)], dw_out.at[rows_there],
                  pair_send.at[slot], pair_recv.at[k])

    def weight_block(k):
        @pl.when(k >= 2)
        def _():
            pair_copy(k - 2).wait_send()
        weight_grad(wbuf.at[lax.rem(k, 2)], first_degree(block_at(k, -way), other_core))
        pair_copy(k).start()
        block = block_at(k, way)
        weight_grad(work.at[pl.ds(block * block_rows, block_rows)], first_degree(block, core))

    loop(chips, weight_block)
    pair_copy(chips - 2).wait_send()
    pair_copy(last).wait_send()
    own_copy.wait()
    packs[core, chip] = (own[core].astype(F32) + other[...].astype(F32)).astype(BF16)

    def low_degree(l):
        def one(z):
            for c in range(2):
                p = l - z if c == 0 else l + 1
                ours = p >= 0 if c == 0 else p >= n - z
                p = jnp.maximum(p, 0)
                h = jnp.where(p > held - 1, 1, 0)
                for which in range(2):
                    lowx[which, 2 * z + c] = only(ours, packs[h, z, which, :, p - h * (held - 1)])

        loop(chips, one)
        outer(wbuf.at[0], 0, [(lowx[1].reshape(-1, chans), lowx[0].reshape(-1, chans))])
        dw_out[pl.ds(l * wide, wide)] = wbuf[0, head(wide)]

    def final_rows(unit):
        ch, t = unit_of(unit)

        step_in(dg_hbm, unit)
        buf = lax.rem(unit, 2)

        fetch_rows(3, ch, t)
        for b in range(0, nb, 2):
            g = fetch_pair(b)
            change = dot(adj_h[...], g) + dot(adj_l[...], g)
            df_out[ch * nb + b, t] = inbuf[buf, b] + change[:, :chans]
            df_out[ch * nb + b + 1, t] = inbuf[buf, b + 1] + change[:, chans:]

    def place(i, of_core):
        block = block_at(lax.div(i, pieces), way)
        start = lax.rem(i, pieces) * piece
        return pl.ds(block * block_rows + start, piece), pl.ds(first_degree(block, of_core) * wide + start, piece)

    def rs_copy(i):
        here, there = place(i, core)
        return to(onward, work.at[here], dw_out.at[there], rs_send, rs_recv.at[i])

    def add_pair(i):
        here, passed = place(i, other_core)

        @pl.when(lax.rem(i, pieces) == 0)
        def _():
            pair_copy(lax.div(i, pieces)).wait_recv()

        work[here] += dw_out[passed]

    def rs_step(i):
        add_pair(i)

        @pl.when(i >= pieces)
        def _():
            rs_copy(i - pieces).wait_recv()
            here, there = place(i, core)
            work[here] += dw_out[there]

        rs_copy(i).start()

        @pl.when(lax.rem(i, pieces) == 0)
        def _():
            k = lax.div(i, pieces)

            @pl.when(k > 0)
            def _():
                pack_copy(k - 1).wait_recv()

            pack_copy(k).start()
            share(k)


    loop(hops, rs_step)
    pack_copy(chips - 2).wait_recv()
    share(last)

    def own_sum(s):
        i = hops + s
        add_pair(i)
        rs_copy(i - pieces).wait_recv()
        here, there = place(i, core)
        dw_out[there] += work[here]
        ag_copy(i, s).start()

    def second_spot(k):
        return pl.ds((n + first_mode(2 * block_at(k, way) + core)) * wide, wide)

    def second_copy(k, got):
        spot = dw_out.at[second_spot(k)]
        return to(onward, spot, spot, ag_send, ag_recv.at[hops + got])

    def second_publish(k):
        spot = dw_out.at[second_spot(k)]
        to(sibling, spot, spot, pub_send, pub_recv).start()

    def ag_copy(i, got):
        _, there = place(i, core)
        return to(onward, dw_out.at[there], dw_out.at[there], ag_send, ag_recv.at[got])

    def publish(i):
        _, there = place(i, core)
        to(sibling, dw_out.at[there], dw_out.at[there], pub_send, pub_recv).start()

    firsts = second.at[:, head(n - 1), :, head(tile)]
    pltpu.make_async_copy(firsts, firsts, always_recv).wait()

    comes, goes = first_mode(me), n - 1 - first_mode(me)

    def wait_some(count, sem):
        for k in range(1, n):
            @pl.when(count == k)
            def _():
                part = second.at[:, head(k), :, pl.ds(tile, tile)]
                pltpu.make_async_copy(part, part, sem).wait()

    wait_some(comes, some_recv)
    outer(wbuf.at[0], 0, [(second[1].reshape(-1, chans), second[0].reshape(-1, chans))])
    dw_out[second_spot(last)] = wbuf[0, head(wide)]
    loop(pieces, own_sum)
    second_copy(last, 0).start()

    pl.semaphore_signal(free_sem, inc=1, device_id={axis: sibling}, device_id_type=pl.DeviceIdType.MESH)
    pl.semaphore_wait(free_sem, 1)

    def own_piece(s):
        publish(hops + s)

    loop(pieces, own_piece)
    second_publish(last)
    gathered = packs.at[other_core]
    pltpu.make_async_copy(gathered, gathered, share_recv).wait()

    def task(i):
        @pl.when(i < chips)
        def _():
            for ch in range(chunks):
                @pl.when(i == 0)
                def _():
                    arrived(3, ch)
                apply_top(0, ch, i)

        @pl.when((i >= chips) & (i < chips + units))
        def _():
            final_rows(i - chips)

        @pl.when(i < n)
        def _():
            low_degree(i)

    def ag_step(i):
        ag_copy(i, i).wait_recv()

        @pl.when(i + pieces < hops)
        def _():
            ag_copy(i, i + pieces).start()

        publish(i)

        @pl.when(lax.rem(i, pieces) == pieces - 1)
        def _():
            k = lax.div(i, pieces)
            second_copy(k, k).wait_recv()

            @pl.when(k < chips - 2)
            def _():
                second_copy(k, k + 1).start()

            second_publish(k)

        task(i)

    loop(hops, ag_step)

    def rest(i):
        task(i)

    loop(max(hops, chips + units, n), rest, hops)

    wait_sent(2 * chunks + final, 2)
    for ch in range(chunks):
        wait_sent(3 * chunks + ch, 3)
    for ch in range(chunks):
        pltpu.make_async_copy(sums.at[ch], sums.at[ch], sum_send.at[ch]).wait()
    sent = work.at[head((last) * block_rows)]
    pltpu.make_async_copy(sent, sent, rs_send).wait()
    sent = dw_out.at[head((last) * (block_rows + wide))]
    pltpu.make_async_copy(sent, sent, ag_send).wait()
    pltpu.make_async_copy(firsts, firsts, always_send).wait()

    wait_some(goes, some_send)
    sent = packs.at[0, head(last)]
    pltpu.make_async_copy(sent, sent, pack_send).wait()
    pltpu.make_async_copy(packs.at[0], packs.at[0], share_send).wait()
    shared = dw_out.at[head(chips * (block_rows + wide))]
    pltpu.make_async_copy(shared, shared, pub_send).wait()
    pltpu.make_async_copy(shared, shared, pub_recv).wait()


def put_kernel(df_ref, dw_ref, df_hbm, dw_hbm, sems):
    copies = []
    for source, target, parts in ((df_ref, df_hbm, 6), (dw_ref, dw_hbm, 12)):
        size = source.shape[0] // parts
        for k in range(parts):
            part = pl.ds(k * size, size)
            copies.append(pltpu.make_async_copy(source.at[part], target.at[part], sems.at[len(copies)]))
    for copy in copies:
        copy.start()
    for copy in copies:
        copy.wait()


def solution(mesh):
    n = mesh.shape['lat']
    field_spec = P('member', None, 'lat')

    def local_step(field_loc, grad_loc, p_fwd, p_inv, w_mix):
        batch, chans, tl, lons = field_loc.shape
        degs, lats = p_fwd.shape[1:]
        ml = p_fwd.shape[0] // n
        nb = 4
        chunks = batch // nb
        rows = ml * 2 * nb
        pitch = rows + 1
        half = degs // n - 2
        pieces = 4 if half * 2 * chans % 32 == 0 else 1
        hops = (n // 2 - 1) * pieces
        per = 4
        area = max(2 * lats * pitch, n // 2 * half * 2 * chans)
        depth = min(degs // per, area // (per * 2 * chans))
        held = n // 2 + 1
        packed = (3, chunks, held, 2 * nb, chans)
        tables = fourier_tables(n, ml, lons)
        anywhere = pl.BlockSpec(memory_space=pl.ANY)
        vmem = pl.BlockSpec(memory_space=pltpu.VMEM)
        grad_field, grad_w = pl.pallas_call(
            functools.partial(layer_kernel, 'lat', n, nb, pieces, per, depth),
            name='layer',
            out_shape=(
                pltpu.VMEM((batch, tl, lons, chans), F32),
                pltpu.VMEM((degs * 2 * chans, chans), F32),
            ),
            in_specs=[anywhere] * 6,
            out_specs=(vmem, vmem),
            scratch_shapes=[
                pltpu.VMEM((2, chunks, n, tl, rows, chans), BF16),
                pltpu.VMEM((chunks + 1, n, tl, rows, chans), BF16),
                pltpu.VMEM((area, chans), F32),
                pltpu.VMEM((lats, 2 * nb * chans), BF16),
                pltpu.VMEM((degs, chunks, rows, chans), BF16),
                pltpu.VMEM((degs, chunks, rows, chans), BF16),
                pltpu.VMEM((degs, 2 * chans, chans), BF16),
                pltpu.VMEM((2, max(per, half) * 2 * chans, chans), F32),
                pltpu.VMEM((2, nb, lons, chans), F32),
                pltpu.VMEM((n * rows, chans), F32),
                pltpu.VMEM((2, ml, degs, lats), F32),
                pltpu.VMEM((2, ml, degs, lats), BF16),
                pltpu.VMEM((2, n, n, lats), F32),
                pltpu.VMEM((2, n // 2, 16, 32), F32),
                pltpu.VMEM((32 * 2 * nb, chans), F32),
                pltpu.VMEM((2,) + packed, BF16),
                pltpu.VMEM(packed, BF16),
                pltpu.VMEM((2, n // 2) + packed, BF16),
                pltpu.VMEM((2, n, chunks, 2 * nb, chans), BF16),
                pltpu.VMEM(tables.shape, BF16),
                pltpu.VMEM((chunks, 5, 6, tl, 2 * nb, chans), BF16),
                pltpu.VMEM((2, 4, held, 2 * nb, chans), F32),
                pltpu.VMEM((chunks, 4, held, 2 * nb, chans), F32),
                pltpu.VMEM((chunks, 4, held, 2 * nb, chans), F32),
                pltpu.VMEM((chunks, 2, held, 2 * nb, chans), F32),
                pltpu.VMEM((chunks, 2, held, 2 * nb, chans), F32),
                pltpu.VMEM((chunks, 2, held, 2 * nb, chans), F32),
                pltpu.VMEM((2, n, chunks, 4 * nb, chans), BF16),
                pltpu.SemaphoreType.DMA((4 * chunks,)),
                pltpu.SemaphoreType.DMA((4 * chunks,)),
                pltpu.SemaphoreType.DMA((2,)),
                pltpu.SemaphoreType.DMA((depth,)),
                pltpu.SemaphoreType.DMA((2,)),
                pltpu.SemaphoreType.DMA((2,)),
                pltpu.SemaphoreType.DMA((2,)),
                pltpu.SemaphoreType.DMA((n // 2,)),
                pltpu.SemaphoreType.DMA,
                pltpu.SemaphoreType.DMA((hops,)),
                pltpu.SemaphoreType.DMA,
                pltpu.SemaphoreType.DMA((hops + n // 2 - 1,)),
                pltpu.SemaphoreType.REGULAR,
                pltpu.SemaphoreType.DMA,
                pltpu.SemaphoreType.DMA,
                pltpu.SemaphoreType.DMA,
                pltpu.SemaphoreType.DMA,
                pltpu.SemaphoreType.DMA,
                pltpu.SemaphoreType.DMA((n // 2 - 1,)),
                pltpu.SemaphoreType.DMA,
                pltpu.SemaphoreType.DMA,
                pltpu.SemaphoreType.DMA((2,)),
                pltpu.SemaphoreType.DMA,
                pltpu.SemaphoreType.DMA((chunks,)),
                pltpu.SemaphoreType.DMA((chunks,)),
                pltpu.SemaphoreType.DMA((chunks,)),
                pltpu.SemaphoreType.DMA((chunks,)),
                pltpu.SemaphoreType.DMA((chunks,)),
                pltpu.SemaphoreType.DMA((chunks,)),
                pltpu.SemaphoreType.DMA((chunks,)),
                pltpu.SemaphoreType.DMA((chunks,)),
                pltpu.SemaphoreType.DMA((chunks,)),
                pltpu.SemaphoreType.DMA((chunks,)),
                pltpu.SemaphoreType.DMA((chunks,)),
                pltpu.SemaphoreType.DMA((chunks,)),
                pltpu.SemaphoreType.DMA((chunks,)),
                pltpu.SemaphoreType.DMA,
                pltpu.SemaphoreType.DMA,
                pltpu.SemaphoreType.DMA,
                pltpu.SemaphoreType.DMA,
                pltpu.SemaphoreType.DMA((chunks,)),
            ],
            compiler_params=pltpu.CompilerParams(
                collective_id=0, has_side_effects=True, vmem_limit_bytes=43 << 20),
        )(
            field_loc.transpose(0, 2, 3, 1), grad_loc.transpose(0, 2, 3, 1),
            w_mix.transpose(0, 1, 3, 2).reshape(degs * 2 * chans, chans),
            p_fwd, p_inv, tables)
        grad_field, grad_w = pl.pallas_call(
            put_kernel,
            name='put',
            out_shape=(
                jax.ShapeDtypeStruct(grad_field.shape, F32),
                jax.ShapeDtypeStruct(grad_w.shape, F32),
            ),
            in_specs=[vmem] * 2,
            out_specs=(anywhere, anywhere),
            scratch_shapes=[pltpu.SemaphoreType.DMA((18,))],
            compiler_params=pltpu.CompilerParams(vmem_limit_bytes=1 << 20),
        )(grad_field, grad_w)
        return grad_field.transpose(0, 3, 1, 2), grad_w.reshape(degs, chans, 2, chans).transpose(0, 1, 3, 2)

    return jax.shard_map(
        local_step, mesh=mesh, in_specs=(field_spec, field_spec, P(), P(), P()),
        out_specs=(field_spec, P('member')), check_vma=False)
```

```python
import functools
import math

import jax
import jax.numpy as jnp
import numpy as np
from jax import lax
from jax.experimental import pallas as pl
from jax.experimental.pallas import tpu as pltpu
from jax.sharding import PartitionSpec as P

F32 = jnp.float32
BF16 = jnp.bfloat16


def split_const(matrix):
    head = matrix.astype(BF16)
    tail = (matrix - head.astype(np.float64)).astype(BF16)
    return [head, tail]


def fourier_tables(n, ml, lons):
    modes = n * ml
    device = np.arange(n)
    first = np.where(device % 2 == 0, device // 2, n - 1 - device // 2)
    order = (first[:, None] + n * np.arange(ml)[None, :]).reshape(-1)
    angle = math.tau * (np.outer(order, np.arange(lons)) % lons) / lons
    forward = np.stack([np.cos(angle), -np.sin(angle)], axis=1).reshape(2 * modes, lons) / math.sqrt(lons)
    gains = np.repeat(2.0 - (order == 0), 2)[:, None]
    doubled = forward * gains
    tables = split_const(forward) + split_const(doubled) + split_const(doubled.T) + split_const(forward.T)
    return jnp.stack([jnp.asarray(t) for t in tables])


def gelu_grad(values):
    cumulative = 0.5 * (1.0 + lax.erf(values * math.sqrt(0.5)))
    density = jnp.exp(-0.5 * values * values) / math.sqrt(math.tau)
    return cumulative + values * density


def loop(stop, step, start=0, **options):
    def one(i, carry):
        step(i)
        return carry

    lax.fori_loop(start, stop, one, 0, **options)


def head(size):
    return pl.ds(0, size)


def dot(a, b, dims=((1,), (0,))):
    return lax.dot_general(a, b, (dims, ((), ())), preferred_element_type=F32)


def layer_kernel(
    axis, n, nb, pieces, per, depth,
    f_hbm, dg_hbm, w_hbm, pf_hbm, pv_hbm, tab_hbm,
    df_out, dw_out,
    recv, send, work, xb, coef, dq, vmix, wbuf, inbuf, gather, pbuf, pmat, band, cmat, qs, own, other, packs, lowx, tab,
    topin, partial, mid, sums, sumin, joined, handed, second,
    send_sem, recv_sem, in_sem, w_sem, p_sem, band_sem, pair_send, pair_recv, rs_send, rs_recv, ag_send, ag_recv,
    free_sem, pub_send, pub_recv, own_send, own_recv, pack_send, pack_recv, share_send, share_recv,
    tab_sem, top_send, near_recv, far_recv, next_recv, swap_send, swap_recv,
    row_send, row_recv, mid_send, mid_recv, sum_send, sum_recv, join_send, join_recv,
    always_send, always_recv, some_send, some_recv, hand_recv,
):
    me = lax.axis_index(axis)
    batch, tl, lons, chans = f_hbm.shape
    ml, degs, lats = pmat.shape[1:]
    chunks = batch // nb
    tile = 2 * nb
    rows = ml * tile
    pitch = rows + 1
    modes2 = 2 * n * ml
    units = chunks * tl
    final = chunks - 1
    slots = chunks + 1
    fwd_h, fwd_l, dbl_h, dbl_l, syn_h, syn_l, adj_h, adj_l = (tab.at[k] for k in range(8))
    area = lats * pitch
    top = n * (ml - 1)
    held = n // 2 + 1
    chip, core = lax.div(me, 2), lax.rem(me, 2)
    other_core = 1 - core
    chips = n // 2
    last = chips - 1
    way = 1 - 2 * core
    sides = (-1, 1)
    sibling = me + way

    def chip_at(away):
        return lax.rem(chip + away + chips, chips)

    def across(away, its_core):
        return 2 * chip_at(away) + its_core

    onward = across(way, core)

    def around(k):
        far = chips // 2 - lax.div(k + 1, 2)
        return jnp.where(lax.rem(k, 2) == 0, far, -far)

    def first_mode(device):
        z = lax.div(device, 2)
        return jnp.where(lax.rem(device, 2) == 0, z, n - 1 - z)

    def to(device, src, dst, sent, got):
        return pltpu.make_async_remote_copy(
            src_ref=src, dst_ref=dst, send_sem=sent, recv_sem=got,
            device_id={axis: device}, device_id_type=pl.DeviceIdType.MESH)

    def unit_of(unit):
        return lax.div(unit, tl), lax.rem(unit, tl)

    def unit_in(src, unit):
        ch, t = unit_of(unit)
        slot = lax.rem(unit, 2)
        return pltpu.make_async_copy(src.at[pl.ds(ch * nb, nb), t], inbuf.at[slot], in_sem.at[slot])

    def step_in(src, unit):
        @pl.when(unit + 1 < units)
        def _():
            unit_in(src, unit + 1).start()
        unit_in(src, unit).wait()

    body, peak = head(rows - tile), pl.ds(rows - tile, tile)

    def ship(stage, ch, t0, nt):
        index = stage * chunks + ch
        slot = lax.rem(index, slots)
        part = pl.ds(t0, nt)

        def one(k):
            away = around(k)
            for its_core in (core, other_core):
                peer = across(away, its_core)
                to(peer, send.at[slot, peer, part, body], recv.at[stage % 2, ch, me, part, body],
                   send_sem.at[slot], recv_sem.at[index]).start()

        loop(last, one)
        to(sibling, send.at[slot, sibling, part, body], recv.at[stage % 2, ch, me, part, body],
           send_sem.at[slot], recv_sem.at[index]).start()
        recv[stage % 2, ch, me, part, body] = send[slot, me, part, body]

    def arrived(stage, ch):
        others = recv.at[stage % 2, ch, head(n - 1), :, body]
        pltpu.make_async_copy(others, others, recv_sem.at[stage * chunks + ch]).wait()

    def peaks():
        return send.at[0, head(n - 5), :, peak]

    def wait_sent(index, stage):
        slot = lax.rem(index, slots)
        others = send.at[slot, head(n - 1), :, body]
        pltpu.make_async_copy(others, others, send_sem.at[slot]).wait()
        if stage % 2 == 0:
            ch = index - stage * chunks
            pltpu.make_async_copy(peaks(), peaks(), row_send.at[ch]).wait()

    def send_peak(stage, ch):
        slot = lax.rem(stage * chunks + ch, slots)
        far = chips // 2
        for same in (True, False):
            its_core = core if same else other_core
            for away in range(1 - far, far + 1):
                near = max(-2, min(2, away))
                hop, target, apart = away - near, (0, 2, 4, 3, 1)[near], abs(away - near)
                if away == far:
                    hop = jnp.where(its_core == 0, 2 - far, far - 2)
                    target = jnp.where(its_core == 0, 3, 4)
                source = send.at[slot, across(away, its_core), :, peak]
                place = topin.at[ch, target, 2 * apart + core]
                if same and not apart:
                    place[...] = source[...]
                else:
                    to(across(hop, its_core), source, place,
                       row_send.at[ch], row_recv.at[ch]).start()

    def free_slot(stage, ch):
        index = stage * chunks + ch
        if stage >= 1:
            @pl.when(ch >= 1)
            def _():
                wait_sent(index - slots, stage - 1)
        if stage >= 2:
            @pl.when(ch == 0)
            def _():
                wait_sent(index - slots, stage - 2)
        return lax.rem(index, slots)

    def put_rows(slot, t):
        send[slot, :, t] = gather[...].reshape(n, rows, chans).astype(BF16)

    def transform(values, head, tail):
        high = values.astype(BF16)
        low = (values - high.astype(F32)).astype(BF16)
        return dot(head[...], high) + (dot(tail[...], high) + dot(head[...], low))

    unit_in(f_hbm, 0).start()
    first_tables = pltpu.make_async_copy(tab_hbm.at[head(2)], tab.at[head(2)], tab_sem.at[0])
    other_tables = pltpu.make_async_copy(tab_hbm.at[pl.ds(2, 6)], tab.at[pl.ds(2, 6)], tab_sem.at[1])
    first_tables.start()
    barrier = pltpu.get_barrier_semaphore()

    def announce(k):
        pl.semaphore_signal(barrier, inc=1, device_id={axis: lax.rem(me + k, n)}, device_id_type=pl.DeviceIdType.MESH)

    loop(n, announce, 1)

    first_tables.wait()

    group = max(1, tl // 3)

    parts = degs // per

    def w_in(k):
        slot = lax.rem(k, depth)
        return pltpu.make_async_copy(
            w_hbm.at[pl.ds(k * per * 2 * chans, per * 2 * chans)],
            work.at[pl.ds(slot * per * 2 * chans, per * 2 * chans)], w_sem.at[slot])

    def band_in(d):
        for which, source in enumerate((pf_hbm, pv_hbm)):
            pltpu.make_async_copy(
                source.at[top + first_mode(d), pl.ds(top, n)], band.at[which, d], band_sem.at[which]).start()

    def step1_chunk(ch):
        slot = free_slot(0, ch)

        def row(t):
            unit = ch * tl + t
            step_in(f_hbm, unit)
            buf = lax.rem(unit, 2)
            for b in range(0, nb, 2):
                pair = jnp.concatenate([inbuf[buf, b], inbuf[buf, b + 1]], axis=1)
                spec = transform(pair, fwd_h, fwd_l)
                gather[pl.ds(b, modes2, stride=nb), :] = spec[:, :chans]
                gather[pl.ds(b + 1, modes2, stride=nb), :] = spec[:, chans:]
            put_rows(slot, t)

            @pl.when((ch == 0) & (t == group - 1))
            def _():
                pl.semaphore_wait(barrier, n - 1)
                ship(0, 0, 0, group)


        loop(tl, row)
        send_peak(0, ch)

        @pl.when(ch == 0)
        def _():
            ship(0, 0, group, tl - group)
            other_tables.start()
            for which, source in enumerate((pf_hbm, pv_hbm)):
                for k in range(ml):
                    pltpu.make_async_copy(
                        source.at[first_mode(me) + n * k], pbuf.at[which, k], p_sem.at[which]).start()
            loop(n, band_in)
            for k in range(depth):
                w_in(k).start()


    loop(chunks, step1_chunk)

    unit_in(dg_hbm, 0).start()
    for which in range(2):
        pltpu.make_async_copy(band.at[which], band.at[which], band_sem.at[which]).wait()
    qs[...] = jnp.zeros_like(qs)

    def pack(z, store):
        def one(index):
            half_at, row = lax.div(index, held), lax.rem(index, held)
            p = half_at * (held - 1) + row
            degree = jnp.where(core == 0, jnp.minimum(z + p, n - 1), jnp.maximum(p - 1, 0))
            store(half_at, row, degree, (p < n - z) == (core == 0))

        loop(2 * held, one)

    def project(which, ch, target, device):
        gather[...] = jnp.zeros_like(gather)
        side = 1 if target == 3 else -1

        def place_rows(apart):
            for c in range(2):
                src = across(side * apart, c)
                gather[pl.ds(pl.multiple_of(src * tl * tile, tile), tl * tile), :] = topin[
                    ch, target, 2 * apart + c].reshape(tl * tile, chans).astype(F32)

        place_rows(0)
        if target > 2:
            place_rows(1)

            @pl.when(core == target - 3)
            def _():
                place_rows(2)

        for k in range(tile):
            xb[:, k * chans:(k + 1) * chans] = gather[pl.ds(k, lats, stride=tile), :].astype(BF16)
        out = dot(band[which, device].astype(BF16), xb[...])
        for k in range(tile):
            qs[pl.ds(k, n, stride=tile), :] = out[:, k * chans:(k + 1) * chans]

    def sum_rows(which, ch):
        pltpu.make_async_copy(peaks(), peaks(), row_recv.at[ch]).wait()
        for target, away in enumerate((-1, 1, -2, 2)):
            project(which, ch, target + 1, across(away, core))

            def keep(half_at, row, degree, ours):
                values = qs[pl.ds(pl.multiple_of(degree * tile, tile), tile), :]
                partial[half_at, target, row] = jnp.where(ours, values, jnp.zeros_like(values))

            pack(chip_at(away), keep)
        swap = to(sibling, partial.at[other_core], mid.at[ch], mid_send, mid_recv.at[ch])
        swap.start()
        if which == 1:
            pltpu.make_async_copy(sums.at[ch], sums.at[ch], sum_send.at[ch]).wait()
        swap.wait()
        sums[ch] = partial[core] + mid[ch]
        for side, away in enumerate(sides):
            to(across(away, core), sums.at[ch, 2 + side], handed.at[ch, side],
               sum_send.at[ch], hand_recv.at[ch]).start()

    def pass_sums(ch):
        pltpu.make_async_copy(handed.at[ch], handed.at[ch], hand_recv.at[ch]).wait()
        for side, away in enumerate(sides):
            sums[ch, side] += handed[ch, side]
            to(across(away, core), sums.at[ch, side], sumin.at[ch, side],
               sum_send.at[ch], sum_recv.at[ch]).start()

    def finish_peak(which, ch):
        pltpu.make_async_copy(sumin.at[ch], sumin.at[ch], sum_recv.at[ch]).wait()
        joined[ch, core] = sumin[ch, 0] + sumin[ch, 1]
        swap = to(sibling, joined.at[ch, core], joined.at[ch, core], join_send, join_recv.at[ch])
        swap.start()
        project(which, ch, 0, me)
        swap.wait()

        def one(degree):
            p = jnp.where(core == 0, degree - chip, degree + 1)
            ours = degree >= first_mode(me)
            p = jnp.maximum(p, 0)
            h = jnp.where(p > held - 1, 1, 0)
            come = joined[ch, h, p - h * (held - 1)]
            work[pl.ds(area + (top + degree) * pitch + rows - tile, tile), :] = qs[
                pl.ds(pl.multiple_of(degree * tile, tile), tile), :] + jnp.where(ours, come, jnp.zeros_like(come))

        loop(n, one)

    sum_rows(0, 0)

    def ship_rows(ch):
        ship(0, ch, 0, tl)

    loop(final, ship_rows, 1)
    for which in range(2):
        pltpu.make_async_copy(pbuf.at[which], pbuf.at[which], p_sem.at[which]).wait()
    pmat[...] = pbuf[...].astype(BF16)
    other_tables.wait()

    def load_w(k):
        w_in(k).wait()
        base = lax.rem(k, depth) * per * 2 * chans
        for j in range(per):
            for part in range(2):
                vmix[k * per + j, pl.ds(part * chans, chans)] = work[
                    pl.ds(base + j * 2 * chans + part, chans, stride=2), :].astype(BF16)

        @pl.when(k + depth < parts)
        def _():
            w_in(k + depth).start()


    loop(parts, load_w)

    span = cmat.shape[3]
    mine_t = (lax.broadcasted_iota(jnp.int32, (8, lats), 1) == me * tl + lax.broadcasted_iota(jnp.int32, (8, lats), 0))
    mine_t &= lax.broadcasted_iota(jnp.int32, (8, lats), 0) < tl
    mine_t = jnp.where(mine_t, 1.0, 0.0).astype(BF16)

    def tabulate(d):
        z, of_core = lax.div(d, 2), lax.rem(d, 2)
        row = lax.broadcasted_iota(jnp.int32, (n, span), 0)
        p = jnp.where(of_core == 0, row - z, row + 1)
        target = jnp.where(p > held - 1, p + 1, p)
        moved = jnp.where(target == lax.broadcasted_iota(jnp.int32, (n, span), 1), 1.0, 0.0).astype(BF16)
        for which in range(2):
            picked = dot(mine_t, band[which, d].astype(BF16), ((1,), (1,))).astype(BF16)
            cmat[which, z, pl.ds(pl.multiple_of(of_core * 8, 8), 8), :] = dot(picked, moved)

    loop(n, tabulate)

    def no_degree(l):
        work[pl.ds(area + l * pitch + rows - tile, tile), :] = jnp.zeros((tile, chans), F32)

    loop(top, no_degree)

    pass_sums(0)

    def sum_first(ch):
        sum_rows(0, ch)

    loop(chunks, sum_first, 1)
    ship(0, final, 0, tl)
    loop(chunks, pass_sums, 1)

    sign = jnp.where(lax.broadcasted_iota(jnp.int32, (tile, chans), 0) < nb, -1.0, 1.0).astype(F32)

    def turn(values):
        groups = values.reshape(-1, tile, chans)
        return (pltpu.roll(groups, nb, 1) * sign[None]).reshape(values.shape)

    def legendre(src, dst, which, over):
        def mode(m):
            for k in range(tile):
                xb[:, k * chans:(k + 1) * chans] = work[
                    pl.ds(src + m * tile + k, lats, stride=pitch), :].astype(BF16)
            out = dot(pmat[which, m], xb[...], ((over,), (0,)))
            for k in range(tile):
                work[pl.ds(dst + m * tile + k, degs, stride=pitch), :] = out[:, k * chans:(k + 1) * chans]

        loop(ml - 1, mode)

    def unload(stage, ch):
        def body(src):
            for t in range(tl):
                work[pl.ds((src * tl + t) * pitch, rows), :] = recv[stage % 2, ch, src, t].astype(F32)

        loop(n, body)

    def load(slot):
        def body(dev):
            for t in range(tl):
                send[slot, dev, t] = work[pl.ds(area + (dev * tl + t) * pitch, rows), :].astype(BF16)

        loop(n, body)

    def only(ours, values):
        values = values.astype(F32)
        return jnp.where(ours, values, jnp.zeros_like(values)).astype(BF16)

    def spectral(stage, ch, into, kept, mix):
        arrived(stage - 1, ch)
        unload(stage - 1, ch)
        legendre(0, area, into, 1)
        finish_peak(into, ch)

        def degree(l):
            x = work[pl.ds(area + l * pitch, rows), :].astype(BF16)
            kept[l, ch] = x
            work[pl.ds(l * pitch, rows), :] = mix(l, x)

        loop(degs, degree, unroll=8)

        def keep_top(half_at, row, degree, ours):
            own[half_at, 2, ch, row] = only(ours, work[pl.ds((top + degree) * pitch + rows - tile, tile), :])

        pack(chip, keep_top)
        if stage == 1:
            swap = to(sibling, own.at[other_core, 2, ch], other.at[2, ch], swap_send, swap_recv.at[ch])
            swap.start()
        legendre(0, area, 1 - into, 0)
        load(free_slot(stage, ch))
        if stage == 1:
            swap.wait()
            packs[core, chip, 2, ch] = (own[core, 2, ch].astype(F32) + other[2, ch].astype(F32)).astype(BF16)

            @pl.when(ch == final - 1)
            def _():
                relay_near(ch - 1)

            for away in sides:
                top_copy(0, away, ch, near_recv).start()
        else:
            @pl.when(ch == 0)
            def _():
                pass_sums(final - 1)
                sum_rows(1, final)

            @pl.when(ch == 1)
            def _():
                pass_sums(final)

        if stage == 1:
            @pl.when(ch < final)
            def _():
                ship(stage, ch, 0, tl)
        else:
            ship(stage, ch, 0, tl)

    def top_copy(source, away, ch, got):
        block = packs.at[core, chip_at(source), 2, ch]
        return to(across(away, core), block, block, top_send, got.at[ch])

    def top_blocks(count, ch):
        return packs.at[core, head(count), 2, ch]

    def relay_near(ch):
        pltpu.make_async_copy(top_blocks(2, ch), top_blocks(2, ch), near_recv.at[ch]).wait()
        for side in sides:
            top_copy(-side, side, ch, next_recv).start()

    def relay_next(ch):
        pltpu.make_async_copy(top_blocks(2, ch), top_blocks(2, ch), next_recv.at[ch]).wait()
        for side in sides:
            top_copy(-2 * side, side, ch, far_recv).start()
        top_copy(-2 * way, 2 * way, ch, far_recv).start()

    def apply_top(which, ch, z):
        for h in range(2):
            qs[pl.ds(h * held * tile, held * tile), :] = packs[h, z, 2, ch].reshape(held * tile, chans).astype(F32)
        for k in range(tile):
            xb[0:span, k * chans:(k + 1) * chans] = qs[pl.ds(k, span, stride=tile), :].astype(BF16)
        out = dot(cmat[which, z].astype(BF16), xb[0:span, :])
        for k in range(tile):
            gather[pl.ds(k, 16, stride=tile), :] = out[:, k * chans:(k + 1) * chans]
        for c in range(2):
            for t in range(tl):
                recv[1, ch, 2 * z + c, t, pl.ds(rows - tile, tile)] = gather[
                    pl.ds((8 * c + t) * tile, tile), :].astype(BF16)

    def mix_forward(l, x):
        both = dot(x, vmix[l], ((1,), (1,)))
        return both[:, :chans] + turn(both[:, chans:])

    def mix_adjoint(l, x):
        both = dot(x, jnp.concatenate([vmix[l, head(chans)], vmix[l, pl.ds(chans, chans)]], axis=1))
        return both[:, :chans] - turn(both[:, chans:])

    def step2_chunk(ch):
        spectral(1, ch, 0, coef, mix_forward)

    loop(chunks, step2_chunk)
    relay_next(final - 2)
    relay_near(final - 1)
    ship(1, final, 0, tl)

    def fetch_rows(stage, ch, t):
        for src in range(n):
            gather[pl.ds(src * rows, rows), :] = recv[stage % 2, ch, src, t].astype(F32)

    def fetch_pair(b):
        return jnp.concatenate(
            [gather[pl.ds(b, modes2, stride=nb), :], gather[pl.ds(b + 1, modes2, stride=nb), :]], axis=1).astype(BF16)

    def step3_chunk(ch):
        arrived(1, ch)

        @pl.when(ch == 0)
        def _():
            relay_near(final)
            relay_next(final - 1)

        pltpu.make_async_copy(top_blocks(3, ch), top_blocks(3, ch), far_recv.at[ch]).wait()
        swap = to(sibling, top_blocks(chips, ch), top_blocks(chips, ch), swap_send, swap_recv.at[ch])
        swap.start()

        @pl.when(ch == 1)
        def _():
            relay_next(final)

        swap.wait()

        @pl.when(ch == final)
        def _():
            all_sent = packs.at[0, head(7), 2]
            pltpu.make_async_copy(all_sent, all_sent, top_send).wait()

        def apply(z):
            apply_top(1, ch, z)

        loop(chips, apply)

        @pl.when(ch == 1)
        def _():
            sum_rows(1, 0)

        slot = free_slot(2, ch)

        def row(t):
            unit = ch * tl + t
            step_in(dg_hbm, unit)
            buf = lax.rem(unit, 2)
            fetch_rows(1, ch, t)
            for b in range(0, nb, 2):
                g = fetch_pair(b)
                hidden = dot(syn_h[...], g) + dot(syn_l[...], g)
                pair = jnp.concatenate([inbuf[buf, b], inbuf[buf, b + 1]], axis=1)
                spec = transform(pair * gelu_grad(hidden), dbl_h, dbl_l)
                gather[pl.ds(b, modes2, stride=nb), :] = spec[:, :chans]
                gather[pl.ds(b + 1, modes2, stride=nb), :] = spec[:, chans:]
            put_rows(slot, t)

        loop(tl, row)
        send_peak(2, ch)

        @pl.when(ch < final)
        def _():
            ship(2, ch, 0, tl)


    loop(chunks, step3_chunk)

    def sum_second(ch):
        pass_sums(ch - 1)
        sum_rows(1, ch)

    loop(final, sum_second, 1)
    ship(2, final, 0, tl)
    unit_in(dg_hbm, 0).start()

    def step4_chunk(ch):
        spectral(3, ch, 1, dq, mix_adjoint)

    loop(chunks, step4_chunk)

    for which, kept in enumerate((coef, dq)):
        def keep_low(half_at, row, degree, ours):
            own[half_at, which, :, row] = only(ours, kept[degree, :, head(tile)])

        pack(chip, keep_low)

    def both_parts(peer, action):
        degree = n + first_mode(peer)
        for which, kept in enumerate((coef, dq)):
            action(to(peer, kept.at[degree, :, head(tile)], second.at[which, me, :, head(tile)],
                      always_send, always_recv))

            @pl.when(first_mode(me) <= first_mode(peer))
            def _():
                more = pl.ds(tile, tile)
                action(to(peer, kept.at[degree, :, more], second.at[which, me, :, more],
                          some_send, some_recv))

    def send_second(k):
        both_parts(lax.rem(me + k, n), lambda copy: copy.start())

    loop(n, send_second, 1)
    for which, kept in enumerate((coef, dq)):
        second[which, me] = kept[n + first_mode(me), :, head(2 * tile)]

    def clear_second(src):
        @pl.when(first_mode(src) > first_mode(me))
        def _():
            for which in range(2):
                second[which, src, :, pl.ds(tile, tile)] = jnp.zeros((chunks, tile, chans), BF16)

    loop(n, clear_second)
    own_copy = to(sibling, own.at[other_core], other, own_send, own_recv)
    own_copy.start()

    def pack_block(k):
        return packs.at[core, chip_at(-way * k)]

    def pack_copy(k):
        return to(onward, pack_block(k), pack_block(k), pack_send, pack_recv.at[k])

    def share(k):
        to(sibling, pack_block(k), pack_block(k), share_send, share_recv).start()

    half = degs // n - 2
    wide = 2 * chans
    block_rows = half * wide
    piece = block_rows // pieces
    hops = (last) * pieces

    def block_at(k, direction):
        return lax.rem(chip - direction * (1 + k) + 2 * chips, chips)

    def outer(dst, row, pairs):
        real = jnp.zeros((chans, chans), F32)
        imag = jnp.zeros((chans, chans), F32)
        for y, x in pairs:
            real += dot(y, x, ((0,), (0,)))
            imag -= dot(turn(y.astype(F32)).astype(BF16), x, ((0,), (0,)))
        dst[pl.ds(row, chans, stride=2), :] = real
        dst[pl.ds(row + 1, chans, stride=2), :] = imag

    def first_degree(block, of_core):
        return 2 * n + (2 * block + of_core) * half

    def weight_grad(dst, degree):
        def one(j):
            outer(dst, j * wide, [(dq[degree + j, ch], coef[degree + j, ch]) for ch in range(chunks)])

        loop(half, one)

    def pair_copy(k):
        slot = lax.rem(k, 2)
        rows_there = pl.ds(first_degree(block_at(k, -way), core) * wide, block_rows)
        return to(sibling, wbuf.at[slot, head(block_rows)], dw_out.at[rows_there],
                  pair_send.at[slot], pair_recv.at[k])

    def weight_block(k):
        @pl.when(k >= 2)
        def _():
            pair_copy(k - 2).wait_send()
        weight_grad(wbuf.at[lax.rem(k, 2)], first_degree(block_at(k, -way), other_core))
        pair_copy(k).start()
        block = block_at(k, way)
        weight_grad(work.at[pl.ds(block * block_rows, block_rows)], first_degree(block, core))

    loop(chips, weight_block)
    pair_copy(chips - 2).wait_send()
    pair_copy(last).wait_send()
    own_copy.wait()
    packs[core, chip] = (own[core].astype(F32) + other[...].astype(F32)).astype(BF16)

    def low_degree(l):
        def one(z):
            for c in range(2):
                p = l - z if c == 0 else l + 1
                ours = p >= 0 if c == 0 else p >= n - z
                p = jnp.maximum(p, 0)
                h = jnp.where(p > held - 1, 1, 0)
                for which in range(2):
                    lowx[which, 2 * z + c] = only(ours, packs[h, z, which, :, p - h * (held - 1)])

        loop(chips, one)
        outer(wbuf.at[0], 0, [(lowx[1].reshape(-1, chans), lowx[0].reshape(-1, chans))])
        dw_out[pl.ds(l * wide, wide)] = wbuf[0, head(wide)]

    def final_rows(unit):
        ch, t = unit_of(unit)

        step_in(dg_hbm, unit)
        buf = lax.rem(unit, 2)

        fetch_rows(3, ch, t)
        for b in range(0, nb, 2):
            g = fetch_pair(b)
            change = dot(adj_h[...], g) + dot(adj_l[...], g)
            df_out[ch * nb + b, t] = inbuf[buf, b] + change[:, :chans]
            df_out[ch * nb + b + 1, t] = inbuf[buf, b + 1] + change[:, chans:]

    def place(i, of_core):
        block = block_at(lax.div(i, pieces), way)
        start = lax.rem(i, pieces) * piece
        return pl.ds(block * block_rows + start, piece), pl.ds(first_degree(block, of_core) * wide + start, piece)

    def rs_copy(i):
        here, there = place(i, core)
        return to(onward, work.at[here], dw_out.at[there], rs_send, rs_recv.at[i])

    def add_pair(i):
        here, passed = place(i, other_core)

        @pl.when(lax.rem(i, pieces) == 0)
        def _():
            pair_copy(lax.div(i, pieces)).wait_recv()

        work[here] += dw_out[passed]

    def rs_step(i):
        add_pair(i)

        @pl.when(i >= pieces)
        def _():
            rs_copy(i - pieces).wait_recv()
            here, there = place(i, core)
            work[here] += dw_out[there]

        rs_copy(i).start()

        @pl.when(lax.rem(i, pieces) == 0)
        def _():
            k = lax.div(i, pieces)

            @pl.when(k > 0)
            def _():
                pack_copy(k - 1).wait_recv()

            pack_copy(k).start()
            share(k)


    loop(hops, rs_step)
    pack_copy(chips - 2).wait_recv()
    share(last)

    def own_sum(s):
        i = hops + s
        add_pair(i)
        rs_copy(i - pieces).wait_recv()
        here, there = place(i, core)
        dw_out[there] += work[here]
        ag_copy(i, s).start()

    def second_spot(k):
        return pl.ds((n + first_mode(2 * block_at(k, way) + core)) * wide, wide)

    def second_copy(k, got):
        spot = dw_out.at[second_spot(k)]
        return to(onward, spot, spot, ag_send, ag_recv.at[hops + got])

    def second_publish(k):
        spot = dw_out.at[second_spot(k)]
        to(sibling, spot, spot, pub_send, pub_recv).start()

    def ag_copy(i, got):
        _, there = place(i, core)
        return to(onward, dw_out.at[there], dw_out.at[there], ag_send, ag_recv.at[got])

    def publish(i):
        _, there = place(i, core)
        to(sibling, dw_out.at[there], dw_out.at[there], pub_send, pub_recv).start()

    firsts = second.at[:, head(n - 1), :, head(tile)]
    pltpu.make_async_copy(firsts, firsts, always_recv).wait()

    comes, goes = first_mode(me), n - 1 - first_mode(me)

    def wait_some(count, sem):
        for k in range(1, n):
            @pl.when(count == k)
            def _():
                part = second.at[:, head(k), :, pl.ds(tile, tile)]
                pltpu.make_async_copy(part, part, sem).wait()

    wait_some(comes, some_recv)
    outer(wbuf.at[0], 0, [(second[1].reshape(-1, chans), second[0].reshape(-1, chans))])
    dw_out[second_spot(last)] = wbuf[0, head(wide)]
    loop(pieces, own_sum)
    second_copy(last, 0).start()

    pl.semaphore_signal(free_sem, inc=1, device_id={axis: sibling}, device_id_type=pl.DeviceIdType.MESH)
    pl.semaphore_wait(free_sem, 1)

    def own_piece(s):
        publish(hops + s)

    loop(pieces, own_piece)
    second_publish(last)
    gathered = packs.at[other_core]
    pltpu.make_async_copy(gathered, gathered, share_recv).wait()

    def task(i):
        @pl.when(i < chips)
        def _():
            for ch in range(chunks):
                @pl.when(i == 0)
                def _():
                    arrived(3, ch)
                apply_top(0, ch, i)

        @pl.when((i >= chips) & (i < chips + units))
        def _():
            final_rows(i - chips)

        @pl.when(i < n)
        def _():
            low_degree(i)

    def ag_step(i):
        ag_copy(i, i).wait_recv()

        @pl.when(i + pieces < hops)
        def _():
            ag_copy(i, i + pieces).start()

        publish(i)

        @pl.when(lax.rem(i, pieces) == pieces - 1)
        def _():
            k = lax.div(i, pieces)
            second_copy(k, k).wait_recv()

            @pl.when(k < chips - 2)
            def _():
                second_copy(k, k + 1).start()

            second_publish(k)

        task(i)

    loop(hops, ag_step)

    def rest(i):
        task(i)

    loop(max(hops, chips + units, n), rest, hops)

    wait_sent(2 * chunks + final, 2)
    for ch in range(chunks):
        wait_sent(3 * chunks + ch, 3)
    for ch in range(chunks):
        pltpu.make_async_copy(sums.at[ch], sums.at[ch], sum_send.at[ch]).wait()
    sent = work.at[head((last) * block_rows)]
    pltpu.make_async_copy(sent, sent, rs_send).wait()
    sent = dw_out.at[head((last) * (block_rows + wide))]
    pltpu.make_async_copy(sent, sent, ag_send).wait()
    pltpu.make_async_copy(firsts, firsts, always_send).wait()

    wait_some(goes, some_send)
    sent = packs.at[0, head(last)]
    pltpu.make_async_copy(sent, sent, pack_send).wait()
    pltpu.make_async_copy(packs.at[0], packs.at[0], share_send).wait()
    shared = dw_out.at[head(chips * (block_rows + wide))]
    pltpu.make_async_copy(shared, shared, pub_send).wait()
    pltpu.make_async_copy(shared, shared, pub_recv).wait()


def put_kernel(df_ref, dw_ref, df_hbm, dw_hbm, sems):
    copies = []
    for source, target, parts in ((df_ref, df_hbm, 6), (dw_ref, dw_hbm, 12)):
        size = source.shape[0] // parts
        for k in range(parts):
            part = pl.ds(k * size, size)
            copies.append(pltpu.make_async_copy(source.at[part], target.at[part], sems.at[len(copies)]))
    for copy in copies:
        copy.start()
    for copy in copies:
        copy.wait()


def solution(mesh):
    n = mesh.shape['lat']
    field_spec = P('member', None, 'lat')

    def local_step(field_loc, grad_loc, p_fwd, p_inv, w_mix):
        batch, chans, tl, lons = field_loc.shape
        degs, lats = p_fwd.shape[1:]
        ml = p_fwd.shape[0] // n
        nb = 4
        chunks = batch // nb
        rows = ml * 2 * nb
        pitch = rows + 1
        half = degs // n - 2
        pieces = 4 if half * 2 * chans % 32 == 0 else 1
        hops = (n // 2 - 1) * pieces
        per = 4
        area = max(2 * lats * pitch, n // 2 * half * 2 * chans)
        depth = min(degs // per, area // (per * 2 * chans))
        held = n // 2 + 1
        packed = (3, chunks, held, 2 * nb, chans)
        tables = fourier_tables(n, ml, lons)
        anywhere = pl.BlockSpec(memory_space=pl.ANY)
        vmem = pl.BlockSpec(memory_space=pltpu.VMEM)
        grad_field, grad_w = pl.pallas_call(
            functools.partial(layer_kernel, 'lat', n, nb, pieces, per, depth),
            name='layer',
            out_shape=(
                pltpu.VMEM((batch, tl, lons, chans), F32),
                pltpu.VMEM((degs * 2 * chans, chans), F32),
            ),
            in_specs=[anywhere] * 6,
            out_specs=(vmem, vmem),
            scratch_shapes=[
                pltpu.VMEM((2, chunks, n, tl, rows, chans), BF16),
                pltpu.VMEM((chunks + 1, n, tl, rows, chans), BF16),
                pltpu.VMEM((area, chans), F32),
                pltpu.VMEM((lats, 2 * nb * chans), BF16),
                pltpu.VMEM((degs, chunks, rows, chans), BF16),
                pltpu.VMEM((degs, chunks, rows, chans), BF16),
                pltpu.VMEM((degs, 2 * chans, chans), BF16),
                pltpu.VMEM((2, max(per, half) * 2 * chans, chans), F32),
                pltpu.VMEM((2, nb, lons, chans), F32),
                pltpu.VMEM((n * rows, chans), F32),
                pltpu.VMEM((2, ml, degs, lats), F32),
                pltpu.VMEM((2, ml, degs, lats), BF16),
                pltpu.VMEM((2, n, n, lats), F32),
                pltpu.VMEM((2, n // 2, 16, 32), F32),
                pltpu.VMEM((32 * 2 * nb, chans), F32),
                pltpu.VMEM((2,) + packed, BF16),
                pltpu.VMEM(packed, BF16),
                pltpu.VMEM((2, n // 2) + packed, BF16),
                pltpu.VMEM((2, n, chunks, 2 * nb, chans), BF16),
                pltpu.VMEM(tables.shape, BF16),
                pltpu.VMEM((chunks, 5, 6, tl, 2 * nb, chans), BF16),
                pltpu.VMEM((2, 4, held, 2 * nb, chans), F32),
                pltpu.VMEM((chunks, 4, held, 2 * nb, chans), F32),
                pltpu.VMEM((chunks, 4, held, 2 * nb, chans), F32),
                pltpu.VMEM((chunks, 2, held, 2 * nb, chans), F32),
                pltpu.VMEM((chunks, 2, held, 2 * nb, chans), F32),
                pltpu.VMEM((chunks, 2, held, 2 * nb, chans), F32),
                pltpu.VMEM((2, n, chunks, 4 * nb, chans), BF16),
                pltpu.SemaphoreType.DMA((chunks + 1,)),
                pltpu.SemaphoreType.DMA((4 * chunks,)),
                pltpu.SemaphoreType.DMA((2,)),
                pltpu.SemaphoreType.DMA((depth,)),
                pltpu.SemaphoreType.DMA((2,)),
                pltpu.SemaphoreType.DMA((2,)),
                pltpu.SemaphoreType.DMA((2,)),
                pltpu.SemaphoreType.DMA((n // 2,)),
                pltpu.SemaphoreType.DMA,
                pltpu.SemaphoreType.DMA((hops,)),
                pltpu.SemaphoreType.DMA,
                pltpu.SemaphoreType.DMA((hops + n // 2 - 1,)),
                pltpu.SemaphoreType.REGULAR,
                pltpu.SemaphoreType.DMA,
                pltpu.SemaphoreType.DMA,
                pltpu.SemaphoreType.DMA,
                pltpu.SemaphoreType.DMA,
                pltpu.SemaphoreType.DMA,
                pltpu.SemaphoreType.DMA((n // 2 - 1,)),
                pltpu.SemaphoreType.DMA,
                pltpu.SemaphoreType.DMA,
                pltpu.SemaphoreType.DMA((2,)),
                pltpu.SemaphoreType.DMA,
                pltpu.SemaphoreType.DMA((chunks,)),
                pltpu.SemaphoreType.DMA((chunks,)),
                pltpu.SemaphoreType.DMA((chunks,)),
                pltpu.SemaphoreType.DMA,
                pltpu.SemaphoreType.DMA((chunks,)),
                pltpu.SemaphoreType.DMA((chunks,)),
                pltpu.SemaphoreType.DMA((chunks,)),
                pltpu.SemaphoreType.DMA,
                pltpu.SemaphoreType.DMA((chunks,)),
                pltpu.SemaphoreType.DMA((chunks,)),
                pltpu.SemaphoreType.DMA((chunks,)),
                pltpu.SemaphoreType.DMA,
                pltpu.SemaphoreType.DMA((chunks,)),
                pltpu.SemaphoreType.DMA,
                pltpu.SemaphoreType.DMA,
                pltpu.SemaphoreType.DMA,
                pltpu.SemaphoreType.DMA,
                pltpu.SemaphoreType.DMA((chunks,)),
            ],
            compiler_params=pltpu.CompilerParams(
                collective_id=0, has_side_effects=True, vmem_limit_bytes=43 << 20),
        )(
            field_loc.transpose(0, 2, 3, 1), grad_loc.transpose(0, 2, 3, 1),
            w_mix.transpose(0, 1, 3, 2).reshape(degs * 2 * chans, chans),
            p_fwd, p_inv, tables)
        grad_field, grad_w = pl.pallas_call(
            put_kernel,
            name='put',
            out_shape=(
                jax.ShapeDtypeStruct(grad_field.shape, F32),
                jax.ShapeDtypeStruct(grad_w.shape, F32),
            ),
            in_specs=[vmem] * 2,
            out_specs=(anywhere, anywhere),
            scratch_shapes=[pltpu.SemaphoreType.DMA((18,))],
            compiler_params=pltpu.CompilerParams(vmem_limit_bytes=1 << 20),
        )(grad_field, grad_w)
        return grad_field.transpose(0, 3, 1, 2), grad_w.reshape(degs, chans, 2, chans).transpose(0, 1, 3, 2)

    return jax.shard_map(
        local_step, mesh=mesh, in_specs=(field_spec, field_spec, P(), P(), P()),
        out_specs=(field_spec, P('member')), check_vma=False)
```

```python
import functools
import math

import jax
import jax.numpy as jnp
import numpy as np
from jax import lax
from jax.experimental import pallas as pl
from jax.experimental.pallas import tpu as pltpu
from jax.sharding import PartitionSpec as P

F32 = jnp.float32
BF16 = jnp.bfloat16


def split_const(matrix):
    head = matrix.astype(BF16)
    tail = (matrix - head.astype(np.float64)).astype(BF16)
    return [head, tail]


def fourier_tables(n, ml, lons):
    modes = n * ml
    device = np.arange(n)
    first = np.where(device % 2 == 0, device // 2, n - 1 - device // 2)
    order = (first[:, None] + n * np.arange(ml)[None, :]).reshape(-1)
    angle = math.tau * (np.outer(order, np.arange(lons)) % lons) / lons
    forward = np.stack([np.cos(angle), -np.sin(angle)], axis=1).reshape(2 * modes, lons) / math.sqrt(lons)
    gains = np.repeat(2.0 - (order == 0), 2)[:, None]
    doubled = forward * gains
    tables = split_const(forward) + split_const(doubled) + split_const(doubled.T) + split_const(forward.T)
    return jnp.stack([jnp.asarray(t) for t in tables])


def gelu_grad(values):
    cumulative = 0.5 * (1.0 + lax.erf(values * math.sqrt(0.5)))
    density = jnp.exp(-0.5 * values * values) / math.sqrt(math.tau)
    return cumulative + values * density


def loop(stop, step, start=0, **options):
    def one(i, carry):
        step(i)
        return carry

    lax.fori_loop(start, stop, one, 0, **options)


def head(size):
    return pl.ds(0, size)


def dot(a, b, dims=((1,), (0,))):
    return lax.dot_general(a, b, (dims, ((), ())), preferred_element_type=F32)


def layer_kernel(
    axis, n, nb, pieces, per, depth,
    f_hbm, dg_hbm, w_hbm, pf_hbm, pv_hbm, tab_hbm,
    df_out, dw_out,
    recv, send, work, xb, coef, dq, vmix, wbuf, inbuf, gather, pbuf, pmat, band, cmat, qs, own, other, packs, lowx, tab,
    topin, partial, mid, sums, sumin, joined, handed, second,
    send_sem, recv_sem, in_sem, w_sem, p_sem, band_sem, pair_send, pair_recv, rs_send, rs_recv, ag_send, ag_recv,
    free_sem, pub_send, pub_recv, own_send, own_recv, pack_send, pack_recv, share_send, share_recv,
    tab_sem, top_send, near_recv, far_recv, next_recv, swap_send, swap_recv,
    row_send, row_recv, mid_send, mid_recv, sum_send, sum_recv, join_send, join_recv,
    always_send, always_recv, some_send, some_recv, hand_recv,
):
    me = lax.axis_index(axis)
    batch, tl, lons, chans = f_hbm.shape
    ml, degs, lats = pmat.shape[1:]
    chunks = batch // nb
    tile = 2 * nb
    rows = ml * tile
    pitch = rows + 1
    modes2 = 2 * n * ml
    units = chunks * tl
    final = chunks - 1
    slots = chunks + 1
    fwd_h, fwd_l, dbl_h, dbl_l, syn_h, syn_l, adj_h, adj_l = (tab.at[k] for k in range(8))
    area = lats * pitch
    top = n * (ml - 1)
    held = n // 2 + 1
    chip, core = lax.div(me, 2), lax.rem(me, 2)
    other_core = 1 - core
    chips = n // 2
    last = chips - 1
    way = 1 - 2 * core
    sides = (-1, 1)
    sibling = me + way

    def chip_at(away):
        return lax.rem(chip + away + chips, chips)

    def across(away, its_core):
        return 2 * chip_at(away) + its_core

    onward = across(way, core)

    def around(k):
        far = chips // 2 - lax.div(k + 1, 2)
        return jnp.where(lax.rem(k, 2) == 0, far, -far)

    def first_mode(device):
        z = lax.div(device, 2)
        return jnp.where(lax.rem(device, 2) == 0, z, n - 1 - z)

    def to(device, src, dst, sent, got):
        return pltpu.make_async_remote_copy(
            src_ref=src, dst_ref=dst, send_sem=sent, recv_sem=got,
            device_id={axis: device}, device_id_type=pl.DeviceIdType.MESH)

    def unit_of(unit):
        return lax.div(unit, tl), lax.rem(unit, tl)

    def unit_in(src, unit):
        ch, t = unit_of(unit)
        slot = lax.rem(unit, 2)
        return pltpu.make_async_copy(src.at[pl.ds(ch * nb, nb), t], inbuf.at[slot], in_sem.at[slot])

    def step_in(src, unit):
        @pl.when(unit + 1 < units)
        def _():
            unit_in(src, unit + 1).start()
        unit_in(src, unit).wait()

    body, peak = head(rows - tile), pl.ds(rows - tile, tile)

    def ship(stage, ch, t0, nt):
        index = stage * chunks + ch
        slot = lax.rem(index, slots)
        part = pl.ds(t0, nt)

        def one(k):
            away = around(k)
            for its_core in (core, other_core):
                peer = across(away, its_core)
                to(peer, send.at[slot, peer, part, body], recv.at[stage % 2, ch, me, part, body],
                   send_sem.at[slot], recv_sem.at[index]).start()

        loop(last, one)
        to(sibling, send.at[slot, sibling, part, body], recv.at[stage % 2, ch, me, part, body],
           send_sem.at[slot], recv_sem.at[index]).start()
        recv[stage % 2, ch, me, part, body] = send[slot, me, part, body]

    def arrived(stage, ch):
        others = recv.at[stage % 2, ch, head(n - 1), :, body]
        pltpu.make_async_copy(others, others, recv_sem.at[stage * chunks + ch]).wait()

    def peaks():
        return send.at[0, head(n - 5), :, peak]

    def wait_sent(index, stage):
        slot = lax.rem(index, slots)
        others = send.at[slot, head(n - 1), :, body]
        pltpu.make_async_copy(others, others, send_sem.at[slot]).wait()
        if stage % 2 == 0:
            ch = index - stage * chunks
            pltpu.make_async_copy(peaks(), peaks(), row_send.at[ch]).wait()

    def send_peak(stage, ch):
        slot = lax.rem(stage * chunks + ch, slots)
        far = chips // 2
        for same in (True, False):
            its_core = core if same else other_core
            for away in range(1 - far, far + 1):
                near = max(-2, min(2, away))
                hop, target, apart = away - near, (0, 2, 4, 3, 1)[near], abs(away - near)
                if away == far:
                    hop = jnp.where(its_core == 0, 2 - far, far - 2)
                    target = jnp.where(its_core == 0, 3, 4)
                source = send.at[slot, across(away, its_core), :, peak]
                place = topin.at[ch, target, 2 * apart + core]
                if same and not apart:
                    place[...] = source[...]
                else:
                    to(across(hop, its_core), source, place,
                       row_send.at[ch], row_recv.at[ch]).start()

    def free_slot(stage, ch):
        index = stage * chunks + ch
        if stage >= 1:
            @pl.when(ch >= 1)
            def _():
                wait_sent(index - slots, stage - 1)
        if stage >= 2:
            @pl.when(ch == 0)
            def _():
                wait_sent(index - slots, stage - 2)
        return lax.rem(index, slots)

    def put_rows(slot, t):
        send[slot, :, t] = gather[...].reshape(n, rows, chans).astype(BF16)

    def transform(values, head, tail):
        high = values.astype(BF16)
        low = (values - high.astype(F32)).astype(BF16)
        return dot(head[...], high) + (dot(tail[...], high) + dot(head[...], low))

    unit_in(f_hbm, 0).start()
    first_tables = pltpu.make_async_copy(tab_hbm.at[head(2)], tab.at[head(2)], tab_sem.at[0])
    other_tables = pltpu.make_async_copy(tab_hbm.at[pl.ds(2, 6)], tab.at[pl.ds(2, 6)], tab_sem.at[1])
    first_tables.start()
    barrier = pltpu.get_barrier_semaphore()

    def announce(k):
        pl.semaphore_signal(barrier, inc=1, device_id={axis: lax.rem(me + k, n)}, device_id_type=pl.DeviceIdType.MESH)

    loop(n, announce, 1)

    first_tables.wait()

    group = max(1, tl // 3)

    parts = degs // per

    def w_in(k):
        slot = lax.rem(k, depth)
        return pltpu.make_async_copy(
            w_hbm.at[pl.ds(k * per * 2 * chans, per * 2 * chans)],
            work.at[pl.ds(slot * per * 2 * chans, per * 2 * chans)], w_sem.at[slot])

    def band_in(d):
        for which, source in enumerate((pf_hbm, pv_hbm)):
            pltpu.make_async_copy(
                source.at[top + first_mode(d), pl.ds(top, n)], band.at[which, d], band_sem.at[which]).start()

    def step1_chunk(ch):
        slot = free_slot(0, ch)

        def row(t):
            unit = ch * tl + t
            step_in(f_hbm, unit)
            buf = lax.rem(unit, 2)
            for b in range(0, nb, 2):
                pair = jnp.concatenate([inbuf[buf, b], inbuf[buf, b + 1]], axis=1)
                spec = transform(pair, fwd_h, fwd_l)
                gather[pl.ds(b, modes2, stride=nb), :] = spec[:, :chans]
                gather[pl.ds(b + 1, modes2, stride=nb), :] = spec[:, chans:]
            put_rows(slot, t)

            @pl.when((ch == 0) & (t == group - 1))
            def _():
                pl.semaphore_wait(barrier, n - 1)
                ship(0, 0, 0, group)


        loop(tl, row)
        send_peak(0, ch)

        @pl.when(ch == 0)
        def _():
            ship(0, 0, group, tl - group)
            other_tables.start()
            for which, source in enumerate((pf_hbm, pv_hbm)):
                for k in range(ml):
                    pltpu.make_async_copy(
                        source.at[first_mode(me) + n * k], pbuf.at[which, k], p_sem.at[which]).start()
            loop(n, band_in)
            for k in range(depth):
                w_in(k).start()


    loop(chunks, step1_chunk)

    unit_in(dg_hbm, 0).start()
    for which in range(2):
        pltpu.make_async_copy(band.at[which], band.at[which], band_sem.at[which]).wait()
    qs[...] = jnp.zeros_like(qs)

    def pack(z, store):
        def one(index):
            half_at, row = lax.div(index, held), lax.rem(index, held)
            p = half_at * (held - 1) + row
            degree = jnp.where(core == 0, jnp.minimum(z + p, n - 1), jnp.maximum(p - 1, 0))
            store(half_at, row, degree, (p < n - z) == (core == 0))

        loop(2 * held, one)

    def project(which, ch, target, device):
        gather[...] = jnp.zeros_like(gather)
        side = 1 if target == 3 else -1

        def place_rows(apart):
            for c in range(2):
                src = across(side * apart, c)
                gather[pl.ds(pl.multiple_of(src * tl * tile, tile), tl * tile), :] = topin[
                    ch, target, 2 * apart + c].reshape(tl * tile, chans).astype(F32)

        place_rows(0)
        if target > 2:
            place_rows(1)

            @pl.when(core == target - 3)
            def _():
                place_rows(2)

        for k in range(tile):
            xb[:, k * chans:(k + 1) * chans] = gather[pl.ds(k, lats, stride=tile), :].astype(BF16)
        out = dot(band[which, device].astype(BF16), xb[...])
        for k in range(tile):
            qs[pl.ds(k, n, stride=tile), :] = out[:, k * chans:(k + 1) * chans]

    def sum_rows(which, ch):
        pltpu.make_async_copy(peaks(), peaks(), row_recv.at[ch]).wait()
        for target, away in enumerate((-1, 1, -2, 2)):
            project(which, ch, target + 1, across(away, core))

            def keep(half_at, row, degree, ours):
                values = qs[pl.ds(pl.multiple_of(degree * tile, tile), tile), :]
                partial[half_at, target, row] = jnp.where(ours, values, jnp.zeros_like(values))

            pack(chip_at(away), keep)
        swap = to(sibling, partial.at[other_core], mid.at[ch], mid_send, mid_recv.at[ch])
        swap.start()
        if which == 1:
            pltpu.make_async_copy(sums.at[ch], sums.at[ch], sum_send.at[ch]).wait()
        swap.wait()
        sums[ch] = partial[core] + mid[ch]
        for side, away in enumerate(sides):
            to(across(away, core), sums.at[ch, 2 + side], handed.at[ch, side],
               sum_send.at[ch], hand_recv.at[ch]).start()

    def pass_sums(ch):
        pltpu.make_async_copy(handed.at[ch], handed.at[ch], hand_recv.at[ch]).wait()
        for side, away in enumerate(sides):
            sums[ch, side] += handed[ch, side]
            to(across(away, core), sums.at[ch, side], sumin.at[ch, side],
               sum_send.at[ch], sum_recv.at[ch]).start()

    def finish_peak(which, ch):
        pltpu.make_async_copy(sumin.at[ch], sumin.at[ch], sum_recv.at[ch]).wait()
        joined[ch, core] = sumin[ch, 0] + sumin[ch, 1]
        swap = to(sibling, joined.at[ch, core], joined.at[ch, core], join_send, join_recv.at[ch])
        swap.start()
        project(which, ch, 0, me)
        swap.wait()

        def one(degree):
            p = jnp.where(core == 0, degree - chip, degree + 1)
            ours = degree >= first_mode(me)
            p = jnp.maximum(p, 0)
            h = jnp.where(p > held - 1, 1, 0)
            come = joined[ch, h, p - h * (held - 1)]
            work[pl.ds(area + (top + degree) * pitch + rows - tile, tile), :] = qs[
                pl.ds(pl.multiple_of(degree * tile, tile), tile), :] + jnp.where(ours, come, jnp.zeros_like(come))

        loop(n, one)

    sum_rows(0, 0)

    def ship_rows(ch):
        ship(0, ch, 0, tl)

    loop(final, ship_rows, 1)
    for which in range(2):
        pltpu.make_async_copy(pbuf.at[which], pbuf.at[which], p_sem.at[which]).wait()
    pmat[...] = pbuf[...].astype(BF16)
    other_tables.wait()

    def load_w(k):
        w_in(k).wait()
        base = lax.rem(k, depth) * per * 2 * chans
        for j in range(per):
            for part in range(2):
                vmix[k * per + j, pl.ds(part * chans, chans)] = work[
                    pl.ds(base + j * 2 * chans + part, chans, stride=2), :].astype(BF16)

        @pl.when(k + depth < parts)
        def _():
            w_in(k + depth).start()


    loop(parts, load_w)

    span = cmat.shape[3]
    mine_t = (lax.broadcasted_iota(jnp.int32, (8, lats), 1) == me * tl + lax.broadcasted_iota(jnp.int32, (8, lats), 0))
    mine_t &= lax.broadcasted_iota(jnp.int32, (8, lats), 0) < tl
    mine_t = jnp.where(mine_t, 1.0, 0.0).astype(BF16)

    def tabulate(d):
        z, of_core = lax.div(d, 2), lax.rem(d, 2)
        row = lax.broadcasted_iota(jnp.int32, (n, span), 0)
        p = jnp.where(of_core == 0, row - z, row + 1)
        target = jnp.where(p > held - 1, p + 1, p)
        moved = jnp.where(target == lax.broadcasted_iota(jnp.int32, (n, span), 1), 1.0, 0.0).astype(BF16)
        for which in range(2):
            picked = dot(mine_t, band[which, d].astype(BF16), ((1,), (1,))).astype(BF16)
            cmat[which, z, pl.ds(pl.multiple_of(of_core * 8, 8), 8), :] = dot(picked, moved)

    loop(n, tabulate)

    def no_degree(l):
        work[pl.ds(area + l * pitch + rows - tile, tile), :] = jnp.zeros((tile, chans), F32)

    loop(top, no_degree)

    pass_sums(0)

    def sum_first(ch):
        sum_rows(0, ch)

    loop(chunks, sum_first, 1)
    ship(0, final, 0, tl)
    loop(chunks, pass_sums, 1)

    sign = jnp.where(lax.broadcasted_iota(jnp.int32, (tile, chans), 0) < nb, -1.0, 1.0).astype(F32)

    def turn(values):
        groups = values.reshape(-1, tile, chans)
        return (pltpu.roll(groups, nb, 1) * sign[None]).reshape(values.shape)

    def legendre(src, dst, which, over):
        def mode(m):
            for k in range(tile):
                xb[:, k * chans:(k + 1) * chans] = work[
                    pl.ds(src + m * tile + k, lats, stride=pitch), :].astype(BF16)
            out = dot(pmat[which, m], xb[...], ((over,), (0,)))
            for k in range(tile):
                work[pl.ds(dst + m * tile + k, degs, stride=pitch), :] = out[:, k * chans:(k + 1) * chans]

        loop(ml - 1, mode)

    def unload(stage, ch):
        def body(src):
            for t in range(tl):
                work[pl.ds((src * tl + t) * pitch, rows), :] = recv[stage % 2, ch, src, t].astype(F32)

        loop(n, body)

    def load(slot):
        def body(dev):
            for t in range(tl):
                send[slot, dev, t] = work[pl.ds(area + (dev * tl + t) * pitch, rows), :].astype(BF16)

        loop(n, body)

    def only(ours, values):
        values = values.astype(F32)
        return jnp.where(ours, values, jnp.zeros_like(values)).astype(BF16)

    def spectral(stage, ch, into, kept, mix):
        arrived(stage - 1, ch)
        unload(stage - 1, ch)
        legendre(0, area, into, 1)
        finish_peak(into, ch)

        def degree(l):
            x = work[pl.ds(area + l * pitch, rows), :].astype(BF16)
            kept[l, ch] = x
            work[pl.ds(l * pitch, rows), :] = mix(l, x)

        loop(degs, degree, unroll=8)

        def keep_top(half_at, row, degree, ours):
            own[half_at, 2, ch, row] = only(ours, work[pl.ds((top + degree) * pitch + rows - tile, tile), :])

        pack(chip, keep_top)
        if stage == 1:
            swap = to(sibling, own.at[other_core, 2, ch], other.at[2, ch], swap_send, swap_recv.at[ch])
            swap.start()
        legendre(0, area, 1 - into, 0)
        load(free_slot(stage, ch))
        if stage == 1:
            swap.wait()
            packs[core, chip, 2, ch] = (own[core, 2, ch].astype(F32) + other[2, ch].astype(F32)).astype(BF16)

            @pl.when(ch == final - 1)
            def _():
                relay_near(ch - 1)

            for away in sides:
                top_copy(0, away, ch, near_recv).start()
        else:
            @pl.when(ch == 0)
            def _():
                pass_sums(final - 1)
                sum_rows(1, final)

            @pl.when(ch == 1)
            def _():
                pass_sums(final)

        if stage == 1:
            @pl.when(ch < final)
            def _():
                ship(stage, ch, 0, tl)
        else:
            ship(stage, ch, 0, tl)

    def top_copy(source, away, ch, got):
        block = packs.at[core, chip_at(source), 2, ch]
        return to(across(away, core), block, block, top_send, got.at[ch])

    def top_blocks(count, ch):
        return packs.at[core, head(count), 2, ch]

    def relay_near(ch):
        pltpu.make_async_copy(top_blocks(2, ch), top_blocks(2, ch), near_recv.at[ch]).wait()
        for side in sides:
            top_copy(-side, side, ch, next_recv).start()

    def relay_next(ch):
        pltpu.make_async_copy(top_blocks(2, ch), top_blocks(2, ch), next_recv.at[ch]).wait()
        for side in sides:
            top_copy(-2 * side, side, ch, far_recv).start()
        top_copy(-2 * way, 2 * way, ch, far_recv).start()

    def apply_top(which, ch, z):
        for h in range(2):
            qs[pl.ds(h * held * tile, held * tile), :] = packs[h, z, 2, ch].reshape(held * tile, chans).astype(F32)
        for k in range(tile):
            xb[0:span, k * chans:(k + 1) * chans] = qs[pl.ds(k, span, stride=tile), :].astype(BF16)
        out = dot(cmat[which, z].astype(BF16), xb[0:span, :])
        for k in range(tile):
            gather[pl.ds(k, 16, stride=tile), :] = out[:, k * chans:(k + 1) * chans]
        for c in range(2):
            for t in range(tl):
                recv[1, ch, 2 * z + c, t, pl.ds(rows - tile, tile)] = gather[
                    pl.ds((8 * c + t) * tile, tile), :].astype(BF16)

    def mix_forward(l, x):
        both = dot(x, vmix[l], ((1,), (1,)))
        return both[:, :chans] + turn(both[:, chans:])

    def mix_adjoint(l, x):
        both = dot(x, jnp.concatenate([vmix[l, head(chans)], vmix[l, pl.ds(chans, chans)]], axis=1))
        return both[:, :chans] - turn(both[:, chans:])

    def step2_chunk(ch):
        spectral(1, ch, 0, coef, mix_forward)

    loop(chunks, step2_chunk)
    relay_next(final - 2)
    relay_near(final - 1)
    ship(1, final, 0, tl)

    def fetch_rows(stage, ch, t):
        for src in range(n):
            gather[pl.ds(src * rows, rows), :] = recv[stage % 2, ch, src, t].astype(F32)

    def fetch_pair(b):
        return jnp.concatenate(
            [gather[pl.ds(b, modes2, stride=nb), :], gather[pl.ds(b + 1, modes2, stride=nb), :]], axis=1).astype(BF16)

    def step3_chunk(ch):
        arrived(1, ch)

        @pl.when(ch == 0)
        def _():
            relay_near(final)
            relay_next(final - 1)

        pltpu.make_async_copy(top_blocks(3, ch), top_blocks(3, ch), far_recv.at[ch]).wait()
        swap = to(sibling, top_blocks(chips, ch), top_blocks(chips, ch), swap_send, swap_recv.at[ch])
        swap.start()

        @pl.when(ch == 1)
        def _():
            relay_next(final)

        swap.wait()

        @pl.when(ch == final)
        def _():
            all_sent = packs.at[0, head(7), 2]
            pltpu.make_async_copy(all_sent, all_sent, top_send).wait()

        def apply(z):
            apply_top(1, ch, z)

        loop(chips, apply)

        @pl.when(ch == 1)
        def _():
            sum_rows(1, 0)

        slot = free_slot(2, ch)

        def row(t):
            unit = ch * tl + t
            step_in(dg_hbm, unit)
            buf = lax.rem(unit, 2)
            fetch_rows(1, ch, t)
            for b in range(0, nb, 2):
                g = fetch_pair(b)
                hidden = dot(syn_h[...], g) + dot(syn_l[...], g)
                pair = jnp.concatenate([inbuf[buf, b], inbuf[buf, b + 1]], axis=1)
                spec = transform(pair * gelu_grad(hidden), dbl_h, dbl_l)
                gather[pl.ds(b, modes2, stride=nb), :] = spec[:, :chans]
                gather[pl.ds(b + 1, modes2, stride=nb), :] = spec[:, chans:]
            put_rows(slot, t)

        loop(tl, row)
        send_peak(2, ch)

        @pl.when(ch < final)
        def _():
            ship(2, ch, 0, tl)


    loop(chunks, step3_chunk)

    def sum_second(ch):
        pass_sums(ch - 1)
        sum_rows(1, ch)

    loop(final, sum_second, 1)
    ship(2, final, 0, tl)
    unit_in(dg_hbm, 0).start()

    def step4_chunk(ch):
        spectral(3, ch, 1, dq, mix_adjoint)

    loop(chunks, step4_chunk)

    for which, kept in enumerate((coef, dq)):
        def keep_low(half_at, row, degree, ours):
            own[half_at, which, :, row] = only(ours, kept[degree, :, head(tile)])

        pack(chip, keep_low)

    def both_parts(peer, action):
        degree = n + first_mode(peer)
        for which, kept in enumerate((coef, dq)):
            action(to(peer, kept.at[degree, :, head(tile)], second.at[which, me, :, head(tile)],
                      always_send, always_recv))

            @pl.when(first_mode(me) <= first_mode(peer))
            def _():
                more = pl.ds(tile, tile)
                action(to(peer, kept.at[degree, :, more], second.at[which, me, :, more],
                          some_send, some_recv))

    def send_second(k):
        both_parts(lax.rem(me + k, n), lambda copy: copy.start())

    loop(n, send_second, 1)
    for which, kept in enumerate((coef, dq)):
        second[which, me] = kept[n + first_mode(me), :, head(2 * tile)]

    def clear_second(src):
        @pl.when(first_mode(src) > first_mode(me))
        def _():
            for which in range(2):
                second[which, src, :, pl.ds(tile, tile)] = jnp.zeros((chunks, tile, chans), BF16)

    loop(n, clear_second)
    own_copy = to(sibling, own.at[other_core], other, own_send, own_recv)
    own_copy.start()

    def pack_block(k):
        return packs.at[core, chip_at(-way * k)]

    def pack_copy(k):
        return to(onward, pack_block(k), pack_block(k), pack_send, pack_recv.at[k])

    def share(k):
        to(sibling, pack_block(k), pack_block(k), share_send, share_recv).start()

    half = degs // n - 2
    wide = 2 * chans
    block_rows = half * wide
    piece = block_rows // pieces
    hops = (last) * pieces

    def block_at(k, direction):
        return lax.rem(chip - direction * (1 + k) + 2 * chips, chips)

    def outer(dst, row, pairs):
        real = jnp.zeros((chans, chans), F32)
        imag = jnp.zeros((chans, chans), F32)
        for y, x in pairs:
            real += dot(y, x, ((0,), (0,)))
            imag -= dot(turn(y.astype(F32)).astype(BF16), x, ((0,), (0,)))
        dst[pl.ds(row, chans, stride=2), :] = real
        dst[pl.ds(row + 1, chans, stride=2), :] = imag

    def first_degree(block, of_core):
        return 2 * n + (2 * block + of_core) * half

    def weight_grad(dst, degree):
        def one(j):
            outer(dst, j * wide, [(dq[degree + j, ch], coef[degree + j, ch]) for ch in range(chunks)])

        loop(half, one)

    def pair_copy(k):
        slot = lax.rem(k, 2)
        rows_there = pl.ds(first_degree(block_at(k, -way), core) * wide, block_rows)
        return to(sibling, wbuf.at[slot, head(block_rows)], dw_out.at[rows_there],
                  pair_send.at[slot], pair_recv.at[k])

    def weight_block(k):
        @pl.when(k >= 2)
        def _():
            pair_copy(k - 2).wait_send()
        weight_grad(wbuf.at[lax.rem(k, 2)], first_degree(block_at(k, -way), other_core))
        pair_copy(k).start()
        block = block_at(k, way)
        weight_grad(work.at[pl.ds(block * block_rows, block_rows)], first_degree(block, core))

    loop(chips, weight_block)
    pair_copy(chips - 2).wait_send()
    pair_copy(last).wait_send()
    own_copy.wait()
    packs[core, chip] = (own[core].astype(F32) + other[...].astype(F32)).astype(BF16)

    def low_degree(l):
        def one(z):
            for c in range(2):
                p = l - z if c == 0 else l + 1
                ours = p >= 0 if c == 0 else p >= n - z
                p = jnp.maximum(p, 0)
                h = jnp.where(p > held - 1, 1, 0)
                for which in range(2):
                    lowx[which, 2 * z + c] = only(ours, packs[h, z, which, :, p - h * (held - 1)])

        loop(chips, one)
        outer(wbuf.at[0], 0, [(lowx[1].reshape(-1, chans), lowx[0].reshape(-1, chans))])
        dw_out[pl.ds(l * wide, wide)] = wbuf[0, head(wide)]

    def final_rows(unit):
        ch, t = unit_of(unit)

        step_in(dg_hbm, unit)
        buf = lax.rem(unit, 2)

        fetch_rows(3, ch, t)
        for b in range(0, nb, 2):
            g = fetch_pair(b)
            change = dot(adj_h[...], g) + dot(adj_l[...], g)
            df_out[ch * nb + b, t] = inbuf[buf, b] + change[:, :chans]
            df_out[ch * nb + b + 1, t] = inbuf[buf, b + 1] + change[:, chans:]

    def place(i, of_core):
        block = block_at(lax.div(i, pieces), way)
        start = lax.rem(i, pieces) * piece
        return pl.ds(block * block_rows + start, piece), pl.ds(first_degree(block, of_core) * wide + start, piece)

    def rs_copy(i):
        here, there = place(i, core)
        return to(onward, work.at[here], dw_out.at[there], rs_send, rs_recv.at[i])

    def add_pair(i):
        here, passed = place(i, other_core)

        @pl.when(lax.rem(i, pieces) == 0)
        def _():
            pair_copy(lax.div(i, pieces)).wait_recv()

        work[here] += dw_out[passed]

    def rs_step(i):
        add_pair(i)

        @pl.when(i >= pieces)
        def _():
            rs_copy(i - pieces).wait_recv()
            here, there = place(i, core)
            work[here] += dw_out[there]

        rs_copy(i).start()

        @pl.when(lax.rem(i, pieces) == 0)
        def _():
            k = lax.div(i, pieces)

            @pl.when(k > 0)
            def _():
                pack_copy(k - 1).wait_recv()

            pack_copy(k).start()
            share(k)


    loop(hops, rs_step)
    pack_copy(chips - 2).wait_recv()
    share(last)

    def own_sum(s):
        i = hops + s
        add_pair(i)
        rs_copy(i - pieces).wait_recv()
        here, there = place(i, core)
        dw_out[there] += work[here]
        ag_copy(i, s).start()

    def second_spot(k):
        return pl.ds((n + first_mode(2 * block_at(k, way) + core)) * wide, wide)

    def second_copy(k, got):
        spot = dw_out.at[second_spot(k)]
        return to(onward, spot, spot, ag_send, ag_recv.at[hops + got])

    def second_publish(k):
        spot = dw_out.at[second_spot(k)]
        to(sibling, spot, spot, pub_send, pub_recv).start()

    def ag_copy(i, got):
        _, there = place(i, core)
        return to(onward, dw_out.at[there], dw_out.at[there], ag_send, ag_recv.at[got])

    def publish(i):
        _, there = place(i, core)
        to(sibling, dw_out.at[there], dw_out.at[there], pub_send, pub_recv).start()

    firsts = second.at[:, head(n - 1), :, head(tile)]
    pltpu.make_async_copy(firsts, firsts, always_recv).wait()

    comes, goes = first_mode(me), n - 1 - first_mode(me)

    def wait_some(count, sem):
        for k in range(1, n):
            @pl.when(count == k)
            def _():
                part = second.at[:, head(k), :, pl.ds(tile, tile)]
                pltpu.make_async_copy(part, part, sem).wait()

    wait_some(comes, some_recv)
    outer(wbuf.at[0], 0, [(second[1].reshape(-1, chans), second[0].reshape(-1, chans))])
    dw_out[second_spot(last)] = wbuf[0, head(wide)]
    loop(pieces, own_sum)
    second_copy(last, 0).start()

    pl.semaphore_signal(free_sem, inc=1, device_id={axis: sibling}, device_id_type=pl.DeviceIdType.MESH)
    pl.semaphore_wait(free_sem, 1)

    def own_piece(s):
        publish(hops + s)

    loop(pieces, own_piece)
    second_publish(last)
    gathered = packs.at[other_core]
    pltpu.make_async_copy(gathered, gathered, share_recv).wait()

    def task(i):
        @pl.when(i < chips)
        def _():
            for ch in range(chunks):
                @pl.when(i == 0)
                def _():
                    arrived(3, ch)
                apply_top(0, ch, i)

        @pl.when((i >= chips) & (i < chips + units))
        def _():
            final_rows(i - chips)

        @pl.when(i < n)
        def _():
            low_degree(i)

    share_of = -(-(chips + units) // hops)

    def ag_step(i):
        ag_copy(i, i).wait_recv()

        @pl.when(i + pieces < hops)
        def _():
            ag_copy(i, i + pieces).start()

        publish(i)

        @pl.when(lax.rem(i, pieces) == pieces - 1)
        def _():
            k = lax.div(i, pieces)
            second_copy(k, k).wait_recv()

            @pl.when(k < chips - 2)
            def _():
                second_copy(k, k + 1).start()

            second_publish(k)

        for j in range(share_of):
            task(i * share_of + j)

    loop(hops, ag_step)

    wait_sent(2 * chunks + final, 2)
    for ch in range(chunks):
        wait_sent(3 * chunks + ch, 3)
    for ch in range(chunks):
        pltpu.make_async_copy(sums.at[ch], sums.at[ch], sum_send.at[ch]).wait()
    sent = work.at[head((last) * block_rows)]
    pltpu.make_async_copy(sent, sent, rs_send).wait()
    sent = dw_out.at[head((last) * (block_rows + wide))]
    pltpu.make_async_copy(sent, sent, ag_send).wait()
    pltpu.make_async_copy(firsts, firsts, always_send).wait()

    wait_some(goes, some_send)
    sent = packs.at[0, head(last)]
    pltpu.make_async_copy(sent, sent, pack_send).wait()
    pltpu.make_async_copy(packs.at[0], packs.at[0], share_send).wait()
    shared = dw_out.at[head(chips * (block_rows + wide))]
    pltpu.make_async_copy(shared, shared, pub_send).wait()
    pltpu.make_async_copy(shared, shared, pub_recv).wait()


def put_kernel(df_ref, dw_ref, df_hbm, dw_hbm, sems):
    copies = []
    for source, target, parts in ((df_ref, df_hbm, 6), (dw_ref, dw_hbm, 12)):
        size = source.shape[0] // parts
        for k in range(parts):
            part = pl.ds(k * size, size)
            copies.append(pltpu.make_async_copy(source.at[part], target.at[part], sems.at[len(copies)]))
    for copy in copies:
        copy.start()
    for copy in copies:
        copy.wait()


def solution(mesh):
    n = mesh.shape['lat']
    field_spec = P('member', None, 'lat')

    def local_step(field_loc, grad_loc, p_fwd, p_inv, w_mix):
        batch, chans, tl, lons = field_loc.shape
        degs, lats = p_fwd.shape[1:]
        ml = p_fwd.shape[0] // n
        nb = 4
        chunks = batch // nb
        rows = ml * 2 * nb
        pitch = rows + 1
        half = degs // n - 2
        pieces = 2 if half * 2 * chans % 32 == 0 else 1
        hops = (n // 2 - 1) * pieces
        per = 4
        area = max(2 * lats * pitch, n // 2 * half * 2 * chans)
        depth = min(degs // per, area // (per * 2 * chans))
        held = n // 2 + 1
        packed = (3, chunks, held, 2 * nb, chans)
        tables = fourier_tables(n, ml, lons)
        anywhere = pl.BlockSpec(memory_space=pl.ANY)
        vmem = pl.BlockSpec(memory_space=pltpu.VMEM)
        grad_field, grad_w = pl.pallas_call(
            functools.partial(layer_kernel, 'lat', n, nb, pieces, per, depth),
            name='layer',
            out_shape=(
                pltpu.VMEM((batch, tl, lons, chans), F32),
                pltpu.VMEM((degs * 2 * chans, chans), F32),
            ),
            in_specs=[anywhere] * 6,
            out_specs=(vmem, vmem),
            scratch_shapes=[
                pltpu.VMEM((2, chunks, n, tl, rows, chans), BF16),
                pltpu.VMEM((chunks + 1, n, tl, rows, chans), BF16),
                pltpu.VMEM((area, chans), F32),
                pltpu.VMEM((lats, 2 * nb * chans), BF16),
                pltpu.VMEM((degs, chunks, rows, chans), BF16),
                pltpu.VMEM((degs, chunks, rows, chans), BF16),
                pltpu.VMEM((degs, 2 * chans, chans), BF16),
                pltpu.VMEM((2, max(per, half) * 2 * chans, chans), F32),
                pltpu.VMEM((2, nb, lons, chans), F32),
                pltpu.VMEM((n * rows, chans), F32),
                pltpu.VMEM((2, ml, degs, lats), F32),
                pltpu.VMEM((2, ml, degs, lats), BF16),
                pltpu.VMEM((2, n, n, lats), F32),
                pltpu.VMEM((2, n // 2, 16, 32), F32),
                pltpu.VMEM((32 * 2 * nb, chans), F32),
                pltpu.VMEM((2,) + packed, BF16),
                pltpu.VMEM(packed, BF16),
                pltpu.VMEM((2, n // 2) + packed, BF16),
                pltpu.VMEM((2, n, chunks, 2 * nb, chans), BF16),
                pltpu.VMEM(tables.shape, BF16),
                pltpu.VMEM((chunks, 5, 6, tl, 2 * nb, chans), BF16),
                pltpu.VMEM((2, 4, held, 2 * nb, chans), F32),
                pltpu.VMEM((chunks, 4, held, 2 * nb, chans), F32),
                pltpu.VMEM((chunks, 4, held, 2 * nb, chans), F32),
                pltpu.VMEM((chunks, 2, held, 2 * nb, chans), F32),
                pltpu.VMEM((chunks, 2, held, 2 * nb, chans), F32),
                pltpu.VMEM((chunks, 2, held, 2 * nb, chans), F32),
                pltpu.VMEM((2, n, chunks, 4 * nb, chans), BF16),
                pltpu.SemaphoreType.DMA((chunks + 1,)),
                pltpu.SemaphoreType.DMA((4 * chunks,)),
                pltpu.SemaphoreType.DMA((2,)),
                pltpu.SemaphoreType.DMA((depth,)),
                pltpu.SemaphoreType.DMA((2,)),
                pltpu.SemaphoreType.DMA((2,)),
                pltpu.SemaphoreType.DMA((2,)),
                pltpu.SemaphoreType.DMA((n // 2,)),
                pltpu.SemaphoreType.DMA,
                pltpu.SemaphoreType.DMA((hops,)),
                pltpu.SemaphoreType.DMA,
                pltpu.SemaphoreType.DMA((hops + n // 2 - 1,)),
                pltpu.SemaphoreType.REGULAR,
                pltpu.SemaphoreType.DMA,
                pltpu.SemaphoreType.DMA,
                pltpu.SemaphoreType.DMA,
                pltpu.SemaphoreType.DMA,
                pltpu.SemaphoreType.DMA,
                pltpu.SemaphoreType.DMA((n // 2 - 1,)),
                pltpu.SemaphoreType.DMA,
                pltpu.SemaphoreType.DMA,
                pltpu.SemaphoreType.DMA((2,)),
                pltpu.SemaphoreType.DMA,
                pltpu.SemaphoreType.DMA((chunks,)),
                pltpu.SemaphoreType.DMA((chunks,)),
                pltpu.SemaphoreType.DMA((chunks,)),
                pltpu.SemaphoreType.DMA,
                pltpu.SemaphoreType.DMA((chunks,)),
                pltpu.SemaphoreType.DMA((chunks,)),
                pltpu.SemaphoreType.DMA((chunks,)),
                pltpu.SemaphoreType.DMA,
                pltpu.SemaphoreType.DMA((chunks,)),
                pltpu.SemaphoreType.DMA((chunks,)),
                pltpu.SemaphoreType.DMA((chunks,)),
                pltpu.SemaphoreType.DMA,
                pltpu.SemaphoreType.DMA((chunks,)),
                pltpu.SemaphoreType.DMA,
                pltpu.SemaphoreType.DMA,
                pltpu.SemaphoreType.DMA,
                pltpu.SemaphoreType.DMA,
                pltpu.SemaphoreType.DMA((chunks,)),
            ],
            compiler_params=pltpu.CompilerParams(
                collective_id=0, has_side_effects=True, vmem_limit_bytes=43 << 20),
        )(
            field_loc.transpose(0, 2, 3, 1), grad_loc.transpose(0, 2, 3, 1),
            w_mix.transpose(0, 1, 3, 2).reshape(degs * 2 * chans, chans),
            p_fwd, p_inv, tables)
        grad_field, grad_w = pl.pallas_call(
            put_kernel,
            name='put',
            out_shape=(
                jax.ShapeDtypeStruct(grad_field.shape, F32),
                jax.ShapeDtypeStruct(grad_w.shape, F32),
            ),
            in_specs=[vmem] * 2,
            out_specs=(anywhere, anywhere),
            scratch_shapes=[pltpu.SemaphoreType.DMA((18,))],
            compiler_params=pltpu.CompilerParams(vmem_limit_bytes=1 << 20),
        )(grad_field, grad_w)
        return grad_field.transpose(0, 3, 1, 2), grad_w.reshape(degs, chans, 2, chans).transpose(0, 1, 3, 2)

    return jax.shard_map(
        local_step, mesh=mesh, in_specs=(field_spec, field_spec, P(), P(), P()),
        out_specs=(field_spec, P('member')), check_vma=False)
```

```python
import functools
import math

import jax
import jax.numpy as jnp
import numpy as np
from jax import lax
from jax.experimental import pallas as pl
from jax.experimental.pallas import tpu as pltpu
from jax.sharding import PartitionSpec as P

F32 = jnp.float32
BF16 = jnp.bfloat16


def split_const(matrix):
    head = matrix.astype(BF16)
    tail = (matrix - head.astype(np.float64)).astype(BF16)
    return [head, tail]


def fourier_tables(n, ml, lons):
    modes = n * ml
    device = np.arange(n)
    first = np.where(device % 2 == 0, device // 2, n - 1 - device // 2)
    order = (first[:, None] + n * np.arange(ml)[None, :]).reshape(-1)
    angle = math.tau * (np.outer(order, np.arange(lons)) % lons) / lons
    forward = np.stack([np.cos(angle), -np.sin(angle)], axis=1).reshape(2 * modes, lons) / math.sqrt(lons)
    gains = np.repeat(2.0 - (order == 0), 2)[:, None]
    doubled = forward * gains
    tables = split_const(forward) + split_const(doubled) + split_const(doubled.T) + split_const(forward.T)
    return jnp.stack([jnp.asarray(t) for t in tables])


def gelu_grad(values):
    cumulative = 0.5 * (1.0 + lax.erf(values * math.sqrt(0.5)))
    density = jnp.exp(-0.5 * values * values) / math.sqrt(math.tau)
    return cumulative + values * density


def loop(stop, step, start=0, **options):
    def one(i, carry):
        step(i)
        return carry

    lax.fori_loop(start, stop, one, 0, **options)


def head(size):
    return pl.ds(0, size)


def dot(a, b, dims=((1,), (0,))):
    return lax.dot_general(a, b, (dims, ((), ())), preferred_element_type=F32)


def layer_kernel(
    axis, n, nb, pieces, per, depth,
    f_hbm, dg_hbm, w_hbm, pf_hbm, pv_hbm, tab_hbm,
    df_out, dw_out,
    recv, send, work, xb, coef, dq, vmix, wbuf, inbuf, gather, pbuf, pmat, band, cmat, qs, own, other, packs, lowx, tab,
    topin, partial, mid, sums, sumin, joined, handed, second,
    send_sem, recv_sem, in_sem, w_sem, p_sem, band_sem, pair_send, pair_recv, rs_send, rs_recv, ag_send, ag_recv,
    free_sem, pub_send, pub_recv, own_send, own_recv, pack_send, pack_recv, share_send, share_recv,
    tab_sem, top_send, near_recv, far_recv, next_recv, swap_send, swap_recv,
    row_send, row_recv, mid_send, mid_recv, sum_send, sum_recv, join_send, join_recv,
    always_send, always_recv, some_send, some_recv, hand_recv,
):
    me = lax.axis_index(axis)
    batch, tl, lons, chans = f_hbm.shape
    ml, degs, lats = pmat.shape[1:]
    chunks = batch // nb
    tile = 2 * nb
    rows = ml * tile
    pitch = rows + 1
    modes2 = 2 * n * ml
    units = chunks * tl
    final = chunks - 1
    slots = chunks + 1
    fwd_h, fwd_l, dbl_h, dbl_l, syn_h, syn_l, adj_h, adj_l = (tab.at[k] for k in range(8))
    area = lats * pitch
    top = n * (ml - 1)
    held = n // 2 + 1
    chip, core = lax.div(me, 2), lax.rem(me, 2)
    other_core = 1 - core
    chips = n // 2
    last = chips - 1
    way = 1 - 2 * core
    sides = (-1, 1)
    sibling = me + way

    def chip_at(away):
        return lax.rem(chip + away + chips, chips)

    def across(away, its_core):
        return 2 * chip_at(away) + its_core

    onward = across(way, core)

    def around(k):
        far = chips // 2 - lax.div(k + 1, 2)
        return jnp.where(lax.rem(k, 2) == 0, far, -far)

    def first_mode(device):
        z = lax.div(device, 2)
        return jnp.where(lax.rem(device, 2) == 0, z, n - 1 - z)

    def to(device, src, dst, sent, got):
        return pltpu.make_async_remote_copy(
            src_ref=src, dst_ref=dst, send_sem=sent, recv_sem=got,
            device_id={axis: device}, device_id_type=pl.DeviceIdType.MESH)

    def unit_of(unit):
        return lax.div(unit, tl), lax.rem(unit, tl)

    def unit_in(src, unit):
        ch, t = unit_of(unit)
        slot = lax.rem(unit, 2)
        return pltpu.make_async_copy(src.at[pl.ds(ch * nb, nb), t], inbuf.at[slot], in_sem.at[slot])

    def step_in(src, unit):
        @pl.when(unit + 1 < units)
        def _():
            unit_in(src, unit + 1).start()
        unit_in(src, unit).wait()

    body, peak = head(rows - tile), pl.ds(rows - tile, tile)

    def ship(stage, ch, t0, nt):
        index = stage * chunks + ch
        slot = lax.rem(index, slots)
        part = pl.ds(t0, nt)

        def one(k):
            away = around(k)
            for its_core in (core, other_core):
                peer = across(away, its_core)
                to(peer, send.at[slot, peer, part, body], recv.at[stage % 2, ch, me, part, body],
                   send_sem.at[slot], recv_sem.at[index]).start()

        loop(last, one)
        to(sibling, send.at[slot, sibling, part, body], recv.at[stage % 2, ch, me, part, body],
           send_sem.at[slot], recv_sem.at[index]).start()
        recv[stage % 2, ch, me, part, body] = send[slot, me, part, body]

    def arrived(stage, ch):
        others = recv.at[stage % 2, ch, head(n - 1), :, body]
        pltpu.make_async_copy(others, others, recv_sem.at[stage * chunks + ch]).wait()

    def peaks():
        return send.at[0, head(n - 5), :, peak]

    def wait_sent(index, stage):
        slot = lax.rem(index, slots)
        others = send.at[slot, head(n - 1), :, body]
        pltpu.make_async_copy(others, others, send_sem.at[slot]).wait()
        if stage % 2 == 0:
            ch = index - stage * chunks
            pltpu.make_async_copy(peaks(), peaks(), row_send.at[ch]).wait()

    def send_peak(stage, ch):
        slot = lax.rem(stage * chunks + ch, slots)
        far = chips // 2
        for same in (True, False):
            its_core = core if same else other_core
            for away in range(1 - far, far + 1):
                near = max(-2, min(2, away))
                hop, target, apart = away - near, (0, 2, 4, 3, 1)[near], abs(away - near)
                if away == far:
                    hop = jnp.where(its_core == 0, 2 - far, far - 2)
                    target = jnp.where(its_core == 0, 3, 4)
                source = send.at[slot, across(away, its_core), :, peak]
                place = topin.at[ch, target, 2 * apart + core]
                if same and not apart:
                    place[...] = source[...]
                else:
                    to(across(hop, its_core), source, place,
                       row_send.at[ch], row_recv.at[ch]).start()

    def free_slot(stage, ch):
        index = stage * chunks + ch
        if stage >= 1:
            @pl.when(ch >= 1)
            def _():
                wait_sent(index - slots, stage - 1)
        if stage >= 2:
            @pl.when(ch == 0)
            def _():
                wait_sent(index - slots, stage - 2)
        return lax.rem(index, slots)

    def put_rows(slot, t):
        send[slot, :, t] = gather[...].reshape(n, rows, chans).astype(BF16)

    def transform(values, head, tail):
        high = values.astype(BF16)
        low = (values - high.astype(F32)).astype(BF16)
        return dot(head[...], high) + (dot(tail[...], high) + dot(head[...], low))

    unit_in(f_hbm, 0).start()
    first_tables = pltpu.make_async_copy(tab_hbm.at[head(2)], tab.at[head(2)], tab_sem.at[0])
    other_tables = pltpu.make_async_copy(tab_hbm.at[pl.ds(2, 6)], tab.at[pl.ds(2, 6)], tab_sem.at[1])
    first_tables.start()
    barrier = pltpu.get_barrier_semaphore()

    def announce(k):
        pl.semaphore_signal(barrier, inc=1, device_id={axis: lax.rem(me + k, n)}, device_id_type=pl.DeviceIdType.MESH)

    loop(n, announce, 1)

    first_tables.wait()

    group = 1

    parts = degs // per

    def w_in(k):
        slot = lax.rem(k, depth)
        return pltpu.make_async_copy(
            w_hbm.at[pl.ds(k * per * 2 * chans, per * 2 * chans)],
            work.at[pl.ds(slot * per * 2 * chans, per * 2 * chans)], w_sem.at[slot])

    def band_in(d):
        for which, source in enumerate((pf_hbm, pv_hbm)):
            pltpu.make_async_copy(
                source.at[top + first_mode(d), pl.ds(top, n)], band.at[which, d], band_sem.at[which]).start()

    def step1_chunk(ch):
        slot = free_slot(0, ch)

        def row(t):
            unit = ch * tl + t
            step_in(f_hbm, unit)
            buf = lax.rem(unit, 2)
            for b in range(0, nb, 2):
                pair = jnp.concatenate([inbuf[buf, b], inbuf[buf, b + 1]], axis=1)
                spec = transform(pair, fwd_h, fwd_l)
                gather[pl.ds(b, modes2, stride=nb), :] = spec[:, :chans]
                gather[pl.ds(b + 1, modes2, stride=nb), :] = spec[:, chans:]
            put_rows(slot, t)

            @pl.when((ch == 0) & (t == group - 1))
            def _():
                pl.semaphore_wait(barrier, n - 1)
                ship(0, 0, 0, group)


        loop(tl, row)
        send_peak(0, ch)

        @pl.when(ch == 0)
        def _():
            ship(0, 0, group, tl - group)
            other_tables.start()
            for which, source in enumerate((pf_hbm, pv_hbm)):
                for k in range(ml):
                    pltpu.make_async_copy(
                        source.at[first_mode(me) + n * k], pbuf.at[which, k], p_sem.at[which]).start()
            loop(n, band_in)
            for k in range(depth):
                w_in(k).start()


    loop(chunks, step1_chunk)

    unit_in(dg_hbm, 0).start()
    for which in range(2):
        pltpu.make_async_copy(band.at[which], band.at[which], band_sem.at[which]).wait()
    qs[...] = jnp.zeros_like(qs)

    def pack(z, store):
        def one(index):
            half_at, row = lax.div(index, held), lax.rem(index, held)
            p = half_at * (held - 1) + row
            degree = jnp.where(core == 0, jnp.minimum(z + p, n - 1), jnp.maximum(p - 1, 0))
            store(half_at, row, degree, (p < n - z) == (core == 0))

        loop(2 * held, one)

    def project(which, ch, target, device):
        gather[...] = jnp.zeros_like(gather)
        side = 1 if target == 3 else -1

        def place_rows(apart):
            for c in range(2):
                src = across(side * apart, c)
                gather[pl.ds(pl.multiple_of(src * tl * tile, tile), tl * tile), :] = topin[
                    ch, target, 2 * apart + c].reshape(tl * tile, chans).astype(F32)

        place_rows(0)
        if target > 2:
            place_rows(1)

            @pl.when(core == target - 3)
            def _():
                place_rows(2)

        for k in range(tile):
            xb[:, k * chans:(k + 1) * chans] = gather[pl.ds(k, lats, stride=tile), :].astype(BF16)
        out = dot(band[which, device].astype(BF16), xb[...])
        for k in range(tile):
            qs[pl.ds(k, n, stride=tile), :] = out[:, k * chans:(k + 1) * chans]

    def sum_rows(which, ch):
        pltpu.make_async_copy(peaks(), peaks(), row_recv.at[ch]).wait()
        for target, away in enumerate((-1, 1, -2, 2)):
            project(which, ch, target + 1, across(away, core))

            def keep(half_at, row, degree, ours):
                values = qs[pl.ds(pl.multiple_of(degree * tile, tile), tile), :]
                partial[half_at, target, row] = jnp.where(ours, values, jnp.zeros_like(values))

            pack(chip_at(away), keep)
        swap = to(sibling, partial.at[other_core], mid.at[ch], mid_send, mid_recv.at[ch])
        swap.start()
        if which == 1:
            pltpu.make_async_copy(sums.at[ch], sums.at[ch], sum_send.at[ch]).wait()
        swap.wait()
        sums[ch] = partial[core] + mid[ch]
        for side, away in enumerate(sides):
            to(across(away, core), sums.at[ch, 2 + side], handed.at[ch, side],
               sum_send.at[ch], hand_recv.at[ch]).start()

    def pass_sums(ch):
        pltpu.make_async_copy(handed.at[ch], handed.at[ch], hand_recv.at[ch]).wait()
        for side, away in enumerate(sides):
            sums[ch, side] += handed[ch, side]
            to(across(away, core), sums.at[ch, side], sumin.at[ch, side],
               sum_send.at[ch], sum_recv.at[ch]).start()

    def finish_peak(which, ch):
        pltpu.make_async_copy(sumin.at[ch], sumin.at[ch], sum_recv.at[ch]).wait()
        joined[ch, core] = sumin[ch, 0] + sumin[ch, 1]
        swap = to(sibling, joined.at[ch, core], joined.at[ch, core], join_send, join_recv.at[ch])
        swap.start()
        project(which, ch, 0, me)
        swap.wait()

        def one(degree):
            p = jnp.where(core == 0, degree - chip, degree + 1)
            ours = degree >= first_mode(me)
            p = jnp.maximum(p, 0)
            h = jnp.where(p > held - 1, 1, 0)
            come = joined[ch, h, p - h * (held - 1)]
            work[pl.ds(area + (top + degree) * pitch + rows - tile, tile), :] = qs[
                pl.ds(pl.multiple_of(degree * tile, tile), tile), :] + jnp.where(ours, come, jnp.zeros_like(come))

        loop(n, one)

    sum_rows(0, 0)

    def ship_rows(ch):
        ship(0, ch, 0, tl)

    loop(final, ship_rows, 1)
    for which in range(2):
        pltpu.make_async_copy(pbuf.at[which], pbuf.at[which], p_sem.at[which]).wait()
    pmat[...] = pbuf[...].astype(BF16)
    other_tables.wait()

    def load_w(k):
        w_in(k).wait()
        base = lax.rem(k, depth) * per * 2 * chans
        for j in range(per):
            for part in range(2):
                vmix[k * per + j, pl.ds(part * chans, chans)] = work[
                    pl.ds(base + j * 2 * chans + part, chans, stride=2), :].astype(BF16)

        @pl.when(k + depth < parts)
        def _():
            w_in(k + depth).start()


    loop(parts, load_w)

    span = cmat.shape[3]
    mine_t = (lax.broadcasted_iota(jnp.int32, (8, lats), 1) == me * tl + lax.broadcasted_iota(jnp.int32, (8, lats), 0))
    mine_t &= lax.broadcasted_iota(jnp.int32, (8, lats), 0) < tl
    mine_t = jnp.where(mine_t, 1.0, 0.0).astype(BF16)

    def tabulate(d):
        z, of_core = lax.div(d, 2), lax.rem(d, 2)
        row = lax.broadcasted_iota(jnp.int32, (n, span), 0)
        p = jnp.where(of_core == 0, row - z, row + 1)
        target = jnp.where(p > held - 1, p + 1, p)
        moved = jnp.where(target == lax.broadcasted_iota(jnp.int32, (n, span), 1), 1.0, 0.0).astype(BF16)
        for which in range(2):
            picked = dot(mine_t, band[which, d].astype(BF16), ((1,), (1,))).astype(BF16)
            cmat[which, z, pl.ds(pl.multiple_of(of_core * 8, 8), 8), :] = dot(picked, moved)

    loop(n, tabulate)

    def no_degree(l):
        work[pl.ds(area + l * pitch + rows - tile, tile), :] = jnp.zeros((tile, chans), F32)

    loop(top, no_degree)

    pass_sums(0)

    def sum_first(ch):
        sum_rows(0, ch)

    loop(chunks, sum_first, 1)
    ship(0, final, 0, tl)
    loop(chunks, pass_sums, 1)

    sign = jnp.where(lax.broadcasted_iota(jnp.int32, (tile, chans), 0) < nb, -1.0, 1.0).astype(F32)

    def turn(values):
        groups = values.reshape(-1, tile, chans)
        return (pltpu.roll(groups, nb, 1) * sign[None]).reshape(values.shape)

    def legendre(src, dst, which, over):
        def mode(m):
            for k in range(tile):
                xb[:, k * chans:(k + 1) * chans] = work[
                    pl.ds(src + m * tile + k, lats, stride=pitch), :].astype(BF16)
            out = dot(pmat[which, m], xb[...], ((over,), (0,)))
            for k in range(tile):
                work[pl.ds(dst + m * tile + k, degs, stride=pitch), :] = out[:, k * chans:(k + 1) * chans]

        loop(ml - 1, mode)

    def unload(stage, ch):
        def body(src):
            for t in range(tl):
                work[pl.ds((src * tl + t) * pitch, rows), :] = recv[stage % 2, ch, src, t].astype(F32)

        loop(n, body)

    def load(slot):
        def body(dev):
            for t in range(tl):
                send[slot, dev, t] = work[pl.ds(area + (dev * tl + t) * pitch, rows), :].astype(BF16)

        loop(n, body)

    def only(ours, values):
        values = values.astype(F32)
        return jnp.where(ours, values, jnp.zeros_like(values)).astype(BF16)

    def spectral(stage, ch, into, kept, mix):
        arrived(stage - 1, ch)
        unload(stage - 1, ch)
        legendre(0, area, into, 1)
        finish_peak(into, ch)

        def degree(l):
            x = work[pl.ds(area + l * pitch, rows), :].astype(BF16)
            kept[l, ch] = x
            work[pl.ds(l * pitch, rows), :] = mix(l, x)

        loop(degs, degree, unroll=8)

        def keep_top(half_at, row, degree, ours):
            own[half_at, 2, ch, row] = only(ours, work[pl.ds((top + degree) * pitch + rows - tile, tile), :])

        pack(chip, keep_top)
        if stage == 1:
            swap = to(sibling, own.at[other_core, 2, ch], other.at[2, ch], swap_send, swap_recv.at[ch])
            swap.start()
        legendre(0, area, 1 - into, 0)
        load(free_slot(stage, ch))
        if stage == 1:
            swap.wait()
            packs[core, chip, 2, ch] = (own[core, 2, ch].astype(F32) + other[2, ch].astype(F32)).astype(BF16)

            @pl.when(ch == final - 1)
            def _():
                relay_near(ch - 1)

            for away in sides:
                top_copy(0, away, ch, near_recv).start()
        else:
            @pl.when(ch == 0)
            def _():
                pass_sums(final - 1)
                sum_rows(1, final)

            @pl.when(ch == 1)
            def _():
                pass_sums(final)

        if stage == 1:
            @pl.when(ch < final)
            def _():
                ship(stage, ch, 0, tl)
        else:
            ship(stage, ch, 0, tl)

    def top_copy(source, away, ch, got):
        block = packs.at[core, chip_at(source), 2, ch]
        return to(across(away, core), block, block, top_send, got.at[ch])

    def top_blocks(count, ch):
        return packs.at[core, head(count), 2, ch]

    def relay_near(ch):
        pltpu.make_async_copy(top_blocks(2, ch), top_blocks(2, ch), near_recv.at[ch]).wait()
        for side in sides:
            top_copy(-side, side, ch, next_recv).start()

    def relay_next(ch):
        pltpu.make_async_copy(top_blocks(2, ch), top_blocks(2, ch), next_recv.at[ch]).wait()
        for side in sides:
            top_copy(-2 * side, side, ch, far_recv).start()
        top_copy(-2 * way, 2 * way, ch, far_recv).start()

    def apply_top(which, ch, z):
        for h in range(2):
            qs[pl.ds(h * held * tile, held * tile), :] = packs[h, z, 2, ch].reshape(held * tile, chans).astype(F32)
        for k in range(tile):
            xb[0:span, k * chans:(k + 1) * chans] = qs[pl.ds(k, span, stride=tile), :].astype(BF16)
        out = dot(cmat[which, z].astype(BF16), xb[0:span, :])
        for k in range(tile):
            gather[pl.ds(k, 16, stride=tile), :] = out[:, k * chans:(k + 1) * chans]
        for c in range(2):
            for t in range(tl):
                recv[1, ch, 2 * z + c, t, pl.ds(rows - tile, tile)] = gather[
                    pl.ds((8 * c + t) * tile, tile), :].astype(BF16)

    def mix_forward(l, x):
        both = dot(x, vmix[l], ((1,), (1,)))
        return both[:, :chans] + turn(both[:, chans:])

    def mix_adjoint(l, x):
        both = dot(x, jnp.concatenate([vmix[l, head(chans)], vmix[l, pl.ds(chans, chans)]], axis=1))
        return both[:, :chans] - turn(both[:, chans:])

    def step2_chunk(ch):
        spectral(1, ch, 0, coef, mix_forward)

    loop(chunks, step2_chunk)
    relay_next(final - 2)
    relay_near(final - 1)
    ship(1, final, 0, tl)

    def fetch_rows(stage, ch, t):
        for src in range(n):
            gather[pl.ds(src * rows, rows), :] = recv[stage % 2, ch, src, t].astype(F32)

    def fetch_pair(b):
        return jnp.concatenate(
            [gather[pl.ds(b, modes2, stride=nb), :], gather[pl.ds(b + 1, modes2, stride=nb), :]], axis=1).astype(BF16)

    def step3_chunk(ch):
        arrived(1, ch)

        @pl.when(ch == 0)
        def _():
            relay_near(final)
            relay_next(final - 1)

        pltpu.make_async_copy(top_blocks(3, ch), top_blocks(3, ch), far_recv.at[ch]).wait()
        swap = to(sibling, top_blocks(chips, ch), top_blocks(chips, ch), swap_send, swap_recv.at[ch])
        swap.start()

        @pl.when(ch == 1)
        def _():
            relay_next(final)

        swap.wait()

        @pl.when(ch == final)
        def _():
            all_sent = packs.at[0, head(7), 2]
            pltpu.make_async_copy(all_sent, all_sent, top_send).wait()

        def apply(z):
            apply_top(1, ch, z)

        loop(chips, apply)

        @pl.when(ch == 1)
        def _():
            sum_rows(1, 0)

        slot = free_slot(2, ch)

        def row(t):
            unit = ch * tl + t
            step_in(dg_hbm, unit)
            buf = lax.rem(unit, 2)
            fetch_rows(1, ch, t)
            for b in range(0, nb, 2):
                g = fetch_pair(b)
                hidden = dot(syn_h[...], g) + dot(syn_l[...], g)
                pair = jnp.concatenate([inbuf[buf, b], inbuf[buf, b + 1]], axis=1)
                spec = transform(pair * gelu_grad(hidden), dbl_h, dbl_l)
                gather[pl.ds(b, modes2, stride=nb), :] = spec[:, :chans]
                gather[pl.ds(b + 1, modes2, stride=nb), :] = spec[:, chans:]
            put_rows(slot, t)

        loop(tl, row)
        send_peak(2, ch)

        @pl.when(ch < final)
        def _():
            ship(2, ch, 0, tl)


    loop(chunks, step3_chunk)

    def sum_second(ch):
        pass_sums(ch - 1)
        sum_rows(1, ch)

    loop(final, sum_second, 1)
    ship(2, final, 0, tl)
    unit_in(dg_hbm, 0).start()

    def step4_chunk(ch):
        spectral(3, ch, 1, dq, mix_adjoint)

    loop(chunks, step4_chunk)

    for which, kept in enumerate((coef, dq)):
        def keep_low(half_at, row, degree, ours):
            own[half_at, which, :, row] = only(ours, kept[degree, :, head(tile)])

        pack(chip, keep_low)

    def both_parts(peer, action):
        degree = n + first_mode(peer)
        for which, kept in enumerate((coef, dq)):
            action(to(peer, kept.at[degree, :, head(tile)], second.at[which, me, :, head(tile)],
                      always_send, always_recv))

            @pl.when(first_mode(me) <= first_mode(peer))
            def _():
                more = pl.ds(tile, tile)
                action(to(peer, kept.at[degree, :, more], second.at[which, me, :, more],
                          some_send, some_recv))

    def send_second(k):
        both_parts(lax.rem(me + k, n), lambda copy: copy.start())

    loop(n, send_second, 1)
    for which, kept in enumerate((coef, dq)):
        second[which, me] = kept[n + first_mode(me), :, head(2 * tile)]

    def clear_second(src):
        @pl.when(first_mode(src) > first_mode(me))
        def _():
            for which in range(2):
                second[which, src, :, pl.ds(tile, tile)] = jnp.zeros((chunks, tile, chans), BF16)

    loop(n, clear_second)
    own_copy = to(sibling, own.at[other_core], other, own_send, own_recv)
    own_copy.start()

    def pack_block(k):
        return packs.at[core, chip_at(-way * k)]

    def pack_copy(k):
        return to(onward, pack_block(k), pack_block(k), pack_send, pack_recv.at[k])

    def share(k):
        to(sibling, pack_block(k), pack_block(k), share_send, share_recv).start()

    half = degs // n - 2
    wide = 2 * chans
    block_rows = half * wide
    piece = block_rows // pieces
    hops = (last) * pieces

    def block_at(k, direction):
        return lax.rem(chip - direction * (1 + k) + 2 * chips, chips)

    def outer(dst, row, pairs):
        real = jnp.zeros((chans, chans), F32)
        imag = jnp.zeros((chans, chans), F32)
        for y, x in pairs:
            real += dot(y, x, ((0,), (0,)))
            imag -= dot(turn(y.astype(F32)).astype(BF16), x, ((0,), (0,)))
        dst[pl.ds(row, chans, stride=2), :] = real
        dst[pl.ds(row + 1, chans, stride=2), :] = imag

    def first_degree(block, of_core):
        return 2 * n + (2 * block + of_core) * half

    def weight_grad(dst, degree):
        def one(j):
            outer(dst, j * wide, [(dq[degree + j, ch], coef[degree + j, ch]) for ch in range(chunks)])

        loop(half, one)

    def pair_copy(k):
        slot = lax.rem(k, 2)
        rows_there = pl.ds(first_degree(block_at(k, -way), core) * wide, block_rows)
        return to(sibling, wbuf.at[slot, head(block_rows)], dw_out.at[rows_there],
                  pair_send.at[slot], pair_recv.at[k])

    def weight_block(k):
        @pl.when(k >= 2)
        def _():
            pair_copy(k - 2).wait_send()
        weight_grad(wbuf.at[lax.rem(k, 2)], first_degree(block_at(k, -way), other_core))
        pair_copy(k).start()
        block = block_at(k, way)
        weight_grad(work.at[pl.ds(block * block_rows, block_rows)], first_degree(block, core))

    loop(chips, weight_block)
    pair_copy(chips - 2).wait_send()
    pair_copy(last).wait_send()
    own_copy.wait()
    packs[core, chip] = (own[core].astype(F32) + other[...].astype(F32)).astype(BF16)

    def low_degree(l):
        def one(z):
            for c in range(2):
                p = l - z if c == 0 else l + 1
                ours = p >= 0 if c == 0 else p >= n - z
                p = jnp.maximum(p, 0)
                h = jnp.where(p > held - 1, 1, 0)
                for which in range(2):
                    lowx[which, 2 * z + c] = only(ours, packs[h, z, which, :, p - h * (held - 1)])

        loop(chips, one)
        outer(wbuf.at[0], 0, [(lowx[1].reshape(-1, chans), lowx[0].reshape(-1, chans))])
        dw_out[pl.ds(l * wide, wide)] = wbuf[0, head(wide)]

    def final_rows(unit):
        ch, t = unit_of(unit)

        step_in(dg_hbm, unit)
        buf = lax.rem(unit, 2)

        fetch_rows(3, ch, t)
        for b in range(0, nb, 2):
            g = fetch_pair(b)
            change = dot(adj_h[...], g) + dot(adj_l[...], g)
            df_out[ch * nb + b, t] = inbuf[buf, b] + change[:, :chans]
            df_out[ch * nb + b + 1, t] = inbuf[buf, b + 1] + change[:, chans:]

    def place(i, of_core):
        block = block_at(lax.div(i, pieces), way)
        start = lax.rem(i, pieces) * piece
        return pl.ds(block * block_rows + start, piece), pl.ds(first_degree(block, of_core) * wide + start, piece)

    def rs_copy(i):
        here, there = place(i, core)
        return to(onward, work.at[here], dw_out.at[there], rs_send, rs_recv.at[i])

    def add_pair(i):
        here, passed = place(i, other_core)

        @pl.when(lax.rem(i, pieces) == 0)
        def _():
            pair_copy(lax.div(i, pieces)).wait_recv()

        work[here] += dw_out[passed]

    def rs_step(i):
        add_pair(i)

        @pl.when(i >= pieces)
        def _():
            rs_copy(i - pieces).wait_recv()
            here, there = place(i, core)
            work[here] += dw_out[there]

        rs_copy(i).start()

        @pl.when(lax.rem(i, pieces) == 0)
        def _():
            k = lax.div(i, pieces)

            @pl.when(k > 0)
            def _():
                pack_copy(k - 1).wait_recv()

            pack_copy(k).start()
            share(k)


    loop(hops, rs_step)
    pack_copy(chips - 2).wait_recv()
    share(last)

    def own_sum(s):
        i = hops + s
        add_pair(i)
        rs_copy(i - pieces).wait_recv()
        here, there = place(i, core)
        dw_out[there] += work[here]
        ag_copy(i, s).start()

    def second_spot(k):
        return pl.ds((n + first_mode(2 * block_at(k, way) + core)) * wide, wide)

    def second_copy(k, got):
        spot = dw_out.at[second_spot(k)]
        return to(onward, spot, spot, ag_send, ag_recv.at[hops + got])

    def second_publish(k):
        spot = dw_out.at[second_spot(k)]
        to(sibling, spot, spot, pub_send, pub_recv).start()

    def ag_copy(i, got):
        _, there = place(i, core)
        return to(onward, dw_out.at[there], dw_out.at[there], ag_send, ag_recv.at[got])

    def publish(i):
        _, there = place(i, core)
        to(sibling, dw_out.at[there], dw_out.at[there], pub_send, pub_recv).start()

    firsts = second.at[:, head(n - 1), :, head(tile)]
    pltpu.make_async_copy(firsts, firsts, always_recv).wait()

    comes, goes = first_mode(me), n - 1 - first_mode(me)

    def wait_some(count, sem):
        for k in range(1, n):
            @pl.when(count == k)
            def _():
                part = second.at[:, head(k), :, pl.ds(tile, tile)]
                pltpu.make_async_copy(part, part, sem).wait()

    wait_some(comes, some_recv)
    outer(wbuf.at[0], 0, [(second[1].reshape(-1, chans), second[0].reshape(-1, chans))])
    dw_out[second_spot(last)] = wbuf[0, head(wide)]
    loop(pieces, own_sum)
    second_copy(last, 0).start()

    pl.semaphore_signal(free_sem, inc=1, device_id={axis: sibling}, device_id_type=pl.DeviceIdType.MESH)
    pl.semaphore_wait(free_sem, 1)

    def own_piece(s):
        publish(hops + s)

    loop(pieces, own_piece)
    second_publish(last)
    gathered = packs.at[other_core]
    pltpu.make_async_copy(gathered, gathered, share_recv).wait()

    def task(i):
        @pl.when(i < chips)
        def _():
            for ch in range(chunks):
                @pl.when(i == 0)
                def _():
                    arrived(3, ch)
                apply_top(0, ch, i)

        @pl.when((i >= chips) & (i < chips + units))
        def _():
            final_rows(i - chips)

        @pl.when(i < n)
        def _():
            low_degree(i)

    share_of = -(-(chips + units) // hops)

    def ag_step(i):
        ag_copy(i, i).wait_recv()

        @pl.when(i + pieces < hops)
        def _():
            ag_copy(i, i + pieces).start()

        publish(i)

        @pl.when(lax.rem(i, pieces) == pieces - 1)
        def _():
            k = lax.div(i, pieces)
            second_copy(k, k).wait_recv()

            @pl.when(k < chips - 2)
            def _():
                second_copy(k, k + 1).start()

            second_publish(k)

        for j in range(share_of):
            task(i * share_of + j)

    loop(hops, ag_step)

    wait_sent(2 * chunks + final, 2)
    for ch in range(chunks):
        wait_sent(3 * chunks + ch, 3)
    for ch in range(chunks):
        pltpu.make_async_copy(sums.at[ch], sums.at[ch], sum_send.at[ch]).wait()
    sent = work.at[head((last) * block_rows)]
    pltpu.make_async_copy(sent, sent, rs_send).wait()
    sent = dw_out.at[head((last) * (block_rows + wide))]
    pltpu.make_async_copy(sent, sent, ag_send).wait()
    pltpu.make_async_copy(firsts, firsts, always_send).wait()

    wait_some(goes, some_send)
    sent = packs.at[0, head(last)]
    pltpu.make_async_copy(sent, sent, pack_send).wait()
    pltpu.make_async_copy(packs.at[0], packs.at[0], share_send).wait()
    shared = dw_out.at[head(chips * (block_rows + wide))]
    pltpu.make_async_copy(shared, shared, pub_send).wait()
    pltpu.make_async_copy(shared, shared, pub_recv).wait()


def put_kernel(df_ref, dw_ref, df_hbm, dw_hbm, sems):
    copies = []
    for source, target, parts in ((df_ref, df_hbm, 6), (dw_ref, dw_hbm, 12)):
        size = source.shape[0] // parts
        for k in range(parts):
            part = pl.ds(k * size, size)
            copies.append(pltpu.make_async_copy(source.at[part], target.at[part], sems.at[len(copies)]))
    for copy in copies:
        copy.start()
    for copy in copies:
        copy.wait()


def solution(mesh):
    n = mesh.shape['lat']
    field_spec = P('member', None, 'lat')

    def local_step(field_loc, grad_loc, p_fwd, p_inv, w_mix):
        batch, chans, tl, lons = field_loc.shape
        degs, lats = p_fwd.shape[1:]
        ml = p_fwd.shape[0] // n
        nb = 4
        chunks = batch // nb
        rows = ml * 2 * nb
        pitch = rows + 1
        half = degs // n - 2
        pieces = 2 if half * 2 * chans % 32 == 0 else 1
        hops = (n // 2 - 1) * pieces
        per = 4
        area = max(2 * lats * pitch, n // 2 * half * 2 * chans)
        depth = min(degs // per, area // (per * 2 * chans))
        held = n // 2 + 1
        packed = (3, chunks, held, 2 * nb, chans)
        tables = fourier_tables(n, ml, lons)
        anywhere = pl.BlockSpec(memory_space=pl.ANY)
        vmem = pl.BlockSpec(memory_space=pltpu.VMEM)
        grad_field, grad_w = pl.pallas_call(
            functools.partial(layer_kernel, 'lat', n, nb, pieces, per, depth),
            name='layer',
            out_shape=(
                pltpu.VMEM((batch, tl, lons, chans), F32),
                pltpu.VMEM((degs * 2 * chans, chans), F32),
            ),
            in_specs=[anywhere] * 6,
            out_specs=(vmem, vmem),
            scratch_shapes=[
                pltpu.VMEM((2, chunks, n, tl, rows, chans), BF16),
                pltpu.VMEM((chunks + 1, n, tl, rows, chans), BF16),
                pltpu.VMEM((area, chans), F32),
                pltpu.VMEM((lats, 2 * nb * chans), BF16),
                pltpu.VMEM((degs, chunks, rows, chans), BF16),
                pltpu.VMEM((degs, chunks, rows, chans), BF16),
                pltpu.VMEM((degs, 2 * chans, chans), BF16),
                pltpu.VMEM((2, max(per, half) * 2 * chans, chans), F32),
                pltpu.VMEM((2, nb, lons, chans), F32),
                pltpu.VMEM((n * rows, chans), F32),
                pltpu.VMEM((2, ml, degs, lats), F32),
                pltpu.VMEM((2, ml, degs, lats), BF16),
                pltpu.VMEM((2, n, n, lats), F32),
                pltpu.VMEM((2, n // 2, 16, 32), F32),
                pltpu.VMEM((32 * 2 * nb, chans), F32),
                pltpu.VMEM((2,) + packed, BF16),
                pltpu.VMEM(packed, BF16),
                pltpu.VMEM((2, n // 2) + packed, BF16),
                pltpu.VMEM((2, n, chunks, 2 * nb, chans), BF16),
                pltpu.VMEM(tables.shape, BF16),
                pltpu.VMEM((chunks, 5, 6, tl, 2 * nb, chans), BF16),
                pltpu.VMEM((2, 4, held, 2 * nb, chans), F32),
                pltpu.VMEM((chunks, 4, held, 2 * nb, chans), F32),
                pltpu.VMEM((chunks, 4, held, 2 * nb, chans), F32),
                pltpu.VMEM((chunks, 2, held, 2 * nb, chans), F32),
                pltpu.VMEM((chunks, 2, held, 2 * nb, chans), F32),
                pltpu.VMEM((chunks, 2, held, 2 * nb, chans), F32),
                pltpu.VMEM((2, n, chunks, 4 * nb, chans), BF16),
                pltpu.SemaphoreType.DMA((chunks + 1,)),
                pltpu.SemaphoreType.DMA((4 * chunks,)),
                pltpu.SemaphoreType.DMA((2,)),
                pltpu.SemaphoreType.DMA((depth,)),
                pltpu.SemaphoreType.DMA((2,)),
                pltpu.SemaphoreType.DMA((2,)),
                pltpu.SemaphoreType.DMA((2,)),
                pltpu.SemaphoreType.DMA((n // 2,)),
                pltpu.SemaphoreType.DMA,
                pltpu.SemaphoreType.DMA((hops,)),
                pltpu.SemaphoreType.DMA,
                pltpu.SemaphoreType.DMA((hops + n // 2 - 1,)),
                pltpu.SemaphoreType.REGULAR,
                pltpu.SemaphoreType.DMA,
                pltpu.SemaphoreType.DMA,
                pltpu.SemaphoreType.DMA,
                pltpu.SemaphoreType.DMA,
                pltpu.SemaphoreType.DMA,
                pltpu.SemaphoreType.DMA((n // 2 - 1,)),
                pltpu.SemaphoreType.DMA,
                pltpu.SemaphoreType.DMA,
                pltpu.SemaphoreType.DMA((2,)),
                pltpu.SemaphoreType.DMA,
                pltpu.SemaphoreType.DMA((chunks,)),
                pltpu.SemaphoreType.DMA((chunks,)),
                pltpu.SemaphoreType.DMA((chunks,)),
                pltpu.SemaphoreType.DMA,
                pltpu.SemaphoreType.DMA((chunks,)),
                pltpu.SemaphoreType.DMA((chunks,)),
                pltpu.SemaphoreType.DMA((chunks,)),
                pltpu.SemaphoreType.DMA,
                pltpu.SemaphoreType.DMA((chunks,)),
                pltpu.SemaphoreType.DMA((chunks,)),
                pltpu.SemaphoreType.DMA((chunks,)),
                pltpu.SemaphoreType.DMA,
                pltpu.SemaphoreType.DMA((chunks,)),
                pltpu.SemaphoreType.DMA,
                pltpu.SemaphoreType.DMA,
                pltpu.SemaphoreType.DMA,
                pltpu.SemaphoreType.DMA,
                pltpu.SemaphoreType.DMA((chunks,)),
            ],
            compiler_params=pltpu.CompilerParams(
                collective_id=0, has_side_effects=True, vmem_limit_bytes=43 << 20),
        )(
            field_loc.transpose(0, 2, 3, 1), grad_loc.transpose(0, 2, 3, 1),
            w_mix.transpose(0, 1, 3, 2).reshape(degs * 2 * chans, chans),
            p_fwd, p_inv, tables)
        grad_field, grad_w = pl.pallas_call(
            put_kernel,
            name='put',
            out_shape=(
                jax.ShapeDtypeStruct(grad_field.shape, F32),
                jax.ShapeDtypeStruct(grad_w.shape, F32),
            ),
            in_specs=[vmem] * 2,
            out_specs=(anywhere, anywhere),
            scratch_shapes=[pltpu.SemaphoreType.DMA((18,))],
            compiler_params=pltpu.CompilerParams(vmem_limit_bytes=1 << 20),
        )(grad_field, grad_w)
        return grad_field.transpose(0, 3, 1, 2), grad_w.reshape(degs, chans, 2, chans).transpose(0, 1, 3, 2)

    return jax.shard_map(
        local_step, mesh=mesh, in_specs=(field_spec, field_spec, P(), P(), P()),
        out_specs=(field_spec, P('member')), check_vma=False)
```
